32 devices in a mesh: dp: 8 (over y, x, core), tensor: 4 (over z).
Axes of the slice: x: 2, y: 2, z: 4, core: 2. Of those that a mesh axis runs over, the one named last changes fastest.
Arguments:
- hidden_in: bfloat16 [4096, 2048], P(('dp', 'tensor')), may hold values from -6 to 6
- segments: int32 [8, 512], P('dp'), may hold values from 0 to 5, never falling along the last dimension, each value on 1 to 256 neighbouring positions
- routes: int32 [4096, 8], P(('dp', 'tensor')), may hold values from 0 to 31, all different within a row; in each aligned block of 128 rows (0 to 127, 128 to 255, ...) at most 64 rows name the same one
- query_weight: bfloat16 [2048, 4096], P('dp', 'tensor'), may hold values from -0.125 to 0.125
- key_weight: bfloat16 [2048, 512], P('dp', 'tensor'), may hold values from -0.125 to 0.125
- value_weight: bfloat16 [2048, 512], P('dp', 'tensor'), may hold values from -0.125 to 0.125
- output_weight: bfloat16 [4096, 2048], P('tensor', 'dp'), may hold values from -0.5 to 0.5
- gain_attn: float32 [2048], replicated, may hold values from 0.5 to 1.5
- gain_moe: float32 [2048], replicated, may hold values from 0.5 to 1.5
- query_gain: float32 [128], replicated, may hold values from 0.5 to 2.5
- key_gain: float32 [128], replicated, may hold values from 0.5 to 2.5
- router: bfloat16 [2048, 32], replicated, may hold values from -0.0625 to 0.0625
- gate_weight: bfloat16 [32, 2048, 768], P(('dp', 'tensor')), may hold values from -0.125 to 0.125
- up_weight: bfloat16 [32, 2048, 768], P(('dp', 'tensor')), may hold values from -0.125 to 0.125
- down_weight: bfloat16 [32, 768, 2048], P(('dp', 'tensor')), may hold values from -0.625 to 0.625
- cotangent: bfloat16 [4096, 2048], P(('dp', 'tensor')), may hold values from -6 to 6
Outputs:
- output: bfloat16 [4096, 2048], P(('dp', 'tensor'))
- grad_input: float32 [4096, 2048], P(('dp', 'tensor'))
- grad_query_weight: float32 [2048, 4096], P('dp', 'tensor')
- grad_key_weight: float32 [2048, 512], P('dp', 'tensor')
- grad_value_weight: float32 [2048, 512], P('dp', 'tensor')
- grad_output_weight: float32 [4096, 2048], P('tensor', 'dp')
- grad_gain_attn: float32 [2048], replicated
- grad_gain_moe: float32 [2048], replicated
- grad_query_gain: float32 [128], replicated
- grad_key_gain: float32 [128], replicated
- grad_router: float32 [2048, 32], replicated
- grad_gate: float32 [32, 2048, 768], P(('dp', 'tensor'))
- grad_up: float32 [32, 2048, 768], P(('dp', 'tensor'))
- grad_down: float32 [32, 768, 2048], P(('dp', 'tensor'))
The draws below stay inside these ranges and needn't reach their ends.
Inputs may be any that keep to these rules, and one draw needn't show every extreme that they name: `routes`: in the rows of one device (128 aligned rows) each expert is named by at most 64 rows, a bound that some block reaches; a row names 8 different experts. `segments`: each row numbers its 6 packed sequences in order, never falling; each sequence has 1 to 256 tokens, one exactly 256.
All inputs are finite; a program needn't handle non-finite values.
Results may differ from the reference program's by a relative error of at most 0.019.
Values may be sent and summed in bfloat16 or wider, within the bound.
A program may use at most 256 MiB of HBM per device.

```python
import math
import jax
import jax.numpy as jnp
import numpy as np
from jax import lax

D = 2048
H = 32
KV = 4
HD = 128
FFE = 768
TOPK = 8
ROWS = 128
SEGS = 6
E = 32
TOK_DEV = 512
TOKENS = 4096
SEQ_MAX = 256
CAP = 64
N_DP = 8
DEVICES = 32


def shard_levels(key, extent, cuts, least, high):
    def one(position, parts):
        steps = jax.random.uniform(jax.random.fold_in(jax.random.fold_in(key, 6), position), (parts,), jnp.float32, least / len(cuts), high / len(cuts))
        return jnp.repeat(jnp.exp(steps), extent[position] // parts).reshape((-1,) + (1,) * (len(extent) - position - 1))

    loudness = one(*cuts[0])
    for cut in cuts[1:]:
        loudness = loudness * one(*cut)
    return loudness


def profile(number_of, total, bound, slope):
    loads = [(1 << 20) // math.isqrt(standing ** slope) + 1 for standing in range(2, number_of + 1)]
    spare, given = total - bound - (number_of - 1), [1] * (number_of - 1)
    while spare > 0:
        movable = [i for i in range(number_of - 1) if given[i] < bound]
        whole, budget = sum([loads[i] for i in movable]), spare
        for i in movable:
            addition = min(bound - given[i], max(1, budget * loads[i] // whole), spare)
            given[i] = given[i] + addition
            spare = spare - addition
    return np.array([bound] + given)


def ragged_sizes(rng, amount, total, reach, slope):
    if amount == 2:
        one = jax.random.randint(rng, (), max(1, total - reach), min(reach, total - 1) + 1)
        return jnp.stack([one, total - one])
    sizes = jnp.asarray(profile(amount, total, reach, slope), jnp.int32)
    twos = (amount - 1) // 2
    source_of, sink = sizes[1:1 + 2 * twos:2], sizes[2:2 + 2 * twos:2]
    room = jnp.minimum(source_of - 1, reach - sink)
    passed = jax.random.randint(jax.random.fold_in(rng, 1), (twos,), 0, 1 << 20) % (room + 1)
    sizes = sizes.at[1:1 + 2 * twos:2].set(source_of - passed).at[2:2 + 2 * twos:2].set(sink + passed)
    return sizes[jax.random.permutation(jax.random.fold_in(rng, 2), amount)]


def routed_block(own_key, own, number, rows, amount, top, bound, skew):
    sequence = jax.random.permutation(own_key, amount)
    crowded, usual = load_shares(amount, rows * top, bound, skew, True), load_shares(amount, rows * top, bound, skew, False)
    places = jnp.arange(amount)

    def named(tallies, offset_by):
        used = int((tallies > 0).sum())
        fixed = max(1, used // 4)
        moved = fixed + (places - fixed + offset_by * (used - fixed)) % max(1, amount - fixed)
        return jnp.zeros((amount,), jnp.int32).at[sequence[jnp.where(places < fixed, places, moved)]].set(jnp.asarray(tallies, jnp.int32))

    tallies = jnp.where(number % 4 == 0, named(crowded, number // 4), named(usual, number - number // 4 - 1))
    mixed = jax.random.permutation(jax.random.fold_in(own, 3), amount)
    source_of, sink = mixed[0:amount // 2 * 2:2], mixed[1:amount // 2 * 2:2]
    margin = jnp.minimum(tallies[source_of] - 1, bound - tallies[sink]) // 2
    margin = jnp.where((source_of == sequence[0]) | (sink == sequence[0]) | (tallies[sink] == 0), 0, jnp.maximum(margin, 0))
    moved = jax.random.randint(jax.random.fold_in(own, 4), (amount // 2,), 0, 1 << 20) % (margin + 1)
    tallies = tallies.at[source_of].add(-moved).at[sink].add(moved)
    labels = jnp.searchsorted(jnp.cumsum(tallies), jnp.arange(rows * top), side="right").astype(jnp.int32)
    listing = labels.reshape(top, rows).T
    listing = listing[jax.random.permutation(jax.random.fold_in(own, 1), rows)]
    offset_by = jax.random.randint(jax.random.fold_in(own, 2), (rows, 1), 0, top)
    return jnp.take_along_axis(listing, (jnp.arange(top)[None, :] + offset_by) % top, axis=1)


def load_shares(number_of, total, reach, lean, full):
    weights = [(1 << 20) // math.isqrt(grade ** lean) + 1 for grade in range(1, number_of + 1)]
    largest = reach if full else min(reach, max(-(-total // number_of), total * weights[0] // sum(weights)))
    least = 1 if total - largest >= number_of - 1 else 0
    holding, surplus = [largest] + [least] * (number_of - 1), total - largest - least * (number_of - 1)
    while surplus > 0:
        free = [i for i in range(1, number_of) if holding[i] < largest] or [i for i in range(1, number_of) if holding[i] < reach]
        whole, left = sum([weights[i] for i in free]), surplus
        for i in free:
            extra = min(reach - holding[i], max(1, left * weights[i] // whole), surplus)
            holding[i] = holding[i] + extra
            surplus = surplus - extra
    return np.array(holding)


def normal_values(key, shape, spread, limit, cuts=(), held_as=jnp.bfloat16):
    level = shard_levels(key, shape, cuts, -0.22, 0.18) if cuts else 1.0
    values = jax.random.normal(key, shape, jnp.float32) * spread * level
    return jnp.minimum(jnp.maximum(values, -limit), limit).astype(held_as)


def setup_inputs(seed: int = 0) -> dict:
    key_list = jax.random.split(jax.random.key(seed), 17)
    hidden_in = normal_values(key_list[0], (TOKENS, D), 1.0, 6.0, ((0, 32),))
    segments = jax.vmap(lambda own: jnp.searchsorted(jnp.cumsum(ragged_sizes(own, SEGS, TOK_DEV, SEQ_MAX, 2)), jnp.arange(TOK_DEV), side="right"))(jax.random.split(key_list[1], N_DP)).reshape((N_DP, TOK_DEV)).astype(jnp.int32)
    routes_keys = jax.random.split(jax.random.fold_in(key_list[2], 1), TOKENS // ROWS)
    routes_turns = jax.random.permutation(jax.random.fold_in(key_list[2], 3), TOKENS // ROWS)
    routes = jax.vmap(lambda own, number: routed_block(jax.random.fold_in(key_list[2], 2), own, number, ROWS, E, TOPK, CAP, 4))(routes_keys, routes_turns).reshape((TOKENS, TOPK))
    query_weight = normal_values(key_list[3], (D, H * HD), D ** -0.5, 0.125, ((0, 8), (1, 4)))
    key_weight = normal_values(key_list[4], (D, KV * HD), D ** -0.5, 0.125, ((0, 8), (1, 4)))
    value_weight = normal_values(key_list[5], (D, KV * HD), D ** -0.5, 0.125, ((0, 8), (1, 4)))
    output_weight = normal_values(key_list[6], (H * HD, D), (H * HD // 32) ** -0.5, 0.5, ((0, 4), (1, 8)))
    gain_attn = jnp.clip(1.0 + 0.1 * jax.random.normal(key_list[7], (D,), jnp.float32), 0.5, 1.5)
    gain_moe = jnp.clip(1.0 + 0.1 * jax.random.normal(key_list[8], (D,), jnp.float32), 0.5, 1.5)
    query_gain = jnp.clip(jnp.exp(jax.random.uniform(key_list[9], (HD,), jnp.float32, math.log(0.5), math.log(2.5))), 0.5, 2.5)
    key_gain = jnp.clip(jnp.exp(jax.random.uniform(key_list[10], (HD,), jnp.float32, math.log(0.5), math.log(2.5))), 0.5, 2.5)
    router = normal_values(key_list[11], (D, E), (4 * D) ** -0.5, 0.0625)
    gate_weight = normal_values(key_list[12], (E, D, FFE), D ** -0.5, 0.125, ((0, 32),))
    up_weight = normal_values(key_list[13], (E, D, FFE), D ** -0.5, 0.125, ((0, 32),))
    down_weight = normal_values(key_list[14], (E, FFE, D), (FFE // 8) ** -0.5, 0.625, ((0, 32),))
    cotangent = normal_values(key_list[15], (TOKENS, D), 1.0, 6.0, ((0, 32),))
    return dict(hidden_in=hidden_in, segments=segments, routes=routes, query_weight=query_weight, key_weight=key_weight, value_weight=value_weight, output_weight=output_weight, gain_attn=gain_attn, gain_moe=gain_moe, query_gain=query_gain, key_gain=key_gain, router=router, gate_weight=gate_weight, up_weight=up_weight, down_weight=down_weight, cotangent=cotangent)


EPSILON = 1e-06
THETA_BASE = 1000000.0
NEG_BIG = -1e+30

def mix(form, left, right):
    return jnp.einsum(form, left.astype(jnp.float32), right.astype(jnp.float32))

def rms_scale(values):
    return lax.rsqrt(lax.optimization_barrier(jnp.mean(values * values, axis=-1, keepdims=True)) + EPSILON)

def rope_tables(seg_ids, head_dim):
    length = seg_ids.shape[0]
    row_index = jnp.arange(length, dtype=jnp.int32)
    starts = lax.optimization_barrier(jnp.sum((seg_ids[None, :] < seg_ids[:, None]).astype(jnp.int32), axis=1))
    places = (row_index - starts).astype(jnp.float32)
    half_dim = head_dim // 2
    frequency = THETA_BASE ** (-(jnp.arange(half_dim, dtype=jnp.float32) * (2.0 / head_dim)))
    angles = places[:, None] * frequency[None, :]
    return (jnp.cos(angles), jnp.sin(angles))

def rotate(values, cosine, sine_table):
    half_dim = values.shape[-1] // 2
    front_part = values[..., :half_dim]
    back_part = values[..., half_dim:]
    cos_rows = cosine[:, None, :]
    sin_rows = sine_table[:, None, :]
    return jnp.concatenate([front_part * cos_rows - back_part * sin_rows, back_part * cos_rows + front_part * sin_rows], axis=-1)

def unrotate(values, cosine, sine_table):
    half_dim = values.shape[-1] // 2
    front_part = values[..., :half_dim]
    back_part = values[..., half_dim:]
    cos_rows = cosine[:, None, :]
    sin_rows = sine_table[:, None, :]
    return jnp.concatenate([front_part * cos_rows + back_part * sin_rows, back_part * cos_rows - front_part * sin_rows], axis=-1)

def head_norm_back(grad_out, normed, factor, gain):
    grad_normed = grad_out * gain
    grad_gain = lax.optimization_barrier(jnp.sum(grad_out * normed, axis=(0, 1)))
    grad_values = factor * (grad_normed - normed * lax.optimization_barrier(jnp.mean(grad_normed * normed, axis=-1, keepdims=True)))
    return (grad_values, grad_gain)

def row_norm_back(grad_out, normed, factor, gain):
    grad_normed = grad_out * gain
    grad_gain = lax.optimization_barrier(jnp.sum(grad_out * normed, axis=0))
    grad_values = factor * (grad_normed - normed * lax.optimization_barrier(jnp.mean(grad_normed * normed, axis=-1, keepdims=True)))
    return (grad_values, grad_gain)

def softmax_rows(logits):
    top_value = lax.optimization_barrier(jnp.max(logits, axis=-1, keepdims=True))
    expo = jnp.exp(logits - top_value)
    return expo / lax.optimization_barrier(jnp.sum(expo, axis=-1, keepdims=True))

def attn_forward(rows, seg_ids, wq_full, wk_full, wv_full, query_gain, key_gain):
    length = rows.shape[0]
    head_dim = query_gain.shape[0]
    num_heads = wq_full.shape[1] // head_dim
    kv_heads = wk_full.shape[1] // head_dim
    per_group = num_heads // kv_heads
    inv_root = 1.0 / math.sqrt(head_dim)
    block_rows = math.gcd(length, 512)
    cosine, sine_table = rope_tables(seg_ids, head_dim)
    query = jnp.dot(rows, wq_full, preferred_element_type=jnp.float32).reshape(length, num_heads, head_dim)
    key_proj = jnp.dot(rows, wk_full, preferred_element_type=jnp.float32).reshape(length, kv_heads, head_dim)
    value_rows = jnp.dot(rows, wv_full, preferred_element_type=jnp.float32).astype(jnp.bfloat16).reshape(length, kv_heads, head_dim)
    query_factor = rms_scale(query)
    query_hat = query * query_factor
    key_factor = rms_scale(key_proj)
    key_hat = key_proj * key_factor
    query_rot = rotate(query_hat * query_gain, cosine, sine_table).astype(jnp.bfloat16).reshape(length, kv_heads, per_group, head_dim)
    key_rot = rotate(key_hat * key_gain, cosine, sine_table).astype(jnp.bfloat16)
    row_index = jnp.arange(length, dtype=jnp.int32)
    outputs = []
    lse_parts = []
    for start_row in range(0, length, block_rows):
        stop_row = start_row + block_rows
        scores = mix('qgrd,kgd->grqk', query_rot[start_row:stop_row], key_rot) * inv_root
        visible = (seg_ids[start_row:stop_row, None] == seg_ids[None, :]) & (row_index[None, :] <= row_index[start_row:stop_row, None])
        scores = jnp.where(visible, scores, NEG_BIG)
        top_value = lax.optimization_barrier(jnp.max(scores, axis=-1, keepdims=True))
        expo = jnp.exp(scores - top_value)
        totals = lax.optimization_barrier(jnp.sum(expo, axis=-1, keepdims=True))
        prob_rows = (expo / totals).astype(jnp.bfloat16)
        outputs.append(mix('grqk,kgd->qgrd', prob_rows, value_rows).astype(jnp.bfloat16))
        lse_parts.append(top_value[..., 0] + jnp.log(totals[..., 0]))
    attn_heads = jnp.concatenate(outputs, axis=0).reshape(length, num_heads * head_dim)
    lse_all = jnp.concatenate(lse_parts, axis=-1)
    return (attn_heads, lse_all, query_rot, key_rot, value_rows, cosine, sine_table, query_hat, query_factor, key_hat, key_factor)

def attn_backward(grad_attn, rows, seg_ids, wq_full, wk_full, wv_full, wo_full, query_gain, key_gain, saved):
    attn_heads, lse_all, query_rot, key_rot, value_rows, cosine, sine_table, query_hat, query_factor, key_hat, key_factor = saved
    length = rows.shape[0]
    head_dim = query_gain.shape[0]
    num_heads = query_hat.shape[1]
    inv_root = 1.0 / math.sqrt(head_dim)
    block_rows = math.gcd(length, 512)
    grad_wo = jnp.dot(attn_heads.T, grad_attn, preferred_element_type=jnp.float32)
    grad_heads = jnp.dot(grad_attn, wo_full.T, preferred_element_type=jnp.float32).astype(jnp.bfloat16).reshape(query_rot.shape)
    heads_view = attn_heads.reshape(query_rot.shape)
    row_delta = jnp.transpose(lax.optimization_barrier(jnp.sum(grad_heads.astype(jnp.float32) * heads_view.astype(jnp.float32), axis=-1)), (1, 2, 0))
    row_index = jnp.arange(length, dtype=jnp.int32)
    grad_value = jnp.zeros(value_rows.shape, jnp.float32)
    grad_key_rot = jnp.zeros(key_rot.shape, jnp.float32)
    pieces = []
    for start_row in range(0, length, block_rows):
        stop_row = start_row + block_rows
        query_block = query_rot[start_row:stop_row]
        grad_block = grad_heads[start_row:stop_row]
        scores = mix('qgrd,kgd->grqk', query_block, key_rot) * inv_root
        visible = (seg_ids[start_row:stop_row, None] == seg_ids[None, :]) & (row_index[None, :] <= row_index[start_row:stop_row, None])
        scores = jnp.where(visible, scores, NEG_BIG)
        prob_f = jnp.where(visible, jnp.exp(scores - lse_all[:, :, start_row:stop_row, None]), 0.0)
        prob_rows = prob_f.astype(jnp.bfloat16)
        grad_value = grad_value + mix('grqk,qgrd->kgd', prob_rows, grad_block)
        grad_probs = mix('qgrd,kgd->grqk', grad_block, value_rows)
        grad_scores = (prob_f * (grad_probs - row_delta[:, :, start_row:stop_row, None])).astype(jnp.bfloat16)
        pieces.append(mix('grqk,kgd->qgrd', grad_scores, key_rot) * inv_root)
        grad_key_rot = grad_key_rot + mix('grqk,qgrd->kgd', grad_scores, query_block) * inv_root
    grad_query_rot = jnp.concatenate(pieces, axis=0).reshape(length, num_heads, head_dim)
    grad_query, grad_qgain = head_norm_back(unrotate(grad_query_rot, cosine, sine_table), query_hat, query_factor, query_gain)
    grad_key, grad_kgain = head_norm_back(unrotate(grad_key_rot, cosine, sine_table), key_hat, key_factor, key_gain)
    query_b = grad_query.astype(jnp.bfloat16).reshape(length, -1)
    key_b = grad_key.astype(jnp.bfloat16).reshape(length, -1)
    value_b = grad_value.astype(jnp.bfloat16).reshape(length, -1)
    grad_rows = jnp.dot(query_b, wq_full.T, preferred_element_type=jnp.float32) + jnp.dot(key_b, wk_full.T, preferred_element_type=jnp.float32) + jnp.dot(value_b, wv_full.T, preferred_element_type=jnp.float32)
    grad_wq = jnp.dot(rows.T, query_b, preferred_element_type=jnp.float32)
    grad_wk = jnp.dot(rows.T, key_b, preferred_element_type=jnp.float32)
    grad_wv = jnp.dot(rows.T, value_b, preferred_element_type=jnp.float32)
    return (grad_rows, grad_wq, grad_wk, grad_wv, grad_wo, grad_qgain, grad_kgain)

def expert_forward(expert_rows, wgate, wup, wdown):
    gate_pre = jnp.dot(expert_rows, wgate, preferred_element_type=jnp.float32)
    up_pre = jnp.dot(expert_rows, wup, preferred_element_type=jnp.float32)
    hidden_units = (jax.nn.silu(gate_pre) * up_pre).astype(jnp.bfloat16)
    result = jnp.dot(hidden_units, wdown, preferred_element_type=jnp.float32).astype(jnp.bfloat16)
    return (result, gate_pre, up_pre, hidden_units)

def expert_backward(expert_rows, grad_result, wgate, wup, wdown, gate_pre, up_pre, hidden_units):
    grad_hidden = jnp.dot(grad_result, wdown.T, preferred_element_type=jnp.float32)
    sigma = jax.nn.sigmoid(gate_pre)
    grad_gate_pre = (grad_hidden * up_pre * sigma * (1.0 + gate_pre * (1.0 - sigma))).astype(jnp.bfloat16)
    grad_up_pre = (grad_hidden * gate_pre * sigma).astype(jnp.bfloat16)
    grad_rows = (jnp.dot(grad_gate_pre, wgate.T, preferred_element_type=jnp.float32) + jnp.dot(grad_up_pre, wup.T, preferred_element_type=jnp.float32)).astype(jnp.bfloat16)
    grad_wd = jnp.dot(hidden_units.T, grad_result, preferred_element_type=jnp.float32)
    grad_wg = jnp.dot(expert_rows.T, grad_gate_pre, preferred_element_type=jnp.float32)
    grad_wu = jnp.dot(expert_rows.T, grad_up_pre, preferred_element_type=jnp.float32)
    return (grad_rows, grad_wg, grad_wu, grad_wd)

def reference(hidden_in, segments, routes, query_weight, key_weight, value_weight, output_weight, gain_attn, gain_moe, query_gain, key_gain, router, gate_weight, up_weight, down_weight, cotangent):
    inputs32 = hidden_in.astype(jnp.float32)
    factor_one = rms_scale(inputs32)
    normed_one = inputs32 * factor_one
    rows_one = (normed_one * gain_attn).astype(jnp.bfloat16)
    grouped = rows_one.reshape(N_DP, TOK_DEV, D)

    def forward_group(carry, pieces):
        group_rows, group_seg = pieces
        saved = attn_forward(group_rows, group_seg, query_weight, key_weight, value_weight, query_gain, key_gain)
        return (carry, jnp.dot(saved[0], output_weight, preferred_element_type=jnp.float32))
    _, attn_add = lax.scan(forward_group, jnp.zeros((), jnp.float32), (grouped, segments))
    residual = inputs32 + attn_add.reshape(TOKENS, D)
    factor_two = rms_scale(residual)
    normed_two = residual * factor_two
    rows_two = (normed_two * gain_moe).astype(jnp.bfloat16)
    router_probs = softmax_rows(jnp.dot(rows_two, router, preferred_element_type=jnp.float32))
    picked = jnp.take_along_axis(router_probs, routes, axis=1)
    total = lax.optimization_barrier(jnp.sum(picked, axis=1, keepdims=True))
    gates = picked / total
    pairs_dev = ROWS * TOPK
    flat_routes = routes.reshape(DEVICES, pairs_dev)
    onehot = (flat_routes[..., None] == jnp.arange(E, dtype=jnp.int32)).astype(jnp.int32)
    ranks = lax.optimization_barrier(jnp.sum(onehot * jnp.cumsum(onehot, axis=1), axis=-1)) - 1
    device_ids = jnp.broadcast_to(jnp.arange(DEVICES, dtype=jnp.int32)[:, None], (DEVICES, pairs_dev))
    pair_ids = jnp.arange(DEVICES * pairs_dev, dtype=jnp.int32).reshape(DEVICES, pairs_dev)
    table = jnp.full((E, DEVICES, CAP), -1, jnp.int32).at[flat_routes, device_ids, ranks].set(pair_ids)
    cot32 = cotangent.astype(jnp.float32)
    gate_flat = gates.reshape(-1)

    def expert_step(carry, pieces):
        mixed, grad_rows_two, grad_gates = carry
        slots, wgate, wup, wdown = pieces
        slots = slots.reshape(-1)
        valid = slots >= 0
        safe = jnp.where(valid, slots, 0)
        token = safe // TOPK
        expert_rows = jnp.where(valid[:, None], rows_two[token], jnp.zeros((), jnp.bfloat16))
        weight_sel = jnp.where(valid, gate_flat[safe], 0.0)
        result, gate_pre, up_pre, hidden_units = expert_forward(expert_rows, wgate, wup, wdown)
        result32 = result.astype(jnp.float32)
        mixed = mixed.at[token].add(weight_sel[:, None] * result32)
        grad_gates = grad_gates.at[safe].add(jnp.where(valid, lax.optimization_barrier(jnp.sum(cot32[token] * result32, axis=-1)), 0.0))
        grad_result = (weight_sel[:, None] * cot32[token]).astype(jnp.bfloat16)
        back = expert_backward(expert_rows, grad_result, wgate, wup, wdown, gate_pre, up_pre, hidden_units)
        grad_rows_two = grad_rows_two.at[token].add(jnp.where(valid[:, None], back[0].astype(jnp.float32), 0.0))
        return ((mixed, grad_rows_two, grad_gates), (back[1], back[2], back[3]))
    start_carry = (jnp.zeros((TOKENS, D), jnp.float32), jnp.zeros((TOKENS, D), jnp.float32), jnp.zeros((TOKENS * TOPK,), jnp.float32))
    (moe_sum, grad_expert_rows, grad_gates), (grad_gate, grad_up, grad_down) = lax.scan(expert_step, start_carry, (table, gate_weight, up_weight, down_weight))
    output = (residual + moe_sum).astype(jnp.bfloat16)
    grad_gates = grad_gates.reshape(TOKENS, TOPK)
    grad_picked = (grad_gates - lax.optimization_barrier(jnp.sum(gates * grad_gates, axis=1, keepdims=True))) / total
    route_hot = (routes[:, :, None] == jnp.arange(E, dtype=jnp.int32)[None, None, :]).astype(jnp.float32)
    grad_probs = lax.optimization_barrier(jnp.sum(route_hot * grad_picked[:, :, None], axis=1))
    grad_logits = (router_probs * (grad_probs - lax.optimization_barrier(jnp.sum(grad_probs * router_probs, axis=-1, keepdims=True)))).astype(jnp.bfloat16)
    grad_router = jnp.dot(rows_two.T, grad_logits, preferred_element_type=jnp.float32)
    grad_rows_two = grad_expert_rows + jnp.dot(grad_logits, router.T, preferred_element_type=jnp.float32)
    grad_res_norm, grad_gain_moe = row_norm_back(grad_rows_two, normed_two, factor_two, gain_moe)
    grad_residual = cot32 + grad_res_norm
    grad_attn = grad_residual.astype(jnp.bfloat16).reshape(N_DP, TOK_DEV, D)

    def backward_group(carry, pieces):
        group_rows, group_seg, group_grad = pieces
        saved = attn_forward(group_rows, group_seg, query_weight, key_weight, value_weight, query_gain, key_gain)
        back = attn_backward(group_grad, group_rows, group_seg, query_weight, key_weight, value_weight, output_weight, query_gain, key_gain, saved)
        new_carry = tuple((carry[slot] + back[slot + 1] for slot in range(6)))
        return (new_carry, back[0])
    zero_carry = (jnp.zeros(query_weight.shape, jnp.float32), jnp.zeros(key_weight.shape, jnp.float32), jnp.zeros(value_weight.shape, jnp.float32), jnp.zeros(output_weight.shape, jnp.float32), jnp.zeros(query_gain.shape, jnp.float32), jnp.zeros(key_gain.shape, jnp.float32))
    sums, grad_rows_one = lax.scan(backward_group, zero_carry, (grouped, segments, grad_attn))
    grad_wq, grad_wk, grad_wv, grad_wo, grad_qgain, grad_kgain = sums
    grad_in_norm, grad_gain_attn = row_norm_back(grad_rows_one.reshape(TOKENS, D), normed_one, factor_one, gain_attn)
    grad_input = grad_residual + grad_in_norm
    return (output, grad_input, grad_wq, grad_wk, grad_wv, grad_wo, grad_gain_attn, grad_gain_moe, grad_qgain, grad_kgain, grad_router, grad_gate, grad_up, grad_down)
```

```python
import math

import jax
import jax.numpy as jnp
from jax import lax
from jax.experimental import pallas as pl
from jax.experimental.pallas import tpu as pltpu
from jax.sharding import PartitionSpec as P

EPSILON = 1e-06
THETA_BASE = 1000000.0
NEG_BIG = -1e30


MESH = pl.DeviceIdType.MESH


class Place:
    def __init__(self, length):
        self.length = length
        self.dp = lax.axis_index("dp")
        self.z = lax.axis_index("tensor")
        core, along_x, along_y = self.dp % 2, (self.dp // 2) % 2, self.dp // 4
        self.to_core = 1 - 2 * core
        self.core = self.dp + self.to_core
        self.x = self.dp + 2 - 4 * along_x
        self.y = self.dp + 4 - 8 * along_y
        self.columns = (self.dp, self.x, self.y, self.x + self.y - self.dp)
        self.has_up = self.z < length - 1
        self.has_down = self.z > 0

    def device(self, kind):
        if kind == "x":
            return (self.x, self.z)
        if kind == "y":
            return (self.y, self.z)
        if kind == "core":
            return (self.core, self.z)
        if kind == "up":
            return (self.dp, self.z + 1)
        return (self.dp, self.z - 1)

    def condition(self, kind):
        return {"up": self.has_up, "down": self.has_down}.get(kind)

    def target(self, turn):
        length, z = self.length, self.z

        def at_least(left, right):
            return (left - right + 2 * length) // (2 * length)

        high = at_least(z, length // 2)
        mirrored = z + high * (length - 1 - 2 * z)
        above = length - 1 - mirrored
        first = at_least(above - 1, turn)
        if turn == length - 1:
            return z
        found = first * (length - 1 - turn) + (1 - first) * (turn - above)
        return found + high * (length - 1 - 2 * found)


def guarded(condition, action):
    if condition is None:
        action()
    else:
        pl.when(condition)(action)


def meet(place, over_z, over_dp):
    barrier = pltpu.get_barrier_semaphore()
    kinds = (("x", "y", "core") if over_dp else ()) + (("up", "down") if over_z else ())
    for kind in kinds:

        def greet(kind=kind):
            pl.semaphore_signal(
                barrier, 1, device_id=place.device(kind), device_id_type=MESH
            )

        guarded(place.condition(kind), greet)
    count = 3 if over_dp else 0
    if over_z:
        length = place.length
        count = count + (place.z + length - 1) // length + (2 * length - 2 - place.z) // length
    pl.semaphore_wait(barrier, count)


class Sends:
    def __init__(self, place):
        self.place = place
        self.started = []

    def start(self, kind, views, condition=None):
        def build():
            source, target, send_sem, recv_sem = views()
            return pltpu.make_async_remote_copy(
                src_ref=source,
                dst_ref=target,
                send_sem=send_sem,
                recv_sem=recv_sem,
                device_id=self.place.device(kind),
                device_id_type=MESH,
            )

        guarded(self.place.condition(kind), lambda: build().start())
        self.started.append((condition, self.place.condition(kind), build))

    def drain(self):
        for outer, inner, build in self.started:

            def finish(inner=inner, build=build):
                guarded(inner, lambda: build().wait_send())

            guarded(outer, finish)


class GatherItem:
    def __init__(self, mode, place, own, slot, recv, send, local):
        self.mode, self.place = mode, place
        self.own, self.slot = own, slot
        self.recv, self.send, self.local = recv, send, local
        self.over_z = mode != "dp"
        self.over_dp = mode != "z"
        self.length = place.length if self.over_z else 1
        self.z = place.z if self.over_z else 0

    def index(self, column, z):
        if self.mode == "all":
            return column * self.length + z
        return column if self.mode == "dp" else z

    @staticmethod
    def semaphores(mode, length):
        blocks = {"all": 8 * length, "dp": 8, "z": length}[mode]
        turns = 2 * length - 1 if mode != "dp" else 1
        return [
            pltpu.SemaphoreType.DMA((blocks, 2)),
            pltpu.SemaphoreType.DMA((10, turns, 2)),
            pltpu.SemaphoreType.DMA((2,)),
        ]

    def turns(self, distance):
        if distance == 0:
            return [(0, self.z, None, None)]
        place = self.place
        return [
            (2 * distance - 1, self.z - distance, place.z - distance >= 0, "up"),
            (2 * distance, self.z + distance, place.z + distance < self.length, "down"),
        ]

    def pass_on(self, sends, lane, kind, column, z, turn, h, source=None, condition=None):

        def views():
            view = self.slot(column, z, h)
            return (
                view if source is None else source(h),
                view,
                self.send.at[lane, turn, h],
                self.recv.at[self.index(column, z), h],
            )

        sends.start(kind, views, condition)

    def arrived(self, column, z, h):
        view = self.slot(column, z, h)
        pltpu.make_async_copy(view, view, self.recv.at[self.index(column, z), h]).wait()

    def begin(self, sends):
        place = self.place
        for h in range(2):
            own = self.own
            if self.over_z:
                self.pass_on(sends, 0, "up", place.dp, self.z, 0, h, own)
                self.pass_on(sends, 1, "down", place.dp, self.z, 0, h, own)
            if self.over_dp:
                self.pass_on(sends, 2, "x", place.dp, self.z, 0, h, own)
                self.pass_on(sends, 3, "y", place.dp, self.z, 0, h, own)
                self.pass_on(sends, 4, "core", place.dp, self.z, 0, h, own)
        for h in range(2):
            pltpu.make_async_copy(
                self.own(h), self.slot(place.dp, self.z, h), self.local.at[h]
            ).start()

    def along_z(self, sends, distance):
        if not self.over_z or distance >= self.length:
            return
        place = self.place
        for turn, z, condition, onward in self.turns(distance):

            def step(turn=turn, z=z, condition=condition, onward=onward):
                for h in range(2):
                    self.arrived(place.dp, z, h)
                    if distance < self.length - 1:
                        self.pass_on(
                            sends, 0 if onward == "up" else 1, onward, place.dp, z, turn, h,
                            condition=condition,
                        )
                    if self.over_dp:
                        for lane, kind in ((2, "x"), (3, "y"), (4, "core")):
                            self.pass_on(
                                sends, lane, kind, place.dp, z, turn, h, condition=condition
                            )

            guarded(condition, step)

    def across(self, sends, distance):
        if not self.over_dp or not 0 <= distance < self.length:
            return
        _, x, y, _ = self.place.columns
        for turn, z, condition, _ in self.turns(distance):

            def step(turn=turn, z=z, condition=condition):
                for h in range(2):
                    self.arrived(x, z, h)
                    if h == 0:
                        self.pass_on(sends, 5, "y", x, z, turn, h, condition=condition)
                    self.pass_on(sends, 7, "core", x, z, turn, h, condition=condition)
                    self.arrived(y, z, h)
                    if h == 1:
                        self.pass_on(sends, 6, "x", y, z, turn, h, condition=condition)
                    self.pass_on(sends, 8, "core", y, z, turn, h, condition=condition)

            guarded(condition, step)

    def diagonal(self, sends, distance):
        if not self.over_dp or not 0 <= distance < self.length:
            return
        corner = self.place.columns[3]
        for turn, z, condition, _ in self.turns(distance):

            def step(turn=turn, z=z, condition=condition):
                for h in range(2):
                    self.arrived(corner, z, h)
                    self.pass_on(sends, 9, "core", corner, z, turn, h, condition=condition)

            guarded(condition, step)

    def finish(self):
        place = self.place
        for h in range(2):
            pltpu.make_async_copy(
                self.own(h), self.slot(place.dp, self.z, h), self.local.at[h]
            ).wait()
        if self.over_dp:
            for column in place.columns:
                for z in range(self.length):
                    for h in range(2):
                        self.arrived(column + place.to_core, z, h)


def run_gather(place, items):
    meet(place, any(i.over_z for i in items), any(i.over_dp for i in items))
    sends = Sends(place)
    for item in items:
        item.begin(sends)
    for step in range(place.length + 2):
        for item in items:
            item.along_z(sends, step + 1)
        for item in items:
            item.across(sends, step)
        for item in items:
            item.diagonal(sends, step - 1)
    for item in items:
        item.finish()
    sends.drain()


def gather(specs, length, collective_id, name):
    modes = [mode for _, mode, _ in specs]
    shapes, sems = [], []
    for array, mode, by_columns in specs:
        blocks = {"all": 8 * length, "dp": 8, "z": length}[mode]
        if by_columns:
            shape = (array.shape[0], blocks * array.shape[1])
        else:
            shape = (blocks,) + array.shape
        shapes.append(jax.ShapeDtypeStruct(shape, array.dtype))
        sems += GatherItem.semaphores(mode, length)
    count = len(specs)

    def kernel(*refs):
        place = Place(length)
        items = []
        for number, (array, mode, by_columns) in enumerate(specs):
            source, target = refs[number], refs[count + number]
            recv, send, local = refs[2 * count + 3 * number : 2 * count + 3 * number + 3]
            half = array.shape[0] // 2
            width = array.shape[1]
            item = GatherItem(mode, place, None, None, recv, send, local)

            def own(h, source=source, half=half):
                return source.at[pl.ds(h * half, half)]

            def slot(column, z, h, target=target, half=half, width=width, item=item, by=by_columns):
                block = item.index(column, z)
                if by:
                    return target.at[
                        pl.ds(h * half, half), pl.ds(pl.multiple_of(block * width, width), width)
                    ]
                return target.at[block, pl.ds(h * half, half)]

            item.own, item.slot = own, slot
            items.append(item)
        run_gather(place, items)

    return pl.pallas_call(
        kernel,
        name=name,
        out_shape=shapes,
        in_specs=[pl.BlockSpec(memory_space=pl.ANY)] * count,
        out_specs=[pl.BlockSpec(memory_space=pl.ANY)] * count,
        scratch_shapes=sems,
        compiler_params=pltpu.CompilerParams(collective_id=collective_id, has_side_effects=True),
    )(*[array for array, _, _ in specs])


class ReduceItem:
    def __init__(self, mode, place, block, bufs, out):
        self.mode, self.place, self.block, self.out = mode, place, block, out
        self.over_z = mode != "dp"
        self.over_dp = mode != "z"
        self.length = place.length if self.over_z else 1
        (self.acc, self.from_core, self.corner, self.from_xy, self.from_z,
         self.load, self.send, self.recv) = bufs

    @staticmethod
    def scratch(mode, length, rows, width):
        t = length if mode != "dp" else 1
        columns = 4 if mode != "z" else 1
        dp = mode != "z"
        half = (rows // 2, width)
        small = (8, 128)
        return [
            pltpu.VMEM((columns, t, 2) + half, jnp.bfloat16),
            pltpu.VMEM(((columns, t, 2) + half) if dp else small, jnp.bfloat16),
            pltpu.VMEM(((2, t) + half) if dp else small, jnp.bfloat16),
            pltpu.VMEM(((2, t, 2) + half) if dp else small, jnp.bfloat16),
            pltpu.VMEM(((t + 1, 2) + half) if mode != "dp" else small, jnp.bfloat16),
            pltpu.SemaphoreType.DMA((columns, t, 2)),
            pltpu.SemaphoreType.DMA((10, t, 2)),
            pltpu.SemaphoreType.DMA((9, t + 1, 2)),
        ]

    def z_of(self, turn):
        return self.place.target(turn) if self.over_z else 0

    def got(self, ref, lane, turn, h):
        pltpu.make_async_copy(ref, ref, self.recv.at[lane, turn, h]).wait()

    def loaded(self, column, turn, h):
        ref = self.acc.at[column, turn, h]
        pltpu.make_async_copy(ref, ref, self.load.at[column, turn, h]).wait()

    def add(self, target, refs, out=None):
        rows = target.shape[0]
        step = 16 if rows % 16 == 0 else rows
        place = target if out is None else out

        def body(i, carry):
            at = pl.ds(pl.multiple_of(i * step, step), step)
            total = target[at, :].astype(jnp.float32)
            for ref in refs:
                total = total + ref[at, :].astype(jnp.float32)
            place[at, :] = total.astype(place.dtype)
            return carry

        lax.fori_loop(0, rows // step, body, 0, unroll=2 if (rows // step) % 2 == 0 else 1)

    def begin(self):
        place = self.place
        if self.over_z:

            @pl.when((place.z == 0) | (place.z == self.length - 1))
            def _():
                def clear(i, carry):
                    self.from_z[i // 2, i % 2] = jnp.zeros(self.from_z.shape[2:], jnp.bfloat16)
                    return carry

                lax.fori_loop(0, 2 * (self.length + 1), clear, 0)

    def start(self, sends):
        place = self.place
        order = (3, 1, 2, 0) if self.over_dp else (0,)
        for column in order:
            for turn in range(self.length):
                for h in range(2):
                    pltpu.make_async_copy(
                        self.block(place.columns[column], self.z_of(turn), h),
                        self.acc.at[column, turn, h],
                        self.load.at[column, turn, h],
                    ).start()
                    if self.over_dp:
                        sends.start(
                            "core",
                            lambda column=column, turn=turn, h=h: (
                                self.block(
                                    place.columns[column] + place.to_core, self.z_of(turn), h
                                ),
                                self.from_core.at[column, turn, h],
                                self.send.at[column, turn, h],
                                self.recv.at[column, turn, h],
                            ),
                        )

    def settle(self, column, turn, h, extra=(), out=None):
        self.loaded(column, turn, h)
        refs = list(extra)
        if self.over_dp:
            ref = self.from_core.at[column, turn, h]
            self.got(ref, column, turn, h)
            refs.append(ref)
        if refs or out is not None:
            self.add(self.acc.at[column, turn, h], refs, out)

    def corners(self, sends, turn):
        if not self.over_dp or turn >= self.length:
            return
        for h, kind in ((0, "y"), (1, "x")):
            self.settle(3, turn, h)
            sends.start(
                kind,
                lambda h=h: (
                    self.acc.at[3, turn, h],
                    self.corner.at[h, turn],
                    self.send.at[4, turn, h],
                    self.recv.at[4, turn, h],
                ),
            )

    def straight(self, sends, turn, second):
        if not self.over_dp or turn >= self.length:
            return
        for column, kind in ((1, "x"), (2, "y")):
            h = (column - 1) if second else (2 - column)
            extra = ()
            if second:
                ref = self.corner.at[h, turn]
                self.got(ref, 4, turn, h)
                extra = (ref,)
            self.settle(column, turn, h, extra)
            sends.start(
                kind,
                lambda column=column, h=h: (
                    self.acc.at[column, turn, h],
                    self.from_xy.at[column - 1, turn, h],
                    self.send.at[4 + column, turn, h],
                    self.recv.at[4 + column, turn, h],
                ),
            )

    def home(self, sends, turn):
        if turn >= self.length:
            return
        place = self.place
        last = turn == self.length - 1
        z = self.z_of(turn)
        for h in range(2):
            extra = []
            if self.over_dp:
                for lane in (0, 1):
                    ref = self.from_xy.at[lane, turn, h]
                    self.got(ref, 5 + lane, turn, h)
                    extra.append(ref)
            if self.over_z:
                slot = self.from_z.at[z, h]

                def got_slot(h=h):
                    self.got(self.from_z.at[z, h], 7, z, h)

                def got_other(h=h):
                    self.got(self.from_z.at[self.length, h], 7, self.length, h)

                if last:
                    guarded(place.has_down, got_slot)
                    guarded(place.has_up, got_other)
                    extra += [slot, self.from_z.at[self.length, h]]
                else:
                    guarded((z > place.z) & place.has_down, got_slot)
                    guarded((z < place.z) & place.has_up, got_slot)
                    extra.append(slot)
            self.settle(
                0, turn, h, extra, self.out(h) if last else None
            )
            if self.over_z and not last:

                def going_up(h=h):
                    return (
                        self.acc.at[0, turn, h],
                        self.from_z.at[z, h],
                        self.send.at[7, turn, h],
                        self.recv.at[7, z, h],
                    )

                def going_down(h=h):
                    arrives = (z - place.z + 1 + self.length) // self.length
                    goal = z + arrives * (self.length - z)
                    return (
                        self.acc.at[0, turn, h],
                        self.from_z.at[goal, h],
                        self.send.at[7, turn, h],
                        self.recv.at[7, goal, h],
                    )

                above, below = z > place.z, z < place.z
                pl.when(above)(lambda: sends.start("up", going_up, above))
                pl.when(below)(lambda: sends.start("down", going_down, below))


def run_reduce(place, items):
    for item in items:
        item.begin()
    meet(place, any(i.over_z for i in items), any(i.over_dp for i in items))
    sends = Sends(place)
    for item in items:
        item.start(sends)
    longest = max(item.length for item in items)
    for turn in range(longest):
        for item in items:
            item.corners(sends, turn)
    for turn in range(longest):
        for item in items:
            item.straight(sends, turn, False)
    for turn in range(longest):
        for item in items:
            item.straight(sends, turn, True)
    for turn in range(longest):
        for item in items:
            item.home(sends, turn)
    sends.drain()


def reduce_scatter(specs, length, collective_id, name):
    count = len(specs)
    shapes, scratch, dims = [], [], []
    for array, mode, by_columns, dtype in specs:
        blocks = {"all": 8 * length, "dp": 8, "z": length}[mode]
        if by_columns:
            rows, width = array.shape[0], array.shape[1] // blocks
        else:
            rows, width = array.shape[0] // blocks, array.shape[1]
        dims.append((rows, width))
        shapes.append(jax.ShapeDtypeStruct((rows, width), dtype))
        scratch += ReduceItem.scratch(mode, length, rows, width)

    def kernel(*refs):
        place = Place(length)
        items = []
        for number, (array, mode, by_columns, dtype) in enumerate(specs):
            rows, width = dims[number]
            source, target = refs[number], refs[count + number]
            bufs = refs[2 * count + 8 * number : 2 * count + 8 * number + 8]
            half = rows // 2

            def block(column, z, h, source=source, half=half, rows=rows, width=width, mode=mode, by=by_columns):
                index = {"all": column * length + z, "dp": column, "z": z}[mode]
                if by:
                    return source.at[
                        pl.ds(h * half, half), pl.ds(pl.multiple_of(index * width, width), width)
                    ]
                return source.at[pl.ds(pl.multiple_of(index * rows + h * half, half), half)]

            def out(h, target=target, half=half):
                return target.at[pl.ds(h * half, half)]

            items.append(ReduceItem(mode, place, block, bufs, out))
        run_reduce(place, items)

    return pl.pallas_call(
        kernel,
        name=name,
        out_shape=shapes,
        in_specs=[pl.BlockSpec(memory_space=pl.ANY)] * count,
        out_specs=[pl.BlockSpec(memory_space=pltpu.VMEM)] * count,
        scratch_shapes=scratch,
        compiler_params=pltpu.CompilerParams(
            collective_id=collective_id, has_side_effects=True, vmem_limit_bytes=56 << 20
        ),
    )(*[array for array, _, _, _ in specs])


def mix(form, left, right):
    return jnp.einsum(form, left, right, preferred_element_type=jnp.float32)


def rms_scale(values):
    return lax.rsqrt(jnp.mean(values * values, axis=-1, keepdims=True) + EPSILON)


def rope_tables(seg_ids, head_dim):
    length = seg_ids.shape[0]
    row_index = jnp.arange(length, dtype=jnp.int32)
    starts = jnp.sum((seg_ids[None, :] < seg_ids[:, None]).astype(jnp.int32), axis=1)
    places = (row_index - starts).astype(jnp.float32)
    half_dim = head_dim // 2
    frequency = THETA_BASE ** (-(jnp.arange(half_dim, dtype=jnp.float32) * (2.0 / head_dim)))
    angles = places[:, None] * frequency[None, :]
    return (jnp.cos(angles), jnp.sin(angles))


def rotate(values, cosine, sine_table):
    half_dim = values.shape[-1] // 2
    front_part = values[..., :half_dim]
    back_part = values[..., half_dim:]
    cos_rows = cosine[:, None, :]
    sin_rows = sine_table[:, None, :]
    return jnp.concatenate(
        [
            front_part * cos_rows - back_part * sin_rows,
            back_part * cos_rows + front_part * sin_rows,
        ],
        axis=-1,
    )


def unrotate(values, cosine, sine_table):
    half_dim = values.shape[-1] // 2
    front_part = values[..., :half_dim]
    back_part = values[..., half_dim:]
    cos_rows = cosine[:, None, :]
    sin_rows = sine_table[:, None, :]
    return jnp.concatenate(
        [
            front_part * cos_rows + back_part * sin_rows,
            back_part * cos_rows - front_part * sin_rows,
        ],
        axis=-1,
    )


def head_norm_back(grad_out, normed, factor, gain):
    grad_normed = grad_out * gain
    grad_gain = jnp.sum(grad_out * normed, axis=(0, 1))
    grad_values = factor * (
        grad_normed - normed * jnp.mean(grad_normed * normed, axis=-1, keepdims=True)
    )
    return (grad_values, grad_gain)


def row_norm_back(grad_out, normed, factor, gain):
    grad_normed = grad_out * gain
    grad_gain = jnp.sum(grad_out * normed, axis=0)
    grad_values = factor * (
        grad_normed - normed * jnp.mean(grad_normed * normed, axis=-1, keepdims=True)
    )
    return (grad_values, grad_gain)


def softmax_rows(logits):
    top_value = jnp.max(logits, axis=-1, keepdims=True)
    expo = jnp.exp(logits - top_value)
    return expo / jnp.sum(expo, axis=-1, keepdims=True)


def attn_forward(rows, seg_ids, wq_full, wk_full, wv_full, query_gain, key_gain):
    length = rows.shape[0]
    head_dim = query_gain.shape[0]
    num_heads = wq_full.shape[1] // head_dim
    kv_heads = wk_full.shape[1] // head_dim
    per_group = num_heads // kv_heads
    inv_root = 1.0 / math.sqrt(head_dim)
    block_rows = math.gcd(length, 512)
    cosine, sine_table = rope_tables(seg_ids, head_dim)
    query = jnp.dot(rows, wq_full, preferred_element_type=jnp.float32).reshape(
        length, num_heads, head_dim
    )
    key_proj = jnp.dot(rows, wk_full, preferred_element_type=jnp.float32).reshape(
        length, kv_heads, head_dim
    )
    value_rows = (
        jnp.dot(rows, wv_full, preferred_element_type=jnp.float32)
        .astype(jnp.bfloat16)
        .reshape(length, kv_heads, head_dim)
    )
    query_factor = rms_scale(query)
    query_hat = query * query_factor
    key_factor = rms_scale(key_proj)
    key_hat = key_proj * key_factor
    query_rot = (
        rotate(query_hat * query_gain, cosine, sine_table)
        .astype(jnp.bfloat16)
        .reshape(length, kv_heads, per_group, head_dim)
    )
    key_rot = rotate(key_hat * key_gain, cosine, sine_table).astype(jnp.bfloat16)
    row_index = jnp.arange(length, dtype=jnp.int32)
    scores = mix("qgrd,kgd->grqk", query_rot, key_rot) * inv_root
    visible = (seg_ids[0:block_rows, None] == seg_ids[None, :]) & (
        row_index[None, :] <= row_index[0:block_rows, None]
    )
    scores = jnp.where(visible, scores, NEG_BIG)
    top_value = jnp.max(scores, axis=-1, keepdims=True)
    expo = jnp.exp(scores - top_value)
    totals = jnp.sum(expo, axis=-1, keepdims=True)
    prob_rows = (expo / totals).astype(jnp.bfloat16)
    outputs = mix("grqk,kgd->qgrd", prob_rows, value_rows).astype(jnp.bfloat16)
    lse_parts = top_value[..., 0] + jnp.log(totals[..., 0])
    attn_heads = outputs.reshape(length, num_heads * head_dim)
    return (
        attn_heads,
        lse_parts,
        query_rot,
        key_rot,
        value_rows,
        cosine,
        sine_table,
        query_hat,
        query_factor,
        key_hat,
        key_factor,
    )


def attn_backward(
    grad_attn, rows, seg_ids, wq_full, wk_full, wv_full, wo_full, query_gain, key_gain, saved
):
    (
        attn_heads,
        lse_all,
        query_rot,
        key_rot,
        value_rows,
        cosine,
        sine_table,
        query_hat,
        query_factor,
        key_hat,
        key_factor,
    ) = saved
    length = rows.shape[0]
    head_dim = query_gain.shape[0]
    num_heads = query_hat.shape[1]
    inv_root = 1.0 / math.sqrt(head_dim)
    block_rows = math.gcd(length, 512)
    grad_wo = jnp.dot(attn_heads.T, grad_attn, preferred_element_type=jnp.float32)
    grad_heads = (
        jnp.dot(grad_attn, wo_full.T, preferred_element_type=jnp.float32)
        .astype(jnp.bfloat16)
        .reshape(query_rot.shape)
    )
    heads_view = attn_heads.reshape(query_rot.shape)
    row_delta = jnp.transpose(
        jnp.sum(grad_heads.astype(jnp.float32) * heads_view.astype(jnp.float32), axis=-1), (1, 2, 0)
    )
    row_index = jnp.arange(length, dtype=jnp.int32)
    scores = mix("qgrd,kgd->grqk", query_rot, key_rot) * inv_root
    visible = (seg_ids[0:block_rows, None] == seg_ids[None, :]) & (
        row_index[None, :] <= row_index[0:block_rows, None]
    )
    scores = jnp.where(visible, scores, NEG_BIG)
    prob_f = jnp.where(visible, jnp.exp(scores - lse_all[:, :, 0:block_rows, None]), 0.0)
    prob_rows = prob_f.astype(jnp.bfloat16)
    grad_value = mix("grqk,qgrd->kgd", prob_rows, grad_heads)
    grad_probs = mix("qgrd,kgd->grqk", grad_heads, value_rows)
    grad_scores = (prob_f * (grad_probs - row_delta[:, :, 0:block_rows, None])).astype(jnp.bfloat16)
    pieces = mix("grqk,kgd->qgrd", grad_scores, key_rot) * inv_root
    grad_key_rot = mix("grqk,qgrd->kgd", grad_scores, query_rot) * inv_root
    grad_query_rot = pieces.reshape(length, num_heads, head_dim)
    grad_query, grad_qgain = head_norm_back(
        unrotate(grad_query_rot, cosine, sine_table), query_hat, query_factor, query_gain
    )
    grad_key, grad_kgain = head_norm_back(
        unrotate(grad_key_rot, cosine, sine_table), key_hat, key_factor, key_gain
    )
    query_b = grad_query.astype(jnp.bfloat16).reshape(length, -1)
    key_b = grad_key.astype(jnp.bfloat16).reshape(length, -1)
    value_b = grad_value.astype(jnp.bfloat16).reshape(length, -1)
    grad_rows = (
        jnp.dot(query_b, wq_full.T, preferred_element_type=jnp.float32)
        + jnp.dot(key_b, wk_full.T, preferred_element_type=jnp.float32)
        + jnp.dot(value_b, wv_full.T, preferred_element_type=jnp.float32)
    )
    grad_wq = jnp.dot(rows.T, query_b, preferred_element_type=jnp.float32)
    grad_wk = jnp.dot(rows.T, key_b, preferred_element_type=jnp.float32)
    grad_wv = jnp.dot(rows.T, value_b, preferred_element_type=jnp.float32)
    return (grad_rows, grad_wq, grad_wk, grad_wv, grad_wo, grad_qgain, grad_kgain)


def expert_forward(expert_rows, wgate, wup, wdown):
    gate_pre = jnp.dot(expert_rows, wgate, preferred_element_type=jnp.float32)
    up_pre = jnp.dot(expert_rows, wup, preferred_element_type=jnp.float32)
    hidden_units = (jax.nn.silu(gate_pre) * up_pre).astype(jnp.bfloat16)
    result = jnp.dot(hidden_units, wdown, preferred_element_type=jnp.float32).astype(jnp.bfloat16)
    return (result, gate_pre, up_pre, hidden_units)


def expert_backward(expert_rows, grad_result, wgate, wup, wdown, gate_pre, up_pre, hidden_units):
    grad_hidden = jnp.dot(grad_result, wdown.T, preferred_element_type=jnp.float32)
    sigma = jax.nn.sigmoid(gate_pre)
    grad_gate_pre = (grad_hidden * up_pre * sigma * (1.0 + gate_pre * (1.0 - sigma))).astype(
        jnp.bfloat16
    )
    grad_up_pre = (grad_hidden * gate_pre * sigma).astype(jnp.bfloat16)
    grad_rows = (
        jnp.dot(grad_gate_pre, wgate.T, preferred_element_type=jnp.float32)
        + jnp.dot(grad_up_pre, wup.T, preferred_element_type=jnp.float32)
    ).astype(jnp.bfloat16)
    grad_wd = jnp.dot(hidden_units.T, grad_result, preferred_element_type=jnp.float32)
    grad_wg = jnp.dot(expert_rows.T, grad_gate_pre, preferred_element_type=jnp.float32)
    grad_wu = jnp.dot(expert_rows.T, grad_up_pre, preferred_element_type=jnp.float32)
    return (grad_rows, grad_wg, grad_wu, grad_wd)


def to_experts(buffer):
    return lax.all_to_all(buffer, ("dp", "tensor"), split_axis=0, concat_axis=0, tiled=True)


def to_sources(buffer):
    return lax.all_to_all(buffer, ("dp", "tensor"), split_axis=0, concat_axis=0, tiled=True)


def shards(
    hidden_in,
    segments,
    routes,
    query_weight,
    key_weight,
    value_weight,
    output_weight,
    gain_attn,
    gain_moe,
    query_gain,
    key_gain,
    router,
    gate_weight,
    up_weight,
    down_weight,
    cotangent,
):
    seg_ids = segments[0]
    rows_dev = hidden_in.shape[0]
    width = hidden_in.shape[1]
    top_count = routes.shape[1]
    experts = router.shape[1]
    capacity = 2 * rows_dev * top_count // experts
    full_query, full_key, full_value, full_output = (
        lax.all_gather(query_weight, "dp", axis=0, tiled=True),
        lax.all_gather(key_weight, "dp", axis=0, tiled=True),
        lax.all_gather(value_weight, "dp", axis=0, tiled=True),
        lax.all_gather(output_weight, "dp", axis=1, tiled=True),
    )
    inputs32 = hidden_in.astype(jnp.float32)
    factor_one = rms_scale(inputs32)
    normed_one = inputs32 * factor_one
    rows_one = (normed_one * gain_attn).astype(jnp.bfloat16)
    group_rows = lax.all_gather(rows_one, "tensor", axis=0, tiled=True)
    saved = attn_forward(
        group_rows, seg_ids, full_query, full_key, full_value, query_gain, key_gain
    )
    partial_add = jnp.dot(saved[0], full_output, preferred_element_type=jnp.float32)
    attn_add = lax.psum_scatter(partial_add, "tensor", scatter_dimension=0, tiled=True)
    residual = inputs32 + attn_add
    factor_two = rms_scale(residual)
    normed_two = residual * factor_two
    rows_two = (normed_two * gain_moe).astype(jnp.bfloat16)
    router_probs = softmax_rows(jnp.dot(rows_two, router, preferred_element_type=jnp.float32))
    route_hot = (routes[:, :, None] == jnp.arange(experts, dtype=jnp.int32)[None, None, :]).astype(
        jnp.float32
    )
    picked = jnp.sum(route_hot * router_probs[:, None, :], axis=-1)
    total = jnp.sum(picked, axis=1, keepdims=True)
    gates = picked / total
    flat_routes = routes.reshape(-1)
    onehot = (flat_routes[:, None] == jnp.arange(experts, dtype=jnp.int32)[None, :]).astype(
        jnp.int32
    )
    ranks = jnp.sum(onehot * jnp.cumsum(onehot, axis=0), axis=1) - 1
    slots = flat_routes * capacity + ranks
    send_rows = (
        jnp.zeros((experts * capacity, width), jnp.bfloat16)
        .at[slots]
        .set(jnp.repeat(rows_two, top_count, axis=0))
    )
    received = to_experts(send_rows.reshape(experts, capacity, width)).reshape(-1, width)
    result, gate_pre, up_pre, hidden_units = expert_forward(
        received, gate_weight[0], up_weight[0], down_weight[0]
    )
    returned = to_sources(result.reshape(-1, capacity, width)).reshape(experts * capacity, width)
    pair_out = returned[slots].astype(jnp.float32).reshape(rows_dev, top_count, width)
    moe_sum = jnp.sum(gates[:, :, None] * pair_out, axis=1)
    output = (residual + moe_sum).astype(jnp.bfloat16)
    cot32 = cotangent.astype(jnp.float32)
    grad_gates = jnp.sum(cot32[:, None, :] * pair_out, axis=-1)
    grad_result = (gates[:, :, None] * cot32[:, None, :]).astype(jnp.bfloat16).reshape(-1, width)
    send_grads = jnp.zeros((experts * capacity, width), jnp.bfloat16).at[slots].set(grad_result)
    received_grads = to_experts(send_grads.reshape(experts, capacity, width)).reshape(-1, width)
    grad_expert_rows, grad_wg, grad_wu, grad_wd = expert_backward(
        received,
        received_grads,
        gate_weight[0],
        up_weight[0],
        down_weight[0],
        gate_pre,
        up_pre,
        hidden_units,
    )
    returned_grads = to_sources(grad_expert_rows.reshape(-1, capacity, width)).reshape(
        experts * capacity, width
    )
    grad_pairs = returned_grads[slots].astype(jnp.float32).reshape(rows_dev, top_count, width)
    grad_picked = (grad_gates - jnp.sum(gates * grad_gates, axis=1, keepdims=True)) / total
    grad_probs = jnp.sum(route_hot * grad_picked[:, :, None], axis=1)
    grad_logits = (
        router_probs * (grad_probs - jnp.sum(grad_probs * router_probs, axis=-1, keepdims=True))
    ).astype(jnp.bfloat16)
    grad_router = jnp.dot(rows_two.T, grad_logits, preferred_element_type=jnp.float32)
    grad_rows_two = jnp.sum(grad_pairs, axis=1) + jnp.dot(
        grad_logits, router.T, preferred_element_type=jnp.float32
    )
    grad_res_norm, grad_gain_moe = row_norm_back(grad_rows_two, normed_two, factor_two, gain_moe)
    grad_residual = cot32 + grad_res_norm
    grad_attn = grad_residual.astype(jnp.bfloat16)
    group_grads = lax.all_gather(grad_attn, "tensor", axis=0, tiled=True)
    back_query, back_key, back_value, back_output = (
        lax.all_gather(query_weight, "dp", axis=0, tiled=True),
        lax.all_gather(key_weight, "dp", axis=0, tiled=True),
        lax.all_gather(value_weight, "dp", axis=0, tiled=True),
        lax.all_gather(output_weight, "dp", axis=1, tiled=True),
    )
    grad_group_rows, grad_wq, grad_wk, grad_wv, grad_wo, grad_qgain, grad_kgain = attn_backward(
        group_grads,
        group_rows,
        seg_ids,
        back_query,
        back_key,
        back_value,
        back_output,
        query_gain,
        key_gain,
        saved,
    )
    grad_rows_one = lax.psum_scatter(
        grad_group_rows.astype(jnp.bfloat16), "tensor", scatter_dimension=0, tiled=True
    ).astype(jnp.float32)
    grad_in_norm, grad_gain_attn = row_norm_back(grad_rows_one, normed_one, factor_one, gain_attn)
    grad_input = grad_residual + grad_in_norm
    grad_wq, grad_wk, grad_wv, grad_wo = (
        lax.psum_scatter(
            grad_wq.astype(jnp.bfloat16), "dp", scatter_dimension=0, tiled=True
        ).astype(jnp.float32),
        lax.psum_scatter(
            grad_wk.astype(jnp.bfloat16), "dp", scatter_dimension=0, tiled=True
        ).astype(jnp.float32),
        lax.psum_scatter(
            grad_wv.astype(jnp.bfloat16), "dp", scatter_dimension=0, tiled=True
        ).astype(jnp.float32),
        lax.psum_scatter(
            grad_wo.astype(jnp.bfloat16), "dp", scatter_dimension=1, tiled=True
        ).astype(jnp.float32),
    )
    grad_gain_attn, grad_gain_moe, grad_qgain, grad_kgain, grad_router = lax.psum(
        (grad_gain_attn, grad_gain_moe, grad_qgain, grad_kgain, grad_router), ("dp", "tensor")
    )
    return (
        output,
        grad_input,
        grad_wq,
        grad_wk,
        grad_wv,
        grad_wo,
        grad_gain_attn,
        grad_gain_moe,
        grad_qgain,
        grad_kgain,
        grad_router,
        grad_wg[None],
        grad_wu[None],
        grad_wd[None],
    )


def attn_backward_joint(
    grad_attn, rows, seg_ids, joint_full, wo_full, query_gain, key_gain, saved
):
    (
        attn_heads,
        lse_all,
        query_rot,
        key_rot,
        value_rows,
        cosine,
        sine_table,
        query_hat,
        query_factor,
        key_hat,
        key_factor,
    ) = saved
    length = rows.shape[0]
    head_dim = query_gain.shape[0]
    num_heads = query_hat.shape[1]
    inv_root = 1.0 / math.sqrt(head_dim)
    block_rows = math.gcd(length, 512)
    grad_wo = jnp.dot(attn_heads.T, grad_attn, preferred_element_type=jnp.float32)
    grad_heads = (
        jnp.dot(grad_attn, wo_full.T, preferred_element_type=jnp.float32)
        .astype(jnp.bfloat16)
        .reshape(query_rot.shape)
    )
    heads_view = attn_heads.reshape(query_rot.shape)
    row_delta = jnp.transpose(
        jnp.sum(grad_heads.astype(jnp.float32) * heads_view.astype(jnp.float32), axis=-1), (1, 2, 0)
    )
    row_index = jnp.arange(length, dtype=jnp.int32)
    scores = mix("qgrd,kgd->grqk", query_rot, key_rot) * inv_root
    visible = (seg_ids[0:block_rows, None] == seg_ids[None, :]) & (
        row_index[None, :] <= row_index[0:block_rows, None]
    )
    scores = jnp.where(visible, scores, NEG_BIG)
    prob_f = jnp.where(visible, jnp.exp(scores - lse_all[:, :, 0:block_rows, None]), 0.0)
    prob_rows = prob_f.astype(jnp.bfloat16)
    grad_value = mix("grqk,qgrd->kgd", prob_rows, grad_heads)
    grad_probs = mix("qgrd,kgd->grqk", grad_heads, value_rows)
    grad_scores = (prob_f * (grad_probs - row_delta[:, :, 0:block_rows, None])).astype(jnp.bfloat16)
    pieces = mix("grqk,kgd->qgrd", grad_scores, key_rot) * inv_root
    grad_key_rot = mix("grqk,qgrd->kgd", grad_scores, query_rot) * inv_root
    grad_query_rot = pieces.reshape(length, num_heads, head_dim)
    grad_query, grad_qgain = head_norm_back(
        unrotate(grad_query_rot, cosine, sine_table), query_hat, query_factor, query_gain
    )
    grad_key, grad_kgain = head_norm_back(
        unrotate(grad_key_rot, cosine, sine_table), key_hat, key_factor, key_gain
    )
    query_b = grad_query.astype(jnp.bfloat16).reshape(length, -1)
    key_b = grad_key.astype(jnp.bfloat16).reshape(length, -1)
    value_b = grad_value.astype(jnp.bfloat16).reshape(length, -1)
    joint_b = jnp.concatenate([query_b, key_b, value_b], axis=1)
    grad_rows = jnp.dot(joint_b, joint_full.T, preferred_element_type=jnp.float32)
    grad_joint = jnp.dot(rows.T, joint_b, preferred_element_type=jnp.float32)
    return (grad_rows, grad_joint, grad_wo, grad_qgain, grad_kgain)


AXES = ("dp", "tensor")


def slots_of(marks, capacity):
    rows = marks.shape[1]
    order = jnp.arange(rows, dtype=jnp.int32)
    upto = (order[:, None] <= order[None, :]).astype(jnp.bfloat16)
    ranks = jnp.dot(marks.astype(jnp.bfloat16), upto, preferred_element_type=jnp.float32) - 1.0
    slot = jnp.arange(capacity, dtype=jnp.float32)
    chosen = (ranks[:, None, :] == slot[None, :, None]) & (marks[:, None, :] > 0.5)
    return chosen.astype(jnp.bfloat16)


def gathered(
    hidden_in,
    segments,
    routes,
    query_weight,
    key_weight,
    value_weight,
    output_weight,
    gain_attn,
    gain_moe,
    query_gain,
    key_gain,
    router,
    gate_weight,
    up_weight,
    down_weight,
    cotangent,
):
    seg_ids = segments[0]
    rows_dev, width = hidden_in.shape
    top_count = routes.shape[1]
    experts = router.shape[1]
    capacity = 2 * rows_dev * top_count // experts
    length = lax.axis_size("tensor")
    devices = lax.axis_size("dp") * length
    expert = lax.axis_index("dp") * length + lax.axis_index("tensor")
    query_cols, key_cols = query_weight.shape[1], key_weight.shape[1]

    inputs32 = hidden_in.astype(jnp.float32)
    factor_one = rms_scale(inputs32)
    normed_one = inputs32 * factor_one
    rows_one = (normed_one * gain_attn).astype(jnp.bfloat16)
    joint_weight = jnp.concatenate([query_weight, key_weight, value_weight], axis=1)
    group_rows, full_joint, full_output = gather(
        [
            (rows_one, "z", False),
            (joint_weight, "dp", False),
            (output_weight, "dp", True),
        ],
        length,
        0,
        "gather_attention",
    )
    group_rows = group_rows.reshape(-1, width)
    full_joint = full_joint.reshape(width, -1)
    full_query = full_joint[:, :query_cols]
    full_key = full_joint[:, query_cols : query_cols + key_cols]
    full_value = full_joint[:, query_cols + key_cols :]
    saved = attn_forward(
        group_rows, seg_ids, full_query, full_key, full_value, query_gain, key_gain
    )
    partial_add = jnp.dot(saved[0], full_output, preferred_element_type=jnp.float32)
    (attn_add,) = reduce_scatter(
        [(partial_add.astype(jnp.bfloat16), "z", False, jnp.float32)], length, 1, "reduce_attention"
    )
    residual = inputs32 + attn_add
    factor_two = rms_scale(residual)
    normed_two = residual * factor_two
    rows_two = (normed_two * gain_moe).astype(jnp.bfloat16)
    router_probs = softmax_rows(jnp.dot(rows_two, router, preferred_element_type=jnp.float32))
    route_hot = (routes[:, :, None] == jnp.arange(experts, dtype=jnp.int32)[None, None, :]).astype(
        jnp.float32
    )
    picked = jnp.sum(route_hot * router_probs[:, None, :], axis=-1)
    total = jnp.sum(picked, axis=1, keepdims=True)
    gates = picked / total
    named = jnp.sum(route_hot, axis=1)
    gate_table = jnp.where(named > 0.5, jnp.sum(route_hot * gates[:, :, None], axis=1), -1.0)
    all_rows, all_cots, all_gates = gather(
        [
            (rows_two, "all", False),
            (cotangent, "all", False),
            (gate_table.T, "all", False),
        ],
        length,
        2,
        "gather_rows",
    )
    own_gates = lax.dynamic_slice_in_dim(all_gates, expert, 1, axis=1)[:, 0, :]
    marks = (own_gates >= 0.0).astype(jnp.float32)
    chosen = slots_of(marks, capacity)
    slot_gates = jnp.sum(chosen.astype(jnp.float32) * own_gates[:, None, :], axis=-1)
    received = mix("bst,btd->bsd", chosen, all_rows).astype(jnp.bfloat16).reshape(-1, width)
    cot_slots = mix("bst,btd->bsd", chosen, all_cots).reshape(-1, width)
    received_grads = (slot_gates.reshape(-1, 1) * cot_slots).astype(jnp.bfloat16)
    result, gate_pre, up_pre, hidden_units = expert_forward(
        received, gate_weight[0], up_weight[0], down_weight[0]
    )
    grad_expert_rows, grad_wg, grad_wu, grad_wd = expert_backward(
        received,
        received_grads,
        gate_weight[0],
        up_weight[0],
        down_weight[0],
        gate_pre,
        up_pre,
        hidden_units,
    )
    result32 = result.astype(jnp.float32)
    slot_grads = jnp.sum(cot_slots * result32, axis=-1).reshape(devices, capacity)
    token_grads = jnp.sum(chosen.astype(jnp.float32) * slot_grads[:, :, None], axis=1)
    back_grads = lax.all_to_all(token_grads, AXES, split_axis=0, concat_axis=0, tiled=True)
    partial_rows = mix(
        "bst,bsd->btd", chosen, grad_expert_rows.reshape(devices, capacity, width)
    ).astype(jnp.bfloat16)
    (grad_sum,) = reduce_scatter(
        [(partial_rows.reshape(-1, width), "all", False, jnp.float32)], length, 3, "reduce_grads"
    )
    scaled = (slot_gates.reshape(-1, 1) * result32).astype(jnp.bfloat16)
    partial_out = mix("bst,bsd->btd", chosen, scaled.reshape(devices, capacity, width)).astype(
        jnp.bfloat16
    )
    (moe_sum,) = reduce_scatter(
        [(partial_out.reshape(-1, width), "all", False, jnp.float32)], length, 4, "reduce_outputs"
    )
    output = (residual + moe_sum).astype(jnp.bfloat16)
    cot32 = cotangent.astype(jnp.float32)
    grad_gates = jnp.sum(route_hot * back_grads.T[:, None, :], axis=-1)
    grad_picked = (grad_gates - jnp.sum(gates * grad_gates, axis=1, keepdims=True)) / total
    grad_probs = jnp.sum(route_hot * grad_picked[:, :, None], axis=1)
    grad_logits = (
        router_probs * (grad_probs - jnp.sum(grad_probs * router_probs, axis=-1, keepdims=True))
    ).astype(jnp.bfloat16)
    all_logits = lax.all_gather(grad_logits, AXES, axis=0, tiled=True)
    grad_router = jnp.dot(
        all_rows.reshape(-1, width).T, all_logits, preferred_element_type=jnp.float32
    )
    grad_rows_two = grad_sum + jnp.dot(grad_logits, router.T, preferred_element_type=jnp.float32)
    grad_res_norm, grad_gain_moe = row_norm_back(grad_rows_two, normed_two, factor_two, gain_moe)
    grad_residual = cot32 + grad_res_norm
    grad_attn = grad_residual.astype(jnp.bfloat16)
    (group_grads,) = gather([(grad_attn, "z", False)], length, 5, "gather_grads")
    grad_group_rows, grad_joint, grad_wo, grad_qgain, grad_kgain = attn_backward_joint(
        group_grads.reshape(-1, width),
        group_rows,
        seg_ids,
        full_joint,
        full_output,
        query_gain,
        key_gain,
        saved,
    )
    grad_rows_one, grad_joint, grad_wo = reduce_scatter(
        [
            (grad_group_rows.astype(jnp.bfloat16), "z", False, jnp.float32),
            (grad_joint.astype(jnp.bfloat16), "dp", False, jnp.float32),
            (grad_wo.astype(jnp.bfloat16), "dp", True, jnp.float32),
        ],
        length,
        6,
        "reduce_weights",
    )
    grad_in_norm, grad_gain_attn = row_norm_back(grad_rows_one, normed_one, factor_one, gain_attn)
    grad_input = grad_residual + grad_in_norm
    small = jnp.concatenate([grad_gain_attn, grad_gain_moe, grad_qgain, grad_kgain]).reshape(-1, 128)
    small = jnp.pad(small, ((0, -small.shape[0] % 16), (0, 0)))
    (all_small,) = gather([(small, "all", False)], length, 7, "gather_small")
    sums = jnp.sum(all_small, axis=0).reshape(-1)
    head_dim = query_gain.shape[0]
    return (
        output,
        grad_input,
        grad_joint[:, :query_cols],
        grad_joint[:, query_cols : query_cols + key_cols],
        grad_joint[:, query_cols + key_cols :],
        grad_wo,
        sums[:width],
        sums[width : 2 * width],
        sums[2 * width : 2 * width + head_dim],
        sums[2 * width + head_dim : 2 * width + 2 * head_dim],
        grad_router,
        grad_wg[None],
        grad_wu[None],
        grad_wd[None],
    )


def solution(mesh):
    placed = (
        P(("dp", "tensor"), None),
        P("dp", None),
        P(("dp", "tensor"), None),
        P("dp", "tensor"),
        P("dp", "tensor"),
        P("dp", "tensor"),
        P("tensor", "dp"),
        P(),
        P(),
        P(),
        P(),
        P(),
        P(("dp", "tensor"), None, None),
        P(("dp", "tensor"), None, None),
        P(("dp", "tensor"), None, None),
        P(("dp", "tensor"), None),
    )
    program = gathered if mesh.shape["dp"] == 8 and mesh.shape["tensor"] <= 4 else shards
    return jax.shard_map(
        program,
        mesh=mesh,
        in_specs=placed,
        out_specs=(
            P(("dp", "tensor"), None),
            P(("dp", "tensor"), None),
            P("dp", "tensor"),
            P("dp", "tensor"),
            P("dp", "tensor"),
            P("tensor", "dp"),
            P(),
            P(),
            P(),
            P(),
            P(),
            P(("dp", "tensor"), None, None),
            P(("dp", "tensor"), None, None),
            P(("dp", "tensor"), None, None),
        ),
        check_vma=False,
    )
```

```python
import math

import jax
import jax.numpy as jnp
from jax import lax
from jax.experimental import pallas as pl
from jax.experimental.pallas import tpu as pltpu
from jax.sharding import PartitionSpec as P

EPSILON = 1e-06
THETA_BASE = 1000000.0
NEG_BIG = -1e30


MESH = pl.DeviceIdType.MESH


class Place:
    def __init__(self, length):
        self.length = length
        self.dp = lax.axis_index("dp")
        self.z = lax.axis_index("tensor")
        core, along_x, along_y = self.dp % 2, (self.dp // 2) % 2, self.dp // 4
        self.to_core = 1 - 2 * core
        self.core = self.dp + self.to_core
        self.x = self.dp + 2 - 4 * along_x
        self.y = self.dp + 4 - 8 * along_y
        self.columns = (self.dp, self.x, self.y, self.x + self.y - self.dp)

    def device(self, kind):
        if kind == "x":
            return (self.x, self.z)
        if kind == "y":
            return (self.y, self.z)
        if kind == "core":
            return (self.core, self.z)
        if kind == "up":
            return (self.dp, self.z + 1)
        return (self.dp, self.z - 1)

    @property
    def has_up(self):
        return self.z < self.length - 1

    @property
    def has_down(self):
        return self.z > 0

    def condition(self, kind):
        if kind == "up":
            return self.has_up
        return self.has_down if kind == "down" else None

    def nearest(self, turn):
        length = self.length

        def equal(left, right):
            far = 2 * length
            return (left - right + far) // far - (left - right - 1 + far) // far

        found = 0
        for mine in range(length):
            order = sorted(range(length), key=lambda other: (abs(other - mine), other))
            for step, other in enumerate(order):
                if other:
                    found = found + equal(self.z, mine) * equal(turn, step) * other
        return found

    def target(self, turn):
        length, z = self.length, self.z

        def at_least(left, right):
            return (left - right + 2 * length) // (2 * length)

        high = at_least(z, length // 2)
        mirrored = z + high * (length - 1 - 2 * z)
        above = length - 1 - mirrored
        first = at_least(above - 1, turn)
        if turn == length - 1:
            return z
        found = first * (length - 1 - turn) + (1 - first) * (turn - above)
        return found + high * (length - 1 - 2 * found)


def guarded(condition, action):
    if condition is None:
        action()
    else:
        pl.when(condition)(action)


def meet(place, over_z, over_dp):
    barrier = pltpu.get_barrier_semaphore()
    kinds = (("x", "y", "core") if over_dp else ()) + (("up", "down") if over_z else ())
    for kind in kinds:

        def greet(kind=kind):
            pl.semaphore_signal(
                barrier, 1, device_id=place.device(kind), device_id_type=MESH
            )

        guarded(place.condition(kind), greet)
    count = 3 if over_dp else 0
    if over_z:
        length = place.length
        count = count + (place.z + length - 1) // length + (2 * length - 2 - place.z) // length
    pl.semaphore_wait(barrier, count)


class Sends:
    def __init__(self, place):
        self.place = place
        self.started = []

    def start(self, kind, views, condition=lambda: None):
        def build():
            source, target, send_sem, recv_sem = views()
            return pltpu.make_async_remote_copy(
                src_ref=source,
                dst_ref=target,
                send_sem=send_sem,
                recv_sem=recv_sem,
                device_id=self.place.device(kind),
                device_id_type=MESH,
            )

        guarded(self.place.condition(kind), lambda: build().start())
        self.started.append((condition, kind, build))

    def drain(self):
        for condition, kind, build in self.started:

            def finish(kind=kind, build=build):
                guarded(self.place.condition(kind), lambda: build().wait_send())

            guarded(condition(), finish)


class GatherItem:
    def __init__(self, mode, place, own, slot, recv, send, local):
        self.mode, self.place = mode, place
        self.own, self.slot = own, slot
        self.recv, self.send, self.local = recv, send, local
        self.over_z = mode != "dp"
        self.over_dp = mode != "z"
        self.length = place.length if self.over_z else 1
        self.z = place.z if self.over_z else 0

    def index(self, column, z):
        if self.mode == "all":
            return column * self.length + z
        return column if self.mode == "dp" else z

    @staticmethod
    def semaphores(mode, length):
        blocks = {"all": 8 * length, "dp": 8, "z": length}[mode]
        turns = 2 * length - 1 if mode != "dp" else 1
        return [
            pltpu.SemaphoreType.DMA((blocks, 2)),
            pltpu.SemaphoreType.DMA((10, turns, 2)),
            pltpu.SemaphoreType.DMA((2,)),
        ]

    def turns(self, distance):
        if distance == 0:
            return [(0, 0, lambda: None, None)]
        place, length = self.place, self.length
        return [
            (2 * distance - 1, -distance, lambda: place.z >= distance, "up"),
            (2 * distance, distance, lambda: place.z < length - distance, "down"),
        ]

    def pass_on(self, sends, lane, kind, column, offset, turn, h, source=None, condition=lambda: None):
        def views():
            z = self.z + offset
            view = self.slot(column, z, h)
            return (
                view if source is None else source(h),
                view,
                self.send.at[lane, turn, h],
                self.recv.at[self.index(column, z), h],
            )

        sends.start(kind, views, condition)

    def arrived(self, column, z, h):
        view = self.slot(column, z, h)
        pltpu.make_async_copy(view, view, self.recv.at[self.index(column, z), h]).wait()

    def begin(self, sends):
        place = self.place
        for h in range(2):
            own = self.own
            if self.over_z:
                self.pass_on(sends, 0, "up", place.dp, 0, 0, h, own)
                self.pass_on(sends, 1, "down", place.dp, 0, 0, h, own)
            if self.over_dp:
                self.pass_on(sends, 2, "x", place.dp, 0, 0, h, own)
                self.pass_on(sends, 3, "y", place.dp, 0, 0, h, own)
                self.pass_on(sends, 4, "core", place.dp, 0, 0, h, own)
        for h in range(2):
            pltpu.make_async_copy(
                self.own(h), self.slot(place.dp, self.z, h), self.local.at[h]
            ).start()

    def along_z(self, sends, distance):
        if not self.over_z or distance >= self.length:
            return
        place = self.place
        for turn, offset, condition, onward in self.turns(distance):

            def step(turn=turn, offset=offset, condition=condition, onward=onward):
                for h in range(2):
                    self.arrived(place.dp, self.z + offset, h)
                    if distance < self.length - 1:
                        self.pass_on(
                            sends, 0 if onward == "up" else 1, onward, place.dp, offset, turn, h,
                            condition=condition,
                        )
                    if self.over_dp:
                        for lane, kind in ((2, "x"), (3, "y"), (4, "core")):
                            self.pass_on(
                                sends, lane, kind, place.dp, offset, turn, h, condition=condition
                            )

            guarded(condition(), step)

    def across(self, sends, distance):
        if not self.over_dp or not 0 <= distance < self.length:
            return
        _, x, y, _ = self.place.columns
        for turn, offset, condition, _ in self.turns(distance):

            def step(turn=turn, offset=offset, condition=condition):
                for h in range(2):
                    self.arrived(x, self.z + offset, h)
                    if h == 0:
                        self.pass_on(sends, 5, "y", x, offset, turn, h, condition=condition)
                    self.pass_on(sends, 7, "core", x, offset, turn, h, condition=condition)
                    self.arrived(y, self.z + offset, h)
                    if h == 1:
                        self.pass_on(sends, 6, "x", y, offset, turn, h, condition=condition)
                    self.pass_on(sends, 8, "core", y, offset, turn, h, condition=condition)

            guarded(condition(), step)

    def diagonal(self, sends, distance):
        if not self.over_dp or not 0 <= distance < self.length:
            return
        corner = self.place.columns[3]
        for turn, offset, condition, _ in self.turns(distance):

            def step(turn=turn, offset=offset, condition=condition):
                for h in range(2):
                    self.arrived(corner, self.z + offset, h)
                    self.pass_on(sends, 9, "core", corner, offset, turn, h, condition=condition)

            guarded(condition(), step)

    def settled(self):
        for h in range(2):
            pltpu.make_async_copy(
                self.own(h), self.slot(self.place.dp, self.z, h), self.local.at[h]
            ).wait()

    def from_core(self, z):
        for column in self.place.columns:
            for h in range(2):
                self.arrived(column + self.place.to_core, z, h)

    def finish(self):
        self.settled()
        if self.over_dp:
            for z in range(self.length):
                self.from_core(z)


def run_gather(place, items):
    meet(place, any(i.over_z for i in items), any(i.over_dp for i in items))
    sends = Sends(place)
    for item in items:
        item.begin(sends)
    for step in range(place.length + 2):
        for item in items:
            item.along_z(sends, step + 1)
        for item in items:
            item.across(sends, step)
        for item in items:
            item.diagonal(sends, step - 1)
    for item in items:
        item.finish()
    sends.drain()


def gather(specs, length, collective_id, name):
    modes = [mode for _, mode, _ in specs]
    shapes, sems = [], []
    for array, mode, by_columns in specs:
        blocks = {"all": 8 * length, "dp": 8, "z": length}[mode]
        if by_columns:
            shape = (array.shape[0], blocks * array.shape[1])
        else:
            shape = (blocks,) + array.shape
        shapes.append(jax.ShapeDtypeStruct(shape, array.dtype))
        sems += GatherItem.semaphores(mode, length)
    count = len(specs)

    def kernel(*refs):
        place = Place(length)
        items = []
        for number, (array, mode, by_columns) in enumerate(specs):
            source, target = refs[number], refs[count + number]
            recv, send, local = refs[2 * count + 3 * number : 2 * count + 3 * number + 3]
            half = array.shape[0] // 2
            width = array.shape[1]
            item = GatherItem(mode, place, None, None, recv, send, local)

            def own(h, source=source, half=half):
                return source.at[pl.ds(h * half, half)]

            def slot(column, z, h, target=target, half=half, width=width, item=item, by=by_columns):
                block = item.index(column, z)
                if by:
                    return target.at[
                        pl.ds(h * half, half), pl.ds(pl.multiple_of(block * width, width), width)
                    ]
                return target.at[block, pl.ds(h * half, half)]

            item.own, item.slot = own, slot
            items.append(item)
        run_gather(place, items)

    return pl.pallas_call(
        kernel,
        name=name,
        out_shape=shapes,
        in_specs=[pl.BlockSpec(memory_space=pl.ANY)] * count,
        out_specs=[pl.BlockSpec(memory_space=pl.ANY)] * count,
        scratch_shapes=sems,
        compiler_params=pltpu.CompilerParams(collective_id=collective_id, has_side_effects=True),
    )(*[array for array, _, _ in specs])


class ReduceItem:
    def __init__(self, mode, place, block, bufs, out):
        self.mode, self.place, self.block, self.out = mode, place, block, out
        self.over_z = mode != "dp"
        self.over_dp = mode != "z"
        self.length = place.length if self.over_z else 1
        (self.acc, self.from_core, self.corner, self.from_xy, self.from_z,
         self.load, self.send, self.recv) = bufs

    @staticmethod
    def scratch(mode, length, rows, width):
        t = length if mode != "dp" else 1
        columns = 4 if mode != "z" else 1
        dp = mode != "z"
        half = (rows // 2, width)
        small = (8, 128)
        return [
            pltpu.VMEM((columns, t, 2) + half, jnp.bfloat16),
            pltpu.VMEM(((columns, t, 2) + half) if dp else small, jnp.bfloat16),
            pltpu.VMEM(((2, t) + half) if dp else small, jnp.bfloat16),
            pltpu.VMEM(((2, t, 2) + half) if dp else small, jnp.bfloat16),
            pltpu.VMEM(((t + 1, 2) + half) if mode != "dp" else small, jnp.bfloat16),
            pltpu.SemaphoreType.DMA((columns, t, 2)),
            pltpu.SemaphoreType.DMA((10, t, 2)),
            pltpu.SemaphoreType.DMA((9, t + 1, 2)),
        ]

    def z_of(self, turn):
        return self.place.target(turn) if self.over_z else 0

    def got(self, ref, lane, turn, h):
        pltpu.make_async_copy(ref, ref, self.recv.at[lane, turn, h]).wait()

    def loaded(self, column, turn, h):
        ref = self.acc.at[column, turn, h]
        pltpu.make_async_copy(ref, ref, self.load.at[column, turn, h]).wait()

    def add(self, target, refs, out=None):
        rows = target.shape[0]
        step = 16 if rows % 16 == 0 else rows
        place = target if out is None else out

        def body(i, carry):
            at = pl.ds(pl.multiple_of(i * step, step), step)
            total = target[at, :].astype(jnp.float32)
            for ref in refs:
                total = total + ref[at, :].astype(jnp.float32)
            place[at, :] = total.astype(place.dtype)
            return carry

        lax.fori_loop(0, rows // step, body, 0, unroll=2 if (rows // step) % 2 == 0 else 1)

    def begin(self):
        place = self.place
        if self.over_z:

            @pl.when((place.z == 0) | (place.z == self.length - 1))
            def _():
                def clear(i, carry):
                    self.from_z[i // 2, i % 2] = jnp.zeros(self.from_z.shape[2:], jnp.bfloat16)
                    return carry

                lax.fori_loop(0, 2 * (self.length + 1), clear, 0)

    def load_all(self):
        place = self.place
        for turn in range(self.length):
            for column in (3, 1, 2, 0) if self.over_dp else (0,):
                for h in range(2):
                    pltpu.make_async_copy(
                        self.block(place.columns[column], self.z_of(turn), h),
                        self.acc.at[column, turn, h],
                        self.load.at[column, turn, h],
                    ).start()

    def hand_over(self, sends, turn):
        if not self.over_dp or turn >= self.length:
            return
        place = self.place
        for column in (3, 1, 2, 0):
            for h in range(2):
                sends.start(
                    "core",
                    lambda column=column, h=h: (
                        self.block(place.columns[column] + place.to_core, self.z_of(turn), h),
                        self.from_core.at[column, turn, h],
                        self.send.at[column, turn, h],
                        self.recv.at[column, turn, h],
                    ),
                )

    def settle(self, column, turn, h, extra=(), out=None):
        self.loaded(column, turn, h)
        refs = list(extra)
        if self.over_dp:
            ref = self.from_core.at[column, turn, h]
            self.got(ref, column, turn, h)
            refs.append(ref)
        if refs or out is not None:
            self.add(self.acc.at[column, turn, h], refs, out)

    def corners(self, sends, turn):
        if not self.over_dp or not 0 <= turn < self.length:
            return
        for h, kind in ((0, "y"), (1, "x")):
            self.settle(3, turn, h)
            sends.start(
                kind,
                lambda h=h: (
                    self.acc.at[3, turn, h],
                    self.corner.at[h, turn],
                    self.send.at[4, turn, h],
                    self.recv.at[4, turn, h],
                ),
            )

    def straight(self, sends, turn, second):
        if not self.over_dp or not 0 <= turn < self.length:
            return
        for column, kind in ((1, "x"), (2, "y")):
            h = (column - 1) if second else (2 - column)
            extra = ()
            if second:
                ref = self.corner.at[h, turn]
                self.got(ref, 4, turn, h)
                extra = (ref,)
            self.settle(column, turn, h, extra)
            sends.start(
                kind,
                lambda column=column, h=h: (
                    self.acc.at[column, turn, h],
                    self.from_xy.at[column - 1, turn, h],
                    self.send.at[4 + column, turn, h],
                    self.recv.at[4 + column, turn, h],
                ),
            )

    def home(self, sends, turn):
        if not 0 <= turn < self.length:
            return
        place = self.place
        last = turn == self.length - 1
        z = self.z_of(turn)
        for h in range(2):
            extra = []
            if self.over_dp:
                for lane in (0, 1):
                    ref = self.from_xy.at[lane, turn, h]
                    self.got(ref, 5 + lane, turn, h)
                    extra.append(ref)
            if self.over_z:
                slot = self.from_z.at[z, h]

                def got_slot(h=h):
                    self.got(self.from_z.at[z, h], 7, z, h)

                def got_other(h=h):
                    self.got(self.from_z.at[self.length, h], 7, self.length, h)

                if last:
                    guarded(place.has_down, got_slot)
                    guarded(place.has_up, got_other)
                    extra += [slot, self.from_z.at[self.length, h]]
                else:
                    guarded((z > place.z) & place.has_down, got_slot)
                    guarded((z < place.z) & place.has_up, got_slot)
                    extra.append(slot)
            self.settle(
                0, turn, h, extra, self.out(h) if last else None
            )
            if self.over_z and not last:

                def going_up(h=h):
                    return (
                        self.acc.at[0, turn, h],
                        self.from_z.at[z, h],
                        self.send.at[7, turn, h],
                        self.recv.at[7, z, h],
                    )

                def going_down(h=h):
                    arrives = (z - place.z + 1 + self.length) // self.length
                    goal = z + arrives * (self.length - z)
                    return (
                        self.acc.at[0, turn, h],
                        self.from_z.at[goal, h],
                        self.send.at[7, turn, h],
                        self.recv.at[7, goal, h],
                    )

                above, below = z > place.z, z < place.z
                pl.when(above)(lambda: sends.start("up", going_up, lambda: above))
                pl.when(below)(lambda: sends.start("down", going_down, lambda: below))


def run_reduce(place, items):
    for item in items:
        item.begin()
    meet(place, any(i.over_z for i in items), any(i.over_dp for i in items))
    sends = Sends(place)
    for item in items:
        item.load_all()
    for turn in range(2):
        for item in items:
            item.hand_over(sends, turn)
    longest = max(item.length for item in items)
    for step in range(longest + 2):
        for item in items:
            item.corners(sends, step)
        for item in items:
            item.straight(sends, step, False)
        for item in items:
            item.hand_over(sends, step + 2)
        for item in items:
            item.straight(sends, step - 1, True)
        for item in items:
            item.home(sends, step - 2 if item.over_dp else step)
    sends.drain()


def reduce_scatter(specs, length, collective_id, name):
    count = len(specs)
    shapes, scratch, dims = [], [], []
    for array, mode, by_columns, dtype in specs:
        blocks = {"all": 8 * length, "dp": 8, "z": length}[mode]
        if by_columns:
            rows, width = array.shape[0], array.shape[1] // blocks
        else:
            rows, width = array.shape[0] // blocks, array.shape[1]
        dims.append((rows, width))
        shapes.append(jax.ShapeDtypeStruct((rows, width), dtype))
        scratch += ReduceItem.scratch(mode, length, rows, width)

    def kernel(*refs):
        place = Place(length)
        items = []
        for number, (array, mode, by_columns, dtype) in enumerate(specs):
            rows, width = dims[number]
            source, target = refs[number], refs[count + number]
            bufs = refs[2 * count + 8 * number : 2 * count + 8 * number + 8]
            half = rows // 2

            def block(column, z, h, source=source, half=half, rows=rows, width=width, mode=mode, by=by_columns):
                index = {"all": column * length + z, "dp": column, "z": z}[mode]
                if by:
                    return source.at[
                        pl.ds(h * half, half), pl.ds(pl.multiple_of(index * width, width), width)
                    ]
                return source.at[pl.ds(pl.multiple_of(index * rows + h * half, half), half)]

            def out(h, target=target, half=half):
                return target.at[pl.ds(h * half, half)]

            items.append(ReduceItem(mode, place, block, bufs, out))
        run_reduce(place, items)

    return pl.pallas_call(
        kernel,
        name=name,
        out_shape=shapes,
        in_specs=[pl.BlockSpec(memory_space=pl.ANY)] * count,
        out_specs=[pl.BlockSpec(memory_space=pltpu.VMEM)] * count,
        scratch_shapes=scratch,
        compiler_params=pltpu.CompilerParams(
            collective_id=collective_id, has_side_effects=True, vmem_limit_bytes=56 << 20
        ),
    )(*[array for array, _, _, _ in specs])


def dot(left, right, left_dim=1, right_dim=0):
    return lax.dot_general(
        left, right, (((left_dim,), (right_dim,)), ((), ())), preferred_element_type=jnp.float32
    )


def experts(rows_own, cots_own, gates_own, wgate, wup, wdown, length, capacity, collective_id):
    rows, width = rows_own.shape
    hidden = wgate.shape[1]
    devices = 8 * length
    count = 4 * capacity
    tile = 512 if width % 512 == 0 else width
    narrow = 256 if hidden % 256 == 0 else hidden
    f32, bf16 = jnp.float32, jnp.bfloat16

    def kernel(
        rows_ref, cots_ref, gates_ref, wg, wu, wd,
        all_rows, all_cots, part_out, part_grad, token_out, out_wg, out_wu, out_wd,
        table, row_buf, cot_buf, picked, cotan, gated, hid, dgate, dup, scaled, back,
        chosen, slot_gate, slot_sum, acc_g, acc_u, acc_d, stage_out, stage_grad,
        recv_r, send_r, local_r, recv_c, send_c, local_c, recv_t, send_t, local_t,
        load_sem, store_sem, final_sem,
    ):
        place = Place(length)
        expert = place.dp * length + place.z

        def item_of(source, target, sems, half):
            item = GatherItem("all", place, None, None, *sems)
            item.own = lambda h: source.at[pl.ds(h * half, half)]
            item.slot = lambda column, z, h: target.at[
                column * length + z, pl.ds(h * half, half)
            ]
            return item

        big = [
            item_of(rows_ref, all_rows, (recv_r, send_r, local_r), rows // 2),
            item_of(cots_ref, all_cots, (recv_c, send_c, local_c), rows // 2),
        ]
        items = [item_of(gates_ref, table, (recv_t, send_t, local_t), gates_ref.shape[0] // 2)] + big
        meet(place, True, True)
        sends = Sends(place)
        for item in items:
            item.begin(sends)

        def along(distance):
            for item in items:
                item.along_z(sends, distance)

        def across(distance):
            for item in items:
                item.across(sends, distance)

        def corner(distance):
            for item in items:
                item.diagonal(sends, distance)

        def clear(i, carry):
            at = pl.ds(pl.multiple_of(i * 64, 64), 64)
            acc_g[at, :] = jnp.zeros((64, hidden), f32)
            acc_u[at, :] = jnp.zeros((64, hidden), f32)
            return carry

        def clear_down(i, carry):
            at = pl.ds(pl.multiple_of(i * 64, 64), 64)
            acc_d[at, :] = jnp.zeros((64, width), f32)
            return carry

        lax.fori_loop(0, width // 64, clear, 0)
        lax.fori_loop(0, hidden // 64, clear_down, 0)
        along(1)
        across(0)
        for item in items:
            item.settled()

        def block_of(j, side, z):
            return (place.columns[j] + side * place.to_core) * length + z

        def load(j, side, z, slot):
            block = block_of(j, side, z)
            return [
                pltpu.make_async_copy(all_rows.at[block], row_buf.at[slot, j], load_sem.at[slot, 0, j]),
                pltpu.make_async_copy(all_cots.at[block], cot_buf.at[slot, j], load_sem.at[slot, 1, j]),
            ]

        def store(j, side, z, slot):
            block = block_of(j, side, z)
            return [
                pltpu.make_async_copy(stage_out.at[slot, j], part_out.at[block], store_sem.at[slot, 0, j]),
                pltpu.make_async_copy(stage_grad.at[slot, j], part_grad.at[block], store_sem.at[slot, 1, j]),
            ]

        order = lax.broadcasted_iota(jnp.int32, (rows, rows), 0)
        upto = (order <= lax.broadcasted_iota(jnp.int32, (rows, rows), 1)).astype(f32).astype(bf16)
        slots = lax.broadcasted_iota(jnp.int32, (capacity, rows), 0).astype(f32)

        def unit(i, carry):
            turn, side = i // 2, i % 2
            z = place.nearest(turn)

            for step in range(length):

                @pl.when(i == 2 * step)
                def _(step=step):
                    along(step + 2)
                    corner(step)
                    across(step + 1)
                    for item in items:
                        item.from_core(place.nearest(step))
                    for other in range(2):
                        for j in range(4):
                            for copy in load(j, other, place.nearest(step), other):
                                copy.start()

            @pl.when(i >= 2)
            def _():
                for j in range(4):
                    for copy in store(j, side, z, side):
                        copy.wait()

            for j in range(4):
                for copy in load(j, side, z, side):
                    copy.wait()
                block = block_of(j, side, z)
                line = table[block, pl.ds(expert, 1), :]
                named = line >= 0.0
                ranks = dot(named.astype(f32).astype(bf16), upto) - 1.0
                pick = jnp.where(named & (ranks == slots), 1.0, 0.0)
                gate = jnp.sum(pick * line, axis=1, keepdims=True)
                chosen[j] = pick.astype(bf16)
                at = pl.ds(j * capacity, capacity)
                slot_gate[at, :] = jnp.broadcast_to(gate, (capacity, 128))

                def select(n, carry, j=j, at=at):
                    lanes = pl.ds(pl.multiple_of(n * tile, tile), tile)
                    picked[at, lanes] = dot(chosen[j], row_buf[side, j, :, lanes]).astype(bf16)
                    cot = dot(chosen[j], cot_buf[side, j, :, lanes])
                    cotan[at, lanes] = cot.astype(bf16)
                    gated[at, lanes] = (slot_gate[at, 0:1] * cot).astype(bf16)
                    return carry

                lax.fori_loop(0, width // tile, select, 0)

            def middle(n, carry):
                lanes = pl.ds(pl.multiple_of(n * narrow, narrow), narrow)
                gate = dot(picked[...], wg[:, lanes])
                up = dot(picked[...], wu[:, lanes])
                grad = dot(gated[...], wd[lanes, :], 1, 1)
                sigma = jax.nn.sigmoid(gate)
                hid[:, lanes] = (gate * sigma * up).astype(bf16)
                dgate[:, lanes] = (grad * up * sigma * (1.0 + gate * (1.0 - sigma))).astype(bf16)
                dup[:, lanes] = (grad * gate * sigma).astype(bf16)
                return carry

            lax.fori_loop(0, hidden // narrow, middle, 0)
            slot_sum[...] = jnp.zeros(slot_sum.shape, f32)

            def outward(n, carry):
                lanes = pl.ds(pl.multiple_of(n * tile, tile), tile)
                result = dot(hid[...], wd[:, lanes]).astype(bf16).astype(f32)
                products = cotan[:, lanes].astype(f32) * result
                total = products[:, 0:128]
                for k in range(1, tile // 128):
                    total = total + products[:, 128 * k : 128 * (k + 1)]
                slot_sum[...] += total
                scaled[:, lanes] = (slot_gate[:, 0:1] * result).astype(bf16)
                back[:, lanes] = (
                    dot(dgate[...], wg[lanes, :], 1, 1) + dot(dup[...], wu[lanes, :], 1, 1)
                ).astype(bf16)
                for j in range(4):
                    at = pl.ds(j * capacity, capacity)
                    stage_out[side, j, :, lanes] = dot(chosen[j], scaled[at, lanes], 0, 0).astype(bf16)
                    stage_grad[side, j, :, lanes] = dot(chosen[j], back[at, lanes], 0, 0).astype(bf16)
                return carry

            lax.fori_loop(0, width // tile, outward, 0)
            for j in range(4):
                for copy in store(j, side, z, side):
                    copy.start()
                at = pl.ds(j * capacity, capacity)
                total = jnp.sum(slot_sum[at, :], axis=1, keepdims=True)
                token_out[pl.ds(block_of(j, side, z), 1), :] = jnp.sum(
                    chosen[j].astype(f32) * total, axis=0, keepdims=True
                )

            def weights(n, carry):
                lanes = pl.ds(pl.multiple_of(n * tile, tile), tile)
                acc_g[lanes, :] += dot(picked[:, lanes], dgate[...], 0, 0)
                acc_u[lanes, :] += dot(picked[:, lanes], dup[...], 0, 0)
                acc_d[:, lanes] += dot(hid[...], gated[:, lanes], 0, 0)
                return carry

            lax.fori_loop(0, width // tile, weights, 0)
            return carry

        lax.fori_loop(0, 2 * length, unit, 0)
        finals = [
            pltpu.make_async_copy(source, target, final_sem.at[n])
            for n, (source, target) in enumerate(
                ((acc_g, out_wg), (acc_u, out_wu), (acc_d, out_wd))
            )
        ]
        for copy in finals:
            copy.start()
        for side in range(2):
            for j in range(4):
                for copy in store(j, side, 0, side):
                    copy.wait()
        for copy in finals:
            copy.wait()
        sends.drain()

    any_spec = pl.BlockSpec(memory_space=pl.ANY)
    vmem = pl.BlockSpec(memory_space=pltpu.VMEM)
    big = (devices, rows, width)
    shape = jax.ShapeDtypeStruct
    sems = pltpu.SemaphoreType.DMA
    return pl.pallas_call(
        kernel,
        name="experts",
        out_shape=[
            shape(big, bf16), shape(big, bf16), shape(big, bf16), shape(big, bf16),
            shape((devices, rows), f32),
            shape((width, hidden), f32), shape((width, hidden), f32), shape((hidden, width), f32),
        ],
        in_specs=[any_spec] * 3 + [vmem] * 3,
        out_specs=[any_spec] * 4 + [vmem] + [any_spec] * 3,
        scratch_shapes=[
            pltpu.VMEM((devices,) + gates_own.shape, f32),
            pltpu.VMEM((2, 4, rows, width), bf16),
            pltpu.VMEM((2, 4, rows, width), bf16),
            pltpu.VMEM((count, width), bf16),
            pltpu.VMEM((count, width), bf16),
            pltpu.VMEM((count, width), bf16),
            pltpu.VMEM((count, hidden), bf16),
            pltpu.VMEM((count, hidden), bf16),
            pltpu.VMEM((count, hidden), bf16),
            pltpu.VMEM((count, width), bf16),
            pltpu.VMEM((count, width), bf16),
            pltpu.VMEM((4, capacity, rows), bf16),
            pltpu.VMEM((count, 128), f32),
            pltpu.VMEM((count, 128), f32),
            pltpu.VMEM((width, hidden), f32),
            pltpu.VMEM((width, hidden), f32),
            pltpu.VMEM((hidden, width), f32),
            pltpu.VMEM((2, 4, rows, width), bf16),
            pltpu.VMEM((2, 4, rows, width), bf16),
        ]
        + GatherItem.semaphores("all", length) * 3
        + [sems((2, 2, 4)), sems((2, 2, 4)), sems((3,))],
        compiler_params=pltpu.CompilerParams(
            collective_id=collective_id, has_side_effects=True, vmem_limit_bytes=63 << 20
        ),
    )(rows_own, cots_own, gates_own, wgate, wup, wdown)


def mix(form, left, right):
    return jnp.einsum(form, left, right, preferred_element_type=jnp.float32)


def rms_scale(values):
    return lax.rsqrt(jnp.mean(values * values, axis=-1, keepdims=True) + EPSILON)


def rope_tables(seg_ids, head_dim):
    length = seg_ids.shape[0]
    row_index = jnp.arange(length, dtype=jnp.int32)
    starts = jnp.sum((seg_ids[None, :] < seg_ids[:, None]).astype(jnp.int32), axis=1)
    places = (row_index - starts).astype(jnp.float32)
    half_dim = head_dim // 2
    frequency = THETA_BASE ** (-(jnp.arange(half_dim, dtype=jnp.float32) * (2.0 / head_dim)))
    angles = places[:, None] * frequency[None, :]
    return (jnp.cos(angles), jnp.sin(angles))


def rotate(values, cosine, sine_table):
    half_dim = values.shape[-1] // 2
    front_part = values[..., :half_dim]
    back_part = values[..., half_dim:]
    cos_rows = cosine[:, None, :]
    sin_rows = sine_table[:, None, :]
    return jnp.concatenate(
        [
            front_part * cos_rows - back_part * sin_rows,
            back_part * cos_rows + front_part * sin_rows,
        ],
        axis=-1,
    )


def unrotate(values, cosine, sine_table):
    half_dim = values.shape[-1] // 2
    front_part = values[..., :half_dim]
    back_part = values[..., half_dim:]
    cos_rows = cosine[:, None, :]
    sin_rows = sine_table[:, None, :]
    return jnp.concatenate(
        [
            front_part * cos_rows + back_part * sin_rows,
            back_part * cos_rows - front_part * sin_rows,
        ],
        axis=-1,
    )


def head_norm_back(grad_out, normed, factor, gain):
    grad_normed = grad_out * gain
    grad_gain = jnp.sum(grad_out * normed, axis=(0, 1))
    grad_values = factor * (
        grad_normed - normed * jnp.mean(grad_normed * normed, axis=-1, keepdims=True)
    )
    return (grad_values, grad_gain)


def row_norm_back(grad_out, normed, factor, gain):
    grad_normed = grad_out * gain
    grad_gain = jnp.sum(grad_out * normed, axis=0)
    grad_values = factor * (
        grad_normed - normed * jnp.mean(grad_normed * normed, axis=-1, keepdims=True)
    )
    return (grad_values, grad_gain)


def softmax_rows(logits):
    top_value = jnp.max(logits, axis=-1, keepdims=True)
    expo = jnp.exp(logits - top_value)
    return expo / jnp.sum(expo, axis=-1, keepdims=True)


def attn_forward(rows, seg_ids, wq_full, wk_full, wv_full, query_gain, key_gain):
    length = rows.shape[0]
    head_dim = query_gain.shape[0]
    num_heads = wq_full.shape[1] // head_dim
    kv_heads = wk_full.shape[1] // head_dim
    per_group = num_heads // kv_heads
    inv_root = 1.0 / math.sqrt(head_dim)
    block_rows = math.gcd(length, 512)
    cosine, sine_table = rope_tables(seg_ids, head_dim)
    query = jnp.dot(rows, wq_full, preferred_element_type=jnp.float32).reshape(
        length, num_heads, head_dim
    )
    key_proj = jnp.dot(rows, wk_full, preferred_element_type=jnp.float32).reshape(
        length, kv_heads, head_dim
    )
    value_rows = (
        jnp.dot(rows, wv_full, preferred_element_type=jnp.float32)
        .astype(jnp.bfloat16)
        .reshape(length, kv_heads, head_dim)
    )
    query_factor = rms_scale(query)
    query_hat = query * query_factor
    key_factor = rms_scale(key_proj)
    key_hat = key_proj * key_factor
    query_rot = (
        rotate(query_hat * query_gain, cosine, sine_table)
        .astype(jnp.bfloat16)
        .reshape(length, kv_heads, per_group, head_dim)
    )
    key_rot = rotate(key_hat * key_gain, cosine, sine_table).astype(jnp.bfloat16)
    row_index = jnp.arange(length, dtype=jnp.int32)
    scores = mix("qgrd,kgd->grqk", query_rot, key_rot) * inv_root
    visible = (seg_ids[0:block_rows, None] == seg_ids[None, :]) & (
        row_index[None, :] <= row_index[0:block_rows, None]
    )
    scores = jnp.where(visible, scores, NEG_BIG)
    top_value = jnp.max(scores, axis=-1, keepdims=True)
    expo = jnp.exp(scores - top_value)
    totals = jnp.sum(expo, axis=-1, keepdims=True)
    prob_rows = (expo / totals).astype(jnp.bfloat16)
    outputs = mix("grqk,kgd->qgrd", prob_rows, value_rows).astype(jnp.bfloat16)
    lse_parts = top_value[..., 0] + jnp.log(totals[..., 0])
    attn_heads = outputs.reshape(length, num_heads * head_dim)
    return (
        attn_heads,
        lse_parts,
        query_rot,
        key_rot,
        value_rows,
        cosine,
        sine_table,
        query_hat,
        query_factor,
        key_hat,
        key_factor,
    )


def attn_backward(
    grad_attn, rows, seg_ids, wq_full, wk_full, wv_full, wo_full, query_gain, key_gain, saved
):
    (
        attn_heads,
        lse_all,
        query_rot,
        key_rot,
        value_rows,
        cosine,
        sine_table,
        query_hat,
        query_factor,
        key_hat,
        key_factor,
    ) = saved
    length = rows.shape[0]
    head_dim = query_gain.shape[0]
    num_heads = query_hat.shape[1]
    inv_root = 1.0 / math.sqrt(head_dim)
    block_rows = math.gcd(length, 512)
    grad_wo = jnp.dot(attn_heads.T, grad_attn, preferred_element_type=jnp.float32)
    grad_heads = (
        jnp.dot(grad_attn, wo_full.T, preferred_element_type=jnp.float32)
        .astype(jnp.bfloat16)
        .reshape(query_rot.shape)
    )
    heads_view = attn_heads.reshape(query_rot.shape)
    row_delta = jnp.transpose(
        jnp.sum(grad_heads.astype(jnp.float32) * heads_view.astype(jnp.float32), axis=-1), (1, 2, 0)
    )
    row_index = jnp.arange(length, dtype=jnp.int32)
    scores = mix("qgrd,kgd->grqk", query_rot, key_rot) * inv_root
    visible = (seg_ids[0:block_rows, None] == seg_ids[None, :]) & (
        row_index[None, :] <= row_index[0:block_rows, None]
    )
    scores = jnp.where(visible, scores, NEG_BIG)
    prob_f = jnp.where(visible, jnp.exp(scores - lse_all[:, :, 0:block_rows, None]), 0.0)
    prob_rows = prob_f.astype(jnp.bfloat16)
    grad_value = mix("grqk,qgrd->kgd", prob_rows, grad_heads)
    grad_probs = mix("qgrd,kgd->grqk", grad_heads, value_rows)
    grad_scores = (prob_f * (grad_probs - row_delta[:, :, 0:block_rows, None])).astype(jnp.bfloat16)
    pieces = mix("grqk,kgd->qgrd", grad_scores, key_rot) * inv_root
    grad_key_rot = mix("grqk,qgrd->kgd", grad_scores, query_rot) * inv_root
    grad_query_rot = pieces.reshape(length, num_heads, head_dim)
    grad_query, grad_qgain = head_norm_back(
        unrotate(grad_query_rot, cosine, sine_table), query_hat, query_factor, query_gain
    )
    grad_key, grad_kgain = head_norm_back(
        unrotate(grad_key_rot, cosine, sine_table), key_hat, key_factor, key_gain
    )
    query_b = grad_query.astype(jnp.bfloat16).reshape(length, -1)
    key_b = grad_key.astype(jnp.bfloat16).reshape(length, -1)
    value_b = grad_value.astype(jnp.bfloat16).reshape(length, -1)
    grad_rows = (
        jnp.dot(query_b, wq_full.T, preferred_element_type=jnp.float32)
        + jnp.dot(key_b, wk_full.T, preferred_element_type=jnp.float32)
        + jnp.dot(value_b, wv_full.T, preferred_element_type=jnp.float32)
    )
    grad_wq = jnp.dot(rows.T, query_b, preferred_element_type=jnp.float32)
    grad_wk = jnp.dot(rows.T, key_b, preferred_element_type=jnp.float32)
    grad_wv = jnp.dot(rows.T, value_b, preferred_element_type=jnp.float32)
    return (grad_rows, grad_wq, grad_wk, grad_wv, grad_wo, grad_qgain, grad_kgain)


def expert_forward(expert_rows, wgate, wup, wdown):
    gate_pre = jnp.dot(expert_rows, wgate, preferred_element_type=jnp.float32)
    up_pre = jnp.dot(expert_rows, wup, preferred_element_type=jnp.float32)
    hidden_units = (jax.nn.silu(gate_pre) * up_pre).astype(jnp.bfloat16)
    result = jnp.dot(hidden_units, wdown, preferred_element_type=jnp.float32).astype(jnp.bfloat16)
    return (result, gate_pre, up_pre, hidden_units)


def expert_backward(expert_rows, grad_result, wgate, wup, wdown, gate_pre, up_pre, hidden_units):
    grad_hidden = jnp.dot(grad_result, wdown.T, preferred_element_type=jnp.float32)
    sigma = jax.nn.sigmoid(gate_pre)
    grad_gate_pre = (grad_hidden * up_pre * sigma * (1.0 + gate_pre * (1.0 - sigma))).astype(
        jnp.bfloat16
    )
    grad_up_pre = (grad_hidden * gate_pre * sigma).astype(jnp.bfloat16)
    grad_rows = (
        jnp.dot(grad_gate_pre, wgate.T, preferred_element_type=jnp.float32)
        + jnp.dot(grad_up_pre, wup.T, preferred_element_type=jnp.float32)
    ).astype(jnp.bfloat16)
    grad_wd = jnp.dot(hidden_units.T, grad_result, preferred_element_type=jnp.float32)
    grad_wg = jnp.dot(expert_rows.T, grad_gate_pre, preferred_element_type=jnp.float32)
    grad_wu = jnp.dot(expert_rows.T, grad_up_pre, preferred_element_type=jnp.float32)
    return (grad_rows, grad_wg, grad_wu, grad_wd)


def to_experts(buffer):
    return lax.all_to_all(buffer, ("dp", "tensor"), split_axis=0, concat_axis=0, tiled=True)


def to_sources(buffer):
    return lax.all_to_all(buffer, ("dp", "tensor"), split_axis=0, concat_axis=0, tiled=True)


def shards(
    hidden_in,
    segments,
    routes,
    query_weight,
    key_weight,
    value_weight,
    output_weight,
    gain_attn,
    gain_moe,
    query_gain,
    key_gain,
    router,
    gate_weight,
    up_weight,
    down_weight,
    cotangent,
):
    seg_ids = segments[0]
    rows_dev = hidden_in.shape[0]
    width = hidden_in.shape[1]
    top_count = routes.shape[1]
    experts = router.shape[1]
    capacity = 2 * rows_dev * top_count // experts
    full_query, full_key, full_value, full_output = (
        lax.all_gather(query_weight, "dp", axis=0, tiled=True),
        lax.all_gather(key_weight, "dp", axis=0, tiled=True),
        lax.all_gather(value_weight, "dp", axis=0, tiled=True),
        lax.all_gather(output_weight, "dp", axis=1, tiled=True),
    )
    inputs32 = hidden_in.astype(jnp.float32)
    factor_one = rms_scale(inputs32)
    normed_one = inputs32 * factor_one
    rows_one = (normed_one * gain_attn).astype(jnp.bfloat16)
    group_rows = lax.all_gather(rows_one, "tensor", axis=0, tiled=True)
    saved = attn_forward(
        group_rows, seg_ids, full_query, full_key, full_value, query_gain, key_gain
    )
    partial_add = jnp.dot(saved[0], full_output, preferred_element_type=jnp.float32)
    attn_add = lax.psum_scatter(partial_add, "tensor", scatter_dimension=0, tiled=True)
    residual = inputs32 + attn_add
    factor_two = rms_scale(residual)
    normed_two = residual * factor_two
    rows_two = (normed_two * gain_moe).astype(jnp.bfloat16)
    router_probs = softmax_rows(jnp.dot(rows_two, router, preferred_element_type=jnp.float32))
    route_hot = (routes[:, :, None] == jnp.arange(experts, dtype=jnp.int32)[None, None, :]).astype(
        jnp.float32
    )
    picked = jnp.sum(route_hot * router_probs[:, None, :], axis=-1)
    total = jnp.sum(picked, axis=1, keepdims=True)
    gates = picked / total
    flat_routes = routes.reshape(-1)
    onehot = (flat_routes[:, None] == jnp.arange(experts, dtype=jnp.int32)[None, :]).astype(
        jnp.int32
    )
    ranks = jnp.sum(onehot * jnp.cumsum(onehot, axis=0), axis=1) - 1
    slots = flat_routes * capacity + ranks
    send_rows = (
        jnp.zeros((experts * capacity, width), jnp.bfloat16)
        .at[slots]
        .set(jnp.repeat(rows_two, top_count, axis=0))
    )
    received = to_experts(send_rows.reshape(experts, capacity, width)).reshape(-1, width)
    result, gate_pre, up_pre, hidden_units = expert_forward(
        received, gate_weight[0], up_weight[0], down_weight[0]
    )
    returned = to_sources(result.reshape(-1, capacity, width)).reshape(experts * capacity, width)
    pair_out = returned[slots].astype(jnp.float32).reshape(rows_dev, top_count, width)
    moe_sum = jnp.sum(gates[:, :, None] * pair_out, axis=1)
    output = (residual + moe_sum).astype(jnp.bfloat16)
    cot32 = cotangent.astype(jnp.float32)
    grad_gates = jnp.sum(cot32[:, None, :] * pair_out, axis=-1)
    grad_result = (gates[:, :, None] * cot32[:, None, :]).astype(jnp.bfloat16).reshape(-1, width)
    send_grads = jnp.zeros((experts * capacity, width), jnp.bfloat16).at[slots].set(grad_result)
    received_grads = to_experts(send_grads.reshape(experts, capacity, width)).reshape(-1, width)
    grad_expert_rows, grad_wg, grad_wu, grad_wd = expert_backward(
        received,
        received_grads,
        gate_weight[0],
        up_weight[0],
        down_weight[0],
        gate_pre,
        up_pre,
        hidden_units,
    )
    returned_grads = to_sources(grad_expert_rows.reshape(-1, capacity, width)).reshape(
        experts * capacity, width
    )
    grad_pairs = returned_grads[slots].astype(jnp.float32).reshape(rows_dev, top_count, width)
    grad_picked = (grad_gates - jnp.sum(gates * grad_gates, axis=1, keepdims=True)) / total
    grad_probs = jnp.sum(route_hot * grad_picked[:, :, None], axis=1)
    grad_logits = (
        router_probs * (grad_probs - jnp.sum(grad_probs * router_probs, axis=-1, keepdims=True))
    ).astype(jnp.bfloat16)
    grad_router = jnp.dot(rows_two.T, grad_logits, preferred_element_type=jnp.float32)
    grad_rows_two = jnp.sum(grad_pairs, axis=1) + jnp.dot(
        grad_logits, router.T, preferred_element_type=jnp.float32
    )
    grad_res_norm, grad_gain_moe = row_norm_back(grad_rows_two, normed_two, factor_two, gain_moe)
    grad_residual = cot32 + grad_res_norm
    grad_attn = grad_residual.astype(jnp.bfloat16)
    group_grads = lax.all_gather(grad_attn, "tensor", axis=0, tiled=True)
    back_query, back_key, back_value, back_output = (
        lax.all_gather(query_weight, "dp", axis=0, tiled=True),
        lax.all_gather(key_weight, "dp", axis=0, tiled=True),
        lax.all_gather(value_weight, "dp", axis=0, tiled=True),
        lax.all_gather(output_weight, "dp", axis=1, tiled=True),
    )
    grad_group_rows, grad_wq, grad_wk, grad_wv, grad_wo, grad_qgain, grad_kgain = attn_backward(
        group_grads,
        group_rows,
        seg_ids,
        back_query,
        back_key,
        back_value,
        back_output,
        query_gain,
        key_gain,
        saved,
    )
    grad_rows_one = lax.psum_scatter(
        grad_group_rows.astype(jnp.bfloat16), "tensor", scatter_dimension=0, tiled=True
    ).astype(jnp.float32)
    grad_in_norm, grad_gain_attn = row_norm_back(grad_rows_one, normed_one, factor_one, gain_attn)
    grad_input = grad_residual + grad_in_norm
    grad_wq, grad_wk, grad_wv, grad_wo = (
        lax.psum_scatter(
            grad_wq.astype(jnp.bfloat16), "dp", scatter_dimension=0, tiled=True
        ).astype(jnp.float32),
        lax.psum_scatter(
            grad_wk.astype(jnp.bfloat16), "dp", scatter_dimension=0, tiled=True
        ).astype(jnp.float32),
        lax.psum_scatter(
            grad_wv.astype(jnp.bfloat16), "dp", scatter_dimension=0, tiled=True
        ).astype(jnp.float32),
        lax.psum_scatter(
            grad_wo.astype(jnp.bfloat16), "dp", scatter_dimension=1, tiled=True
        ).astype(jnp.float32),
    )
    grad_gain_attn, grad_gain_moe, grad_qgain, grad_kgain, grad_router = lax.psum(
        (grad_gain_attn, grad_gain_moe, grad_qgain, grad_kgain, grad_router), ("dp", "tensor")
    )
    return (
        output,
        grad_input,
        grad_wq,
        grad_wk,
        grad_wv,
        grad_wo,
        grad_gain_attn,
        grad_gain_moe,
        grad_qgain,
        grad_kgain,
        grad_router,
        grad_wg[None],
        grad_wu[None],
        grad_wd[None],
    )


def attn_backward_joint(
    grad_attn, rows, seg_ids, joint_full, wo_full, query_gain, key_gain, saved
):
    (
        attn_heads,
        lse_all,
        query_rot,
        key_rot,
        value_rows,
        cosine,
        sine_table,
        query_hat,
        query_factor,
        key_hat,
        key_factor,
    ) = saved
    length = rows.shape[0]
    head_dim = query_gain.shape[0]
    num_heads = query_hat.shape[1]
    inv_root = 1.0 / math.sqrt(head_dim)
    block_rows = math.gcd(length, 512)
    grad_wo = jnp.dot(attn_heads.T, grad_attn, preferred_element_type=jnp.float32)
    grad_heads = (
        jnp.dot(grad_attn, wo_full.T, preferred_element_type=jnp.float32)
        .astype(jnp.bfloat16)
        .reshape(query_rot.shape)
    )
    heads_view = attn_heads.reshape(query_rot.shape)
    row_delta = jnp.transpose(
        jnp.sum(grad_heads.astype(jnp.float32) * heads_view.astype(jnp.float32), axis=-1), (1, 2, 0)
    )
    row_index = jnp.arange(length, dtype=jnp.int32)
    scores = mix("qgrd,kgd->grqk", query_rot, key_rot) * inv_root
    visible = (seg_ids[0:block_rows, None] == seg_ids[None, :]) & (
        row_index[None, :] <= row_index[0:block_rows, None]
    )
    scores = jnp.where(visible, scores, NEG_BIG)
    prob_f = jnp.where(visible, jnp.exp(scores - lse_all[:, :, 0:block_rows, None]), 0.0)
    prob_rows = prob_f.astype(jnp.bfloat16)
    grad_value = mix("grqk,qgrd->kgd", prob_rows, grad_heads)
    grad_probs = mix("qgrd,kgd->grqk", grad_heads, value_rows)
    grad_scores = (prob_f * (grad_probs - row_delta[:, :, 0:block_rows, None])).astype(jnp.bfloat16)
    pieces = mix("grqk,kgd->qgrd", grad_scores, key_rot) * inv_root
    grad_key_rot = mix("grqk,qgrd->kgd", grad_scores, query_rot) * inv_root
    grad_query_rot = pieces.reshape(length, num_heads, head_dim)
    grad_query, grad_qgain = head_norm_back(
        unrotate(grad_query_rot, cosine, sine_table), query_hat, query_factor, query_gain
    )
    grad_key, grad_kgain = head_norm_back(
        unrotate(grad_key_rot, cosine, sine_table), key_hat, key_factor, key_gain
    )
    query_b = grad_query.astype(jnp.bfloat16).reshape(length, -1)
    key_b = grad_key.astype(jnp.bfloat16).reshape(length, -1)
    value_b = grad_value.astype(jnp.bfloat16).reshape(length, -1)
    joint_b = jnp.concatenate([query_b, key_b, value_b], axis=1)
    grad_rows = jnp.dot(joint_b, joint_full.T, preferred_element_type=jnp.float32)
    grad_joint = jnp.dot(rows.T, joint_b, preferred_element_type=jnp.float32)
    return (grad_rows, grad_joint, grad_wo, grad_qgain, grad_kgain)


AXES = ("dp", "tensor")


def gathered(
    hidden_in,
    segments,
    routes,
    query_weight,
    key_weight,
    value_weight,
    output_weight,
    gain_attn,
    gain_moe,
    query_gain,
    key_gain,
    router,
    gate_weight,
    up_weight,
    down_weight,
    cotangent,
):
    seg_ids = segments[0]
    rows_dev, width = hidden_in.shape
    top_count = routes.shape[1]
    expert_count = router.shape[1]
    capacity = 2 * rows_dev * top_count // expert_count
    length = lax.axis_size("tensor")
    query_cols, key_cols = query_weight.shape[1], key_weight.shape[1]

    inputs32 = hidden_in.astype(jnp.float32)
    factor_one = rms_scale(inputs32)
    normed_one = inputs32 * factor_one
    rows_one = (normed_one * gain_attn).astype(jnp.bfloat16)
    joint_weight = jnp.concatenate([query_weight, key_weight, value_weight], axis=1)
    group_rows, full_joint, full_output = gather(
        [
            (rows_one, "z", False),
            (joint_weight, "dp", False),
            (output_weight, "dp", True),
        ],
        length,
        0,
        "gather_attention",
    )
    group_rows = group_rows.reshape(-1, width)
    full_joint = full_joint.reshape(width, -1)
    full_query = full_joint[:, :query_cols]
    full_key = full_joint[:, query_cols : query_cols + key_cols]
    full_value = full_joint[:, query_cols + key_cols :]
    saved = attn_forward(
        group_rows, seg_ids, full_query, full_key, full_value, query_gain, key_gain
    )
    partial_add = jnp.dot(saved[0], full_output, preferred_element_type=jnp.float32)
    (attn_add,) = reduce_scatter(
        [(partial_add.astype(jnp.bfloat16), "z", False, jnp.float32)], length, 1, "reduce_attention"
    )
    residual = inputs32 + attn_add
    factor_two = rms_scale(residual)
    normed_two = residual * factor_two
    rows_two = (normed_two * gain_moe).astype(jnp.bfloat16)
    router_probs = softmax_rows(jnp.dot(rows_two, router, preferred_element_type=jnp.float32))
    route_hot = (routes[:, :, None] == jnp.arange(expert_count, dtype=jnp.int32)[None, None, :]).astype(
        jnp.float32
    )
    picked = jnp.sum(route_hot * router_probs[:, None, :], axis=-1)
    total = jnp.sum(picked, axis=1, keepdims=True)
    gates = picked / total
    named = jnp.sum(route_hot, axis=1)
    gate_table = jnp.where(named > 0.5, jnp.sum(route_hot * gates[:, :, None], axis=1), -1.0)
    all_rows, _, partial_out, partial_rows, token_grads, grad_wg, grad_wu, grad_wd = experts(
        rows_two,
        cotangent,
        gate_table.T,
        gate_weight[0],
        up_weight[0],
        down_weight[0],
        length,
        capacity,
        2,
    )
    back_grads = lax.all_to_all(token_grads, AXES, split_axis=0, concat_axis=0, tiled=True)
    (grad_sum,) = reduce_scatter(
        [(partial_rows.reshape(-1, width), "all", False, jnp.float32)], length, 3, "reduce_grads"
    )
    (moe_sum,) = reduce_scatter(
        [(partial_out.reshape(-1, width), "all", False, jnp.float32)], length, 4, "reduce_outputs"
    )
    output = (residual + moe_sum).astype(jnp.bfloat16)
    cot32 = cotangent.astype(jnp.float32)
    grad_gates = jnp.sum(route_hot * back_grads.T[:, None, :], axis=-1)
    grad_picked = (grad_gates - jnp.sum(gates * grad_gates, axis=1, keepdims=True)) / total
    grad_probs = jnp.sum(route_hot * grad_picked[:, :, None], axis=1)
    grad_logits = (
        router_probs * (grad_probs - jnp.sum(grad_probs * router_probs, axis=-1, keepdims=True))
    ).astype(jnp.bfloat16)
    grad_rows_two = grad_sum + jnp.dot(grad_logits, router.T, preferred_element_type=jnp.float32)
    grad_res_norm, grad_gain_moe = row_norm_back(grad_rows_two, normed_two, factor_two, gain_moe)
    grad_residual = cot32 + grad_res_norm
    grad_attn = grad_residual.astype(jnp.bfloat16)
    group_grads, all_logits = gather(
        [(grad_attn, "z", False), (grad_logits.T, "all", False)], length, 5, "gather_grads"
    )
    grad_router = mix("btd,bet->de", all_rows, all_logits)
    grad_group_rows, grad_joint, grad_wo, grad_qgain, grad_kgain = attn_backward_joint(
        group_grads.reshape(-1, width),
        group_rows,
        seg_ids,
        full_joint,
        full_output,
        query_gain,
        key_gain,
        saved,
    )
    grad_rows_one, grad_joint, grad_wo = reduce_scatter(
        [
            (grad_group_rows.astype(jnp.bfloat16), "z", False, jnp.float32),
            (grad_joint.astype(jnp.bfloat16), "dp", False, jnp.float32),
            (grad_wo.astype(jnp.bfloat16), "dp", True, jnp.float32),
        ],
        length,
        6,
        "reduce_weights",
    )
    grad_in_norm, grad_gain_attn = row_norm_back(grad_rows_one, normed_one, factor_one, gain_attn)
    grad_input = grad_residual + grad_in_norm
    small = jnp.concatenate([grad_gain_attn, grad_gain_moe, grad_qgain, grad_kgain]).reshape(-1, 128)
    small = jnp.pad(small, ((0, -small.shape[0] % 16), (0, 0)))
    (all_small,) = gather([(small, "all", False)], length, 7, "gather_small")
    sums = jnp.sum(all_small, axis=0).reshape(-1)
    head_dim = query_gain.shape[0]
    return (
        output,
        grad_input,
        grad_joint[:, :query_cols],
        grad_joint[:, query_cols : query_cols + key_cols],
        grad_joint[:, query_cols + key_cols :],
        grad_wo,
        sums[:width],
        sums[width : 2 * width],
        sums[2 * width : 2 * width + head_dim],
        sums[2 * width + head_dim : 2 * width + 2 * head_dim],
        grad_router,
        grad_wg[None],
        grad_wu[None],
        grad_wd[None],
    )


def solution(mesh):
    placed = (
        P(("dp", "tensor"), None),
        P("dp", None),
        P(("dp", "tensor"), None),
        P("dp", "tensor"),
        P("dp", "tensor"),
        P("dp", "tensor"),
        P("tensor", "dp"),
        P(),
        P(),
        P(),
        P(),
        P(),
        P(("dp", "tensor"), None, None),
        P(("dp", "tensor"), None, None),
        P(("dp", "tensor"), None, None),
        P(("dp", "tensor"), None),
    )
    program = gathered if mesh.shape["dp"] == 8 and mesh.shape["tensor"] <= 4 else shards
    return jax.shard_map(
        program,
        mesh=mesh,
        in_specs=placed,
        out_specs=(
            P(("dp", "tensor"), None),
            P(("dp", "tensor"), None),
            P("dp", "tensor"),
            P("dp", "tensor"),
            P("dp", "tensor"),
            P("tensor", "dp"),
            P(),
            P(),
            P(),
            P(),
            P(),
            P(("dp", "tensor"), None, None),
            P(("dp", "tensor"), None, None),
            P(("dp", "tensor"), None, None),
        ),
        check_vma=False,
    )
```

```python
import math

import jax
import jax.numpy as jnp
from jax import lax
from jax.experimental import pallas as pl
from jax.experimental.pallas import tpu as pltpu
from jax.sharding import PartitionSpec as P

EPSILON = 1e-06
THETA_BASE = 1000000.0
NEG_BIG = -1e30


MESH = pl.DeviceIdType.MESH


class Place:
    def __init__(self, length):
        self.length = length
        self.dp = lax.axis_index("dp")
        self.z = lax.axis_index("tensor")
        core, along_x, along_y = self.dp % 2, (self.dp // 2) % 2, self.dp // 4
        self.to_core = 1 - 2 * core
        self.core = self.dp + self.to_core
        self.x = self.dp + 2 - 4 * along_x
        self.y = self.dp + 4 - 8 * along_y
        self.columns = (self.dp, self.x, self.y, self.x + self.y - self.dp)

    def device(self, kind):
        if kind == "x":
            return (self.x, self.z)
        if kind == "y":
            return (self.y, self.z)
        if kind == "core":
            return (self.core, self.z)
        if kind == "up":
            return (self.dp, self.z + 1)
        return (self.dp, self.z - 1)

    @property
    def has_up(self):
        return self.z < self.length - 1

    @property
    def has_down(self):
        return self.z > 0

    def condition(self, kind):
        if kind == "up":
            return self.has_up
        return self.has_down if kind == "down" else None

    def nearest(self, turn):
        length = self.length

        def equal(left, right):
            far = 2 * length
            return (left - right + far) // far - (left - right - 1 + far) // far

        found = 0
        for mine in range(length):
            order = sorted(range(length), key=lambda other: (abs(other - mine), other))
            for step, other in enumerate(order):
                if other:
                    found = found + equal(self.z, mine) * equal(turn, step) * other
        return found

    def target(self, turn):
        length, z = self.length, self.z

        def at_least(left, right):
            return (left - right + 2 * length) // (2 * length)

        high = at_least(z, length // 2)
        mirrored = z + high * (length - 1 - 2 * z)
        above = length - 1 - mirrored
        first = at_least(above - 1, turn)
        if turn == length - 1:
            return z
        found = first * (length - 1 - turn) + (1 - first) * (turn - above)
        return found + high * (length - 1 - 2 * found)


def guarded(condition, action):
    if condition is None:
        action()
    else:
        pl.when(condition)(action)


def meet(place, over_z, over_dp):
    barrier = pltpu.get_barrier_semaphore()
    kinds = (("x", "y", "core") if over_dp else ()) + (("up", "down") if over_z else ())
    for kind in kinds:

        def greet(kind=kind):
            pl.semaphore_signal(
                barrier, 1, device_id=place.device(kind), device_id_type=MESH
            )

        guarded(place.condition(kind), greet)
    count = 3 if over_dp else 0
    if over_z:
        length = place.length
        count = count + (place.z + length - 1) // length + (2 * length - 2 - place.z) // length
    pl.semaphore_wait(barrier, count)


def other_device(place, distance):
    there = lax.rem(place.dp * place.length + place.z + distance, 8 * place.length)
    return (there // place.length, lax.rem(there, place.length)), there


def meet_all(place):
    barrier = pltpu.get_barrier_semaphore()
    others = 8 * place.length - 1

    def greet(n, carry):
        device, _ = other_device(place, n + 1)
        pl.semaphore_signal(barrier, 1, device_id=device, device_id_type=MESH)
        return carry

    lax.fori_loop(0, others, greet, 0)
    pl.semaphore_wait(barrier, others)


class Sends:
    def __init__(self, place):
        self.place = place
        self.started = []

    def start(self, kind, views, condition=lambda: None):
        def build():
            source, target, send_sem, recv_sem = views()
            return pltpu.make_async_remote_copy(
                src_ref=source,
                dst_ref=target,
                send_sem=send_sem,
                recv_sem=recv_sem,
                device_id=self.place.device(kind),
                device_id_type=MESH,
            )

        guarded(self.place.condition(kind), lambda: build().start())
        self.started.append((condition, kind, build))

    def drain(self):
        for condition, kind, build in self.started:

            def finish(kind=kind, build=build):
                guarded(self.place.condition(kind), lambda: build().wait_send())

            guarded(condition(), finish)


class GatherItem:
    def __init__(self, mode, place, own, slot, recv, send, local):
        self.mode, self.place = mode, place
        self.own, self.slot = own, slot
        self.recv, self.send, self.local = recv, send, local
        self.over_z = mode != "dp"
        self.over_dp = mode != "z"
        self.length = place.length if self.over_z else 1
        self.z = place.z if self.over_z else 0

    def index(self, column, z):
        if self.mode == "all":
            return column * self.length + z
        return column if self.mode == "dp" else z

    @staticmethod
    def semaphores(mode, length):
        blocks = {"all": 8 * length, "dp": 8, "z": length}[mode]
        turns = 2 * length - 1 if mode != "dp" else 1
        return [
            pltpu.SemaphoreType.DMA((blocks, 2)),
            pltpu.SemaphoreType.DMA((10, turns, 2)),
            pltpu.SemaphoreType.DMA((2,)),
        ]

    def turns(self, distance):
        if distance == 0:
            return [(0, 0, lambda: None, None)]
        place, length = self.place, self.length
        return [
            (2 * distance - 1, -distance, lambda: place.z >= distance, "up"),
            (2 * distance, distance, lambda: place.z < length - distance, "down"),
        ]

    def pass_on(self, sends, lane, kind, column, offset, turn, h, source=None, condition=lambda: None):
        def views():
            z = self.z + offset
            view = self.slot(column, z, h)
            return (
                view if source is None else source(h),
                view,
                self.send.at[lane, turn, h],
                self.recv.at[self.index(column, z), h],
            )

        sends.start(kind, views, condition)

    def arrived(self, column, z, h):
        view = self.slot(column, z, h)
        pltpu.make_async_copy(view, view, self.recv.at[self.index(column, z), h]).wait()

    def begin(self, sends):
        place = self.place
        for h in range(2):
            own = self.own
            if self.over_z:
                self.pass_on(sends, 0, "up", place.dp, 0, 0, h, own)
                self.pass_on(sends, 1, "down", place.dp, 0, 0, h, own)
            if self.over_dp:
                self.pass_on(sends, 2, "x", place.dp, 0, 0, h, own)
                self.pass_on(sends, 3, "y", place.dp, 0, 0, h, own)
                self.pass_on(sends, 4, "core", place.dp, 0, 0, h, own)
        for h in range(2):
            pltpu.make_async_copy(
                self.own(h), self.slot(place.dp, self.z, h), self.local.at[h]
            ).start()

    def along_z(self, sends, distance):
        if not self.over_z or distance >= self.length:
            return
        place = self.place
        for turn, offset, condition, onward in self.turns(distance):

            def step(turn=turn, offset=offset, condition=condition, onward=onward):
                for h in range(2):
                    self.arrived(place.dp, self.z + offset, h)
                    if distance < self.length - 1:
                        self.pass_on(
                            sends, 0 if onward == "up" else 1, onward, place.dp, offset, turn, h,
                            condition=condition,
                        )
                    if self.over_dp:
                        for lane, kind in ((2, "x"), (3, "y"), (4, "core")):
                            self.pass_on(
                                sends, lane, kind, place.dp, offset, turn, h, condition=condition
                            )

            guarded(condition(), step)

    def across(self, sends, distance):
        if not self.over_dp or not 0 <= distance < self.length:
            return
        _, x, y, _ = self.place.columns
        for turn, offset, condition, _ in self.turns(distance):

            def step(turn=turn, offset=offset, condition=condition):
                for h in range(2):
                    self.arrived(x, self.z + offset, h)
                    if h == 0:
                        self.pass_on(sends, 5, "y", x, offset, turn, h, condition=condition)
                    self.pass_on(sends, 7, "core", x, offset, turn, h, condition=condition)
                    self.arrived(y, self.z + offset, h)
                    if h == 1:
                        self.pass_on(sends, 6, "x", y, offset, turn, h, condition=condition)
                    self.pass_on(sends, 8, "core", y, offset, turn, h, condition=condition)

            guarded(condition(), step)

    def diagonal(self, sends, distance):
        if not self.over_dp or not 0 <= distance < self.length:
            return
        corner = self.place.columns[3]
        for turn, offset, condition, _ in self.turns(distance):

            def step(turn=turn, offset=offset, condition=condition):
                for h in range(2):
                    self.arrived(corner, self.z + offset, h)
                    self.pass_on(sends, 9, "core", corner, offset, turn, h, condition=condition)

            guarded(condition(), step)

    def settled(self):
        for h in range(2):
            pltpu.make_async_copy(
                self.own(h), self.slot(self.place.dp, self.z, h), self.local.at[h]
            ).wait()

    def from_core(self, z):
        for column in self.place.columns:
            for h in range(2):
                self.arrived(column + self.place.to_core, z, h)

    def finish(self):
        self.settled()
        if self.over_dp:
            for z in range(self.length):
                self.from_core(z)


def run_gather(place, items):
    meet(place, any(i.over_z for i in items), any(i.over_dp for i in items))
    sends = Sends(place)
    for item in items:
        item.begin(sends)
    for step in range(place.length + 2):
        for item in items:
            item.along_z(sends, step + 1)
        for item in items:
            item.across(sends, step)
        for item in items:
            item.diagonal(sends, step - 1)
    for item in items:
        item.finish()
    sends.drain()


def gather(specs, length, collective_id, name):
    modes = [mode for _, mode, _ in specs]
    shapes, sems = [], []
    for array, mode, by_columns in specs:
        blocks = {"all": 8 * length, "dp": 8, "z": length}[mode]
        if by_columns:
            shape = (array.shape[0], blocks * array.shape[1])
        else:
            shape = (blocks,) + array.shape
        shapes.append(jax.ShapeDtypeStruct(shape, array.dtype))
        sems += GatherItem.semaphores(mode, length)
    count = len(specs)

    def kernel(*refs):
        place = Place(length)
        items = []
        for number, (array, mode, by_columns) in enumerate(specs):
            source, target = refs[number], refs[count + number]
            recv, send, local = refs[2 * count + 3 * number : 2 * count + 3 * number + 3]
            half = array.shape[0] // 2
            width = array.shape[1]
            item = GatherItem(mode, place, None, None, recv, send, local)

            def own(h, source=source, half=half):
                return source.at[pl.ds(h * half, half)]

            def slot(column, z, h, target=target, half=half, width=width, item=item, by=by_columns):
                block = item.index(column, z)
                if by:
                    return target.at[
                        pl.ds(h * half, half), pl.ds(pl.multiple_of(block * width, width), width)
                    ]
                return target.at[block, pl.ds(h * half, half)]

            item.own, item.slot = own, slot
            items.append(item)
        run_gather(place, items)

    return pl.pallas_call(
        kernel,
        name=name,
        out_shape=shapes,
        in_specs=[pl.BlockSpec(memory_space=pl.ANY)] * count,
        out_specs=[pl.BlockSpec(memory_space=pl.ANY)] * count,
        scratch_shapes=sems,
        compiler_params=pltpu.CompilerParams(collective_id=collective_id, has_side_effects=True),
    )(*[array for array, _, _ in specs])


class ReduceItem:
    def __init__(self, mode, place, block, bufs, out):
        self.mode, self.place, self.block, self.out = mode, place, block, out
        self.over_z = mode != "dp"
        self.over_dp = mode != "z"
        self.length = place.length if self.over_z else 1
        (self.acc, self.from_core, self.corner, self.from_xy, self.from_z,
         self.load, self.send, self.recv) = bufs

    @staticmethod
    def scratch(mode, length, rows, width, in_place=False):
        t = length if mode != "dp" else 1
        columns = 4 if mode != "z" else 1
        dp = mode != "z"
        half = (rows // 2, width)
        small = (8, 128)
        return [
            pltpu.VMEM(small if in_place else (columns, t, 2) + half, jnp.bfloat16),
            pltpu.VMEM(((columns, t, 2) + half) if dp else small, jnp.bfloat16),
            pltpu.VMEM(((2, t) + half) if dp else small, jnp.bfloat16),
            pltpu.VMEM(((2, t, 2) + half) if dp else small, jnp.bfloat16),
            pltpu.VMEM(((t + 1, 2) + half) if mode != "dp" else small, jnp.bfloat16),
            pltpu.SemaphoreType.DMA((columns, t, 2)),
            pltpu.SemaphoreType.DMA((10, t, 2)),
            pltpu.SemaphoreType.DMA((9, t + 1, 2)),
        ]

    def z_of(self, turn):
        return self.place.target(turn) if self.over_z else 0

    def got(self, ref, lane, turn, h):
        pltpu.make_async_copy(ref, ref, self.recv.at[lane, turn, h]).wait()

    computed = False
    in_place = False

    def partial(self, column, turn, h):
        if self.in_place:
            return self.block(self.place.columns[column], self.z_of(turn), h)
        return self.acc.at[column, turn, h]

    def loaded(self, column, turn, h):
        if self.computed or self.in_place:
            return
        ref = self.acc.at[column, turn, h]
        pltpu.make_async_copy(ref, ref, self.load.at[column, turn, h]).wait()

    def add(self, target, refs, out=None):
        rows = target.shape[0]
        step = 16 if rows % 16 == 0 else rows
        place = target if out is None else out

        def body(i, carry):
            at = pl.ds(pl.multiple_of(i * step, step), step)
            total = target[at, :].astype(jnp.float32)
            for ref in refs:
                total = total + ref[at, :].astype(jnp.float32)
            place[at, :] = total.astype(place.dtype)
            return carry

        lax.fori_loop(0, rows // step, body, 0, unroll=2 if (rows // step) % 2 == 0 else 1)

    def begin(self):
        place = self.place
        if self.over_z:

            @pl.when((place.z == 0) | (place.z == self.length - 1))
            def _():
                def clear(i, carry):
                    self.from_z[i // 2, i % 2] = jnp.zeros(self.from_z.shape[2:], jnp.bfloat16)
                    return carry

                lax.fori_loop(0, 2 * (self.length + 1), clear, 0)

    def load_all(self):
        place = self.place
        for turn in range(self.length):
            for column in (3, 1, 2, 0) if self.over_dp else (0,):
                for h in range(2):
                    pltpu.make_async_copy(
                        self.block(place.columns[column], self.z_of(turn), h),
                        self.acc.at[column, turn, h],
                        self.load.at[column, turn, h],
                    ).start()

    def hand_over(self, sends, turn):
        if not self.over_dp or turn >= self.length:
            return
        place = self.place
        for column in (3, 1, 2, 0):
            for h in range(2):
                sends.start(
                    "core",
                    lambda column=column, h=h: (
                        self.block(place.columns[column] + place.to_core, self.z_of(turn), h),
                        self.from_core.at[column, turn, h],
                        self.send.at[column, turn, h],
                        self.recv.at[column, turn, h],
                    ),
                )

    def settle(self, column, turn, h, extra=(), out=None):
        self.loaded(column, turn, h)
        refs = list(extra)
        if self.over_dp:
            ref = self.from_core.at[column, turn, h]
            self.got(ref, column, turn, h)
            refs.append(ref)
        if refs or out is not None:
            self.add(self.partial(column, turn, h), refs, out)

    def corners(self, sends, turn):
        if not self.over_dp or not 0 <= turn < self.length:
            return
        for h, kind in ((0, "y"), (1, "x")):
            self.settle(3, turn, h)
            sends.start(
                kind,
                lambda h=h: (
                    self.partial(3, turn, h),
                    self.corner.at[h, turn],
                    self.send.at[4, turn, h],
                    self.recv.at[4, turn, h],
                ),
            )

    def straight(self, sends, turn, second):
        if not self.over_dp or not 0 <= turn < self.length:
            return
        for column, kind in ((1, "x"), (2, "y")):
            h = (column - 1) if second else (2 - column)
            extra = ()
            if second:
                ref = self.corner.at[h, turn]
                self.got(ref, 4, turn, h)
                extra = (ref,)
            self.settle(column, turn, h, extra)
            sends.start(
                kind,
                lambda column=column, h=h: (
                    self.partial(column, turn, h),
                    self.from_xy.at[column - 1, turn, h],
                    self.send.at[4 + column, turn, h],
                    self.recv.at[4 + column, turn, h],
                ),
            )

    def home(self, sends, turn):
        if not 0 <= turn < self.length:
            return
        place = self.place
        last = turn == self.length - 1
        z = self.z_of(turn)
        for h in range(2):
            extra = []
            if self.over_dp:
                for lane in (0, 1):
                    ref = self.from_xy.at[lane, turn, h]
                    self.got(ref, 5 + lane, turn, h)
                    extra.append(ref)
            if self.over_z:
                slot = self.from_z.at[z, h]

                def got_slot(h=h):
                    self.got(self.from_z.at[z, h], 7, z, h)

                def got_other(h=h):
                    self.got(self.from_z.at[self.length, h], 7, self.length, h)

                if last:
                    guarded(place.has_down, got_slot)
                    guarded(place.has_up, got_other)
                    extra += [slot, self.from_z.at[self.length, h]]
                else:
                    guarded((z > place.z) & place.has_down, got_slot)
                    guarded((z < place.z) & place.has_up, got_slot)
                    extra.append(slot)
            self.settle(
                0, turn, h, extra, self.out(h) if last else None
            )
            if self.over_z and not last:

                def going_up(h=h):
                    return (
                        self.partial(0, turn, h),
                        self.from_z.at[z, h],
                        self.send.at[7, turn, h],
                        self.recv.at[7, z, h],
                    )

                def going_down(h=h):
                    arrives = (z - place.z + 1 + self.length) // self.length
                    goal = z + arrives * (self.length - z)
                    return (
                        self.partial(0, turn, h),
                        self.from_z.at[goal, h],
                        self.send.at[7, turn, h],
                        self.recv.at[7, goal, h],
                    )

                above, below = z > place.z, z < place.z
                pl.when(above)(lambda: sends.start("up", going_up, lambda: above))
                pl.when(below)(lambda: sends.start("down", going_down, lambda: below))


def advance(item, sends, step):
    item.corners(sends, step)
    item.straight(sends, step, False)
    item.hand_over(sends, step + 2)
    item.straight(sends, step - 1, True)
    item.home(sends, step - 2 if item.over_dp else step)


def run_reduce(place, items, gathers=()):
    for item in items:
        item.begin()
    meet(place, any(i.over_z for i in items), any(i.over_dp for i in items))
    sends = Sends(place)
    for item in gathers:
        item.begin(sends)
    for item in items:
        item.load_all()
    for turn in range(2):
        for item in items:
            item.hand_over(sends, turn)
    longest = max(item.length for item in items)
    for step in range(longest + 2):
        for item in items:
            item.corners(sends, step)
        for item in items:
            item.straight(sends, step, False)
        for item in items:
            item.hand_over(sends, step + 2)
        for item in items:
            item.straight(sends, step - 1, True)
        for item in items:
            item.home(sends, step - 2 if item.over_dp else step)
        for item in gathers:
            item.along_z(sends, step + 1)
            item.across(sends, step)
            item.diagonal(sends, step - 1)
    for item in gathers:
        item.finish()
    sends.drain()


def reduce_rows(partials, small, length, collective_id):
    devices, rows, width = partials.shape
    half, low = rows // 2, small.shape[0] // 2

    def kernel(source, small_ref, target, small_all, *rest):
        place = Place(length)
        item = ReduceItem(
            "all",
            place,
            lambda c, z, h: source.at[c * length + z, pl.ds(h * half, half)],
            rest[:8],
            lambda h: target.at[pl.ds(h * half, half)],
        )
        beside = GatherItem("all", place, None, None, *rest[8:])
        beside.own = lambda h: small_ref.at[pl.ds(h * low, low)]
        beside.slot = lambda c, z, h: small_all.at[c * length + z, pl.ds(h * low, low)]
        run_reduce(place, [item], [beside])

    any_spec = pl.BlockSpec(memory_space=pl.ANY)
    return pl.pallas_call(
        kernel,
        name="reduce_rows",
        out_shape=[
            jax.ShapeDtypeStruct((rows, width), jnp.float32),
            jax.ShapeDtypeStruct((devices,) + small.shape, small.dtype),
        ],
        in_specs=[any_spec, any_spec],
        out_specs=[pl.BlockSpec(memory_space=pltpu.VMEM), any_spec],
        scratch_shapes=ReduceItem.scratch("all", length, rows, width)
        + GatherItem.semaphores("all", length),
        compiler_params=pltpu.CompilerParams(
            collective_id=collective_id, has_side_effects=True, vmem_limit_bytes=56 << 20
        ),
    )(partials, small)


def dot(left, right, left_dim=1, right_dim=0):
    return lax.dot_general(
        left, right, (((left_dim,), (right_dim,)), ((), ())), preferred_element_type=jnp.float32
    )


def experts(rows_own, all_cots, gates_own, wgate, wup, wdown, length, capacity, collective_id):
    rows, width = rows_own.shape
    hidden = wgate.shape[1]
    devices = 8 * length
    count = 4 * capacity
    tile = 512 if width % 512 == 0 else width
    narrow = 256 if hidden % 256 == 0 else hidden
    f32, bf16 = jnp.float32, jnp.bfloat16

    def kernel(
        rows_ref, all_cots, gates_ref, wg, wu, wd,
        all_rows, part_out, part_grad, token_in, out_wg, out_wu, out_wd,
        table, row_buf, cot_buf, picked, cotan, gated, hid, dgate, dup, scaled, back,
        chosen, slot_gate, slot_sum, acc_g, acc_u, acc_d, stage_out, stage_grad, token_out,
        recv_r, send_r, local_r, recv_t, send_t, local_t,
        load_sem, store_sem, final_sem, token_sem,
    ):
        place = Place(length)
        expert = place.dp * length + place.z

        def item_of(source, target, sems, half):
            item = GatherItem("all", place, None, None, *sems)
            item.own = lambda h: source.at[pl.ds(h * half, half)]
            item.slot = lambda column, z, h: target.at[
                column * length + z, pl.ds(h * half, half)
            ]
            return item

        big = [
            item_of(rows_ref, all_rows, (recv_r, send_r, local_r), rows // 2),
        ]
        items = [item_of(gates_ref, table, (recv_t, send_t, local_t), gates_ref.shape[0] // 2)] + big
        meet_all(place)
        sends = Sends(place)
        for item in items:
            item.begin(sends)

        def along(distance):
            for item in items:
                item.along_z(sends, distance)

        def across(distance):
            for item in items:
                item.across(sends, distance)

        def corner(distance):
            for item in items:
                item.diagonal(sends, distance)

        def clear(i, carry):
            at = pl.ds(pl.multiple_of(i * 64, 64), 64)
            acc_g[at, :] = jnp.zeros((64, hidden), f32)
            acc_u[at, :] = jnp.zeros((64, hidden), f32)
            return carry

        def clear_down(i, carry):
            at = pl.ds(pl.multiple_of(i * 64, 64), 64)
            acc_d[at, :] = jnp.zeros((64, width), f32)
            return carry

        lax.fori_loop(0, width // 64, clear, 0)
        lax.fori_loop(0, hidden // 64, clear_down, 0)
        along(1)
        across(0)
        for item in items:
            item.settled()

        def block_of(j, side, z):
            return (place.columns[j] + side * place.to_core) * length + z

        def load(j, side, z, slot):
            block = block_of(j, side, z)
            return [
                pltpu.make_async_copy(all_rows.at[block], row_buf.at[slot, j], load_sem.at[slot, 0, j]),
                pltpu.make_async_copy(all_cots.at[block], cot_buf.at[slot, j], load_sem.at[slot, 1, j]),
            ]

        def store(j, side, z, slot):
            block = block_of(j, side, z)
            return [
                pltpu.make_async_copy(stage_out.at[slot, j], part_out.at[block], store_sem.at[slot, 0, j]),
                pltpu.make_async_copy(stage_grad.at[slot, j], part_grad.at[block], store_sem.at[slot, 1, j]),
            ]

        order = lax.broadcasted_iota(jnp.int32, (rows, rows), 0)
        upto = (order <= lax.broadcasted_iota(jnp.int32, (rows, rows), 1)).astype(f32).astype(bf16)
        slots = lax.broadcasted_iota(jnp.int32, (capacity, rows), 0).astype(f32)

        def unit(i, carry):
            turn, side = i // 2, i % 2
            z = place.nearest(turn)

            for step in range(length):

                @pl.when(i == 2 * step)
                def _(step=step):
                    along(step + 2)
                    corner(step)
                    across(step + 1)
                    for item in items:
                        item.from_core(place.nearest(step))
                    for other in range(2):
                        for j in range(4):
                            for copy in load(j, other, place.nearest(step), other):
                                copy.start()

            @pl.when(i >= 2)
            def _():
                for j in range(4):
                    for copy in store(j, side, z, side):
                        copy.wait()

            for j in range(4):
                for copy in load(j, side, z, side):
                    copy.wait()
                block = block_of(j, side, z)
                line = table[block, pl.ds(expert, 1), :]
                named = line >= 0.0
                ranks = dot(named.astype(f32).astype(bf16), upto) - 1.0
                pick = jnp.where(named & (ranks == slots), 1.0, 0.0)
                gate = jnp.sum(pick * line, axis=1, keepdims=True)
                chosen[j] = pick.astype(bf16)
                at = pl.ds(j * capacity, capacity)
                slot_gate[at, :] = jnp.broadcast_to(gate, (capacity, 128))

                def select(n, carry, j=j, at=at):
                    lanes = pl.ds(pl.multiple_of(n * tile, tile), tile)
                    picked[at, lanes] = dot(chosen[j], row_buf[side, j, :, lanes]).astype(bf16)
                    cot = dot(chosen[j], cot_buf[side, j, :, lanes])
                    cotan[at, lanes] = cot.astype(bf16)
                    gated[at, lanes] = (slot_gate[at, 0:1] * cot).astype(bf16)
                    return carry

                lax.fori_loop(0, width // tile, select, 0)

            def middle(n, carry):
                lanes = pl.ds(pl.multiple_of(n * narrow, narrow), narrow)
                gate = dot(picked[...], wg[:, lanes])
                up = dot(picked[...], wu[:, lanes])
                grad = dot(gated[...], wd[lanes, :], 1, 1)
                sigma = jax.nn.sigmoid(gate)
                hid[:, lanes] = (gate * sigma * up).astype(bf16)
                dgate[:, lanes] = (grad * up * sigma * (1.0 + gate * (1.0 - sigma))).astype(bf16)
                dup[:, lanes] = (grad * gate * sigma).astype(bf16)
                return carry

            lax.fori_loop(0, hidden // narrow, middle, 0)
            slot_sum[...] = jnp.zeros(slot_sum.shape, f32)

            def outward(n, carry):
                lanes = pl.ds(pl.multiple_of(n * tile, tile), tile)
                result = dot(hid[...], wd[:, lanes]).astype(bf16).astype(f32)
                products = cotan[:, lanes].astype(f32) * result
                total = products[:, 0:128]
                for k in range(1, tile // 128):
                    total = total + products[:, 128 * k : 128 * (k + 1)]
                slot_sum[...] += total
                scaled[:, lanes] = (slot_gate[:, 0:1] * result).astype(bf16)
                back[:, lanes] = (
                    dot(dgate[...], wg[lanes, :], 1, 1) + dot(dup[...], wu[lanes, :], 1, 1)
                ).astype(bf16)
                for j in range(4):
                    at = pl.ds(j * capacity, capacity)
                    stage_out[side, j, :, lanes] = dot(chosen[j], scaled[at, lanes], 0, 0).astype(bf16)
                    stage_grad[side, j, :, lanes] = dot(chosen[j], back[at, lanes], 0, 0).astype(bf16)
                return carry

            lax.fori_loop(0, width // tile, outward, 0)
            for j in range(4):
                for copy in store(j, side, z, side):
                    copy.start()
                at = pl.ds(j * capacity, capacity)
                total = jnp.sum(slot_sum[at, :], axis=1, keepdims=True)
                sums = jnp.sum(chosen[j].astype(f32) * total, axis=0, keepdims=True)
                token_out[block_of(j, side, z)] = jnp.broadcast_to(sums, (8, rows))

            def weights(n, carry):
                lanes = pl.ds(pl.multiple_of(n * tile, tile), tile)
                acc_g[lanes, :] += dot(picked[:, lanes], dgate[...], 0, 0)
                acc_u[lanes, :] += dot(picked[:, lanes], dup[...], 0, 0)
                acc_d[:, lanes] += dot(hid[...], gated[:, lanes], 0, 0)
                return carry

            lax.fori_loop(0, width // tile, weights, 0)
            return carry

        lax.fori_loop(0, 2 * length, unit, 0)
        finals = [
            pltpu.make_async_copy(source, target, final_sem.at[n])
            for n, (source, target) in enumerate(
                ((acc_g, out_wg), (acc_u, out_wu), (acc_d, out_wd))
            )
        ]
        for copy in finals:
            copy.start()

        def token_send(n):
            device, there = other_device(place, n + 1)
            return pltpu.make_async_remote_copy(
                src_ref=token_out.at[there],
                dst_ref=token_in.at[expert],
                send_sem=token_sem.at[0],
                recv_sem=token_sem.at[1],
                device_id=device,
                device_id_type=MESH,
            )

        def send(n, carry):
            token_send(n).start()
            return carry

        lax.fori_loop(0, devices - 1, send, 0)
        pltpu.make_async_copy(token_out.at[expert], token_in.at[expert], token_sem.at[1]).start()
        for side in range(2):
            for j in range(4):
                for copy in store(j, side, 0, side):
                    copy.wait()
        for copy in finals:
            copy.wait()
        sends.drain()
        pltpu.make_async_copy(token_out, token_in, token_sem.at[1]).wait()
        sent = token_out.at[pl.ds(0, devices - 1)]
        pltpu.make_async_copy(sent, sent, token_sem.at[0]).wait()

    any_spec = pl.BlockSpec(memory_space=pl.ANY)
    vmem = pl.BlockSpec(memory_space=pltpu.VMEM)
    big = (devices, rows, width)
    shape = jax.ShapeDtypeStruct
    sems = pltpu.SemaphoreType.DMA
    return pl.pallas_call(
        kernel,
        name="experts",
        out_shape=[
            shape(big, bf16), shape(big, bf16), shape(big, bf16),
            shape((devices, 8, rows), f32),
            shape((width, hidden), f32), shape((width, hidden), f32), shape((hidden, width), f32),
        ],
        in_specs=[any_spec] * 3 + [vmem] * 3,
        out_specs=[any_spec] * 3 + [vmem] + [any_spec] * 3,
        scratch_shapes=[
            pltpu.VMEM((devices,) + gates_own.shape, f32),
            pltpu.VMEM((2, 4, rows, width), bf16),
            pltpu.VMEM((2, 4, rows, width), bf16),
            pltpu.VMEM((count, width), bf16),
            pltpu.VMEM((count, width), bf16),
            pltpu.VMEM((count, width), bf16),
            pltpu.VMEM((count, hidden), bf16),
            pltpu.VMEM((count, hidden), bf16),
            pltpu.VMEM((count, hidden), bf16),
            pltpu.VMEM((count, width), bf16),
            pltpu.VMEM((count, width), bf16),
            pltpu.VMEM((4, capacity, rows), bf16),
            pltpu.VMEM((count, 128), f32),
            pltpu.VMEM((count, 128), f32),
            pltpu.VMEM((width, hidden), f32),
            pltpu.VMEM((width, hidden), f32),
            pltpu.VMEM((hidden, width), f32),
            pltpu.VMEM((2, 4, rows, width), bf16),
            pltpu.VMEM((2, 4, rows, width), bf16),
            pltpu.VMEM((devices, 8, rows), f32),
        ]
        + GatherItem.semaphores("all", length) * 2
        + [sems((2, 2, 4)), sems((2, 2, 4)), sems((3,)), sems((2,))],
        compiler_params=pltpu.CompilerParams(
            collective_id=collective_id, has_side_effects=True, vmem_limit_bytes=63 << 20
        ),
    )(rows_own, all_cots, gates_own, wgate, wup, wdown)


def rope(values, cosine, sine):
    return values * cosine + pltpu.roll(values, values.shape[-1] // 2, 1) * sine


def unrope(values, cosine, sine):
    return values * cosine - pltpu.roll(values, values.shape[-1] // 2, 1) * sine


def row_factor(values):
    return lax.rsqrt(jnp.mean(values * values, axis=-1, keepdims=True) + EPSILON)


def visible_pairs(seg_col, seg_row, start, stop, reach):
    shape = (stop - start, reach)
    query = lax.broadcasted_iota(jnp.int32, shape, 0) + start
    key = lax.broadcasted_iota(jnp.int32, shape, 1)
    return (seg_col[start:stop, :] == seg_row[:, 0:reach]) & (key <= query)


def attend(rows_own, joint_own, output_own, cots_own, seg_col, seg_row, cosine, sine, query_gain, key_gain, length, collective_id):
    rows, width = rows_own.shape
    depth, joint = joint_own.shape
    head_width, part = output_own.shape
    head = query_gain.shape[-1]
    heads = head_width // head
    tokens = rows * length
    block = tokens // 2
    tile = 512
    scale = 1.0 / math.sqrt(head)
    f32, bf16 = jnp.float32, jnp.bfloat16

    def kernel(
        rows_ref, joint_ref, output_ref, cots_ref, segc, segr, cos_ref, sin_ref, qgain, kgain,
        out_add, out_rows, out_joint, out_weight, out_cots, out_qkv, out_heads,
        rows_v, joint_v, weight_v, qkv, att, key_v, value_v,
        r0, r1, r2, r3, r4, r5, r6, r7,
        g0, g1, g2, j0, j1, j2, w0, w1, w2, c0, c1, c2, save_sem,
    ):
        place = Place(length)

        def item_of(mode, source, half, slot, sems):
            item = GatherItem(mode, place, None, None, *sems)
            item.own = lambda h: source.at[pl.ds(h * half, half)]
            item.slot = slot
            return item

        half, deep, tall = rows // 2, depth // 2, head_width // 2
        own_rows = item_of(
            "z", rows_ref, half, lambda c, z, h: rows_v.at[z, pl.ds(h * half, half)], (g0, g1, g2)
        )
        own_joint = item_of(
            "dp", joint_ref, deep, lambda c, z, h: joint_v.at[c, pl.ds(h * deep, deep)], (j0, j1, j2)
        )
        own_weight = item_of(
            "dp",
            output_ref,
            tall,
            lambda c, z, h: weight_v.at[
                pl.ds(h * tall, tall), pl.ds(pl.multiple_of(c * part, part), part)
            ],
            (w0, w1, w2),
        )
        cots = item_of(
            "all",
            cots_ref,
            half,
            lambda c, z, h: out_cots.at[c * length + z, pl.ds(h * half, half)],
            (c0, c1, c2),
        )
        total = ReduceItem(
            "z", place, None, (r0, r1, r2, r3, r4, r5, r6, r7),
            lambda h: out_add.at[pl.ds(h * half, half)],
        )
        total.computed = True
        total.begin()
        meet(place, True, True)
        sends = Sends(place)
        own_joint.begin(sends)
        own_rows.begin(sends)
        own_weight.begin(sends)
        own_joint.across(sends, 0)
        own_rows.along_z(sends, 1)
        own_weight.across(sends, 0)
        own_joint.diagonal(sends, 0)
        own_rows.along_z(sends, 2)
        own_weight.diagonal(sends, 0)
        for distance in range(3, length):
            own_rows.along_z(sends, distance)
        cots.begin(sends)
        own_joint.finish()
        own_rows.finish()

        def projection(n, carry):
            lanes = pl.ds(pl.multiple_of(n * 256, 256), 256)
            left = rows_v[...].reshape(tokens, width)
            right = joint_v[:, :, lanes].reshape(width, 256)
            qkv[:, lanes] = dot(left, right)
            return carry

        lax.fori_loop(0, joint // 256, projection, 0)
        saves = [
            pltpu.make_async_copy(source, target, save_sem.at[n])
            for n, (source, target) in enumerate(
                ((rows_v, out_rows), (joint_v, out_joint), (qkv, out_qkv), (weight_v, out_weight), (att, out_heads))
            )
        ]
        for copy in saves[:3]:
            copy.start()
        key = qkv[:, head_width : head_width + head]
        key_v[...] = rope(key * row_factor(key) * kgain[...], cos_ref[...], sin_ref[...]).astype(bf16)
        value_v[...] = qkv[:, head_width + head : head_width + 2 * head].astype(bf16)

        def one_head(n, carry):
            lanes = pl.ds(pl.multiple_of(n * head, head), head)
            for start in range(0, tokens, block):
                stop = start + block
                query = qkv[start:stop, lanes]
                turned = rope(
                    query * row_factor(query) * qgain[...], cos_ref[start:stop, :], sin_ref[start:stop, :]
                ).astype(bf16)
                scores = dot(turned, key_v[0:stop, :], 1, 1) * scale
                seen = visible_pairs(segc, segr, start, stop, stop)
                scores = jnp.where(seen, scores, NEG_BIG)
                top = jnp.max(scores, axis=-1, keepdims=True)
                powers = jnp.exp(scores - top)
                probs = (powers / jnp.sum(powers, axis=-1, keepdims=True)).astype(bf16)
                att[start:stop, lanes] = dot(probs, value_v[0:stop, :]).astype(bf16)
            return carry

        lax.fori_loop(0, heads // 2, one_head, 0)
        cots.along_z(sends, 1)
        cots.across(sends, 0)
        lax.fori_loop(heads // 2, heads, one_head, 0)
        saves[4].start()
        own_weight.finish()
        saves[3].start()

        def outward(turn):
            z = total.z_of(turn)

            def body(n, carry):
                lanes = pl.ds(pl.multiple_of(n * tile, tile), tile)
                left = att[pl.ds(pl.multiple_of(z * rows, rows), rows), :]
                found = dot(left, weight_v[:, lanes]).astype(bf16)
                for h in range(2):
                    total.acc[0, turn, h, :, lanes] = found[h * half : (h + 1) * half, :]
                return carry

            lax.fori_loop(0, width // tile, body, 0)

        for turn in range(length):
            outward(turn)
            total.home(sends, turn)
            cots.along_z(sends, turn + 2)
            cots.diagonal(sends, turn)
            cots.across(sends, turn + 1)
        cots.finish()
        for copy in saves:
            copy.wait()
        sends.drain()

    any_spec = pl.BlockSpec(memory_space=pl.ANY)
    vmem = pl.BlockSpec(memory_space=pltpu.VMEM)
    shape = jax.ShapeDtypeStruct
    return pl.pallas_call(
        kernel,
        name="attend",
        out_shape=[
            shape((rows, width), f32),
            shape((length, rows, width), bf16),
            shape((8, depth, joint), bf16),
            shape((head_width, 8 * part), bf16),
            shape((8 * length, rows, width), bf16),
            shape((tokens, joint), f32),
            shape((tokens, head_width), bf16),
        ],
        in_specs=[any_spec] * 4 + [vmem] * 6,
        out_specs=[vmem] + [any_spec] * 6,
        scratch_shapes=[
            pltpu.VMEM((length, rows, width), bf16),
            pltpu.VMEM((8, depth, joint), bf16),
            pltpu.VMEM((head_width, 8 * part), bf16),
            pltpu.VMEM((tokens, joint), f32),
            pltpu.VMEM((tokens, head_width), bf16),
            pltpu.VMEM((tokens, head), bf16),
            pltpu.VMEM((tokens, head), bf16),
        ]
        + ReduceItem.scratch("z", length, rows, width)
        + GatherItem.semaphores("z", length)
        + GatherItem.semaphores("dp", length) * 2
        + GatherItem.semaphores("all", length)
        + [pltpu.SemaphoreType.DMA((5,))],
        compiler_params=pltpu.CompilerParams(
            collective_id=collective_id, has_side_effects=True, vmem_limit_bytes=56 << 20
        ),
    )(rows_own, joint_own, output_own, cots_own, seg_col, seg_row, cosine, sine, query_gain, key_gain)


def attend_back(grad_own, rows_all, joint_all, output_all, qkv_all, heads_all, part_out, seg_col, seg_row, cosine, sine, query_gain, key_gain, length, collective_id):
    rows, width = grad_own.shape
    _, depth, joint = joint_all.shape
    head_width = output_all.shape[0]
    part = width // 8
    head = query_gain.shape[-1]
    heads = head_width // head
    tokens = rows * length
    block = tokens // 2
    scale = 1.0 / math.sqrt(head)
    f32, bf16 = jnp.float32, jnp.bfloat16
    half, deep, tall = rows // 2, depth // 2, head_width // 2

    def kernel(
        grad_ref, rows_ref, joint_ref, output_ref, qkv_ref, heads_ref, part_ref,
        segc, segr, cos_ref, sin_ref, qgain, kgain,
        out_rows, out_joint, out_weight, out_moe, out_qgain, out_kgain,
        grads, joint_v, weight_v, qkv, att, gatt, joint_b, part_w, key_v, value_v, dkey, dvalue,
        *rest,
    ):
        place = Place(length)
        o_bufs, z_bufs, j_bufs, w_bufs = (rest[8 * n : 8 * n + 8] for n in range(4))
        gather_sems, load_sem = rest[32:35], rest[35]

        outs = ReduceItem(
            "all",
            place,
            lambda c, z, h: part_ref.at[c * length + z, pl.ds(h * half, half)],
            o_bufs,
            lambda h: out_moe.at[pl.ds(h * half, half)],
        )
        back = ReduceItem(
            "z",
            place,
            lambda c, z, h: grads.at[z, pl.ds(h * half, half)],
            z_bufs,
            lambda h: out_rows.at[pl.ds(h * half, half)],
        )
        joints = ReduceItem(
            "dp",
            place,
            lambda c, z, h: joint_v.at[c, pl.ds(h * deep, deep)],
            j_bufs,
            lambda h: out_joint.at[pl.ds(h * deep, deep)],
        )
        weights = ReduceItem(
            "dp",
            place,
            lambda c, z, h: part_w.at[
                pl.ds(h * tall, tall), pl.ds(pl.multiple_of(c * part, part), part)
            ],
            w_bufs,
            lambda h: out_weight.at[pl.ds(h * tall, tall)],
        )
        for item in (back, joints, weights):
            item.in_place = True
        gathers = GatherItem("z", place, None, None, *gather_sems)
        gathers.own = lambda h: grad_ref.at[pl.ds(h * half, half)]
        gathers.slot = lambda c, z, h: grads.at[z, pl.ds(h * half, half)]

        outs.begin()
        back.begin()
        meet(place, True, True)
        first, sends = Sends(place), Sends(place)
        gathers.begin(first)
        outs.load_all()
        outs.hand_over(sends, 0)
        outs.hand_over(sends, 1)
        loads = [
            pltpu.make_async_copy(source, target, load_sem.at[n])
            for n, (source, target) in enumerate(
                ((output_ref, weight_v), (heads_ref, att), (qkv_ref, qkv), (joint_ref, joint_v))
            )
        ]
        for copy in loads:
            copy.start()
        advance(outs, sends, 0)
        for distance in range(1, length):
            gathers.along_z(first, distance)
            if distance < length - 1:
                advance(outs, sends, distance)
        gathers.finish()
        first.drain()
        for copy in loads[:3]:
            copy.wait()

        def to_heads(n, carry):
            lanes = pl.ds(pl.multiple_of(n * 256, 256), 256)
            left = grads[...].reshape(tokens, width)
            gatt[:, lanes] = dot(left, weight_v[lanes, :], 1, 1).astype(bf16)
            return carry

        def to_weight(n, carry):
            lanes = pl.ds(pl.multiple_of(n * 256, 256), 256)
            right = grads[:, :, lanes].reshape(tokens, 256)
            part_w[:, lanes] = dot(att[...], right, 0, 0).astype(bf16)
            return carry

        lax.fori_loop(0, width // 256, to_weight, 0)
        weights.hand_over(sends, 0)
        lax.fori_loop(0, head_width // 256, to_heads, 0)
        rows_v = weight_v.at[pl.ds(0, tokens)]
        rows_loads = [
            pltpu.make_async_copy(
                rows_ref.at[z], weight_v.at[pl.ds(z * rows, rows)], load_sem.at[4 + z]
            )
            for z in range(length)
        ]
        for copy in rows_loads:
            copy.start()
        advance(weights, sends, 0)
        key = qkv[:, head_width : head_width + head]
        key_v[...] = rope(key * row_factor(key) * kgain[...], cos_ref[...], sin_ref[...]).astype(bf16)
        value_v[...] = qkv[:, head_width + head : head_width + 2 * head].astype(bf16)
        dkey[...] = jnp.zeros((tokens, head), f32)
        dvalue[...] = jnp.zeros((tokens, head), f32)
        out_qgain[...] = jnp.zeros(out_qgain.shape, f32)

        def normed_back(grad, raw, gain, start, stop):
            factor = row_factor(raw)
            hat = raw * factor
            turned = unrope(grad, cos_ref[start:stop, :], sin_ref[start:stop, :])
            scaled = turned * gain
            found = factor * (scaled - hat * jnp.mean(scaled * hat, axis=-1, keepdims=True))
            return found, jnp.sum(turned * hat, axis=0, keepdims=True)

        def one_head(n, carry):
            lanes = pl.ds(pl.multiple_of(n * head, head), head)
            for start in range(0, tokens, block):
                stop = start + block
                raw = qkv[start:stop, lanes]
                turned = rope(
                    raw * row_factor(raw) * qgain[...], cos_ref[start:stop, :], sin_ref[start:stop, :]
                ).astype(bf16)
                grad = gatt[start:stop, lanes]
                delta = jnp.sum(
                    grad.astype(f32) * att[start:stop, lanes].astype(f32), axis=-1, keepdims=True
                )
                scores = dot(turned, key_v[0:stop, :], 1, 1) * scale
                seen = visible_pairs(segc, segr, start, stop, stop)
                scores = jnp.where(seen, scores, NEG_BIG)
                powers = jnp.exp(scores - jnp.max(scores, axis=-1, keepdims=True))
                probs = powers / jnp.sum(powers, axis=-1, keepdims=True)
                dprobs = dot(grad, value_v[0:stop, :], 1, 1)
                dscores = (probs * (dprobs - delta)).astype(bf16)
                dvalue[0:stop, :] += dot(probs.astype(bf16), grad, 0, 0)
                dkey[0:stop, :] += dot(dscores, turned, 0, 0) * scale
                dquery = dot(dscores, key_v[0:stop, :]) * scale
                found, gain_part = normed_back(dquery, raw, qgain[...], start, stop)
                joint_b[start:stop, lanes] = found.astype(bf16)
                out_qgain[...] += gain_part
            return carry

        lax.fori_loop(0, heads // 2, one_head, 0)
        advance(outs, sends, length - 1)
        advance(weights, sends, 1)
        lax.fori_loop(heads // 2, heads, one_head, 0)
        found, gain_part = normed_back(
            dkey[...], qkv[:, head_width : head_width + head], kgain[...], 0, tokens
        )
        out_kgain[...] = gain_part
        joint_b[:, head_width : head_width + head] = found.astype(bf16)
        joint_b[:, head_width + head : head_width + 2 * head] = dvalue[...].astype(bf16)
        advance(outs, sends, length)
        advance(weights, sends, 2)
        loads[3].wait()

        def to_rows(n, carry):
            lanes = pl.ds(pl.multiple_of(n * depth, depth), depth)
            found = dot(joint_b[...], joint_v[n], 1, 1).astype(bf16)
            grads[:, :, lanes] = found.reshape(length, rows, depth)
            return carry

        lax.fori_loop(0, 8, to_rows, 0)
        back.home(sends, 0)
        for copy in rows_loads:
            copy.wait()

        def to_joint(n, carry):
            lanes = pl.ds(pl.multiple_of(n * depth, depth), depth)
            joint_v[n] = dot(weight_v[0:tokens, lanes], joint_b[...], 0, 0).astype(bf16)
            return carry

        lax.fori_loop(0, 8, to_joint, 0)
        joints.hand_over(sends, 0)
        back.home(sends, 1)
        advance(joints, sends, 0)
        for turn in range(2, length):
            back.home(sends, turn)
        advance(joints, sends, 1)
        advance(outs, sends, length + 1)
        advance(joints, sends, 2)
        sends.drain()

    any_spec = pl.BlockSpec(memory_space=pl.ANY)
    vmem = pl.BlockSpec(memory_space=pltpu.VMEM)
    shape = jax.ShapeDtypeStruct
    return pl.pallas_call(
        kernel,
        name="attend_back",
        out_shape=[
            shape((rows, width), f32),
            shape((depth, joint), f32),
            shape((head_width, part), f32),
            shape((rows, width), f32),
            shape((1, head), f32),
            shape((1, head), f32),
        ],
        in_specs=[any_spec] * 7 + [vmem] * 6,
        out_specs=[vmem] * 6,
        scratch_shapes=[
            pltpu.VMEM((length, rows, width), bf16),
            pltpu.VMEM((8, depth, joint), bf16),
            pltpu.VMEM((head_width, width), bf16),
            pltpu.VMEM((tokens, joint), f32),
            pltpu.VMEM((tokens, head_width), bf16),
            pltpu.VMEM((tokens, head_width), bf16),
            pltpu.VMEM((tokens, joint), bf16),
            pltpu.VMEM((head_width, width), bf16),
            pltpu.VMEM((tokens, head), bf16),
            pltpu.VMEM((tokens, head), bf16),
            pltpu.VMEM((tokens, head), f32),
            pltpu.VMEM((tokens, head), f32),
        ]
        + ReduceItem.scratch("all", length, rows, width)
        + ReduceItem.scratch("z", length, rows, width, True)
        + ReduceItem.scratch("dp", length, depth, joint, True)
        + ReduceItem.scratch("dp", length, head_width, part, True)
        + GatherItem.semaphores("z", length)
        + [pltpu.SemaphoreType.DMA((4 + length,))],
        compiler_params=pltpu.CompilerParams(
            collective_id=collective_id, has_side_effects=True, vmem_limit_bytes=67043328
        ),
    )(grad_own, rows_all, joint_all, output_all, qkv_all, heads_all, part_out, seg_col, seg_row, cosine, sine, query_gain, key_gain)


def mix(form, left, right):
    return jnp.einsum(form, left, right, preferred_element_type=jnp.float32)


def rms_scale(values):
    return lax.rsqrt(jnp.mean(values * values, axis=-1, keepdims=True) + EPSILON)


def rope_tables(seg_ids, head_dim):
    length = seg_ids.shape[0]
    row_index = jnp.arange(length, dtype=jnp.int32)
    starts = jnp.sum((seg_ids[None, :] < seg_ids[:, None]).astype(jnp.int32), axis=1)
    places = (row_index - starts).astype(jnp.float32)
    half_dim = head_dim // 2
    frequency = THETA_BASE ** (-(jnp.arange(half_dim, dtype=jnp.float32) * (2.0 / head_dim)))
    angles = places[:, None] * frequency[None, :]
    return (jnp.cos(angles), jnp.sin(angles))


def rotate(values, cosine, sine_table):
    half_dim = values.shape[-1] // 2
    front_part = values[..., :half_dim]
    back_part = values[..., half_dim:]
    cos_rows = cosine[:, None, :]
    sin_rows = sine_table[:, None, :]
    return jnp.concatenate(
        [
            front_part * cos_rows - back_part * sin_rows,
            back_part * cos_rows + front_part * sin_rows,
        ],
        axis=-1,
    )


def unrotate(values, cosine, sine_table):
    half_dim = values.shape[-1] // 2
    front_part = values[..., :half_dim]
    back_part = values[..., half_dim:]
    cos_rows = cosine[:, None, :]
    sin_rows = sine_table[:, None, :]
    return jnp.concatenate(
        [
            front_part * cos_rows + back_part * sin_rows,
            back_part * cos_rows - front_part * sin_rows,
        ],
        axis=-1,
    )


def head_norm_back(grad_out, normed, factor, gain):
    grad_normed = grad_out * gain
    grad_gain = jnp.sum(grad_out * normed, axis=(0, 1))
    grad_values = factor * (
        grad_normed - normed * jnp.mean(grad_normed * normed, axis=-1, keepdims=True)
    )
    return (grad_values, grad_gain)


def row_norm_back(grad_out, normed, factor, gain):
    grad_normed = grad_out * gain
    grad_gain = jnp.sum(grad_out * normed, axis=0)
    grad_values = factor * (
        grad_normed - normed * jnp.mean(grad_normed * normed, axis=-1, keepdims=True)
    )
    return (grad_values, grad_gain)


def softmax_rows(logits):
    top_value = jnp.max(logits, axis=-1, keepdims=True)
    expo = jnp.exp(logits - top_value)
    return expo / jnp.sum(expo, axis=-1, keepdims=True)


def attn_forward(rows, seg_ids, wq_full, wk_full, wv_full, query_gain, key_gain):
    length = rows.shape[0]
    head_dim = query_gain.shape[0]
    num_heads = wq_full.shape[1] // head_dim
    kv_heads = wk_full.shape[1] // head_dim
    per_group = num_heads // kv_heads
    inv_root = 1.0 / math.sqrt(head_dim)
    block_rows = math.gcd(length, 512)
    cosine, sine_table = rope_tables(seg_ids, head_dim)
    query = jnp.dot(rows, wq_full, preferred_element_type=jnp.float32).reshape(
        length, num_heads, head_dim
    )
    key_proj = jnp.dot(rows, wk_full, preferred_element_type=jnp.float32).reshape(
        length, kv_heads, head_dim
    )
    value_rows = (
        jnp.dot(rows, wv_full, preferred_element_type=jnp.float32)
        .astype(jnp.bfloat16)
        .reshape(length, kv_heads, head_dim)
    )
    query_factor = rms_scale(query)
    query_hat = query * query_factor
    key_factor = rms_scale(key_proj)
    key_hat = key_proj * key_factor
    query_rot = (
        rotate(query_hat * query_gain, cosine, sine_table)
        .astype(jnp.bfloat16)
        .reshape(length, kv_heads, per_group, head_dim)
    )
    key_rot = rotate(key_hat * key_gain, cosine, sine_table).astype(jnp.bfloat16)
    row_index = jnp.arange(length, dtype=jnp.int32)
    scores = mix("qgrd,kgd->grqk", query_rot, key_rot) * inv_root
    visible = (seg_ids[0:block_rows, None] == seg_ids[None, :]) & (
        row_index[None, :] <= row_index[0:block_rows, None]
    )
    scores = jnp.where(visible, scores, NEG_BIG)
    top_value = jnp.max(scores, axis=-1, keepdims=True)
    expo = jnp.exp(scores - top_value)
    totals = jnp.sum(expo, axis=-1, keepdims=True)
    prob_rows = (expo / totals).astype(jnp.bfloat16)
    outputs = mix("grqk,kgd->qgrd", prob_rows, value_rows).astype(jnp.bfloat16)
    lse_parts = top_value[..., 0] + jnp.log(totals[..., 0])
    attn_heads = outputs.reshape(length, num_heads * head_dim)
    return (
        attn_heads,
        lse_parts,
        query_rot,
        key_rot,
        value_rows,
        cosine,
        sine_table,
        query_hat,
        query_factor,
        key_hat,
        key_factor,
    )


def attn_backward(
    grad_attn, rows, seg_ids, wq_full, wk_full, wv_full, wo_full, query_gain, key_gain, saved
):
    (
        attn_heads,
        lse_all,
        query_rot,
        key_rot,
        value_rows,
        cosine,
        sine_table,
        query_hat,
        query_factor,
        key_hat,
        key_factor,
    ) = saved
    length = rows.shape[0]
    head_dim = query_gain.shape[0]
    num_heads = query_hat.shape[1]
    inv_root = 1.0 / math.sqrt(head_dim)
    block_rows = math.gcd(length, 512)
    grad_wo = jnp.dot(attn_heads.T, grad_attn, preferred_element_type=jnp.float32)
    grad_heads = (
        jnp.dot(grad_attn, wo_full.T, preferred_element_type=jnp.float32)
        .astype(jnp.bfloat16)
        .reshape(query_rot.shape)
    )
    heads_view = attn_heads.reshape(query_rot.shape)
    row_delta = jnp.transpose(
        jnp.sum(grad_heads.astype(jnp.float32) * heads_view.astype(jnp.float32), axis=-1), (1, 2, 0)
    )
    row_index = jnp.arange(length, dtype=jnp.int32)
    scores = mix("qgrd,kgd->grqk", query_rot, key_rot) * inv_root
    visible = (seg_ids[0:block_rows, None] == seg_ids[None, :]) & (
        row_index[None, :] <= row_index[0:block_rows, None]
    )
    scores = jnp.where(visible, scores, NEG_BIG)
    prob_f = jnp.where(visible, jnp.exp(scores - lse_all[:, :, 0:block_rows, None]), 0.0)
    prob_rows = prob_f.astype(jnp.bfloat16)
    grad_value = mix("grqk,qgrd->kgd", prob_rows, grad_heads)
    grad_probs = mix("qgrd,kgd->grqk", grad_heads, value_rows)
    grad_scores = (prob_f * (grad_probs - row_delta[:, :, 0:block_rows, None])).astype(jnp.bfloat16)
    pieces = mix("grqk,kgd->qgrd", grad_scores, key_rot) * inv_root
    grad_key_rot = mix("grqk,qgrd->kgd", grad_scores, query_rot) * inv_root
    grad_query_rot = pieces.reshape(length, num_heads, head_dim)
    grad_query, grad_qgain = head_norm_back(
        unrotate(grad_query_rot, cosine, sine_table), query_hat, query_factor, query_gain
    )
    grad_key, grad_kgain = head_norm_back(
        unrotate(grad_key_rot, cosine, sine_table), key_hat, key_factor, key_gain
    )
    query_b = grad_query.astype(jnp.bfloat16).reshape(length, -1)
    key_b = grad_key.astype(jnp.bfloat16).reshape(length, -1)
    value_b = grad_value.astype(jnp.bfloat16).reshape(length, -1)
    grad_rows = (
        jnp.dot(query_b, wq_full.T, preferred_element_type=jnp.float32)
        + jnp.dot(key_b, wk_full.T, preferred_element_type=jnp.float32)
        + jnp.dot(value_b, wv_full.T, preferred_element_type=jnp.float32)
    )
    grad_wq = jnp.dot(rows.T, query_b, preferred_element_type=jnp.float32)
    grad_wk = jnp.dot(rows.T, key_b, preferred_element_type=jnp.float32)
    grad_wv = jnp.dot(rows.T, value_b, preferred_element_type=jnp.float32)
    return (grad_rows, grad_wq, grad_wk, grad_wv, grad_wo, grad_qgain, grad_kgain)


def expert_forward(expert_rows, wgate, wup, wdown):
    gate_pre = jnp.dot(expert_rows, wgate, preferred_element_type=jnp.float32)
    up_pre = jnp.dot(expert_rows, wup, preferred_element_type=jnp.float32)
    hidden_units = (jax.nn.silu(gate_pre) * up_pre).astype(jnp.bfloat16)
    result = jnp.dot(hidden_units, wdown, preferred_element_type=jnp.float32).astype(jnp.bfloat16)
    return (result, gate_pre, up_pre, hidden_units)


def expert_backward(expert_rows, grad_result, wgate, wup, wdown, gate_pre, up_pre, hidden_units):
    grad_hidden = jnp.dot(grad_result, wdown.T, preferred_element_type=jnp.float32)
    sigma = jax.nn.sigmoid(gate_pre)
    grad_gate_pre = (grad_hidden * up_pre * sigma * (1.0 + gate_pre * (1.0 - sigma))).astype(
        jnp.bfloat16
    )
    grad_up_pre = (grad_hidden * gate_pre * sigma).astype(jnp.bfloat16)
    grad_rows = (
        jnp.dot(grad_gate_pre, wgate.T, preferred_element_type=jnp.float32)
        + jnp.dot(grad_up_pre, wup.T, preferred_element_type=jnp.float32)
    ).astype(jnp.bfloat16)
    grad_wd = jnp.dot(hidden_units.T, grad_result, preferred_element_type=jnp.float32)
    grad_wg = jnp.dot(expert_rows.T, grad_gate_pre, preferred_element_type=jnp.float32)
    grad_wu = jnp.dot(expert_rows.T, grad_up_pre, preferred_element_type=jnp.float32)
    return (grad_rows, grad_wg, grad_wu, grad_wd)


def to_experts(buffer):
    return lax.all_to_all(buffer, ("dp", "tensor"), split_axis=0, concat_axis=0, tiled=True)


def to_sources(buffer):
    return lax.all_to_all(buffer, ("dp", "tensor"), split_axis=0, concat_axis=0, tiled=True)


def shards(
    hidden_in,
    segments,
    routes,
    query_weight,
    key_weight,
    value_weight,
    output_weight,
    gain_attn,
    gain_moe,
    query_gain,
    key_gain,
    router,
    gate_weight,
    up_weight,
    down_weight,
    cotangent,
):
    seg_ids = segments[0]
    rows_dev = hidden_in.shape[0]
    width = hidden_in.shape[1]
    top_count = routes.shape[1]
    experts = router.shape[1]
    capacity = 2 * rows_dev * top_count // experts
    full_query, full_key, full_value, full_output = (
        lax.all_gather(query_weight, "dp", axis=0, tiled=True),
        lax.all_gather(key_weight, "dp", axis=0, tiled=True),
        lax.all_gather(value_weight, "dp", axis=0, tiled=True),
        lax.all_gather(output_weight, "dp", axis=1, tiled=True),
    )
    inputs32 = hidden_in.astype(jnp.float32)
    factor_one = rms_scale(inputs32)
    normed_one = inputs32 * factor_one
    rows_one = (normed_one * gain_attn).astype(jnp.bfloat16)
    group_rows = lax.all_gather(rows_one, "tensor", axis=0, tiled=True)
    saved = attn_forward(
        group_rows, seg_ids, full_query, full_key, full_value, query_gain, key_gain
    )
    partial_add = jnp.dot(saved[0], full_output, preferred_element_type=jnp.float32)
    attn_add = lax.psum_scatter(partial_add, "tensor", scatter_dimension=0, tiled=True)
    residual = inputs32 + attn_add
    factor_two = rms_scale(residual)
    normed_two = residual * factor_two
    rows_two = (normed_two * gain_moe).astype(jnp.bfloat16)
    router_probs = softmax_rows(jnp.dot(rows_two, router, preferred_element_type=jnp.float32))
    route_hot = (routes[:, :, None] == jnp.arange(experts, dtype=jnp.int32)[None, None, :]).astype(
        jnp.float32
    )
    picked = jnp.sum(route_hot * router_probs[:, None, :], axis=-1)
    total = jnp.sum(picked, axis=1, keepdims=True)
    gates = picked / total
    flat_routes = routes.reshape(-1)
    onehot = (flat_routes[:, None] == jnp.arange(experts, dtype=jnp.int32)[None, :]).astype(
        jnp.int32
    )
    ranks = jnp.sum(onehot * jnp.cumsum(onehot, axis=0), axis=1) - 1
    slots = flat_routes * capacity + ranks
    send_rows = (
        jnp.zeros((experts * capacity, width), jnp.bfloat16)
        .at[slots]
        .set(jnp.repeat(rows_two, top_count, axis=0))
    )
    received = to_experts(send_rows.reshape(experts, capacity, width)).reshape(-1, width)
    result, gate_pre, up_pre, hidden_units = expert_forward(
        received, gate_weight[0], up_weight[0], down_weight[0]
    )
    returned = to_sources(result.reshape(-1, capacity, width)).reshape(experts * capacity, width)
    pair_out = returned[slots].astype(jnp.float32).reshape(rows_dev, top_count, width)
    moe_sum = jnp.sum(gates[:, :, None] * pair_out, axis=1)
    output = (residual + moe_sum).astype(jnp.bfloat16)
    cot32 = cotangent.astype(jnp.float32)
    grad_gates = jnp.sum(cot32[:, None, :] * pair_out, axis=-1)
    grad_result = (gates[:, :, None] * cot32[:, None, :]).astype(jnp.bfloat16).reshape(-1, width)
    send_grads = jnp.zeros((experts * capacity, width), jnp.bfloat16).at[slots].set(grad_result)
    received_grads = to_experts(send_grads.reshape(experts, capacity, width)).reshape(-1, width)
    grad_expert_rows, grad_wg, grad_wu, grad_wd = expert_backward(
        received,
        received_grads,
        gate_weight[0],
        up_weight[0],
        down_weight[0],
        gate_pre,
        up_pre,
        hidden_units,
    )
    returned_grads = to_sources(grad_expert_rows.reshape(-1, capacity, width)).reshape(
        experts * capacity, width
    )
    grad_pairs = returned_grads[slots].astype(jnp.float32).reshape(rows_dev, top_count, width)
    grad_picked = (grad_gates - jnp.sum(gates * grad_gates, axis=1, keepdims=True)) / total
    grad_probs = jnp.sum(route_hot * grad_picked[:, :, None], axis=1)
    grad_logits = (
        router_probs * (grad_probs - jnp.sum(grad_probs * router_probs, axis=-1, keepdims=True))
    ).astype(jnp.bfloat16)
    grad_router = jnp.dot(rows_two.T, grad_logits, preferred_element_type=jnp.float32)
    grad_rows_two = jnp.sum(grad_pairs, axis=1) + jnp.dot(
        grad_logits, router.T, preferred_element_type=jnp.float32
    )
    grad_res_norm, grad_gain_moe = row_norm_back(grad_rows_two, normed_two, factor_two, gain_moe)
    grad_residual = cot32 + grad_res_norm
    grad_attn = grad_residual.astype(jnp.bfloat16)
    group_grads = lax.all_gather(grad_attn, "tensor", axis=0, tiled=True)
    back_query, back_key, back_value, back_output = (
        lax.all_gather(query_weight, "dp", axis=0, tiled=True),
        lax.all_gather(key_weight, "dp", axis=0, tiled=True),
        lax.all_gather(value_weight, "dp", axis=0, tiled=True),
        lax.all_gather(output_weight, "dp", axis=1, tiled=True),
    )
    grad_group_rows, grad_wq, grad_wk, grad_wv, grad_wo, grad_qgain, grad_kgain = attn_backward(
        group_grads,
        group_rows,
        seg_ids,
        back_query,
        back_key,
        back_value,
        back_output,
        query_gain,
        key_gain,
        saved,
    )
    grad_rows_one = lax.psum_scatter(
        grad_group_rows.astype(jnp.bfloat16), "tensor", scatter_dimension=0, tiled=True
    ).astype(jnp.float32)
    grad_in_norm, grad_gain_attn = row_norm_back(grad_rows_one, normed_one, factor_one, gain_attn)
    grad_input = grad_residual + grad_in_norm
    grad_wq, grad_wk, grad_wv, grad_wo = (
        lax.psum_scatter(
            grad_wq.astype(jnp.bfloat16), "dp", scatter_dimension=0, tiled=True
        ).astype(jnp.float32),
        lax.psum_scatter(
            grad_wk.astype(jnp.bfloat16), "dp", scatter_dimension=0, tiled=True
        ).astype(jnp.float32),
        lax.psum_scatter(
            grad_wv.astype(jnp.bfloat16), "dp", scatter_dimension=0, tiled=True
        ).astype(jnp.float32),
        lax.psum_scatter(
            grad_wo.astype(jnp.bfloat16), "dp", scatter_dimension=1, tiled=True
        ).astype(jnp.float32),
    )
    grad_gain_attn, grad_gain_moe, grad_qgain, grad_kgain, grad_router = lax.psum(
        (grad_gain_attn, grad_gain_moe, grad_qgain, grad_kgain, grad_router), ("dp", "tensor")
    )
    return (
        output,
        grad_input,
        grad_wq,
        grad_wk,
        grad_wv,
        grad_wo,
        grad_gain_attn,
        grad_gain_moe,
        grad_qgain,
        grad_kgain,
        grad_router,
        grad_wg[None],
        grad_wu[None],
        grad_wd[None],
    )


AXES = ("dp", "tensor")


def gathered(
    hidden_in,
    segments,
    routes,
    query_weight,
    key_weight,
    value_weight,
    output_weight,
    gain_attn,
    gain_moe,
    query_gain,
    key_gain,
    router,
    gate_weight,
    up_weight,
    down_weight,
    cotangent,
):
    seg_ids = segments[0]
    rows_dev, width = hidden_in.shape
    top_count = routes.shape[1]
    expert_count = router.shape[1]
    capacity = 2 * rows_dev * top_count // expert_count
    length = lax.axis_size("tensor")
    query_cols, key_cols = query_weight.shape[1], key_weight.shape[1]

    inputs32 = hidden_in.astype(jnp.float32)
    factor_one = rms_scale(inputs32)
    normed_one = inputs32 * factor_one
    rows_one = (normed_one * gain_attn).astype(jnp.bfloat16)
    joint_weight = jnp.concatenate([query_weight, key_weight, value_weight], axis=1)
    cosine, sine_table = rope_tables(seg_ids, query_gain.shape[0])
    turns = (
        seg_ids[:, None],
        seg_ids[None, :],
        jnp.concatenate([cosine, cosine], axis=1),
        jnp.concatenate([-sine_table, sine_table], axis=1),
        query_gain[None, :],
        key_gain[None, :],
    )
    attn_add, group_rows, full_joint, full_output, all_cots, projected, attn_heads = attend(
        rows_one, joint_weight, output_weight, cotangent, *turns, length, 0
    )
    residual = inputs32 + attn_add
    factor_two = rms_scale(residual)
    normed_two = residual * factor_two
    rows_two = (normed_two * gain_moe).astype(jnp.bfloat16)
    router_probs = softmax_rows(jnp.dot(rows_two, router, preferred_element_type=jnp.float32))
    route_hot = (routes[:, :, None] == jnp.arange(expert_count, dtype=jnp.int32)[None, None, :]).astype(
        jnp.float32
    )
    picked = jnp.sum(route_hot * router_probs[:, None, :], axis=-1)
    total = jnp.sum(picked, axis=1, keepdims=True)
    gates = picked / total
    named = jnp.sum(route_hot, axis=1)
    gate_table = jnp.where(named > 0.5, jnp.sum(route_hot * gates[:, :, None], axis=1), -1.0)
    all_rows, partial_out, partial_rows, token_grads, grad_wg, grad_wu, grad_wd = experts(
        rows_two,
        all_cots,
        gate_table.T,
        gate_weight[0],
        up_weight[0],
        down_weight[0],
        length,
        capacity,
        1,
    )
    back_grads = token_grads[:, 0, :]
    cot32 = cotangent.astype(jnp.float32)
    grad_gates = jnp.sum(route_hot * back_grads.T[:, None, :], axis=-1)
    grad_picked = (grad_gates - jnp.sum(gates * grad_gates, axis=1, keepdims=True)) / total
    grad_probs = jnp.sum(route_hot * grad_picked[:, :, None], axis=1)
    grad_logits = (
        router_probs * (grad_probs - jnp.sum(grad_probs * router_probs, axis=-1, keepdims=True))
    ).astype(jnp.bfloat16)
    grad_sum, all_logits = reduce_rows(partial_rows, grad_logits.T, length, 2)
    grad_router = mix("btd,bet->de", all_rows, all_logits)
    grad_rows_two = grad_sum + jnp.dot(grad_logits, router.T, preferred_element_type=jnp.float32)
    grad_res_norm, grad_gain_moe = row_norm_back(grad_rows_two, normed_two, factor_two, gain_moe)
    grad_residual = cot32 + grad_res_norm
    grad_attn = grad_residual.astype(jnp.bfloat16)
    grad_rows_one, grad_joint, grad_wo, moe_sum, grad_qgain, grad_kgain = attend_back(
        grad_attn,
        group_rows,
        full_joint,
        full_output,
        projected,
        attn_heads,
        partial_out,
        *turns,
        length,
        3,
    )
    output = (residual + moe_sum).astype(jnp.bfloat16)
    grad_in_norm, grad_gain_attn = row_norm_back(grad_rows_one, normed_one, factor_one, gain_attn)
    grad_input = grad_residual + grad_in_norm
    small = jnp.concatenate([grad_gain_attn, grad_gain_moe, grad_qgain[0], grad_kgain[0]]).reshape(-1, 128)
    small = jnp.pad(small, ((0, -small.shape[0] % 16), (0, 0)))
    (all_small,) = gather([(small, "all", False)], length, 4, "gather_small")
    sums = jnp.sum(all_small, axis=0).reshape(-1)
    head_dim = query_gain.shape[0]
    return (
        output,
        grad_input,
        grad_joint[:, :query_cols],
        grad_joint[:, query_cols : query_cols + key_cols],
        grad_joint[:, query_cols + key_cols :],
        grad_wo,
        sums[:width],
        sums[width : 2 * width],
        sums[2 * width : 2 * width + head_dim],
        sums[2 * width + head_dim : 2 * width + 2 * head_dim],
        grad_router,
        grad_wg[None],
        grad_wu[None],
        grad_wd[None],
    )


def solution(mesh):
    placed = (
        P(("dp", "tensor"), None),
        P("dp", None),
        P(("dp", "tensor"), None),
        P("dp", "tensor"),
        P("dp", "tensor"),
        P("dp", "tensor"),
        P("tensor", "dp"),
        P(),
        P(),
        P(),
        P(),
        P(),
        P(("dp", "tensor"), None, None),
        P(("dp", "tensor"), None, None),
        P(("dp", "tensor"), None, None),
        P(("dp", "tensor"), None),
    )
    program = gathered if mesh.shape["dp"] == 8 and mesh.shape["tensor"] <= 4 else shards
    return jax.shard_map(
        program,
        mesh=mesh,
        in_specs=placed,
        out_specs=(
            P(("dp", "tensor"), None),
            P(("dp", "tensor"), None),
            P("dp", "tensor"),
            P("dp", "tensor"),
            P("dp", "tensor"),
            P("tensor", "dp"),
            P(),
            P(),
            P(),
            P(),
            P(),
            P(("dp", "tensor"), None, None),
            P(("dp", "tensor"), None, None),
            P(("dp", "tensor"), None, None),
        ),
        check_vma=False,
    )
```

```python
import math

import jax
import jax.numpy as jnp
from jax import lax
from jax.experimental import pallas as pl
from jax.experimental.pallas import tpu as pltpu
from jax.sharding import PartitionSpec as P

EPSILON = 1e-06
THETA_BASE = 1000000.0
NEG_BIG = -1e30


MESH = pl.DeviceIdType.MESH


class Place:
    def __init__(self, length):
        self.length = length
        self.dp = lax.axis_index("dp")
        self.z = lax.axis_index("tensor")
        core, along_x, along_y = self.dp % 2, (self.dp // 2) % 2, self.dp // 4
        self.to_core = 1 - 2 * core
        self.core = self.dp + self.to_core
        self.x = self.dp + 2 - 4 * along_x
        self.y = self.dp + 4 - 8 * along_y
        self.columns = (self.dp, self.x, self.y, self.x + self.y - self.dp)

    def device(self, kind):
        if kind == "x":
            return (self.x, self.z)
        if kind == "y":
            return (self.y, self.z)
        if kind == "core":
            return (self.core, self.z)
        if kind == "up":
            return (self.dp, self.z + 1)
        return (self.dp, self.z - 1)

    @property
    def has_up(self):
        return self.z < self.length - 1

    @property
    def has_down(self):
        return self.z > 0

    def condition(self, kind):
        if kind == "up":
            return self.has_up
        return self.has_down if kind == "down" else None

    def nearest(self, turn):
        length = self.length

        def equal(left, right):
            far = 2 * length
            return (left - right + far) // far - (left - right - 1 + far) // far

        found = 0
        for mine in range(length):
            order = sorted(range(length), key=lambda other: (abs(other - mine), other))
            for step, other in enumerate(order):
                if other:
                    found = found + equal(self.z, mine) * equal(turn, step) * other
        return found

    def target(self, turn):
        length, z = self.length, self.z

        def at_least(left, right):
            return (left - right + 2 * length) // (2 * length)

        high = at_least(z, length // 2)
        mirrored = z + high * (length - 1 - 2 * z)
        above = length - 1 - mirrored
        first = at_least(above - 1, turn)
        if turn == length - 1:
            return z
        found = first * (length - 1 - turn) + (1 - first) * (turn - above)
        return found + high * (length - 1 - 2 * found)


def piece(rows, h):
    return pl.ds(0, rows) if h is None else pl.ds(h * (rows // 2), rows // 2)


def guarded(condition, action):
    if condition is None:
        action()
    else:
        pl.when(condition)(action)


def meet(place, over_z, over_dp):
    barrier = pltpu.get_barrier_semaphore()
    kinds = (("x", "y", "core") if over_dp else ()) + (("up", "down") if over_z else ())
    for kind in kinds:

        def greet(kind=kind):
            pl.semaphore_signal(
                barrier, 1, device_id=place.device(kind), device_id_type=MESH
            )

        guarded(place.condition(kind), greet)
    count = 3 if over_dp else 0
    if over_z:
        length = place.length
        count = count + (place.z + length - 1) // length + (2 * length - 2 - place.z) // length
    pl.semaphore_wait(barrier, count)


def other_device(place, distance):
    there = lax.rem(place.dp * place.length + place.z + distance, 8 * place.length)
    return (there // place.length, lax.rem(there, place.length)), there


def meet_all(place):
    barrier = pltpu.get_barrier_semaphore()
    others = 8 * place.length - 1

    def greet(n, carry):
        device, _ = other_device(place, n + 1)
        pl.semaphore_signal(barrier, 1, device_id=device, device_id_type=MESH)
        return carry

    lax.fori_loop(0, others, greet, 0)
    pl.semaphore_wait(barrier, others)


class Sends:
    def __init__(self, place):
        self.place = place
        self.started = []

    def start(self, kind, views, condition=lambda: None):
        def build():
            source, target, send_sem, recv_sem = views()
            return pltpu.make_async_remote_copy(
                src_ref=source,
                dst_ref=target,
                send_sem=send_sem,
                recv_sem=recv_sem,
                device_id=self.place.device(kind),
                device_id_type=MESH,
            )

        guarded(self.place.condition(kind), lambda: build().start())
        self.started.append((condition, kind, build))

    def drain(self):
        for condition, kind, build in self.started:

            def finish(kind=kind, build=build):
                guarded(self.place.condition(kind), lambda: build().wait_send())

            guarded(condition(), finish)


class GatherItem:
    def __init__(self, mode, place, own, slot, recv, send, local):
        self.mode, self.place = mode, place
        self.own, self.slot = own, slot
        self.recv, self.send, self.local = recv, send, local
        self.over_z = mode != "dp"
        self.over_dp = mode != "z"
        self.length = place.length if self.over_z else 1
        self.z = place.z if self.over_z else 0

    def index(self, column, z):
        if self.mode == "all":
            return column * self.length + z
        return column if self.mode == "dp" else z

    @staticmethod
    def semaphores(mode, length):
        blocks = {"all": 8 * length, "dp": 8, "z": length}[mode]
        turns = 2 * length - 1 if mode != "dp" else 1
        return [
            pltpu.SemaphoreType.DMA((blocks, 2)),
            pltpu.SemaphoreType.DMA((10, turns, 2)),
            pltpu.SemaphoreType.DMA((2,)),
        ]

    def turns(self, distance):
        if distance == 0:
            return [(0, 0, lambda: None, None)]
        place, length = self.place, self.length
        return [
            (2 * distance - 1, -distance, lambda: place.z >= distance, "up"),
            (2 * distance, distance, lambda: place.z < length - distance, "down"),
        ]

    def pass_on(self, sends, lane, kind, column, offset, turn, h, source=None, condition=lambda: None):
        at = 0 if h is None else h

        def views():
            z = self.z + offset
            view = self.slot(column, z, h)
            return (
                view if source is None else source(h),
                view,
                self.send.at[lane, turn, at],
                self.recv.at[self.index(column, z), at],
            )

        sends.start(kind, views, condition)

    def arrived(self, column, z, h):
        view = self.slot(column, z, h)
        at = 0 if h is None else h
        pltpu.make_async_copy(view, view, self.recv.at[self.index(column, z), at]).wait()

    def local_copy(self):
        return pltpu.make_async_copy(
            self.own(None), self.slot(self.place.dp, self.z, None), self.local.at[0]
        )

    def begin(self, sends):
        place = self.place
        if self.over_z:
            self.pass_on(sends, 0, "up", place.dp, 0, 0, None, self.own)
            self.pass_on(sends, 1, "down", place.dp, 0, 0, None, self.own)
        if self.over_dp:
            self.pass_on(sends, 2, "x", place.dp, 0, 0, None, self.own)
            self.pass_on(sends, 3, "y", place.dp, 0, 0, None, self.own)
            self.pass_on(sends, 4, "core", place.dp, 0, 0, None, self.own)
        self.local_copy().start()

    def along_z(self, sends, distance):
        if not self.over_z or distance >= self.length:
            return
        place = self.place
        for turn, offset, condition, onward in self.turns(distance):

            def step(turn=turn, offset=offset, condition=condition, onward=onward):
                self.arrived(place.dp, self.z + offset, None)
                lanes = []
                if distance < self.length - 1:
                    lanes.append((0 if onward == "up" else 1, onward))
                if self.over_dp:
                    lanes += [(2, "x"), (3, "y"), (4, "core")]
                for lane, kind in lanes:
                    self.pass_on(
                        sends, lane, kind, place.dp, offset, turn, None, condition=condition
                    )

            guarded(condition(), step)

    def across(self, sends, distance):
        if not self.over_dp or not 0 <= distance < self.length:
            return
        _, x, y, _ = self.place.columns
        for turn, offset, condition, _ in self.turns(distance):

            def step(turn=turn, offset=offset, condition=condition):
                self.arrived(x, self.z + offset, None)
                self.pass_on(sends, 5, "y", x, offset, turn, 0, condition=condition)
                self.pass_on(sends, 7, "core", x, offset, turn, None, condition=condition)
                self.arrived(y, self.z + offset, None)
                self.pass_on(sends, 6, "x", y, offset, turn, 1, condition=condition)
                self.pass_on(sends, 8, "core", y, offset, turn, None, condition=condition)

            guarded(condition(), step)

    def diagonal(self, sends, distance):
        if not self.over_dp or not 0 <= distance < self.length:
            return
        corner = self.place.columns[3]
        for turn, offset, condition, _ in self.turns(distance):

            def step(turn=turn, offset=offset, condition=condition):
                for h in range(2):
                    self.arrived(corner, self.z + offset, h)
                    self.pass_on(sends, 9, "core", corner, offset, turn, h, condition=condition)

            guarded(condition(), step)

    def settled(self):
        self.local_copy().wait()

    def from_core(self, z):
        for number, column in enumerate(self.place.columns):
            for h in (0, 1) if number == 3 else (None,):
                self.arrived(column + self.place.to_core, z, h)

    def finish(self):
        self.settled()
        if self.over_dp:
            for z in range(self.length):
                self.from_core(z)


class ReduceItem:
    def __init__(self, mode, place, block, bufs, out):
        self.mode, self.place, self.block, self.out = mode, place, block, out
        self.over_z = mode != "dp"
        self.over_dp = mode != "z"
        self.length = place.length if self.over_z else 1
        (self.acc, self.from_core, self.corner, self.from_xy, self.from_z,
         self.load, self.send, self.recv) = bufs

    @staticmethod
    def scratch(mode, length, rows, width, in_place=False):
        t = length if mode != "dp" else 1
        columns = 4 if mode != "z" else 1
        dp = mode != "z"
        small = (8, 128)
        return [
            pltpu.VMEM(small if in_place else (columns, t, rows, width), jnp.bfloat16),
            pltpu.VMEM((columns, t, rows, width) if dp else small, jnp.bfloat16),
            pltpu.VMEM((2, t, rows // 2, width) if dp else small, jnp.bfloat16),
            pltpu.VMEM((2, t, rows, width) if dp else small, jnp.bfloat16),
            pltpu.VMEM((t + 1, rows, width) if mode != "dp" else small, jnp.bfloat16),
            pltpu.SemaphoreType.DMA((columns, t)),
            pltpu.SemaphoreType.DMA((10, t, 2)),
            pltpu.SemaphoreType.DMA((9, t + 1, 2)),
        ]

    def z_of(self, turn):
        return self.place.target(turn) if self.over_z else 0

    def got(self, ref, lane, turn, h=0):
        pltpu.make_async_copy(ref, ref, self.recv.at[lane, turn, h]).wait()

    computed = False
    in_place = False

    def partial(self, column, turn, h):
        if self.in_place:
            return self.block(self.place.columns[column], self.z_of(turn), h)
        return self.acc.at[column, turn, piece(self.acc.shape[2], h)]

    def add(self, target, refs, out=None):
        rows = target.shape[0]
        step = 16 if rows % 16 == 0 else rows
        place = target if out is None else out

        def body(i, carry):
            at = pl.ds(pl.multiple_of(i * step, step), step)
            total = target[at, :].astype(jnp.float32)
            for ref in refs:
                total = total + ref[at, :].astype(jnp.float32)
            place[at, :] = total.astype(place.dtype)
            return carry

        lax.fori_loop(0, rows // step, body, 0, unroll=2 if (rows // step) % 2 == 0 else 1)

    def begin(self):
        place = self.place
        if self.over_z:

            @pl.when((place.z == 0) | (place.z == self.length - 1))
            def _():
                def clear(i, carry):
                    self.from_z[i] = jnp.zeros(self.from_z.shape[1:], jnp.bfloat16)
                    return carry

                lax.fori_loop(0, self.length + 1, clear, 0)

    def load_all(self):
        place = self.place
        for turn in range(self.length):
            for column in (3, 1, 2, 0) if self.over_dp else (0,):
                pltpu.make_async_copy(
                    self.block(place.columns[column], self.z_of(turn), None),
                    self.acc.at[column, turn],
                    self.load.at[column, turn],
                ).start()

    def hand_over(self, sends, turn):
        if not self.over_dp or turn >= self.length:
            return
        place = self.place
        for column in (3, 1, 2, 0):
            sends.start(
                "core",
                lambda column=column: (
                    self.block(place.columns[column] + place.to_core, self.z_of(turn), None),
                    self.from_core.at[column, turn],
                    self.send.at[column, turn, 0],
                    self.recv.at[column, turn, 0],
                ),
            )

    def ready(self, column, turn):
        if not (self.computed or self.in_place):
            ref = self.acc.at[column, turn]
            pltpu.make_async_copy(ref, ref, self.load.at[column, turn]).wait()
        if self.over_dp:
            self.got(self.from_core.at[column, turn], column, turn)

    def settle(self, column, turn, h, extra=(), out=None):
        refs = list(extra)
        if self.over_dp:
            rows = self.from_core.shape[2]
            refs.append(self.from_core.at[column, turn, piece(rows, h)])
        if refs or out is not None:
            self.add(self.partial(column, turn, h), refs, out)

    def corners(self, sends, turn):
        if not self.over_dp or not 0 <= turn < self.length:
            return
        self.ready(3, turn)
        for h, kind in ((0, "y"), (1, "x")):
            self.settle(3, turn, h)
            sends.start(
                kind,
                lambda h=h: (
                    self.partial(3, turn, h),
                    self.corner.at[h, turn],
                    self.send.at[4, turn, h],
                    self.recv.at[4, turn, h],
                ),
            )

    def straight(self, sends, turn, second):
        if not self.over_dp or not 0 <= turn < self.length:
            return
        rows = self.from_xy.shape[2]
        for column, kind in ((1, "x"), (2, "y")):
            h = (column - 1) if second else (2 - column)
            extra = ()
            if second:
                ref = self.corner.at[h, turn]
                self.got(ref, 4, turn, h)
                extra = (ref,)
            else:
                self.ready(column, turn)
            self.settle(column, turn, h, extra)
            sends.start(
                kind,
                lambda column=column, h=h: (
                    self.partial(column, turn, h),
                    self.from_xy.at[column - 1, turn, piece(rows, h)],
                    self.send.at[4 + column, turn, h],
                    self.recv.at[4 + column, turn, h],
                ),
            )

    def home(self, sends, turn):
        if not 0 <= turn < self.length:
            return
        place = self.place
        last = turn == self.length - 1
        z = self.z_of(turn)
        extra = []
        self.ready(0, turn)
        if self.over_dp:
            for lane in (0, 1):
                rows = self.from_xy.shape[2]
                for h in range(2):
                    self.got(self.from_xy.at[lane, turn, piece(rows, h)], 5 + lane, turn, h)
                extra.append(self.from_xy.at[lane, turn])
        if self.over_z:

            def got_slot():
                self.got(self.from_z.at[z], 7, z)

            def got_other():
                self.got(self.from_z.at[self.length], 7, self.length)

            extra.append(self.from_z.at[z])
            if last:
                guarded(place.has_down, got_slot)
                guarded(place.has_up, got_other)
                extra.append(self.from_z.at[self.length])
            else:
                guarded((z > place.z) & place.has_down, got_slot)
                guarded((z < place.z) & place.has_up, got_slot)
        self.settle(0, turn, None, extra, self.out(None) if last else None)
        if self.over_z and not last:

            def going_up():
                goal = self.z_of(turn)
                return (
                    self.partial(0, turn, None),
                    self.from_z.at[goal],
                    self.send.at[7, turn, 0],
                    self.recv.at[7, goal, 0],
                )

            def going_down():
                there = self.z_of(turn)
                arrives = (there - place.z + 1 + self.length) // self.length
                goal = there + arrives * (self.length - there)
                return (
                    self.partial(0, turn, None),
                    self.from_z.at[goal],
                    self.send.at[7, turn, 0],
                    self.recv.at[7, goal, 0],
                )

            def above():
                return self.z_of(turn) > place.z

            def below():
                return self.z_of(turn) < place.z

            pl.when(above())(lambda: sends.start("up", going_up, above))
            pl.when(below())(lambda: sends.start("down", going_down, below))


def advance(item, sends, step):
    item.corners(sends, step)
    item.straight(sends, step, False)
    item.hand_over(sends, step + 2)
    item.straight(sends, step - 1, True)
    item.home(sends, step - 2 if item.over_dp else step)


def reduce_rows(partials, small, picked, gated, hid, dgate, dup, length, collective_id):
    devices, rows, width = partials.shape
    slots, hidden = dup.shape
    half, low = rows // 2, small.shape[0] // 2
    tile, narrow = width // 4, hidden // 3
    f32, bf16 = jnp.float32, jnp.bfloat16

    def kernel(
        source, small_ref, picked_ref, gated_ref, hid_ref, dgate_ref, dup_ref,
        target, small_all, out_g, out_u, out_d,
        hid_v, dgate_v, dup_v, picked_v, gated_v, tile_g, tile_u, tile_d, load_sem, tile_sem, store_sem,
        *rest,
    ):
        place = Place(length)
        item = ReduceItem(
            "all",
            place,
            lambda c, z, h: source.at[c * length + z, piece(2 * half, h)],
            rest[:8],
            lambda h: target.at[piece(2 * half, h)],
        )
        beside = GatherItem("all", place, None, None, *rest[8:])
        beside.own = lambda h: small_ref.at[piece(2 * low, h)]
        beside.slot = lambda c, z, h: small_all.at[c * length + z, piece(2 * low, h)]
        item.begin()
        meet(place, True, True)
        sends = Sends(place)
        beside.begin(sends)
        item.load_all()
        item.hand_over(sends, 0)
        item.hand_over(sends, 1)
        resident = [
            pltpu.make_async_copy(left, right, load_sem.at[n])
            for n, (left, right) in enumerate(
                ((hid_ref, hid_v), (dgate_ref, dgate_v), (dup_ref, dup_v))
            )
        ]
        for copy in resident:
            copy.start()

        def lanes_of(n):
            return pl.ds(pl.multiple_of(n * tile, tile), tile)

        def tiles(n, slot):
            return [
                pltpu.make_async_copy(picked_ref.at[:, lanes_of(n)], picked_v.at[slot], tile_sem.at[slot, 0]),
                pltpu.make_async_copy(gated_ref.at[:, lanes_of(n)], gated_v.at[slot], tile_sem.at[slot, 1]),
            ]

        def stores(n, slot):
            return [
                pltpu.make_async_copy(tile_g.at[slot], out_g.at[lanes_of(n)], store_sem.at[slot, 0]),
                pltpu.make_async_copy(tile_u.at[slot], out_u.at[lanes_of(n)], store_sem.at[slot, 1]),
                pltpu.make_async_copy(tile_d.at[slot], out_d.at[:, lanes_of(n)], store_sem.at[slot, 2]),
            ]

        for copy in tiles(0, 0):
            copy.start()

        def narrow_of(m):
            return pl.ds(pl.multiple_of(m * narrow, narrow), narrow)

        def turn_of(i, carry):
            for step in range(length + 2):

                @pl.when(i == 2 * step)
                def _(step=step):
                    item.corners(sends, step)
                    item.straight(sends, step, False)
                    item.hand_over(sends, step + 2)
                    beside.along_z(sends, step + 1)
                    beside.across(sends, step)

                @pl.when(i == 2 * step + 1)
                def _(step=step):
                    item.straight(sends, step - 1, True)
                    item.home(sends, step - 2)
                    beside.diagonal(sends, step)

            n, kind = i // 3, i % 3
            slot = n % 2

            @pl.when(i == 0)
            def _():
                for copy in resident:
                    copy.wait()

            @pl.when((kind == 0) & (n < 4))
            def _():
                for copy in tiles(n, slot):
                    copy.wait()

                @pl.when(n < 3)
                def _():
                    for copy in tiles(n + 1, 1 - slot):
                        copy.start()

                @pl.when(n >= 2)
                def _():
                    for copy in stores(n, slot):
                        copy.wait()

                def body(m, carry):
                    tile_g[slot, :, narrow_of(m)] = dot(picked_v[slot], dgate_v[:, narrow_of(m)], 0, 0)
                    return carry

                lax.fori_loop(0, 3, body, 0)
                stores(n, slot)[0].start()

            @pl.when((kind == 1) & (n < 4))
            def _():
                def body(m, carry):
                    tile_u[slot, :, narrow_of(m)] = dot(picked_v[slot], dup_v[:, narrow_of(m)], 0, 0)
                    return carry

                lax.fori_loop(0, 3, body, 0)
                stores(n, slot)[1].start()

            @pl.when((kind == 2) & (n < 4))
            def _():
                def body(m, carry):
                    tile_d[slot, narrow_of(m), :] = dot(hid_v[:, narrow_of(m)], gated_v[slot], 0, 0)
                    return carry

                lax.fori_loop(0, 3, body, 0)
                stores(n, slot)[2].start()

            return carry

        lax.fori_loop(0, max(12, 2 * (length + 2)), turn_of, 0)
        beside.finish()
        for slot in range(2):
            for copy in stores(slot, slot):
                copy.wait()
        sends.drain()

    any_spec = pl.BlockSpec(memory_space=pl.ANY)
    shape = jax.ShapeDtypeStruct
    sems = pltpu.SemaphoreType.DMA
    return pl.pallas_call(
        kernel,
        name="reduce_rows",
        out_shape=[
            shape((rows, width), f32),
            shape((devices,) + small.shape, small.dtype),
            shape((width, hidden), f32),
            shape((width, hidden), f32),
            shape((hidden, width), f32),
        ],
        in_specs=[any_spec] * 7,
        out_specs=[pl.BlockSpec(memory_space=pltpu.VMEM)] + [any_spec] * 4,
        scratch_shapes=[
            pltpu.VMEM((slots, hidden), bf16),
            pltpu.VMEM((slots, hidden), bf16),
            pltpu.VMEM((slots, hidden), bf16),
            pltpu.VMEM((2, slots, tile), bf16),
            pltpu.VMEM((2, slots, tile), bf16),
            pltpu.VMEM((2, tile, hidden), f32),
            pltpu.VMEM((2, tile, hidden), f32),
            pltpu.VMEM((2, hidden, tile), f32),
            sems((3,)),
            sems((2, 2)),
            sems((2, 3)),
        ]
        + ReduceItem.scratch("all", length, rows, width)
        + GatherItem.semaphores("all", length),
        compiler_params=pltpu.CompilerParams(
            collective_id=collective_id, has_side_effects=True, vmem_limit_bytes=67043328
        ),
    )(partials, small, picked, gated, hid, dgate, dup)


def dot(left, right, left_dim=1, right_dim=0):
    return lax.dot_general(
        left, right, (((left_dim,), (right_dim,)), ((), ())), preferred_element_type=jnp.float32
    )


def experts(rows_own, all_cots, gates_own, wgate, wup, wdown, length, capacity, collective_id):
    rows, width = rows_own.shape
    hidden = wgate.shape[1]
    devices = 8 * length
    count = 4 * capacity
    tile = 512 if width % 512 == 0 else width
    narrow = 256 if hidden % 256 == 0 else hidden
    f32, bf16 = jnp.float32, jnp.bfloat16

    def kernel(
        rows_ref, all_cots, gates_ref, wg_ref, wu_ref, wd_ref,
        all_rows, part_out, part_grad, token_in, picked_all, gated_all, hid_all, dgate_all, dup_all,
        wg, wu, wd, chosen_all, gates_all, rank_v, table, row_buf, cot_buf, picked, cotan, gated, hid, dgate, dup, scaled, back,
        chosen, slot_gate, slot_sum, stage_out, stage_grad, token_out,
        recv_r, send_r, local_r,
        load_sem, store_sem, save_sem, token_sem, gate_sem, weight_sem,
    ):
        place = Place(length)
        expert = place.dp * length + place.z

        def item_of(source, target, sems, half):
            item = GatherItem("all", place, None, None, *sems)
            item.own = lambda h: source.at[piece(2 * half, h)]
            item.slot = lambda column, z, h: target.at[
                column * length + z, piece(2 * half, h)
            ]
            return item

        big = [
            item_of(rows_ref, all_rows, (recv_r, send_r, local_r), rows // 2),
        ]
        items = big
        meet_all(place)
        sends = Sends(place)

        def gate_send(n):
            device, there = other_device(place, n + 1)
            return pltpu.make_async_remote_copy(
                src_ref=gates_ref.at[there],
                dst_ref=table.at[expert],
                send_sem=gate_sem.at[0],
                recv_sem=gate_sem.at[1],
                device_id=device,
                device_id_type=MESH,
            )

        def send_gates(n, carry):
            gate_send(n).start()
            return carry

        lax.fori_loop(0, devices - 1, send_gates, 0)
        pltpu.make_async_copy(gates_ref.at[expert], table.at[expert], gate_sem.at[1]).start()
        for item in items:
            item.begin(sends)

        weights = [
            pltpu.make_async_copy(source, target, weight_sem.at[n])
            for n, (source, target) in enumerate(((wg_ref, wg), (wu_ref, wu), (wd_ref, wd)))
        ]
        for copy in weights:
            copy.start()

        def along(distance):
            for item in items:
                item.along_z(sends, distance)

        def across(distance):
            for item in items:
                item.across(sends, distance)

        def corner(distance):
            for item in items:
                item.diagonal(sends, distance)

        along(1)
        pltpu.make_async_copy(table, table, gate_sem.at[1]).wait()
        order = lax.broadcasted_iota(jnp.int32, (rows, rows), 0)
        upto = (order <= lax.broadcasted_iota(jnp.int32, (rows, rows), 1)).astype(f32).astype(bf16)
        slots = lax.broadcasted_iota(jnp.int32, (capacity, rows), 0).astype(f32)
        lines = table[:, 0, :]
        rank_v[...] = dot((lines >= 0.0).astype(f32).astype(bf16), upto) - 1.0

        def choose(block, carry):
            line = table[block, 0:1, :]
            ranks = rank_v[pl.ds(block, 1), :]
            pick = jnp.where((line >= 0.0) & (ranks == slots), 1.0, 0.0)
            gate = jnp.sum(pick * line, axis=1, keepdims=True)
            chosen_all[block] = pick.astype(bf16)
            gates_all[block] = jnp.broadcast_to(gate, (capacity, 128))
            return carry

        lax.fori_loop(0, devices, choose, 0, unroll=4)
        across(0)
        for item in items:
            item.settled()

        def block_of(j, side, z):
            return (place.columns[j] + side * place.to_core) * length + z

        def load(j, side, z, slot):
            block = block_of(j, side, z)
            return [
                pltpu.make_async_copy(all_rows.at[block], row_buf.at[slot, j], load_sem.at[slot, 0, j]),
                pltpu.make_async_copy(all_cots.at[block], cot_buf.at[slot, j], load_sem.at[slot, 1, j]),
            ]

        def store(j, side, z, slot):
            block = block_of(j, side, z)
            return [
                pltpu.make_async_copy(stage_out.at[slot, j], part_out.at[block], store_sem.at[slot, 0, j]),
                pltpu.make_async_copy(stage_grad.at[slot, j], part_grad.at[block], store_sem.at[slot, 1, j]),
            ]

        def saved(i):
            first = [
                pltpu.make_async_copy(picked, picked_all.at[i], save_sem.at[0]),
                pltpu.make_async_copy(gated, gated_all.at[i], save_sem.at[1]),
            ]
            second = [
                pltpu.make_async_copy(hid, hid_all.at[i], save_sem.at[2]),
                pltpu.make_async_copy(dgate, dgate_all.at[i], save_sem.at[3]),
                pltpu.make_async_copy(dup, dup_all.at[i], save_sem.at[4]),
            ]
            return first, second

        def start_loads(step, side):
            for j in range(4):
                for copy in load(j, side, place.nearest(step), side):
                    copy.start()

        corner(0)
        for item in items:
            item.from_core(place.nearest(0))
        start_loads(0, 0)
        start_loads(0, 1)
        for copy in weights:
            copy.wait()

        def unit(i, carry):
            turn, side = i // 2, i % 2
            z = place.nearest(turn)

            @pl.when(i == 1)
            def _():
                along(2)
                across(1)

            for step in range(1, length):

                @pl.when(i == max(2, 2 * step - 1))
                def _(step=step):
                    corner(step)
                    along(step + 2)
                    across(step + 1)
                    for item in items:
                        item.from_core(place.nearest(step))
                    start_loads(step, 0)
                    if step == 1:
                        start_loads(step, 1)

            @pl.when(i >= 1)
            def _():
                for copy in saved(i)[0]:
                    copy.wait()

            for j in range(4):
                for copy in load(j, side, z, side):
                    copy.wait()
            for j in range(4):
                block = block_of(j, side, z)
                chosen[j] = chosen_all[block]
                slot_gate[pl.ds(j * capacity, capacity), :] = gates_all[block]

            def select(n, carry):
                lanes = pl.ds(pl.multiple_of(n * tile, tile), tile)
                for j in range(4):
                    at = pl.ds(j * capacity, capacity)
                    picked[at, lanes] = dot(chosen[j], row_buf[side, j, :, lanes]).astype(bf16)
                    cot = dot(chosen[j], cot_buf[side, j, :, lanes])
                    cotan[at, lanes] = cot.astype(bf16)
                    gated[at, lanes] = (slot_gate[at, 0:1] * cot).astype(bf16)
                return carry

            lax.fori_loop(0, width // tile, select, 0)

            for copy in saved(i)[0]:
                copy.start()
            for step in range(2, length):

                @pl.when(i == 2 * step - 1)
                def _(step=step):
                    start_loads(step, 1)

            @pl.when(i >= 1)
            def _():
                for copy in saved(i)[1]:
                    copy.wait()

            def middle(n, carry):
                lanes = pl.ds(pl.multiple_of(n * narrow, narrow), narrow)
                gate = dot(picked[...], wg[:, lanes])
                up = dot(picked[...], wu[:, lanes])
                grad = dot(gated[...], wd[lanes, :], 1, 1)
                sigma = jax.nn.sigmoid(gate)
                hid[:, lanes] = (gate * sigma * up).astype(bf16)
                dgate[:, lanes] = (grad * up * sigma * (1.0 + gate * (1.0 - sigma))).astype(bf16)
                dup[:, lanes] = (grad * gate * sigma).astype(bf16)
                return carry

            lax.fori_loop(0, hidden // narrow, middle, 0)
            for copy in saved(i)[1]:
                copy.start()
            slot_sum[...] = jnp.zeros(slot_sum.shape, f32)

            @pl.when(i >= 2)
            def _():
                for j in range(4):
                    for copy in store(j, side, z, side):
                        copy.wait()

            def outward(n, carry):
                lanes = pl.ds(pl.multiple_of(n * tile, tile), tile)
                result = dot(hid[...], wd[:, lanes]).astype(bf16).astype(f32)
                products = cotan[:, lanes].astype(f32) * result
                total = products[:, 0:128]
                for k in range(1, tile // 128):
                    total = total + products[:, 128 * k : 128 * (k + 1)]
                slot_sum[...] += total
                scaled[:, lanes] = (slot_gate[:, 0:1] * result).astype(bf16)
                back[:, lanes] = (
                    dot(dgate[...], wg[lanes, :], 1, 1) + dot(dup[...], wu[lanes, :], 1, 1)
                ).astype(bf16)
                for j in range(4):
                    at = pl.ds(j * capacity, capacity)
                    stage_out[side, j, :, lanes] = dot(chosen[j], scaled[at, lanes], 0, 0).astype(bf16)
                    stage_grad[side, j, :, lanes] = dot(chosen[j], back[at, lanes], 0, 0).astype(bf16)
                return carry

            lax.fori_loop(0, width // tile, outward, 0)
            for j in range(4):
                for copy in store(j, side, z, side):
                    copy.start()
            total = jnp.sum(slot_sum[...], axis=1, keepdims=True).reshape(4, capacity, 1)
            sums = jnp.sum(chosen[...].astype(f32) * total, axis=1)
            for j in range(4):
                token_out[block_of(j, side, z)] = jnp.broadcast_to(sums[j : j + 1], (8, rows))
            return carry

        lax.fori_loop(0, 2 * length, unit, 0)

        def token_send(n):
            device, there = other_device(place, n + 1)
            return pltpu.make_async_remote_copy(
                src_ref=token_out.at[there],
                dst_ref=token_in.at[expert],
                send_sem=token_sem.at[0],
                recv_sem=token_sem.at[1],
                device_id=device,
                device_id_type=MESH,
            )

        def send(n, carry):
            token_send(n).start()
            return carry

        lax.fori_loop(0, devices - 1, send, 0)
        pltpu.make_async_copy(token_out.at[expert], token_in.at[expert], token_sem.at[1]).start()
        for side in range(2):
            for j in range(4):
                for copy in store(j, side, 0, side):
                    copy.wait()
        for copies in saved(0):
            for copy in copies:
                copy.wait()
        sends.drain()
        pltpu.make_async_copy(token_out, token_in, token_sem.at[1]).wait()
        sent = token_out.at[pl.ds(0, devices - 1)]
        pltpu.make_async_copy(sent, sent, token_sem.at[0]).wait()
        pltpu.make_async_copy(sent, sent, gate_sem.at[0]).wait()

    any_spec = pl.BlockSpec(memory_space=pl.ANY)
    vmem = pl.BlockSpec(memory_space=pltpu.VMEM)
    big = (devices, rows, width)
    shape = jax.ShapeDtypeStruct
    sems = pltpu.SemaphoreType.DMA
    return pl.pallas_call(
        kernel,
        name="experts",
        out_shape=[
            shape(big, bf16), shape(big, bf16), shape(big, bf16),
            shape((devices, 8, rows), f32),
            shape((2 * length, count, width), bf16), shape((2 * length, count, width), bf16),
            shape((2 * length, count, hidden), bf16), shape((2 * length, count, hidden), bf16),
            shape((2 * length, count, hidden), bf16),
        ],
        in_specs=[any_spec] * 6,
        out_specs=[any_spec] * 3 + [vmem] + [any_spec] * 5,
        scratch_shapes=[
            pltpu.VMEM((width, hidden), bf16),
            pltpu.VMEM((width, hidden), bf16),
            pltpu.VMEM((hidden, width), bf16),
            pltpu.VMEM((devices, capacity, rows), bf16),
            pltpu.VMEM((devices, capacity, 128), f32),
            pltpu.VMEM((devices, rows), f32),
            pltpu.VMEM((devices, 8, rows), f32),
            pltpu.VMEM((2, 4, rows, width), bf16),
            pltpu.VMEM((2, 4, rows, width), bf16),
            pltpu.VMEM((count, width), bf16),
            pltpu.VMEM((count, width), bf16),
            pltpu.VMEM((count, width), bf16),
            pltpu.VMEM((count, hidden), bf16),
            pltpu.VMEM((count, hidden), bf16),
            pltpu.VMEM((count, hidden), bf16),
            pltpu.VMEM((count, width), bf16),
            pltpu.VMEM((count, width), bf16),
            pltpu.VMEM((4, capacity, rows), bf16),
            pltpu.VMEM((count, 128), f32),
            pltpu.VMEM((count, 128), f32),
            pltpu.VMEM((2, 4, rows, width), bf16),
            pltpu.VMEM((2, 4, rows, width), bf16),
            pltpu.VMEM((devices, 8, rows), f32),
        ]
        + GatherItem.semaphores("all", length)
        + [sems((2, 2, 4)), sems((2, 2, 4)), sems((5,)), sems((2,)), sems((2,)), sems((3,))],
        compiler_params=pltpu.CompilerParams(
            collective_id=collective_id, has_side_effects=True, vmem_limit_bytes=63 << 20
        ),
    )(rows_own, all_cots, gates_own, wgate, wup, wdown)


def rope(values, cosine, sine):
    return values * cosine + pltpu.roll(values, values.shape[-1] // 2, 1) * sine


def unrope(values, cosine, sine):
    return values * cosine - pltpu.roll(values, values.shape[-1] // 2, 1) * sine


def row_factor(values):
    return lax.rsqrt(jnp.mean(values * values, axis=-1, keepdims=True) + EPSILON)


def visible_pairs(seg_col, seg_row, start, stop, reach):
    shape = (stop - start, reach)
    query = lax.broadcasted_iota(jnp.int32, shape, 0) + start
    key = lax.broadcasted_iota(jnp.int32, shape, 1)
    return (seg_col[start:stop, :] == seg_row[:, 0:reach]) & (key <= query)


def attend(rows_own, joint_own, output_own, cots_own, seg_col, seg_row, cosine, sine, query_gain, key_gain, length, collective_id):
    rows, width = rows_own.shape
    depth, joint = joint_own.shape
    head_width, part = output_own.shape
    head = query_gain.shape[-1]
    heads = head_width // head
    tokens = rows * length
    block = tokens // 2
    tile = 512
    scale = 1.0 / math.sqrt(head)
    f32, bf16 = jnp.float32, jnp.bfloat16

    def kernel(
        rows_ref, joint_ref, output_ref, cots_ref, segc, segr, cos_ref, sin_ref, qgain, kgain,
        out_add, out_rows, out_joint, out_weight, out_cots, out_qkv, out_heads,
        rows_v, joint_v, weight_v, qkv, att, key_v, value_v,
        r0, r1, r2, r3, r4, r5, r6, r7,
        g0, g1, g2, j0, j1, j2, w0, w1, w2, c0, c1, c2, save_sem,
    ):
        place = Place(length)

        def item_of(mode, source, half, slot, sems):
            item = GatherItem(mode, place, None, None, *sems)
            item.own = lambda h: source.at[piece(2 * half, h)]
            item.slot = slot
            return item

        half, deep, tall = rows // 2, depth // 2, head_width // 2
        own_rows = item_of(
            "z", rows_ref, half, lambda c, z, h: rows_v.at[z, piece(2 * half, h)], (g0, g1, g2)
        )
        own_joint = item_of(
            "dp", joint_ref, deep, lambda c, z, h: joint_v.at[c, piece(2 * deep, h)], (j0, j1, j2)
        )
        own_weight = item_of(
            "dp",
            output_ref,
            tall,
            lambda c, z, h: weight_v.at[
                piece(2 * tall, h), pl.ds(pl.multiple_of(c * part, part), part)
            ],
            (w0, w1, w2),
        )
        cots = item_of(
            "all",
            cots_ref,
            half,
            lambda c, z, h: out_cots.at[c * length + z, piece(2 * half, h)],
            (c0, c1, c2),
        )
        total = ReduceItem(
            "z", place, None, (r0, r1, r2, r3, r4, r5, r6, r7),
            lambda h: out_add.at[piece(2 * half, h)],
        )
        total.computed = True
        total.begin()
        meet(place, True, True)
        sends = Sends(place)
        own_joint.begin(sends)
        own_rows.begin(sends)
        own_weight.begin(sends)
        own_joint.across(sends, 0)
        own_rows.along_z(sends, 1)
        own_weight.across(sends, 0)
        own_joint.diagonal(sends, 0)
        own_rows.along_z(sends, 2)
        own_weight.diagonal(sends, 0)
        for distance in range(3, length):
            own_rows.along_z(sends, distance)
        cots.begin(sends)
        own_joint.finish()
        own_rows.finish()

        def projection(n, carry):
            lanes = pl.ds(pl.multiple_of(n * 256, 256), 256)
            left = rows_v[...].reshape(tokens, width)
            right = joint_v[:, :, lanes].reshape(width, 256)
            qkv[:, lanes] = dot(left, right)
            return carry

        lax.fori_loop(0, joint // 256, projection, 0)
        saves = [
            pltpu.make_async_copy(source, target, save_sem.at[n])
            for n, (source, target) in enumerate(
                ((rows_v, out_rows), (joint_v, out_joint), (qkv, out_qkv), (weight_v, out_weight), (att, out_heads))
            )
        ]
        for copy in saves[:3]:
            copy.start()
        key = qkv[:, head_width : head_width + head]
        key_v[...] = rope(key * row_factor(key) * kgain[...], cos_ref[...], sin_ref[...]).astype(bf16)
        value_v[...] = qkv[:, head_width + head : head_width + 2 * head].astype(bf16)

        def one_head(n, carry):
            lanes = pl.ds(pl.multiple_of(n * head, head), head)
            for start in range(0, tokens, block):
                stop = start + block
                query = qkv[start:stop, lanes]
                turned = rope(
                    query * row_factor(query) * qgain[...], cos_ref[start:stop, :], sin_ref[start:stop, :]
                ).astype(bf16)
                scores = dot(turned, key_v[0:stop, :], 1, 1) * scale
                seen = visible_pairs(segc, segr, start, stop, stop)
                scores = jnp.where(seen, scores, NEG_BIG)
                top = jnp.max(scores, axis=-1, keepdims=True)
                powers = jnp.exp(scores - top)
                probs = (powers / jnp.sum(powers, axis=-1, keepdims=True)).astype(bf16)
                att[start:stop, lanes] = dot(probs, value_v[0:stop, :]).astype(bf16)
            return carry

        lax.fori_loop(0, heads // 2, one_head, 0)
        cots.along_z(sends, 1)
        cots.across(sends, 0)
        lax.fori_loop(heads // 2, heads, one_head, 0)
        saves[4].start()
        own_weight.finish()
        saves[3].start()

        def outward(turn):
            z = total.z_of(turn)

            def body(n, carry):
                lanes = pl.ds(pl.multiple_of(n * tile, tile), tile)
                left = att[pl.ds(pl.multiple_of(z * rows, rows), rows), :]
                found = dot(left, weight_v[:, lanes]).astype(bf16)
                total.acc[0, turn, :, lanes] = found
                return carry

            lax.fori_loop(0, width // tile, body, 0)

        for turn in range(length):
            outward(turn)
            total.home(sends, turn)
            cots.along_z(sends, turn + 2)
            cots.diagonal(sends, turn)
            cots.across(sends, turn + 1)
        cots.finish()
        for copy in saves:
            copy.wait()
        sends.drain()

    any_spec = pl.BlockSpec(memory_space=pl.ANY)
    vmem = pl.BlockSpec(memory_space=pltpu.VMEM)
    shape = jax.ShapeDtypeStruct
    return pl.pallas_call(
        kernel,
        name="attend",
        out_shape=[
            shape((rows, width), f32),
            shape((length, rows, width), bf16),
            shape((8, depth, joint), bf16),
            shape((head_width, 8 * part), bf16),
            shape((8 * length, rows, width), bf16),
            shape((tokens, joint), f32),
            shape((tokens, head_width), bf16),
        ],
        in_specs=[any_spec] * 4 + [vmem] * 6,
        out_specs=[vmem] + [any_spec] * 6,
        scratch_shapes=[
            pltpu.VMEM((length, rows, width), bf16),
            pltpu.VMEM((8, depth, joint), bf16),
            pltpu.VMEM((head_width, 8 * part), bf16),
            pltpu.VMEM((tokens, joint), f32),
            pltpu.VMEM((tokens, head_width), bf16),
            pltpu.VMEM((tokens, head), bf16),
            pltpu.VMEM((tokens, head), bf16),
        ]
        + ReduceItem.scratch("z", length, rows, width)
        + GatherItem.semaphores("z", length)
        + GatherItem.semaphores("dp", length) * 2
        + GatherItem.semaphores("all", length)
        + [pltpu.SemaphoreType.DMA((5,))],
        compiler_params=pltpu.CompilerParams(
            collective_id=collective_id, has_side_effects=True, vmem_limit_bytes=56 << 20
        ),
    )(rows_own, joint_own, output_own, cots_own, seg_col, seg_row, cosine, sine, query_gain, key_gain)


def attend_back(grad_own, rows_all, joint_all, output_all, qkv_all, heads_all, part_out, seg_col, seg_row, cosine, sine, query_gain, key_gain, length, collective_id):
    rows, width = grad_own.shape
    _, depth, joint = joint_all.shape
    head_width = output_all.shape[0]
    part = width // 8
    head = query_gain.shape[-1]
    heads = head_width // head
    tokens = rows * length
    block = tokens // 2
    scale = 1.0 / math.sqrt(head)
    f32, bf16 = jnp.float32, jnp.bfloat16
    half, deep, tall = rows // 2, depth // 2, head_width // 2

    def kernel(
        grad_ref, rows_ref, joint_ref, output_ref, qkv_ref, heads_ref, part_ref,
        segc, segr, cos_ref, sin_ref, qgain, kgain,
        out_rows, out_joint, out_weight, out_moe, out_qgain, out_kgain,
        grads, joint_v, weight_v, qkv, att, gatt, joint_b, part_w, key_v, value_v, dkey, dvalue,
        *rest,
    ):
        place = Place(length)
        o_bufs, z_bufs, j_bufs, w_bufs = (rest[8 * n : 8 * n + 8] for n in range(4))
        gather_sems, load_sem = rest[32:35], rest[35]

        outs = ReduceItem(
            "all",
            place,
            lambda c, z, h: part_ref.at[c * length + z, piece(2 * half, h)],
            o_bufs,
            lambda h: out_moe.at[piece(2 * half, h)],
        )
        back = ReduceItem(
            "z",
            place,
            lambda c, z, h: grads.at[z, piece(2 * half, h)],
            z_bufs,
            lambda h: out_rows.at[piece(2 * half, h)],
        )
        joints = ReduceItem(
            "dp",
            place,
            lambda c, z, h: joint_v.at[c, piece(2 * deep, h)],
            j_bufs,
            lambda h: out_joint.at[piece(2 * deep, h)],
        )
        weights = ReduceItem(
            "dp",
            place,
            lambda c, z, h: part_w.at[
                piece(2 * tall, h), pl.ds(pl.multiple_of(c * part, part), part)
            ],
            w_bufs,
            lambda h: out_weight.at[piece(2 * tall, h)],
        )
        for item in (back, joints, weights):
            item.in_place = True
        gathers = GatherItem("z", place, None, None, *gather_sems)
        gathers.own = lambda h: grad_ref.at[piece(2 * half, h)]
        gathers.slot = lambda c, z, h: grads.at[z, piece(2 * half, h)]

        outs.begin()
        back.begin()
        meet(place, True, True)
        first, sends = Sends(place), Sends(place)
        gathers.begin(first)
        outs.load_all()
        outs.hand_over(sends, 0)
        outs.hand_over(sends, 1)
        loads = [
            pltpu.make_async_copy(source, target, load_sem.at[n])
            for n, (source, target) in enumerate(
                ((output_ref, weight_v), (heads_ref, att), (qkv_ref, qkv), (joint_ref, joint_v))
            )
        ]
        for copy in loads:
            copy.start()
        advance(outs, sends, 0)
        for distance in range(1, length):
            gathers.along_z(first, distance)
            if distance < length - 1:
                advance(outs, sends, distance)
        gathers.finish()
        first.drain()
        for copy in loads[:3]:
            copy.wait()

        def to_heads(n, carry):
            lanes = pl.ds(pl.multiple_of(n * 256, 256), 256)
            left = grads[...].reshape(tokens, width)
            gatt[:, lanes] = dot(left, weight_v[lanes, :], 1, 1).astype(bf16)
            return carry

        def to_weight(n, carry):
            lanes = pl.ds(pl.multiple_of(n * 256, 256), 256)
            right = grads[:, :, lanes].reshape(tokens, 256)
            part_w[:, lanes] = dot(att[...], right, 0, 0).astype(bf16)
            return carry

        lax.fori_loop(0, width // 256, to_weight, 0)
        weights.hand_over(sends, 0)
        lax.fori_loop(0, head_width // 256, to_heads, 0)
        rows_v = weight_v.at[pl.ds(0, tokens)]
        rows_loads = [
            pltpu.make_async_copy(
                rows_ref.at[z], weight_v.at[pl.ds(z * rows, rows)], load_sem.at[4 + z]
            )
            for z in range(length)
        ]
        for copy in rows_loads:
            copy.start()
        advance(weights, sends, 0)
        key = qkv[:, head_width : head_width + head]
        key_v[...] = rope(key * row_factor(key) * kgain[...], cos_ref[...], sin_ref[...]).astype(bf16)
        value_v[...] = qkv[:, head_width + head : head_width + 2 * head].astype(bf16)
        dkey[...] = jnp.zeros((tokens, head), f32)
        dvalue[...] = jnp.zeros((tokens, head), f32)
        out_qgain[...] = jnp.zeros(out_qgain.shape, f32)

        def normed_back(grad, raw, gain, start, stop):
            factor = row_factor(raw)
            hat = raw * factor
            turned = unrope(grad, cos_ref[start:stop, :], sin_ref[start:stop, :])
            scaled = turned * gain
            found = factor * (scaled - hat * jnp.mean(scaled * hat, axis=-1, keepdims=True))
            return found, jnp.sum(turned * hat, axis=0, keepdims=True)

        def one_head(n, carry):
            lanes = pl.ds(pl.multiple_of(n * head, head), head)
            for start in range(0, tokens, block):
                stop = start + block
                raw = qkv[start:stop, lanes]
                turned = rope(
                    raw * row_factor(raw) * qgain[...], cos_ref[start:stop, :], sin_ref[start:stop, :]
                ).astype(bf16)
                grad = gatt[start:stop, lanes]
                delta = jnp.sum(
                    grad.astype(f32) * att[start:stop, lanes].astype(f32), axis=-1, keepdims=True
                )
                scores = dot(turned, key_v[0:stop, :], 1, 1) * scale
                seen = visible_pairs(segc, segr, start, stop, stop)
                scores = jnp.where(seen, scores, NEG_BIG)
                powers = jnp.exp(scores - jnp.max(scores, axis=-1, keepdims=True))
                probs = powers / jnp.sum(powers, axis=-1, keepdims=True)
                dprobs = dot(grad, value_v[0:stop, :], 1, 1)
                dscores = (probs * (dprobs - delta)).astype(bf16)
                dvalue[0:stop, :] += dot(probs.astype(bf16), grad, 0, 0)
                dkey[0:stop, :] += dot(dscores, turned, 0, 0) * scale
                dquery = dot(dscores, key_v[0:stop, :]) * scale
                found, gain_part = normed_back(dquery, raw, qgain[...], start, stop)
                joint_b[start:stop, lanes] = found.astype(bf16)
                out_qgain[...] += gain_part
            return carry

        lax.fori_loop(0, heads // 2, one_head, 0)
        advance(outs, sends, length - 1)
        advance(weights, sends, 1)
        lax.fori_loop(heads // 2, heads, one_head, 0)
        found, gain_part = normed_back(
            dkey[...], qkv[:, head_width : head_width + head], kgain[...], 0, tokens
        )
        out_kgain[...] = gain_part
        joint_b[:, head_width : head_width + head] = found.astype(bf16)
        joint_b[:, head_width + head : head_width + 2 * head] = dvalue[...].astype(bf16)
        advance(outs, sends, length)
        advance(weights, sends, 2)
        loads[3].wait()

        def to_rows(n, carry):
            lanes = pl.ds(pl.multiple_of(n * depth, depth), depth)
            found = dot(joint_b[...], joint_v[n], 1, 1).astype(bf16)
            grads[:, :, lanes] = found.reshape(length, rows, depth)
            return carry

        lax.fori_loop(0, 8, to_rows, 0)
        back.home(sends, 0)
        for copy in rows_loads:
            copy.wait()

        def to_joint(n, carry):
            lanes = pl.ds(pl.multiple_of(n * depth, depth), depth)
            joint_v[n] = dot(weight_v[0:tokens, lanes], joint_b[...], 0, 0).astype(bf16)
            return carry

        lax.fori_loop(0, 8, to_joint, 0)
        joints.hand_over(sends, 0)
        back.home(sends, 1)
        advance(joints, sends, 0)
        for turn in range(2, length):
            back.home(sends, turn)
        advance(joints, sends, 1)
        advance(outs, sends, length + 1)
        advance(joints, sends, 2)
        sends.drain()

    any_spec = pl.BlockSpec(memory_space=pl.ANY)
    vmem = pl.BlockSpec(memory_space=pltpu.VMEM)
    shape = jax.ShapeDtypeStruct
    return pl.pallas_call(
        kernel,
        name="attend_back",
        out_shape=[
            shape((rows, width), f32),
            shape((depth, joint), f32),
            shape((head_width, part), f32),
            shape((rows, width), f32),
            shape((1, head), f32),
            shape((1, head), f32),
        ],
        in_specs=[any_spec] * 7 + [vmem] * 6,
        out_specs=[vmem] * 6,
        scratch_shapes=[
            pltpu.VMEM((length, rows, width), bf16),
            pltpu.VMEM((8, depth, joint), bf16),
            pltpu.VMEM((head_width, width), bf16),
            pltpu.VMEM((tokens, joint), f32),
            pltpu.VMEM((tokens, head_width), bf16),
            pltpu.VMEM((tokens, head_width), bf16),
            pltpu.VMEM((tokens, joint), bf16),
            pltpu.VMEM((head_width, width), bf16),
            pltpu.VMEM((tokens, head), bf16),
            pltpu.VMEM((tokens, head), bf16),
            pltpu.VMEM((tokens, head), f32),
            pltpu.VMEM((tokens, head), f32),
        ]
        + ReduceItem.scratch("all", length, rows, width)
        + ReduceItem.scratch("z", length, rows, width, True)
        + ReduceItem.scratch("dp", length, depth, joint, True)
        + ReduceItem.scratch("dp", length, head_width, part, True)
        + GatherItem.semaphores("z", length)
        + [pltpu.SemaphoreType.DMA((4 + length,))],
        compiler_params=pltpu.CompilerParams(
            collective_id=collective_id, has_side_effects=True, vmem_limit_bytes=67043328
        ),
    )(grad_own, rows_all, joint_all, output_all, qkv_all, heads_all, part_out, seg_col, seg_row, cosine, sine, query_gain, key_gain)


def share_sum(values, length, collective_id):
    devices = 8 * length
    rows, width = values.shape

    def kernel(own, target, land, sem):
        place = Place(length)
        me = place.dp * length + place.z
        meet_all(place)

        def send(n, carry):
            device, _ = other_device(place, n + 1)
            pltpu.make_async_remote_copy(
                src_ref=own,
                dst_ref=land.at[me],
                send_sem=sem.at[0],
                recv_sem=sem.at[1],
                device_id=device,
                device_id_type=MESH,
            ).start()
            return carry

        lax.fori_loop(0, devices - 1, send, 0)
        pltpu.make_async_copy(own, land.at[me], sem.at[1]).start()
        pltpu.make_async_copy(land, land, sem.at[1]).wait()
        sent = land.at[pl.ds(0, devices - 1)]
        pltpu.make_async_copy(sent, sent, sem.at[0]).wait()

        def add(n, total):
            return total + land[n]

        target[...] = lax.fori_loop(1, devices, add, land[0])

    vmem = pl.BlockSpec(memory_space=pltpu.VMEM)
    return pl.pallas_call(
        kernel,
        name="share_sum",
        out_shape=jax.ShapeDtypeStruct((rows, width), values.dtype),
        in_specs=[vmem],
        out_specs=vmem,
        scratch_shapes=[
            pltpu.VMEM((devices, rows, width), values.dtype),
            pltpu.SemaphoreType.DMA((2,)),
        ],
        compiler_params=pltpu.CompilerParams(collective_id=collective_id, has_side_effects=True),
    )(values)


def mix(form, left, right):
    return jnp.einsum(form, left, right, preferred_element_type=jnp.float32)


def rms_scale(values):
    return lax.rsqrt(jnp.mean(values * values, axis=-1, keepdims=True) + EPSILON)


def rope_tables(seg_ids, head_dim):
    length = seg_ids.shape[0]
    row_index = jnp.arange(length, dtype=jnp.int32)
    starts = jnp.sum((seg_ids[None, :] < seg_ids[:, None]).astype(jnp.int32), axis=1)
    places = (row_index - starts).astype(jnp.float32)
    half_dim = head_dim // 2
    frequency = THETA_BASE ** (-(jnp.arange(half_dim, dtype=jnp.float32) * (2.0 / head_dim)))
    angles = places[:, None] * frequency[None, :]
    return (jnp.cos(angles), jnp.sin(angles))


def rotate(values, cosine, sine_table):
    half_dim = values.shape[-1] // 2
    front_part = values[..., :half_dim]
    back_part = values[..., half_dim:]
    cos_rows = cosine[:, None, :]
    sin_rows = sine_table[:, None, :]
    return jnp.concatenate(
        [
            front_part * cos_rows - back_part * sin_rows,
            back_part * cos_rows + front_part * sin_rows,
        ],
        axis=-1,
    )


def unrotate(values, cosine, sine_table):
    half_dim = values.shape[-1] // 2
    front_part = values[..., :half_dim]
    back_part = values[..., half_dim:]
    cos_rows = cosine[:, None, :]
    sin_rows = sine_table[:, None, :]
    return jnp.concatenate(
        [
            front_part * cos_rows + back_part * sin_rows,
            back_part * cos_rows - front_part * sin_rows,
        ],
        axis=-1,
    )


def head_norm_back(grad_out, normed, factor, gain):
    grad_normed = grad_out * gain
    grad_gain = jnp.sum(grad_out * normed, axis=(0, 1))
    grad_values = factor * (
        grad_normed - normed * jnp.mean(grad_normed * normed, axis=-1, keepdims=True)
    )
    return (grad_values, grad_gain)


def row_norm_back(grad_out, normed, factor, gain):
    grad_normed = grad_out * gain
    grad_gain = jnp.sum(grad_out * normed, axis=0)
    grad_values = factor * (
        grad_normed - normed * jnp.mean(grad_normed * normed, axis=-1, keepdims=True)
    )
    return (grad_values, grad_gain)


def softmax_rows(logits):
    top_value = jnp.max(logits, axis=-1, keepdims=True)
    expo = jnp.exp(logits - top_value)
    return expo / jnp.sum(expo, axis=-1, keepdims=True)


def attn_forward(rows, seg_ids, wq_full, wk_full, wv_full, query_gain, key_gain):
    length = rows.shape[0]
    head_dim = query_gain.shape[0]
    num_heads = wq_full.shape[1] // head_dim
    kv_heads = wk_full.shape[1] // head_dim
    per_group = num_heads // kv_heads
    inv_root = 1.0 / math.sqrt(head_dim)
    block_rows = math.gcd(length, 512)
    cosine, sine_table = rope_tables(seg_ids, head_dim)
    query = jnp.dot(rows, wq_full, preferred_element_type=jnp.float32).reshape(
        length, num_heads, head_dim
    )
    key_proj = jnp.dot(rows, wk_full, preferred_element_type=jnp.float32).reshape(
        length, kv_heads, head_dim
    )
    value_rows = (
        jnp.dot(rows, wv_full, preferred_element_type=jnp.float32)
        .astype(jnp.bfloat16)
        .reshape(length, kv_heads, head_dim)
    )
    query_factor = rms_scale(query)
    query_hat = query * query_factor
    key_factor = rms_scale(key_proj)
    key_hat = key_proj * key_factor
    query_rot = (
        rotate(query_hat * query_gain, cosine, sine_table)
        .astype(jnp.bfloat16)
        .reshape(length, kv_heads, per_group, head_dim)
    )
    key_rot = rotate(key_hat * key_gain, cosine, sine_table).astype(jnp.bfloat16)
    row_index = jnp.arange(length, dtype=jnp.int32)
    scores = mix("qgrd,kgd->grqk", query_rot, key_rot) * inv_root
    visible = (seg_ids[0:block_rows, None] == seg_ids[None, :]) & (
        row_index[None, :] <= row_index[0:block_rows, None]
    )
    scores = jnp.where(visible, scores, NEG_BIG)
    top_value = jnp.max(scores, axis=-1, keepdims=True)
    expo = jnp.exp(scores - top_value)
    totals = jnp.sum(expo, axis=-1, keepdims=True)
    prob_rows = (expo / totals).astype(jnp.bfloat16)
    outputs = mix("grqk,kgd->qgrd", prob_rows, value_rows).astype(jnp.bfloat16)
    lse_parts = top_value[..., 0] + jnp.log(totals[..., 0])
    attn_heads = outputs.reshape(length, num_heads * head_dim)
    return (
        attn_heads,
        lse_parts,
        query_rot,
        key_rot,
        value_rows,
        cosine,
        sine_table,
        query_hat,
        query_factor,
        key_hat,
        key_factor,
    )


def attn_backward(
    grad_attn, rows, seg_ids, wq_full, wk_full, wv_full, wo_full, query_gain, key_gain, saved
):
    (
        attn_heads,
        lse_all,
        query_rot,
        key_rot,
        value_rows,
        cosine,
        sine_table,
        query_hat,
        query_factor,
        key_hat,
        key_factor,
    ) = saved
    length = rows.shape[0]
    head_dim = query_gain.shape[0]
    num_heads = query_hat.shape[1]
    inv_root = 1.0 / math.sqrt(head_dim)
    block_rows = math.gcd(length, 512)
    grad_wo = jnp.dot(attn_heads.T, grad_attn, preferred_element_type=jnp.float32)
    grad_heads = (
        jnp.dot(grad_attn, wo_full.T, preferred_element_type=jnp.float32)
        .astype(jnp.bfloat16)
        .reshape(query_rot.shape)
    )
    heads_view = attn_heads.reshape(query_rot.shape)
    row_delta = jnp.transpose(
        jnp.sum(grad_heads.astype(jnp.float32) * heads_view.astype(jnp.float32), axis=-1), (1, 2, 0)
    )
    row_index = jnp.arange(length, dtype=jnp.int32)
    scores = mix("qgrd,kgd->grqk", query_rot, key_rot) * inv_root
    visible = (seg_ids[0:block_rows, None] == seg_ids[None, :]) & (
        row_index[None, :] <= row_index[0:block_rows, None]
    )
    scores = jnp.where(visible, scores, NEG_BIG)
    prob_f = jnp.where(visible, jnp.exp(scores - lse_all[:, :, 0:block_rows, None]), 0.0)
    prob_rows = prob_f.astype(jnp.bfloat16)
    grad_value = mix("grqk,qgrd->kgd", prob_rows, grad_heads)
    grad_probs = mix("qgrd,kgd->grqk", grad_heads, value_rows)
    grad_scores = (prob_f * (grad_probs - row_delta[:, :, 0:block_rows, None])).astype(jnp.bfloat16)
    pieces = mix("grqk,kgd->qgrd", grad_scores, key_rot) * inv_root
    grad_key_rot = mix("grqk,qgrd->kgd", grad_scores, query_rot) * inv_root
    grad_query_rot = pieces.reshape(length, num_heads, head_dim)
    grad_query, grad_qgain = head_norm_back(
        unrotate(grad_query_rot, cosine, sine_table), query_hat, query_factor, query_gain
    )
    grad_key, grad_kgain = head_norm_back(
        unrotate(grad_key_rot, cosine, sine_table), key_hat, key_factor, key_gain
    )
    query_b = grad_query.astype(jnp.bfloat16).reshape(length, -1)
    key_b = grad_key.astype(jnp.bfloat16).reshape(length, -1)
    value_b = grad_value.astype(jnp.bfloat16).reshape(length, -1)
    grad_rows = (
        jnp.dot(query_b, wq_full.T, preferred_element_type=jnp.float32)
        + jnp.dot(key_b, wk_full.T, preferred_element_type=jnp.float32)
        + jnp.dot(value_b, wv_full.T, preferred_element_type=jnp.float32)
    )
    grad_wq = jnp.dot(rows.T, query_b, preferred_element_type=jnp.float32)
    grad_wk = jnp.dot(rows.T, key_b, preferred_element_type=jnp.float32)
    grad_wv = jnp.dot(rows.T, value_b, preferred_element_type=jnp.float32)
    return (grad_rows, grad_wq, grad_wk, grad_wv, grad_wo, grad_qgain, grad_kgain)


def expert_forward(expert_rows, wgate, wup, wdown):
    gate_pre = jnp.dot(expert_rows, wgate, preferred_element_type=jnp.float32)
    up_pre = jnp.dot(expert_rows, wup, preferred_element_type=jnp.float32)
    hidden_units = (jax.nn.silu(gate_pre) * up_pre).astype(jnp.bfloat16)
    result = jnp.dot(hidden_units, wdown, preferred_element_type=jnp.float32).astype(jnp.bfloat16)
    return (result, gate_pre, up_pre, hidden_units)


def expert_backward(expert_rows, grad_result, wgate, wup, wdown, gate_pre, up_pre, hidden_units):
    grad_hidden = jnp.dot(grad_result, wdown.T, preferred_element_type=jnp.float32)
    sigma = jax.nn.sigmoid(gate_pre)
    grad_gate_pre = (grad_hidden * up_pre * sigma * (1.0 + gate_pre * (1.0 - sigma))).astype(
        jnp.bfloat16
    )
    grad_up_pre = (grad_hidden * gate_pre * sigma).astype(jnp.bfloat16)
    grad_rows = (
        jnp.dot(grad_gate_pre, wgate.T, preferred_element_type=jnp.float32)
        + jnp.dot(grad_up_pre, wup.T, preferred_element_type=jnp.float32)
    ).astype(jnp.bfloat16)
    grad_wd = jnp.dot(hidden_units.T, grad_result, preferred_element_type=jnp.float32)
    grad_wg = jnp.dot(expert_rows.T, grad_gate_pre, preferred_element_type=jnp.float32)
    grad_wu = jnp.dot(expert_rows.T, grad_up_pre, preferred_element_type=jnp.float32)
    return (grad_rows, grad_wg, grad_wu, grad_wd)


def to_experts(buffer):
    return lax.all_to_all(buffer, ("dp", "tensor"), split_axis=0, concat_axis=0, tiled=True)


def to_sources(buffer):
    return lax.all_to_all(buffer, ("dp", "tensor"), split_axis=0, concat_axis=0, tiled=True)


def shards(
    hidden_in,
    segments,
    routes,
    query_weight,
    key_weight,
    value_weight,
    output_weight,
    gain_attn,
    gain_moe,
    query_gain,
    key_gain,
    router,
    gate_weight,
    up_weight,
    down_weight,
    cotangent,
):
    seg_ids = segments[0]
    rows_dev = hidden_in.shape[0]
    width = hidden_in.shape[1]
    top_count = routes.shape[1]
    experts = router.shape[1]
    capacity = 2 * rows_dev * top_count // experts
    full_query, full_key, full_value, full_output = (
        lax.all_gather(query_weight, "dp", axis=0, tiled=True),
        lax.all_gather(key_weight, "dp", axis=0, tiled=True),
        lax.all_gather(value_weight, "dp", axis=0, tiled=True),
        lax.all_gather(output_weight, "dp", axis=1, tiled=True),
    )
    inputs32 = hidden_in.astype(jnp.float32)
    factor_one = rms_scale(inputs32)
    normed_one = inputs32 * factor_one
    rows_one = (normed_one * gain_attn).astype(jnp.bfloat16)
    group_rows = lax.all_gather(rows_one, "tensor", axis=0, tiled=True)
    saved = attn_forward(
        group_rows, seg_ids, full_query, full_key, full_value, query_gain, key_gain
    )
    partial_add = jnp.dot(saved[0], full_output, preferred_element_type=jnp.float32)
    attn_add = lax.psum_scatter(partial_add, "tensor", scatter_dimension=0, tiled=True)
    residual = inputs32 + attn_add
    factor_two = rms_scale(residual)
    normed_two = residual * factor_two
    rows_two = (normed_two * gain_moe).astype(jnp.bfloat16)
    router_probs = softmax_rows(jnp.dot(rows_two, router, preferred_element_type=jnp.float32))
    route_hot = (routes[:, :, None] == jnp.arange(experts, dtype=jnp.int32)[None, None, :]).astype(
        jnp.float32
    )
    picked = jnp.sum(route_hot * router_probs[:, None, :], axis=-1)
    total = jnp.sum(picked, axis=1, keepdims=True)
    gates = picked / total
    flat_routes = routes.reshape(-1)
    onehot = (flat_routes[:, None] == jnp.arange(experts, dtype=jnp.int32)[None, :]).astype(
        jnp.int32
    )
    ranks = jnp.sum(onehot * jnp.cumsum(onehot, axis=0), axis=1) - 1
    slots = flat_routes * capacity + ranks
    send_rows = (
        jnp.zeros((experts * capacity, width), jnp.bfloat16)
        .at[slots]
        .set(jnp.repeat(rows_two, top_count, axis=0))
    )
    received = to_experts(send_rows.reshape(experts, capacity, width)).reshape(-1, width)
    result, gate_pre, up_pre, hidden_units = expert_forward(
        received, gate_weight[0], up_weight[0], down_weight[0]
    )
    returned = to_sources(result.reshape(-1, capacity, width)).reshape(experts * capacity, width)
    pair_out = returned[slots].astype(jnp.float32).reshape(rows_dev, top_count, width)
    moe_sum = jnp.sum(gates[:, :, None] * pair_out, axis=1)
    output = (residual + moe_sum).astype(jnp.bfloat16)
    cot32 = cotangent.astype(jnp.float32)
    grad_gates = jnp.sum(cot32[:, None, :] * pair_out, axis=-1)
    grad_result = (gates[:, :, None] * cot32[:, None, :]).astype(jnp.bfloat16).reshape(-1, width)
    send_grads = jnp.zeros((experts * capacity, width), jnp.bfloat16).at[slots].set(grad_result)
    received_grads = to_experts(send_grads.reshape(experts, capacity, width)).reshape(-1, width)
    grad_expert_rows, grad_wg, grad_wu, grad_wd = expert_backward(
        received,
        received_grads,
        gate_weight[0],
        up_weight[0],
        down_weight[0],
        gate_pre,
        up_pre,
        hidden_units,
    )
    returned_grads = to_sources(grad_expert_rows.reshape(-1, capacity, width)).reshape(
        experts * capacity, width
    )
    grad_pairs = returned_grads[slots].astype(jnp.float32).reshape(rows_dev, top_count, width)
    grad_picked = (grad_gates - jnp.sum(gates * grad_gates, axis=1, keepdims=True)) / total
    grad_probs = jnp.sum(route_hot * grad_picked[:, :, None], axis=1)
    grad_logits = (
        router_probs * (grad_probs - jnp.sum(grad_probs * router_probs, axis=-1, keepdims=True))
    ).astype(jnp.bfloat16)
    grad_router = jnp.dot(rows_two.T, grad_logits, preferred_element_type=jnp.float32)
    grad_rows_two = jnp.sum(grad_pairs, axis=1) + jnp.dot(
        grad_logits, router.T, preferred_element_type=jnp.float32
    )
    grad_res_norm, grad_gain_moe = row_norm_back(grad_rows_two, normed_two, factor_two, gain_moe)
    grad_residual = cot32 + grad_res_norm
    grad_attn = grad_residual.astype(jnp.bfloat16)
    group_grads = lax.all_gather(grad_attn, "tensor", axis=0, tiled=True)
    back_query, back_key, back_value, back_output = (
        lax.all_gather(query_weight, "dp", axis=0, tiled=True),
        lax.all_gather(key_weight, "dp", axis=0, tiled=True),
        lax.all_gather(value_weight, "dp", axis=0, tiled=True),
        lax.all_gather(output_weight, "dp", axis=1, tiled=True),
    )
    grad_group_rows, grad_wq, grad_wk, grad_wv, grad_wo, grad_qgain, grad_kgain = attn_backward(
        group_grads,
        group_rows,
        seg_ids,
        back_query,
        back_key,
        back_value,
        back_output,
        query_gain,
        key_gain,
        saved,
    )
    grad_rows_one = lax.psum_scatter(
        grad_group_rows.astype(jnp.bfloat16), "tensor", scatter_dimension=0, tiled=True
    ).astype(jnp.float32)
    grad_in_norm, grad_gain_attn = row_norm_back(grad_rows_one, normed_one, factor_one, gain_attn)
    grad_input = grad_residual + grad_in_norm
    grad_wq, grad_wk, grad_wv, grad_wo = (
        lax.psum_scatter(
            grad_wq.astype(jnp.bfloat16), "dp", scatter_dimension=0, tiled=True
        ).astype(jnp.float32),
        lax.psum_scatter(
            grad_wk.astype(jnp.bfloat16), "dp", scatter_dimension=0, tiled=True
        ).astype(jnp.float32),
        lax.psum_scatter(
            grad_wv.astype(jnp.bfloat16), "dp", scatter_dimension=0, tiled=True
        ).astype(jnp.float32),
        lax.psum_scatter(
            grad_wo.astype(jnp.bfloat16), "dp", scatter_dimension=1, tiled=True
        ).astype(jnp.float32),
    )
    grad_gain_attn, grad_gain_moe, grad_qgain, grad_kgain, grad_router = lax.psum(
        (grad_gain_attn, grad_gain_moe, grad_qgain, grad_kgain, grad_router), ("dp", "tensor")
    )
    return (
        output,
        grad_input,
        grad_wq,
        grad_wk,
        grad_wv,
        grad_wo,
        grad_gain_attn,
        grad_gain_moe,
        grad_qgain,
        grad_kgain,
        grad_router,
        grad_wg[None],
        grad_wu[None],
        grad_wd[None],
    )


AXES = ("dp", "tensor")


def gathered(
    hidden_in,
    segments,
    routes,
    query_weight,
    key_weight,
    value_weight,
    output_weight,
    gain_attn,
    gain_moe,
    query_gain,
    key_gain,
    router,
    gate_weight,
    up_weight,
    down_weight,
    cotangent,
):
    seg_ids = segments[0]
    rows_dev, width = hidden_in.shape
    top_count = routes.shape[1]
    expert_count = router.shape[1]
    capacity = 2 * rows_dev * top_count // expert_count
    length = lax.axis_size("tensor")
    query_cols, key_cols = query_weight.shape[1], key_weight.shape[1]

    inputs32 = hidden_in.astype(jnp.float32)
    factor_one = rms_scale(inputs32)
    normed_one = inputs32 * factor_one
    rows_one = (normed_one * gain_attn).astype(jnp.bfloat16)
    joint_weight = jnp.concatenate([query_weight, key_weight, value_weight], axis=1)
    cosine, sine_table = rope_tables(seg_ids, query_gain.shape[0])
    turns = (
        seg_ids[:, None],
        seg_ids[None, :],
        jnp.concatenate([cosine, cosine], axis=1),
        jnp.concatenate([-sine_table, sine_table], axis=1),
        query_gain[None, :],
        key_gain[None, :],
    )
    attn_add, group_rows, full_joint, full_output, all_cots, projected, attn_heads = attend(
        rows_one, joint_weight, output_weight, cotangent, *turns, length, 0
    )
    residual = inputs32 + attn_add
    factor_two = rms_scale(residual)
    normed_two = residual * factor_two
    rows_two = (normed_two * gain_moe).astype(jnp.bfloat16)
    router_probs = softmax_rows(jnp.dot(rows_two, router, preferred_element_type=jnp.float32))
    route_hot = (routes[:, :, None] == jnp.arange(expert_count, dtype=jnp.int32)[None, None, :]).astype(
        jnp.float32
    )
    picked = jnp.sum(route_hot * router_probs[:, None, :], axis=-1)
    total = jnp.sum(picked, axis=1, keepdims=True)
    gates = picked / total
    named = jnp.sum(route_hot, axis=1)
    gate_table = jnp.where(named > 0.5, jnp.sum(route_hot * gates[:, :, None], axis=1), -1.0)
    all_rows, partial_out, partial_rows, token_grads, *units = experts(
        rows_two,
        all_cots,
        jnp.broadcast_to(gate_table.T[:, None, :], (expert_count, 8, rows_dev)),
        gate_weight[0],
        up_weight[0],
        down_weight[0],
        length,
        capacity,
        1,
    )
    back_grads = token_grads[:, 0, :]
    cot32 = cotangent.astype(jnp.float32)
    grad_gates = jnp.sum(route_hot * back_grads.T[:, None, :], axis=-1)
    grad_picked = (grad_gates - jnp.sum(gates * grad_gates, axis=1, keepdims=True)) / total
    grad_probs = jnp.sum(route_hot * grad_picked[:, :, None], axis=1)
    grad_logits = (
        router_probs * (grad_probs - jnp.sum(grad_probs * router_probs, axis=-1, keepdims=True))
    ).astype(jnp.bfloat16)
    grad_sum, all_logits, grad_wg, grad_wu, grad_wd = reduce_rows(
        partial_rows,
        grad_logits.T,
        *[unit.reshape(-1, unit.shape[-1]) for unit in units],
        length,
        2,
    )
    grad_router = mix("btd,bet->de", all_rows, all_logits)
    grad_rows_two = grad_sum + jnp.dot(grad_logits, router.T, preferred_element_type=jnp.float32)
    grad_res_norm, grad_gain_moe = row_norm_back(grad_rows_two, normed_two, factor_two, gain_moe)
    grad_residual = cot32 + grad_res_norm
    grad_attn = grad_residual.astype(jnp.bfloat16)
    grad_rows_one, grad_joint, grad_wo, moe_sum, grad_qgain, grad_kgain = attend_back(
        grad_attn,
        group_rows,
        full_joint,
        full_output,
        projected,
        attn_heads,
        partial_out,
        *turns,
        length,
        3,
    )
    output = (residual + moe_sum).astype(jnp.bfloat16)
    grad_in_norm, grad_gain_attn = row_norm_back(grad_rows_one, normed_one, factor_one, gain_attn)
    grad_input = grad_residual + grad_in_norm
    small = jnp.concatenate([grad_gain_attn, grad_gain_moe, grad_qgain[0], grad_kgain[0]]).reshape(-1, 128)
    small = jnp.pad(small, ((0, -small.shape[0] % 8), (0, 0)))
    sums = share_sum(small, length, 4).reshape(-1)
    head_dim = query_gain.shape[0]
    return (
        output,
        grad_input,
        grad_joint[:, :query_cols],
        grad_joint[:, query_cols : query_cols + key_cols],
        grad_joint[:, query_cols + key_cols :],
        grad_wo,
        sums[:width],
        sums[width : 2 * width],
        sums[2 * width : 2 * width + head_dim],
        sums[2 * width + head_dim : 2 * width + 2 * head_dim],
        grad_router,
        grad_wg[None],
        grad_wu[None],
        grad_wd[None],
    )


def solution(mesh):
    placed = (
        P(("dp", "tensor"), None),
        P("dp", None),
        P(("dp", "tensor"), None),
        P("dp", "tensor"),
        P("dp", "tensor"),
        P("dp", "tensor"),
        P("tensor", "dp"),
        P(),
        P(),
        P(),
        P(),
        P(),
        P(("dp", "tensor"), None, None),
        P(("dp", "tensor"), None, None),
        P(("dp", "tensor"), None, None),
        P(("dp", "tensor"), None),
    )
    program = gathered if mesh.shape["dp"] == 8 and mesh.shape["tensor"] <= 4 else shards
    return jax.shard_map(
        program,
        mesh=mesh,
        in_specs=placed,
        out_specs=(
            P(("dp", "tensor"), None),
            P(("dp", "tensor"), None),
            P("dp", "tensor"),
            P("dp", "tensor"),
            P("dp", "tensor"),
            P("tensor", "dp"),
            P(),
            P(),
            P(),
            P(),
            P(),
            P(("dp", "tensor"), None, None),
            P(("dp", "tensor"), None, None),
            P(("dp", "tensor"), None, None),
        ),
        check_vma=False,
    )
```

```python
import math

import jax
import jax.numpy as jnp
from jax import lax
from jax.experimental import pallas as pl
from jax.experimental.pallas import tpu as pltpu
from jax.sharding import PartitionSpec as P

EPSILON = 1e-06
THETA_BASE = 1000000.0
NEG_BIG = -1e30


MESH = pl.DeviceIdType.MESH


class Place:
    def __init__(self, length):
        self.length = length
        self.dp = lax.axis_index("dp")
        self.z = lax.axis_index("tensor")
        core, along_x, along_y = self.dp % 2, (self.dp // 2) % 2, self.dp // 4
        self.to_core = 1 - 2 * core
        self.core = self.dp + self.to_core
        self.x = self.dp + 2 - 4 * along_x
        self.y = self.dp + 4 - 8 * along_y
        self.columns = (self.dp, self.x, self.y, self.x + self.y - self.dp)

    def device(self, kind):
        if kind == "x":
            return (self.x, self.z)
        if kind == "y":
            return (self.y, self.z)
        if kind == "core":
            return (self.core, self.z)
        if kind == "up":
            return (self.dp, self.z + 1)
        return (self.dp, self.z - 1)

    @property
    def has_up(self):
        return self.z < self.length - 1

    @property
    def has_down(self):
        return self.z > 0

    def condition(self, kind):
        if kind == "up":
            return self.has_up
        return self.has_down if kind == "down" else None

    def nearest(self, turn):
        length = self.length

        def equal(left, right):
            far = 2 * length
            return (left - right + far) // far - (left - right - 1 + far) // far

        found = 0
        for mine in range(length):
            order = sorted(range(length), key=lambda other: (abs(other - mine), other))
            for step, other in enumerate(order):
                if other:
                    found = found + equal(self.z, mine) * equal(turn, step) * other
        return found

    def target(self, turn):
        length, z = self.length, self.z

        def at_least(left, right):
            return (left - right + 2 * length) // (2 * length)

        high = at_least(z, length // 2)
        mirrored = z + high * (length - 1 - 2 * z)
        above = length - 1 - mirrored
        first = at_least(above - 1, turn)
        if turn == length - 1:
            return z
        found = first * (length - 1 - turn) + (1 - first) * (turn - above)
        return found + high * (length - 1 - 2 * found)


def piece(rows, h):
    return pl.ds(0, rows) if h is None else pl.ds(h * (rows // 2), rows // 2)


def guarded(condition, action):
    if condition is None:
        action()
    else:
        pl.when(condition)(action)


def meet(place, over_z, over_dp):
    barrier = pltpu.get_barrier_semaphore()
    kinds = (("x", "y", "core") if over_dp else ()) + (("up", "down") if over_z else ())
    for kind in kinds:

        def greet(kind=kind):
            pl.semaphore_signal(
                barrier, 1, device_id=place.device(kind), device_id_type=MESH
            )

        guarded(place.condition(kind), greet)
    count = 3 if over_dp else 0
    if over_z:
        length = place.length
        count = count + (place.z + length - 1) // length + (2 * length - 2 - place.z) // length
    pl.semaphore_wait(barrier, count)


def other_device(place, distance):
    there = lax.rem(place.dp * place.length + place.z + distance, 8 * place.length)
    return (there // place.length, lax.rem(there, place.length)), there


def meet_all(place):
    barrier = pltpu.get_barrier_semaphore()
    others = 8 * place.length - 1

    def greet(n, carry):
        device, _ = other_device(place, n + 1)
        pl.semaphore_signal(barrier, 1, device_id=device, device_id_type=MESH)
        return carry

    lax.fori_loop(0, others, greet, 0)
    pl.semaphore_wait(barrier, others)


class Sends:
    def __init__(self, place):
        self.place = place
        self.started = []

    def start(self, kind, views, condition=lambda: None):
        def build():
            source, target, send_sem, recv_sem = views()
            return pltpu.make_async_remote_copy(
                src_ref=source,
                dst_ref=target,
                send_sem=send_sem,
                recv_sem=recv_sem,
                device_id=self.place.device(kind),
                device_id_type=MESH,
            )

        guarded(self.place.condition(kind), lambda: build().start())
        self.started.append((condition, kind, build))

    def drain(self):
        for condition, kind, build in self.started:

            def finish(kind=kind, build=build):
                guarded(self.place.condition(kind), lambda: build().wait_send())

            guarded(condition(), finish)


class GatherItem:
    def __init__(self, mode, place, own, slot, recv, send, local):
        self.mode, self.place = mode, place
        self.own, self.slot = own, slot
        self.recv, self.send, self.local = recv, send, local
        self.over_z = mode != "dp"
        self.over_dp = mode != "z"
        self.length = place.length if self.over_z else 1
        self.z = place.z if self.over_z else 0

    def index(self, column, z):
        if self.mode == "all":
            return column * self.length + z
        return column if self.mode == "dp" else z

    @staticmethod
    def semaphores(mode, length):
        blocks = {"all": 8 * length, "dp": 8, "z": length}[mode]
        turns = 2 * length - 1 if mode != "dp" else 1
        return [
            pltpu.SemaphoreType.DMA((blocks, 2)),
            pltpu.SemaphoreType.DMA((10, turns, 2)),
            pltpu.SemaphoreType.DMA((2,)),
        ]

    def turns(self, distance):
        if distance == 0:
            return [(0, 0, lambda: None, None)]
        place, length = self.place, self.length
        return [
            (2 * distance - 1, -distance, lambda: place.z >= distance, "up"),
            (2 * distance, distance, lambda: place.z < length - distance, "down"),
        ]

    def pass_on(self, sends, lane, kind, column, offset, turn, h, source=None, condition=lambda: None):
        at = 0 if h is None else h

        def views():
            z = self.z + offset
            view = self.slot(column, z, h)
            return (
                view if source is None else source(h),
                view,
                self.send.at[lane, turn, at],
                self.recv.at[self.index(column, z), at],
            )

        sends.start(kind, views, condition)

    def arrived(self, column, z, h):
        view = self.slot(column, z, h)
        at = 0 if h is None else h
        pltpu.make_async_copy(view, view, self.recv.at[self.index(column, z), at]).wait()

    def local_copy(self):
        return pltpu.make_async_copy(
            self.own(None), self.slot(self.place.dp, self.z, None), self.local.at[0]
        )

    def begin(self, sends):
        place = self.place
        if self.over_z:
            self.pass_on(sends, 0, "up", place.dp, 0, 0, None, self.own)
            self.pass_on(sends, 1, "down", place.dp, 0, 0, None, self.own)
        if self.over_dp:
            self.pass_on(sends, 2, "x", place.dp, 0, 0, None, self.own)
            self.pass_on(sends, 3, "y", place.dp, 0, 0, None, self.own)
            self.pass_on(sends, 4, "core", place.dp, 0, 0, None, self.own)
        self.local_copy().start()

    def along_z(self, sends, distance):
        if not self.over_z or distance >= self.length:
            return
        place = self.place
        for turn, offset, condition, onward in self.turns(distance):

            def step(turn=turn, offset=offset, condition=condition, onward=onward):
                self.arrived(place.dp, self.z + offset, None)
                lanes = []
                if distance < self.length - 1:
                    lanes.append((0 if onward == "up" else 1, onward))
                if self.over_dp:
                    lanes += [(2, "x"), (3, "y"), (4, "core")]
                for lane, kind in lanes:
                    self.pass_on(
                        sends, lane, kind, place.dp, offset, turn, None, condition=condition
                    )

            guarded(condition(), step)

    def across(self, sends, distance):
        if not self.over_dp or not 0 <= distance < self.length:
            return
        _, x, y, _ = self.place.columns
        for turn, offset, condition, _ in self.turns(distance):

            def step(turn=turn, offset=offset, condition=condition):
                self.arrived(x, self.z + offset, None)
                self.pass_on(sends, 5, "y", x, offset, turn, 0, condition=condition)
                self.pass_on(sends, 7, "core", x, offset, turn, None, condition=condition)
                self.arrived(y, self.z + offset, None)
                self.pass_on(sends, 6, "x", y, offset, turn, 1, condition=condition)
                self.pass_on(sends, 8, "core", y, offset, turn, None, condition=condition)

            guarded(condition(), step)

    def diagonal(self, sends, distance):
        if not self.over_dp or not 0 <= distance < self.length:
            return
        corner = self.place.columns[3]
        for turn, offset, condition, _ in self.turns(distance):

            def step(turn=turn, offset=offset, condition=condition):
                for h in range(2):
                    self.arrived(corner, self.z + offset, h)
                    self.pass_on(sends, 9, "core", corner, offset, turn, h, condition=condition)

            guarded(condition(), step)

    def settled(self):
        self.local_copy().wait()

    def from_core(self, z):
        for number, column in enumerate(self.place.columns):
            for h in (0, 1) if number == 3 else (None,):
                self.arrived(column + self.place.to_core, z, h)

    def finish(self):
        self.settled()
        if self.over_dp:
            for z in range(self.length):
                self.from_core(z)


class ReduceItem:
    def __init__(self, mode, place, block, bufs, out):
        self.mode, self.place, self.block, self.out = mode, place, block, out
        self.over_z = mode != "dp"
        self.over_dp = mode != "z"
        self.length = place.length if self.over_z else 1
        (self.acc, self.from_core, self.corner, self.from_xy, self.from_z,
         self.load, self.send, self.recv) = bufs

    @staticmethod
    def scratch(mode, length, rows, width, in_place=False):
        t = length if mode != "dp" else 1
        columns = 4 if mode != "z" else 1
        dp = mode != "z"
        small = (8, 128)
        return [
            pltpu.VMEM(small if in_place else (columns, t, rows, width), jnp.bfloat16),
            pltpu.VMEM((columns, t, rows, width) if dp else small, jnp.bfloat16),
            pltpu.VMEM((2, t, rows // 2, width) if dp else small, jnp.bfloat16),
            pltpu.VMEM((2, t, rows, width) if dp else small, jnp.bfloat16),
            pltpu.VMEM((t + 1, rows, width) if mode != "dp" else small, jnp.bfloat16),
            pltpu.SemaphoreType.DMA((columns, t)),
            pltpu.SemaphoreType.DMA((10, t, 2)),
            pltpu.SemaphoreType.DMA((9, t + 1, 2)),
        ]

    def z_of(self, turn):
        return self.place.target(turn) if self.over_z else 0

    def got(self, ref, lane, turn, h=0):
        pltpu.make_async_copy(ref, ref, self.recv.at[lane, turn, h]).wait()

    computed = False
    in_place = False

    def partial(self, column, turn, h):
        if self.in_place:
            return self.block(self.place.columns[column], self.z_of(turn), h)
        return self.acc.at[column, turn, piece(self.acc.shape[2], h)]

    def add(self, target, refs, out=None):
        rows = target.shape[0]
        step = 16 if rows % 16 == 0 else rows
        place = target if out is None else out

        def body(i, carry):
            at = pl.ds(pl.multiple_of(i * step, step), step)
            total = target[at, :].astype(jnp.float32)
            for ref in refs:
                total = total + ref[at, :].astype(jnp.float32)
            place[at, :] = total.astype(place.dtype)
            return carry

        lax.fori_loop(0, rows // step, body, 0, unroll=2 if (rows // step) % 2 == 0 else 1)

    def begin(self):
        place = self.place
        if self.over_z:

            @pl.when((place.z == 0) | (place.z == self.length - 1))
            def _():
                def clear(i, carry):
                    self.from_z[i] = jnp.zeros(self.from_z.shape[1:], jnp.bfloat16)
                    return carry

                lax.fori_loop(0, self.length + 1, clear, 0)

    def load_all(self):
        place = self.place
        for turn in range(self.length):
            for column in (3, 1, 2, 0) if self.over_dp else (0,):
                pltpu.make_async_copy(
                    self.block(place.columns[column], self.z_of(turn), None),
                    self.acc.at[column, turn],
                    self.load.at[column, turn],
                ).start()

    def hand_over(self, sends, turn):
        if not self.over_dp or turn >= self.length:
            return
        place = self.place
        for column in (3, 1, 2, 0):
            sends.start(
                "core",
                lambda column=column: (
                    self.block(place.columns[column] + place.to_core, self.z_of(turn), None),
                    self.from_core.at[column, turn],
                    self.send.at[column, turn, 0],
                    self.recv.at[column, turn, 0],
                ),
            )

    def ready(self, column, turn):
        if not (self.computed or self.in_place):
            ref = self.acc.at[column, turn]
            pltpu.make_async_copy(ref, ref, self.load.at[column, turn]).wait()
        if self.over_dp:
            self.got(self.from_core.at[column, turn], column, turn)

    def settle(self, column, turn, h, extra=(), out=None):
        refs = list(extra)
        if self.over_dp:
            rows = self.from_core.shape[2]
            refs.append(self.from_core.at[column, turn, piece(rows, h)])
        if refs or out is not None:
            self.add(self.partial(column, turn, h), refs, out)

    def corners(self, sends, turn):
        if not self.over_dp or not 0 <= turn < self.length:
            return
        self.ready(3, turn)
        for h, kind in ((0, "y"), (1, "x")):
            self.settle(3, turn, h)
            sends.start(
                kind,
                lambda h=h: (
                    self.partial(3, turn, h),
                    self.corner.at[h, turn],
                    self.send.at[4, turn, h],
                    self.recv.at[4, turn, h],
                ),
            )

    def straight(self, sends, turn, second):
        if not self.over_dp or not 0 <= turn < self.length:
            return
        rows = self.from_xy.shape[2]
        for column, kind in ((1, "x"), (2, "y")):
            h = (column - 1) if second else (2 - column)
            extra = ()
            if second:
                ref = self.corner.at[h, turn]
                self.got(ref, 4, turn, h)
                extra = (ref,)
            else:
                self.ready(column, turn)
            self.settle(column, turn, h, extra)
            sends.start(
                kind,
                lambda column=column, h=h: (
                    self.partial(column, turn, h),
                    self.from_xy.at[column - 1, turn, piece(rows, h)],
                    self.send.at[4 + column, turn, h],
                    self.recv.at[4 + column, turn, h],
                ),
            )

    def home(self, sends, turn):
        if not 0 <= turn < self.length:
            return
        place = self.place
        last = turn == self.length - 1
        z = self.z_of(turn)
        extra = []
        self.ready(0, turn)
        if self.over_dp:
            for lane in (0, 1):
                rows = self.from_xy.shape[2]
                for h in range(2):
                    self.got(self.from_xy.at[lane, turn, piece(rows, h)], 5 + lane, turn, h)
                extra.append(self.from_xy.at[lane, turn])
        if self.over_z:

            def got_slot():
                self.got(self.from_z.at[z], 7, z)

            def got_other():
                self.got(self.from_z.at[self.length], 7, self.length)

            extra.append(self.from_z.at[z])
            if last:
                guarded(place.has_down, got_slot)
                guarded(place.has_up, got_other)
                extra.append(self.from_z.at[self.length])
            else:
                guarded((z > place.z) & place.has_down, got_slot)
                guarded((z < place.z) & place.has_up, got_slot)
        self.settle(0, turn, None, extra, self.out(None) if last else None)
        if self.over_z and not last:

            def going_up():
                goal = self.z_of(turn)
                return (
                    self.partial(0, turn, None),
                    self.from_z.at[goal],
                    self.send.at[7, turn, 0],
                    self.recv.at[7, goal, 0],
                )

            def going_down():
                there = self.z_of(turn)
                arrives = (there - place.z + 1 + self.length) // self.length
                goal = there + arrives * (self.length - there)
                return (
                    self.partial(0, turn, None),
                    self.from_z.at[goal],
                    self.send.at[7, turn, 0],
                    self.recv.at[7, goal, 0],
                )

            def above():
                return self.z_of(turn) > place.z

            def below():
                return self.z_of(turn) < place.z

            pl.when(above())(lambda: sends.start("up", going_up, above))
            pl.when(below())(lambda: sends.start("down", going_down, below))


def advance(item, sends, step):
    item.corners(sends, step)
    item.straight(sends, step, False)
    item.hand_over(sends, step + 2)
    item.straight(sends, step - 1, True)
    item.home(sends, step - 2 if item.over_dp else step)


def reduce_rows(partials, small, all_rows, picked, gated, hid, dgate, dup, length, collective_id):
    devices, rows, width = partials.shape
    slots, hidden = dup.shape
    half, low = rows // 2, small.shape[0] // 2
    tile, narrow = width // 4, hidden // 3
    f32, bf16 = jnp.float32, jnp.bfloat16

    def kernel(
        source, small_ref, all_ref, picked_ref, gated_ref, hid_ref, dgate_ref, dup_ref,
        target, product, out_g, out_u, out_d,
        small_all, rows_v, rows_sem, hid_v, dgate_v, dup_v, picked_v, gated_v, tile_g, tile_u, tile_d, load_sem, tile_sem, store_sem,
        *rest,
    ):
        place = Place(length)
        item = ReduceItem(
            "all",
            place,
            lambda c, z, h: source.at[c * length + z, piece(2 * half, h)],
            rest[:8],
            lambda h: target.at[piece(2 * half, h)],
        )
        beside = GatherItem("all", place, None, None, *rest[8:])
        beside.own = lambda h: small_ref.at[piece(2 * low, h)]
        beside.slot = lambda c, z, h: small_all.at[c * length + z, piece(2 * low, h)]
        item.begin()
        meet(place, True, True)
        sends = Sends(place)
        beside.begin(sends)
        item.load_all()
        item.hand_over(sends, 0)
        item.hand_over(sends, 1)
        resident = [
            pltpu.make_async_copy(left, right, load_sem.at[n])
            for n, (left, right) in enumerate(
                ((hid_ref, hid_v), (dgate_ref, dgate_v), (dup_ref, dup_v))
            )
        ]
        for copy in resident:
            copy.start()

        def lanes_of(n):
            return pl.ds(pl.multiple_of(n * tile, tile), tile)

        def tiles(n, slot):
            return [
                pltpu.make_async_copy(picked_ref.at[:, lanes_of(n)], picked_v.at[slot], tile_sem.at[slot, 0]),
                pltpu.make_async_copy(gated_ref.at[:, lanes_of(n)], gated_v.at[slot], tile_sem.at[slot, 1]),
            ]

        def stores(n, slot):
            return [
                pltpu.make_async_copy(tile_g.at[slot], out_g.at[lanes_of(n)], store_sem.at[slot, 0]),
                pltpu.make_async_copy(tile_u.at[slot], out_u.at[lanes_of(n)], store_sem.at[slot, 1]),
                pltpu.make_async_copy(tile_d.at[slot], out_d.at[:, lanes_of(n)], store_sem.at[slot, 2]),
            ]

        for copy in tiles(0, 0):
            copy.start()

        def rows_load(group, part):
            return pltpu.make_async_copy(
                all_ref.at[pl.ds(group * length, length)], rows_v.at[part], rows_sem.at[part]
            )

        for part in range(2):
            rows_load(part, part).start()

        def narrow_of(m):
            return pl.ds(pl.multiple_of(m * narrow, narrow), narrow)

        def turn_of(i, carry):
            for step in range(length + 2):

                @pl.when(i == 2 * step)
                def _(step=step):
                    item.corners(sends, step)
                    item.straight(sends, step, False)
                    item.hand_over(sends, step + 2)

                @pl.when(i == 2 * step + 1)
                def _(step=step):
                    item.straight(sends, step - 1, True)
                    item.home(sends, step - 2)

            for step in range(length + 2):

                @pl.when(i == step)
                def _(step=step):
                    beside.along_z(sends, step + 1)
                    beside.across(sends, step)
                    beside.diagonal(sends, step - 1)

            @pl.when(i == length + 2)
            def _():
                beside.finish()
                product[...] = jnp.zeros(product.shape, f32)

            @pl.when((i >= length + 2) & (i < length + 6))
            def _():
                for part in range(2):
                    group = 2 * (i - length - 2) + part
                    rows_load(group, part).wait()
                    marks = [
                        small_all[group * length + z] for z in range(length)
                    ]
                    left = jnp.concatenate(marks, axis=1)

                    def body(m, carry, part=part, left=left):
                        lanes = pl.ds(pl.multiple_of(m * tile, tile), tile)
                        right = rows_v[part, :, :, lanes].reshape(length * rows, tile)
                        product[:, lanes] += dot(left, right)
                        return carry

                    lax.fori_loop(0, 4, body, 0)

                    @pl.when(group + 2 < 8)
                    def _(part=part, group=group):
                        rows_load(group + 2, part).start()

            n, kind = i // 3, i % 3
            slot = n % 2

            @pl.when(i == 0)
            def _():
                for copy in resident:
                    copy.wait()

            @pl.when((kind == 0) & (n < 4))
            def _():
                for copy in tiles(n, slot):
                    copy.wait()

                @pl.when(n < 3)
                def _():
                    for copy in tiles(n + 1, 1 - slot):
                        copy.start()

                @pl.when(n >= 2)
                def _():
                    for copy in stores(n, slot):
                        copy.wait()

                def body(m, carry):
                    tile_g[slot, :, narrow_of(m)] = dot(picked_v[slot], dgate_v[:, narrow_of(m)], 0, 0)
                    return carry

                lax.fori_loop(0, 3, body, 0)
                stores(n, slot)[0].start()

            @pl.when((kind == 1) & (n < 4))
            def _():
                def body(m, carry):
                    tile_u[slot, :, narrow_of(m)] = dot(picked_v[slot], dup_v[:, narrow_of(m)], 0, 0)
                    return carry

                lax.fori_loop(0, 3, body, 0)
                stores(n, slot)[1].start()

            @pl.when((kind == 2) & (n < 4))
            def _():
                def body(m, carry):
                    tile_d[slot, narrow_of(m), :] = dot(hid_v[:, narrow_of(m)], gated_v[slot], 0, 0)
                    return carry

                lax.fori_loop(0, 3, body, 0)
                stores(n, slot)[2].start()

            return carry

        lax.fori_loop(0, max(12, 2 * (length + 2), length + 6), turn_of, 0)
        for slot in range(2):
            for copy in stores(slot, slot):
                copy.wait()
        sends.drain()

    any_spec = pl.BlockSpec(memory_space=pl.ANY)
    shape = jax.ShapeDtypeStruct
    sems = pltpu.SemaphoreType.DMA
    return pl.pallas_call(
        kernel,
        name="reduce_rows",
        out_shape=[
            shape((rows, width), f32),
            shape((small.shape[0], width), f32),
            shape((width, hidden), f32),
            shape((width, hidden), f32),
            shape((hidden, width), f32),
        ],
        in_specs=[any_spec] * 8,
        out_specs=[pl.BlockSpec(memory_space=pltpu.VMEM)] * 2 + [any_spec] * 3,
        scratch_shapes=[
            pltpu.VMEM((devices,) + small.shape, small.dtype),
            pltpu.VMEM((2, length, rows, width), bf16),
            sems((2,)),
            pltpu.VMEM((slots, hidden), bf16),
            pltpu.VMEM((slots, hidden), bf16),
            pltpu.VMEM((slots, hidden), bf16),
            pltpu.VMEM((2, slots, tile), bf16),
            pltpu.VMEM((2, slots, tile), bf16),
            pltpu.VMEM((2, tile, hidden), f32),
            pltpu.VMEM((2, tile, hidden), f32),
            pltpu.VMEM((2, hidden, tile), f32),
            sems((3,)),
            sems((2, 2)),
            sems((2, 3)),
        ]
        + ReduceItem.scratch("all", length, rows, width)
        + GatherItem.semaphores("all", length),
        compiler_params=pltpu.CompilerParams(
            collective_id=collective_id, has_side_effects=True, vmem_limit_bytes=67043328
        ),
    )(partials, small, all_rows, picked, gated, hid, dgate, dup)


def dot(left, right, left_dim=1, right_dim=0):
    return lax.dot_general(
        left, right, (((left_dim,), (right_dim,)), ((), ())), preferred_element_type=jnp.float32
    )


def experts(rows_own, all_cots, gates_own, wgate, wup, wdown, length, capacity, collective_id):
    rows, width = rows_own.shape
    hidden = wgate.shape[1]
    devices = 8 * length
    count = 4 * capacity
    tile = 512 if width % 512 == 0 else width
    narrow = 256 if hidden % 256 == 0 else hidden
    f32, bf16 = jnp.float32, jnp.bfloat16

    def kernel(
        rows_ref, all_cots, gates_ref, wg_ref, wu_ref, wd_ref,
        all_rows, part_out, part_grad, token_in, picked_all, gated_all, hid_all, dgate_all, dup_all,
        wg, wu, wd, chosen_all, gates_all, rank_v, table, row_buf, cot_buf, picked, cotan, gated, hid, dgate, dup, scaled, back,
        chosen, slot_gate, slot_sum, stage_out, stage_grad, token_out,
        recv_r, send_r, local_r,
        load_sem, store_sem, save_sem, token_sem, gate_sem, weight_sem,
    ):
        place = Place(length)
        expert = place.dp * length + place.z

        def item_of(source, target, sems, half):
            item = GatherItem("all", place, None, None, *sems)
            item.own = lambda h: source.at[piece(2 * half, h)]
            item.slot = lambda column, z, h: target.at[
                column * length + z, piece(2 * half, h)
            ]
            return item

        big = [
            item_of(rows_ref, all_rows, (recv_r, send_r, local_r), rows // 2),
        ]
        items = big
        meet_all(place)
        sends = Sends(place)

        def gate_send(n):
            device, there = other_device(place, n + 1)
            return pltpu.make_async_remote_copy(
                src_ref=gates_ref.at[there],
                dst_ref=table.at[expert],
                send_sem=gate_sem.at[0],
                recv_sem=gate_sem.at[1],
                device_id=device,
                device_id_type=MESH,
            )

        def send_gates(n, carry):
            gate_send(n).start()
            return carry

        lax.fori_loop(0, devices - 1, send_gates, 0)
        pltpu.make_async_copy(gates_ref.at[expert], table.at[expert], gate_sem.at[1]).start()
        for item in items:
            item.begin(sends)

        weights = [
            pltpu.make_async_copy(source, target, weight_sem.at[n])
            for n, (source, target) in enumerate(((wg_ref, wg), (wu_ref, wu), (wd_ref, wd)))
        ]
        for copy in weights:
            copy.start()

        def along(distance):
            for item in items:
                item.along_z(sends, distance)

        def across(distance):
            for item in items:
                item.across(sends, distance)

        def corner(distance):
            for item in items:
                item.diagonal(sends, distance)

        across(0)
        along(1)
        pltpu.make_async_copy(table, table, gate_sem.at[1]).wait()
        order = lax.broadcasted_iota(jnp.int32, (rows, rows), 0)
        upto = (order <= lax.broadcasted_iota(jnp.int32, (rows, rows), 1)).astype(f32).astype(bf16)
        slots = lax.broadcasted_iota(jnp.int32, (capacity, rows), 0).astype(f32)
        lines = table[:, 0, :]
        rank_v[...] = dot((lines >= 0.0).astype(f32).astype(bf16), upto) - 1.0

        def choose(block, carry):
            line = table[block, 0:1, :]
            ranks = rank_v[pl.ds(block, 1), :]
            pick = jnp.where((line >= 0.0) & (ranks == slots), 1.0, 0.0)
            gate = jnp.sum(pick * line, axis=1, keepdims=True)
            chosen_all[block] = pick.astype(bf16)
            gates_all[block] = jnp.broadcast_to(gate, (capacity, 128))
            return carry

        lax.fori_loop(0, devices, choose, 0, unroll=4)
        for item in items:
            item.settled()

        def block_of(j, side, z):
            return (place.columns[j] + side * place.to_core) * length + z

        def load(j, side, z, slot):
            block = block_of(j, side, z)
            return [
                pltpu.make_async_copy(all_rows.at[block], row_buf.at[slot, j], load_sem.at[slot, 0, j]),
                pltpu.make_async_copy(all_cots.at[block], cot_buf.at[slot, j], load_sem.at[slot, 1, j]),
            ]

        def store(j, side, z, slot):
            block = block_of(j, side, z)
            return [
                pltpu.make_async_copy(stage_out.at[slot, j], part_out.at[block], store_sem.at[slot, 0, j]),
                pltpu.make_async_copy(stage_grad.at[slot, j], part_grad.at[block], store_sem.at[slot, 1, j]),
            ]

        def saved(i):
            first = [
                pltpu.make_async_copy(picked, picked_all.at[i], save_sem.at[0]),
                pltpu.make_async_copy(gated, gated_all.at[i], save_sem.at[1]),
            ]
            second = [
                pltpu.make_async_copy(hid, hid_all.at[i], save_sem.at[2]),
                pltpu.make_async_copy(dgate, dgate_all.at[i], save_sem.at[3]),
                pltpu.make_async_copy(dup, dup_all.at[i], save_sem.at[4]),
            ]
            return first, second

        def start_loads(step, side):
            for j in range(4):
                for copy in load(j, side, place.nearest(step), side):
                    copy.start()

        corner(0)
        for item in items:
            item.from_core(place.nearest(0))
        start_loads(0, 0)
        start_loads(0, 1)
        for copy in weights:
            copy.wait()

        def unit(i, carry):
            turn, side = i // 2, i % 2
            z = place.nearest(turn)

            @pl.when(i == 1)
            def _():
                along(2)
                across(1)

            for step in range(1, length):

                @pl.when(i == max(2, 2 * step - 1))
                def _(step=step):
                    corner(step)
                    along(step + 2)
                    across(step + 1)
                    for item in items:
                        item.from_core(place.nearest(step))
                    start_loads(step, 0)
                    if step == 1:
                        start_loads(step, 1)

            @pl.when(i >= 1)
            def _():
                for copy in saved(i)[0]:
                    copy.wait()

            for j in range(4):
                for copy in load(j, side, z, side):
                    copy.wait()
            for j in range(4):
                block = block_of(j, side, z)
                chosen[j] = chosen_all[block]
                slot_gate[pl.ds(j * capacity, capacity), :] = gates_all[block]

            def select(n, carry):
                lanes = pl.ds(pl.multiple_of(n * tile, tile), tile)
                for j in range(4):
                    at = pl.ds(j * capacity, capacity)
                    picked[at, lanes] = dot(chosen[j], row_buf[side, j, :, lanes]).astype(bf16)
                    cot = dot(chosen[j], cot_buf[side, j, :, lanes])
                    cotan[at, lanes] = cot.astype(bf16)
                    gated[at, lanes] = (slot_gate[at, 0:1] * cot).astype(bf16)
                return carry

            lax.fori_loop(0, width // tile, select, 0)

            for copy in saved(i)[0]:
                copy.start()
            for step in range(2, length):

                @pl.when(i == 2 * step - 1)
                def _(step=step):
                    start_loads(step, 1)

            @pl.when(i >= 1)
            def _():
                for copy in saved(i)[1]:
                    copy.wait()

            def middle(n, carry):
                lanes = pl.ds(pl.multiple_of(n * narrow, narrow), narrow)
                gate = dot(picked[...], wg[:, lanes])
                up = dot(picked[...], wu[:, lanes])
                grad = dot(gated[...], wd[lanes, :], 1, 1)
                sigma = jax.nn.sigmoid(gate)
                hid[:, lanes] = (gate * sigma * up).astype(bf16)
                dgate[:, lanes] = (grad * up * sigma * (1.0 + gate * (1.0 - sigma))).astype(bf16)
                dup[:, lanes] = (grad * gate * sigma).astype(bf16)
                return carry

            lax.fori_loop(0, hidden // narrow, middle, 0)
            for copy in saved(i)[1]:
                copy.start()
            slot_sum[...] = jnp.zeros(slot_sum.shape, f32)

            @pl.when(i >= 2)
            def _():
                for j in range(4):
                    for copy in store(j, side, z, side):
                        copy.wait()

            def outward(n, carry):
                lanes = pl.ds(pl.multiple_of(n * tile, tile), tile)
                result = dot(hid[...], wd[:, lanes]).astype(bf16).astype(f32)
                products = cotan[:, lanes].astype(f32) * result
                total = products[:, 0:128]
                for k in range(1, tile // 128):
                    total = total + products[:, 128 * k : 128 * (k + 1)]
                slot_sum[...] += total
                scaled[:, lanes] = (slot_gate[:, 0:1] * result).astype(bf16)
                back[:, lanes] = (
                    dot(dgate[...], wg[lanes, :], 1, 1) + dot(dup[...], wu[lanes, :], 1, 1)
                ).astype(bf16)
                for j in range(4):
                    at = pl.ds(j * capacity, capacity)
                    stage_out[side, j, :, lanes] = dot(chosen[j], scaled[at, lanes], 0, 0).astype(bf16)
                    stage_grad[side, j, :, lanes] = dot(chosen[j], back[at, lanes], 0, 0).astype(bf16)
                return carry

            lax.fori_loop(0, width // tile, outward, 0)
            for j in range(4):
                for copy in store(j, side, z, side):
                    copy.start()
            total = jnp.sum(slot_sum[...], axis=1, keepdims=True).reshape(4, capacity, 1)
            sums = jnp.sum(chosen[...].astype(f32) * total, axis=1)
            for j in range(4):
                token_out[block_of(j, side, z)] = jnp.broadcast_to(sums[j : j + 1], (8, rows))
            return carry

        lax.fori_loop(0, 2 * length, unit, 0)

        def token_send(n):
            device, there = other_device(place, n + 1)
            return pltpu.make_async_remote_copy(
                src_ref=token_out.at[there],
                dst_ref=token_in.at[expert],
                send_sem=token_sem.at[0],
                recv_sem=token_sem.at[1],
                device_id=device,
                device_id_type=MESH,
            )

        def send(n, carry):
            token_send(n).start()
            return carry

        lax.fori_loop(0, devices - 1, send, 0)
        pltpu.make_async_copy(token_out.at[expert], token_in.at[expert], token_sem.at[1]).start()
        for side in range(2):
            for j in range(4):
                for copy in store(j, side, 0, side):
                    copy.wait()
        for copies in saved(0):
            for copy in copies:
                copy.wait()
        sends.drain()
        pltpu.make_async_copy(token_out, token_in, token_sem.at[1]).wait()
        sent = token_out.at[pl.ds(0, devices - 1)]
        pltpu.make_async_copy(sent, sent, token_sem.at[0]).wait()
        pltpu.make_async_copy(sent, sent, gate_sem.at[0]).wait()

    any_spec = pl.BlockSpec(memory_space=pl.ANY)
    vmem = pl.BlockSpec(memory_space=pltpu.VMEM)
    big = (devices, rows, width)
    shape = jax.ShapeDtypeStruct
    sems = pltpu.SemaphoreType.DMA
    return pl.pallas_call(
        kernel,
        name="experts",
        out_shape=[
            shape(big, bf16), shape(big, bf16), shape(big, bf16),
            shape((devices, 8, rows), f32),
            shape((2 * length, count, width), bf16), shape((2 * length, count, width), bf16),
            shape((2 * length, count, hidden), bf16), shape((2 * length, count, hidden), bf16),
            shape((2 * length, count, hidden), bf16),
        ],
        in_specs=[any_spec] * 6,
        out_specs=[any_spec] * 3 + [vmem] + [any_spec] * 5,
        scratch_shapes=[
            pltpu.VMEM((width, hidden), bf16),
            pltpu.VMEM((width, hidden), bf16),
            pltpu.VMEM((hidden, width), bf16),
            pltpu.VMEM((devices, capacity, rows), bf16),
            pltpu.VMEM((devices, capacity, 128), f32),
            pltpu.VMEM((devices, rows), f32),
            pltpu.VMEM((devices, 8, rows), f32),
            pltpu.VMEM((2, 4, rows, width), bf16),
            pltpu.VMEM((2, 4, rows, width), bf16),
            pltpu.VMEM((count, width), bf16),
            pltpu.VMEM((count, width), bf16),
            pltpu.VMEM((count, width), bf16),
            pltpu.VMEM((count, hidden), bf16),
            pltpu.VMEM((count, hidden), bf16),
            pltpu.VMEM((count, hidden), bf16),
            pltpu.VMEM((count, width), bf16),
            pltpu.VMEM((count, width), bf16),
            pltpu.VMEM((4, capacity, rows), bf16),
            pltpu.VMEM((count, 128), f32),
            pltpu.VMEM((count, 128), f32),
            pltpu.VMEM((2, 4, rows, width), bf16),
            pltpu.VMEM((2, 4, rows, width), bf16),
            pltpu.VMEM((devices, 8, rows), f32),
        ]
        + GatherItem.semaphores("all", length)
        + [sems((2, 2, 4)), sems((2, 2, 4)), sems((5,)), sems((2,)), sems((2,)), sems((3,))],
        compiler_params=pltpu.CompilerParams(
            collective_id=collective_id, has_side_effects=True, vmem_limit_bytes=63 << 20
        ),
    )(rows_own, all_cots, gates_own, wgate, wup, wdown)


def rope(values, cosine, sine):
    return values * cosine + pltpu.roll(values, values.shape[-1] // 2, 1) * sine


def unrope(values, cosine, sine):
    return values * cosine - pltpu.roll(values, values.shape[-1] // 2, 1) * sine


def row_factor(values):
    return lax.rsqrt(jnp.mean(values * values, axis=-1, keepdims=True) + EPSILON)


def visible_pairs(seg_col, seg_row, start, stop, reach):
    shape = (stop - start, reach)
    query = lax.broadcasted_iota(jnp.int32, shape, 0) + start
    key = lax.broadcasted_iota(jnp.int32, shape, 1)
    return (seg_col[start:stop, :] == seg_row[:, 0:reach]) & (key <= query)


def attend(rows_own, joint_own, output_own, cots_own, seg_col, seg_row, cosine, sine, query_gain, key_gain, length, collective_id):
    rows, width = rows_own.shape
    depth, joint = joint_own.shape
    head_width, part = output_own.shape
    head = query_gain.shape[-1]
    heads = head_width // head
    tokens = rows * length
    block = tokens // 2
    tile = 512
    scale = 1.0 / math.sqrt(head)
    f32, bf16 = jnp.float32, jnp.bfloat16

    def kernel(
        rows_ref, joint_ref, output_ref, cots_ref, segc, segr, cos_ref, sin_ref, qgain, kgain,
        out_add, out_rows, out_joint, out_weight, out_cots, out_qkv, out_heads,
        rows_v, joint_v, weight_v, qkv, att, key_v, value_v,
        r0, r1, r2, r3, r4, r5, r6, r7,
        g0, g1, g2, j0, j1, j2, w0, w1, w2, c0, c1, c2, save_sem,
    ):
        place = Place(length)

        def item_of(mode, source, half, slot, sems):
            item = GatherItem(mode, place, None, None, *sems)
            item.own = lambda h: source.at[piece(2 * half, h)]
            item.slot = slot
            return item

        half, deep, tall = rows // 2, depth // 2, head_width // 2
        own_rows = item_of(
            "z", rows_ref, half, lambda c, z, h: rows_v.at[z, piece(2 * half, h)], (g0, g1, g2)
        )
        own_joint = item_of(
            "dp", joint_ref, deep, lambda c, z, h: joint_v.at[c, piece(2 * deep, h)], (j0, j1, j2)
        )
        own_weight = item_of(
            "dp",
            output_ref,
            tall,
            lambda c, z, h: weight_v.at[
                piece(2 * tall, h), pl.ds(pl.multiple_of(c * part, part), part)
            ],
            (w0, w1, w2),
        )
        cots = item_of(
            "all",
            cots_ref,
            half,
            lambda c, z, h: out_cots.at[c * length + z, piece(2 * half, h)],
            (c0, c1, c2),
        )
        total = ReduceItem(
            "z", place, None, (r0, r1, r2, r3, r4, r5, r6, r7),
            lambda h: out_add.at[piece(2 * half, h)],
        )
        total.computed = True
        total.begin()
        meet(place, True, True)
        sends = Sends(place)
        own_joint.begin(sends)
        own_rows.begin(sends)
        own_weight.begin(sends)
        own_joint.across(sends, 0)
        own_rows.along_z(sends, 1)
        own_weight.across(sends, 0)
        own_joint.diagonal(sends, 0)
        own_rows.along_z(sends, 2)
        cots.begin(sends)
        own_weight.diagonal(sends, 0)
        for distance in range(3, length):
            own_rows.along_z(sends, distance)
        own_joint.finish()
        own_rows.finish()

        def projection(n, carry):
            lanes = pl.ds(pl.multiple_of(n * 256, 256), 256)
            left = rows_v[...].reshape(tokens, width)
            right = joint_v[:, :, lanes].reshape(width, 256)
            qkv[:, lanes] = dot(left, right)
            return carry

        lax.fori_loop(0, joint // 256, projection, 0)
        saves = [
            pltpu.make_async_copy(source, target, save_sem.at[n])
            for n, (source, target) in enumerate(
                ((rows_v, out_rows), (joint_v, out_joint), (qkv, out_qkv), (weight_v, out_weight), (att, out_heads))
            )
        ]
        for copy in saves[:3]:
            copy.start()
        key = qkv[:, head_width : head_width + head]
        key_v[...] = rope(key * row_factor(key) * kgain[...], cos_ref[...], sin_ref[...]).astype(bf16)
        value_v[...] = qkv[:, head_width + head : head_width + 2 * head].astype(bf16)

        def one_head(n, carry):
            lanes = pl.ds(pl.multiple_of(n * head, head), head)
            for start in range(0, tokens, block):
                stop = start + block
                query = qkv[start:stop, lanes]
                turned = rope(
                    query * row_factor(query) * qgain[...], cos_ref[start:stop, :], sin_ref[start:stop, :]
                ).astype(bf16)
                scores = dot(turned, key_v[0:stop, :], 1, 1) * scale
                seen = visible_pairs(segc, segr, start, stop, stop)
                scores = jnp.where(seen, scores, NEG_BIG)
                top = jnp.max(scores, axis=-1, keepdims=True)
                powers = jnp.exp(scores - top)
                probs = (powers / jnp.sum(powers, axis=-1, keepdims=True)).astype(bf16)
                att[start:stop, lanes] = dot(probs, value_v[0:stop, :]).astype(bf16)
            return carry

        lax.fori_loop(0, heads // 2, one_head, 0)
        cots.across(sends, 0)
        cots.along_z(sends, 1)
        lax.fori_loop(heads // 2, heads, one_head, 0)
        saves[4].start()
        own_weight.finish()
        saves[3].start()

        def outward(turn):
            z = total.z_of(turn)

            def body(n, carry):
                lanes = pl.ds(pl.multiple_of(n * tile, tile), tile)
                left = att[pl.ds(pl.multiple_of(z * rows, rows), rows), :]
                found = dot(left, weight_v[:, lanes]).astype(bf16)
                total.acc[0, turn, :, lanes] = found
                return carry

            lax.fori_loop(0, width // tile, body, 0)

        for turn in range(length):
            outward(turn)
            total.home(sends, turn)
            cots.diagonal(sends, turn)
            cots.across(sends, turn + 1)
            cots.along_z(sends, turn + 2)
        cots.finish()
        for copy in saves:
            copy.wait()
        sends.drain()

    any_spec = pl.BlockSpec(memory_space=pl.ANY)
    vmem = pl.BlockSpec(memory_space=pltpu.VMEM)
    shape = jax.ShapeDtypeStruct
    return pl.pallas_call(
        kernel,
        name="attend",
        out_shape=[
            shape((rows, width), f32),
            shape((length, rows, width), bf16),
            shape((8, depth, joint), bf16),
            shape((head_width, 8 * part), bf16),
            shape((8 * length, rows, width), bf16),
            shape((tokens, joint), f32),
            shape((tokens, head_width), bf16),
        ],
        in_specs=[any_spec] * 4 + [vmem] * 6,
        out_specs=[vmem] + [any_spec] * 6,
        scratch_shapes=[
            pltpu.VMEM((length, rows, width), bf16),
            pltpu.VMEM((8, depth, joint), bf16),
            pltpu.VMEM((head_width, 8 * part), bf16),
            pltpu.VMEM((tokens, joint), f32),
            pltpu.VMEM((tokens, head_width), bf16),
            pltpu.VMEM((tokens, head), bf16),
            pltpu.VMEM((tokens, head), bf16),
        ]
        + ReduceItem.scratch("z", length, rows, width)
        + GatherItem.semaphores("z", length)
        + GatherItem.semaphores("dp", length) * 2
        + GatherItem.semaphores("all", length)
        + [pltpu.SemaphoreType.DMA((5,))],
        compiler_params=pltpu.CompilerParams(
            collective_id=collective_id, has_side_effects=True, vmem_limit_bytes=56 << 20
        ),
    )(rows_own, joint_own, output_own, cots_own, seg_col, seg_row, cosine, sine, query_gain, key_gain)


def attend_back(grad_own, rows_all, joint_all, output_all, qkv_all, heads_all, part_out, seg_col, seg_row, cosine, sine, query_gain, key_gain, length, collective_id):
    rows, width = grad_own.shape
    _, depth, joint = joint_all.shape
    head_width = output_all.shape[0]
    part = width // 8
    head = query_gain.shape[-1]
    heads = head_width // head
    tokens = rows * length
    block = tokens // 2
    scale = 1.0 / math.sqrt(head)
    f32, bf16 = jnp.float32, jnp.bfloat16
    half, deep, tall = rows // 2, depth // 2, head_width // 2

    def kernel(
        grad_ref, rows_ref, joint_ref, output_ref, qkv_ref, heads_ref, part_ref,
        segc, segr, cos_ref, sin_ref, qgain, kgain,
        out_rows, out_joint, out_weight, out_moe, out_qgain, out_kgain,
        grads, joint_v, weight_v, qkv, att, gatt, joint_b, part_w, key_v, value_v, dkey, dvalue,
        *rest,
    ):
        place = Place(length)
        o_bufs, z_bufs, j_bufs, w_bufs = (rest[8 * n : 8 * n + 8] for n in range(4))
        gather_sems, load_sem = rest[32:35], rest[35]

        outs = ReduceItem(
            "all",
            place,
            lambda c, z, h: part_ref.at[c * length + z, piece(2 * half, h)],
            o_bufs,
            lambda h: out_moe.at[piece(2 * half, h)],
        )
        back = ReduceItem(
            "z",
            place,
            lambda c, z, h: grads.at[z, piece(2 * half, h)],
            z_bufs,
            lambda h: out_rows.at[piece(2 * half, h)],
        )
        joints = ReduceItem(
            "dp",
            place,
            lambda c, z, h: joint_v.at[c, piece(2 * deep, h)],
            j_bufs,
            lambda h: out_joint.at[piece(2 * deep, h)],
        )
        weights = ReduceItem(
            "dp",
            place,
            lambda c, z, h: part_w.at[
                piece(2 * tall, h), pl.ds(pl.multiple_of(c * part, part), part)
            ],
            w_bufs,
            lambda h: out_weight.at[piece(2 * tall, h)],
        )
        for item in (back, joints, weights):
            item.in_place = True
        gathers = GatherItem("z", place, None, None, *gather_sems)
        gathers.own = lambda h: grad_ref.at[piece(2 * half, h)]
        gathers.slot = lambda c, z, h: grads.at[z, piece(2 * half, h)]

        outs.begin()
        back.begin()
        meet(place, True, True)
        first, sends = Sends(place), Sends(place)
        gathers.begin(first)
        outs.load_all()
        outs.hand_over(sends, 0)
        outs.hand_over(sends, 1)
        loads = [
            pltpu.make_async_copy(source, target, load_sem.at[n])
            for n, (source, target) in enumerate(
                ((output_ref, weight_v), (heads_ref, att), (qkv_ref, qkv), (joint_ref, joint_v))
            )
        ]
        for copy in loads:
            copy.start()
        advance(outs, sends, 0)
        for distance in range(1, length):
            gathers.along_z(first, distance)
            if distance < length - 1:
                advance(outs, sends, distance)
        gathers.finish()
        first.drain()
        for copy in loads[:3]:
            copy.wait()

        def to_heads(n, carry):
            lanes = pl.ds(pl.multiple_of(n * 256, 256), 256)
            left = grads[...].reshape(tokens, width)
            gatt[:, lanes] = dot(left, weight_v[lanes, :], 1, 1).astype(bf16)
            return carry

        def to_weight(n, carry):
            lanes = pl.ds(pl.multiple_of(n * 256, 256), 256)
            right = grads[:, :, lanes].reshape(tokens, 256)
            part_w[:, lanes] = dot(att[...], right, 0, 0).astype(bf16)
            return carry

        lax.fori_loop(0, width // 256, to_weight, 0)
        weights.hand_over(sends, 0)
        lax.fori_loop(0, head_width // 256, to_heads, 0)
        rows_v = weight_v.at[pl.ds(0, tokens)]
        rows_loads = [
            pltpu.make_async_copy(
                rows_ref.at[z], weight_v.at[pl.ds(z * rows, rows)], load_sem.at[4 + z]
            )
            for z in range(length)
        ]
        for copy in rows_loads:
            copy.start()
        advance(weights, sends, 0)
        key = qkv[:, head_width : head_width + head]
        key_v[...] = rope(key * row_factor(key) * kgain[...], cos_ref[...], sin_ref[...]).astype(bf16)
        value_v[...] = qkv[:, head_width + head : head_width + 2 * head].astype(bf16)
        dkey[...] = jnp.zeros((tokens, head), f32)
        dvalue[...] = jnp.zeros((tokens, head), f32)
        out_qgain[...] = jnp.zeros(out_qgain.shape, f32)

        def normed_back(grad, raw, gain, start, stop):
            factor = row_factor(raw)
            hat = raw * factor
            turned = unrope(grad, cos_ref[start:stop, :], sin_ref[start:stop, :])
            scaled = turned * gain
            found = factor * (scaled - hat * jnp.mean(scaled * hat, axis=-1, keepdims=True))
            return found, jnp.sum(turned * hat, axis=0, keepdims=True)

        def one_head(n, carry):
            lanes = pl.ds(pl.multiple_of(n * head, head), head)
            for start in range(0, tokens, block):
                stop = start + block
                raw = qkv[start:stop, lanes]
                turned = rope(
                    raw * row_factor(raw) * qgain[...], cos_ref[start:stop, :], sin_ref[start:stop, :]
                ).astype(bf16)
                grad = gatt[start:stop, lanes]
                delta = jnp.sum(
                    grad.astype(f32) * att[start:stop, lanes].astype(f32), axis=-1, keepdims=True
                )
                scores = dot(turned, key_v[0:stop, :], 1, 1) * scale
                seen = visible_pairs(segc, segr, start, stop, stop)
                scores = jnp.where(seen, scores, NEG_BIG)
                powers = jnp.exp(scores - jnp.max(scores, axis=-1, keepdims=True))
                probs = powers / jnp.sum(powers, axis=-1, keepdims=True)
                dprobs = dot(grad, value_v[0:stop, :], 1, 1)
                dscores = (probs * (dprobs - delta)).astype(bf16)
                dvalue[0:stop, :] += dot(probs.astype(bf16), grad, 0, 0)
                dkey[0:stop, :] += dot(dscores, turned, 0, 0) * scale
                dquery = dot(dscores, key_v[0:stop, :]) * scale
                found, gain_part = normed_back(dquery, raw, qgain[...], start, stop)
                joint_b[start:stop, lanes] = found.astype(bf16)
                out_qgain[...] += gain_part
            return carry

        lax.fori_loop(0, heads // 2, one_head, 0)
        advance(outs, sends, length - 1)
        advance(weights, sends, 1)
        lax.fori_loop(heads // 2, heads, one_head, 0)
        found, gain_part = normed_back(
            dkey[...], qkv[:, head_width : head_width + head], kgain[...], 0, tokens
        )
        out_kgain[...] = gain_part
        joint_b[:, head_width : head_width + head] = found.astype(bf16)
        joint_b[:, head_width + head : head_width + 2 * head] = dvalue[...].astype(bf16)
        advance(outs, sends, length)
        advance(weights, sends, 2)
        loads[3].wait()

        def to_rows(n, carry):
            lanes = pl.ds(pl.multiple_of(n * depth, depth), depth)
            found = dot(joint_b[...], joint_v[n], 1, 1).astype(bf16)
            grads[:, :, lanes] = found.reshape(length, rows, depth)
            return carry

        lax.fori_loop(0, 8, to_rows, 0)
        back.home(sends, 0)
        for copy in rows_loads:
            copy.wait()

        def to_joint(n, carry):
            lanes = pl.ds(pl.multiple_of(n * depth, depth), depth)
            joint_v[n] = dot(weight_v[0:tokens, lanes], joint_b[...], 0, 0).astype(bf16)
            return carry

        lax.fori_loop(0, 8, to_joint, 0)
        joints.hand_over(sends, 0)
        back.home(sends, 1)
        advance(joints, sends, 0)
        for turn in range(2, length):
            back.home(sends, turn)
        advance(joints, sends, 1)
        advance(outs, sends, length + 1)
        advance(joints, sends, 2)
        sends.drain()

    any_spec = pl.BlockSpec(memory_space=pl.ANY)
    vmem = pl.BlockSpec(memory_space=pltpu.VMEM)
    shape = jax.ShapeDtypeStruct
    return pl.pallas_call(
        kernel,
        name="attend_back",
        out_shape=[
            shape((rows, width), f32),
            shape((depth, joint), f32),
            shape((head_width, part), f32),
            shape((rows, width), f32),
            shape((1, head), f32),
            shape((1, head), f32),
        ],
        in_specs=[any_spec] * 7 + [vmem] * 6,
        out_specs=[vmem] * 6,
        scratch_shapes=[
            pltpu.VMEM((length, rows, width), bf16),
            pltpu.VMEM((8, depth, joint), bf16),
            pltpu.VMEM((head_width, width), bf16),
            pltpu.VMEM((tokens, joint), f32),
            pltpu.VMEM((tokens, head_width), bf16),
            pltpu.VMEM((tokens, head_width), bf16),
            pltpu.VMEM((tokens, joint), bf16),
            pltpu.VMEM((head_width, width), bf16),
            pltpu.VMEM((tokens, head), bf16),
            pltpu.VMEM((tokens, head), bf16),
            pltpu.VMEM((tokens, head), f32),
            pltpu.VMEM((tokens, head), f32),
        ]
        + ReduceItem.scratch("all", length, rows, width)
        + ReduceItem.scratch("z", length, rows, width, True)
        + ReduceItem.scratch("dp", length, depth, joint, True)
        + ReduceItem.scratch("dp", length, head_width, part, True)
        + GatherItem.semaphores("z", length)
        + [pltpu.SemaphoreType.DMA((4 + length,))],
        compiler_params=pltpu.CompilerParams(
            collective_id=collective_id, has_side_effects=True, vmem_limit_bytes=67043328
        ),
    )(grad_own, rows_all, joint_all, output_all, qkv_all, heads_all, part_out, seg_col, seg_row, cosine, sine, query_gain, key_gain)


def share_sum(values, length, collective_id):
    rows, width = values.shape
    jumps = []
    while 2 ** len(jumps) < length:
        jumps.append(2 ** len(jumps))
    stages = 3 + len(jumps)

    def kernel(own, target, sums, land, send_sem, recv_sem):
        place = Place(length)
        z = place.z
        partners = [(place.core, z), (place.x, z), (place.y, z)] + [
            (place.dp, z + jump - 2 * jump * ((z // jump) % 2)) for jump in jumps
        ]
        barrier = pltpu.get_barrier_semaphore()
        for device in partners:
            pl.semaphore_signal(barrier, 1, device_id=device, device_id_type=MESH)
        pl.semaphore_wait(barrier, stages)
        sums[0] = own[...]
        copies = []
        for stage, device in enumerate(partners):
            copy = pltpu.make_async_remote_copy(
                src_ref=sums.at[stage],
                dst_ref=land.at[stage],
                send_sem=send_sem.at[stage],
                recv_sem=recv_sem.at[stage],
                device_id=device,
                device_id_type=MESH,
            )
            copy.start()
            copies.append(copy)
            copy.wait_recv()
            total = sums[stage] + land[stage]
            if stage + 1 < stages:
                sums[stage + 1] = total
            else:
                target[...] = total
        for copy in copies:
            copy.wait_send()

    vmem = pl.BlockSpec(memory_space=pltpu.VMEM)
    return pl.pallas_call(
        kernel,
        name="share_sum",
        out_shape=jax.ShapeDtypeStruct((rows, width), values.dtype),
        in_specs=[vmem],
        out_specs=vmem,
        scratch_shapes=[
            pltpu.VMEM((stages, rows, width), values.dtype),
            pltpu.VMEM((stages, rows, width), values.dtype),
            pltpu.SemaphoreType.DMA((stages,)),
            pltpu.SemaphoreType.DMA((stages,)),
        ],
        compiler_params=pltpu.CompilerParams(collective_id=collective_id, has_side_effects=True),
    )(values)


def mix(form, left, right):
    return jnp.einsum(form, left, right, preferred_element_type=jnp.float32)


def rms_scale(values):
    return lax.rsqrt(jnp.mean(values * values, axis=-1, keepdims=True) + EPSILON)


def rope_tables(seg_ids, head_dim):
    length = seg_ids.shape[0]
    row_index = jnp.arange(length, dtype=jnp.int32)
    starts = jnp.sum((seg_ids[None, :] < seg_ids[:, None]).astype(jnp.int32), axis=1)
    places = (row_index - starts).astype(jnp.float32)
    half_dim = head_dim // 2
    frequency = THETA_BASE ** (-(jnp.arange(half_dim, dtype=jnp.float32) * (2.0 / head_dim)))
    angles = places[:, None] * frequency[None, :]
    return (jnp.cos(angles), jnp.sin(angles))


def rotate(values, cosine, sine_table):
    half_dim = values.shape[-1] // 2
    front_part = values[..., :half_dim]
    back_part = values[..., half_dim:]
    cos_rows = cosine[:, None, :]
    sin_rows = sine_table[:, None, :]
    return jnp.concatenate(
        [
            front_part * cos_rows - back_part * sin_rows,
            back_part * cos_rows + front_part * sin_rows,
        ],
        axis=-1,
    )


def unrotate(values, cosine, sine_table):
    half_dim = values.shape[-1] // 2
    front_part = values[..., :half_dim]
    back_part = values[..., half_dim:]
    cos_rows = cosine[:, None, :]
    sin_rows = sine_table[:, None, :]
    return jnp.concatenate(
        [
            front_part * cos_rows + back_part * sin_rows,
            back_part * cos_rows - front_part * sin_rows,
        ],
        axis=-1,
    )


def head_norm_back(grad_out, normed, factor, gain):
    grad_normed = grad_out * gain
    grad_gain = jnp.sum(grad_out * normed, axis=(0, 1))
    grad_values = factor * (
        grad_normed - normed * jnp.mean(grad_normed * normed, axis=-1, keepdims=True)
    )
    return (grad_values, grad_gain)


def row_norm_back(grad_out, normed, factor, gain):
    grad_normed = grad_out * gain
    grad_gain = jnp.sum(grad_out * normed, axis=0)
    grad_values = factor * (
        grad_normed - normed * jnp.mean(grad_normed * normed, axis=-1, keepdims=True)
    )
    return (grad_values, grad_gain)


def softmax_rows(logits):
    top_value = jnp.max(logits, axis=-1, keepdims=True)
    expo = jnp.exp(logits - top_value)
    return expo / jnp.sum(expo, axis=-1, keepdims=True)


def attn_forward(rows, seg_ids, wq_full, wk_full, wv_full, query_gain, key_gain):
    length = rows.shape[0]
    head_dim = query_gain.shape[0]
    num_heads = wq_full.shape[1] // head_dim
    kv_heads = wk_full.shape[1] // head_dim
    per_group = num_heads // kv_heads
    inv_root = 1.0 / math.sqrt(head_dim)
    block_rows = math.gcd(length, 512)
    cosine, sine_table = rope_tables(seg_ids, head_dim)
    query = jnp.dot(rows, wq_full, preferred_element_type=jnp.float32).reshape(
        length, num_heads, head_dim
    )
    key_proj = jnp.dot(rows, wk_full, preferred_element_type=jnp.float32).reshape(
        length, kv_heads, head_dim
    )
    value_rows = (
        jnp.dot(rows, wv_full, preferred_element_type=jnp.float32)
        .astype(jnp.bfloat16)
        .reshape(length, kv_heads, head_dim)
    )
    query_factor = rms_scale(query)
    query_hat = query * query_factor
    key_factor = rms_scale(key_proj)
    key_hat = key_proj * key_factor
    query_rot = (
        rotate(query_hat * query_gain, cosine, sine_table)
        .astype(jnp.bfloat16)
        .reshape(length, kv_heads, per_group, head_dim)
    )
    key_rot = rotate(key_hat * key_gain, cosine, sine_table).astype(jnp.bfloat16)
    row_index = jnp.arange(length, dtype=jnp.int32)
    scores = mix("qgrd,kgd->grqk", query_rot, key_rot) * inv_root
    visible = (seg_ids[0:block_rows, None] == seg_ids[None, :]) & (
        row_index[None, :] <= row_index[0:block_rows, None]
    )
    scores = jnp.where(visible, scores, NEG_BIG)
    top_value = jnp.max(scores, axis=-1, keepdims=True)
    expo = jnp.exp(scores - top_value)
    totals = jnp.sum(expo, axis=-1, keepdims=True)
    prob_rows = (expo / totals).astype(jnp.bfloat16)
    outputs = mix("grqk,kgd->qgrd", prob_rows, value_rows).astype(jnp.bfloat16)
    lse_parts = top_value[..., 0] + jnp.log(totals[..., 0])
    attn_heads = outputs.reshape(length, num_heads * head_dim)
    return (
        attn_heads,
        lse_parts,
        query_rot,
        key_rot,
        value_rows,
        cosine,
        sine_table,
        query_hat,
        query_factor,
        key_hat,
        key_factor,
    )


def attn_backward(
    grad_attn, rows, seg_ids, wq_full, wk_full, wv_full, wo_full, query_gain, key_gain, saved
):
    (
        attn_heads,
        lse_all,
        query_rot,
        key_rot,
        value_rows,
        cosine,
        sine_table,
        query_hat,
        query_factor,
        key_hat,
        key_factor,
    ) = saved
    length = rows.shape[0]
    head_dim = query_gain.shape[0]
    num_heads = query_hat.shape[1]
    inv_root = 1.0 / math.sqrt(head_dim)
    block_rows = math.gcd(length, 512)
    grad_wo = jnp.dot(attn_heads.T, grad_attn, preferred_element_type=jnp.float32)
    grad_heads = (
        jnp.dot(grad_attn, wo_full.T, preferred_element_type=jnp.float32)
        .astype(jnp.bfloat16)
        .reshape(query_rot.shape)
    )
    heads_view = attn_heads.reshape(query_rot.shape)
    row_delta = jnp.transpose(
        jnp.sum(grad_heads.astype(jnp.float32) * heads_view.astype(jnp.float32), axis=-1), (1, 2, 0)
    )
    row_index = jnp.arange(length, dtype=jnp.int32)
    scores = mix("qgrd,kgd->grqk", query_rot, key_rot) * inv_root
    visible = (seg_ids[0:block_rows, None] == seg_ids[None, :]) & (
        row_index[None, :] <= row_index[0:block_rows, None]
    )
    scores = jnp.where(visible, scores, NEG_BIG)
    prob_f = jnp.where(visible, jnp.exp(scores - lse_all[:, :, 0:block_rows, None]), 0.0)
    prob_rows = prob_f.astype(jnp.bfloat16)
    grad_value = mix("grqk,qgrd->kgd", prob_rows, grad_heads)
    grad_probs = mix("qgrd,kgd->grqk", grad_heads, value_rows)
    grad_scores = (prob_f * (grad_probs - row_delta[:, :, 0:block_rows, None])).astype(jnp.bfloat16)
    pieces = mix("grqk,kgd->qgrd", grad_scores, key_rot) * inv_root
    grad_key_rot = mix("grqk,qgrd->kgd", grad_scores, query_rot) * inv_root
    grad_query_rot = pieces.reshape(length, num_heads, head_dim)
    grad_query, grad_qgain = head_norm_back(
        unrotate(grad_query_rot, cosine, sine_table), query_hat, query_factor, query_gain
    )
    grad_key, grad_kgain = head_norm_back(
        unrotate(grad_key_rot, cosine, sine_table), key_hat, key_factor, key_gain
    )
    query_b = grad_query.astype(jnp.bfloat16).reshape(length, -1)
    key_b = grad_key.astype(jnp.bfloat16).reshape(length, -1)
    value_b = grad_value.astype(jnp.bfloat16).reshape(length, -1)
    grad_rows = (
        jnp.dot(query_b, wq_full.T, preferred_element_type=jnp.float32)
        + jnp.dot(key_b, wk_full.T, preferred_element_type=jnp.float32)
        + jnp.dot(value_b, wv_full.T, preferred_element_type=jnp.float32)
    )
    grad_wq = jnp.dot(rows.T, query_b, preferred_element_type=jnp.float32)
    grad_wk = jnp.dot(rows.T, key_b, preferred_element_type=jnp.float32)
    grad_wv = jnp.dot(rows.T, value_b, preferred_element_type=jnp.float32)
    return (grad_rows, grad_wq, grad_wk, grad_wv, grad_wo, grad_qgain, grad_kgain)


def expert_forward(expert_rows, wgate, wup, wdown):
    gate_pre = jnp.dot(expert_rows, wgate, preferred_element_type=jnp.float32)
    up_pre = jnp.dot(expert_rows, wup, preferred_element_type=jnp.float32)
    hidden_units = (jax.nn.silu(gate_pre) * up_pre).astype(jnp.bfloat16)
    result = jnp.dot(hidden_units, wdown, preferred_element_type=jnp.float32).astype(jnp.bfloat16)
    return (result, gate_pre, up_pre, hidden_units)


def expert_backward(expert_rows, grad_result, wgate, wup, wdown, gate_pre, up_pre, hidden_units):
    grad_hidden = jnp.dot(grad_result, wdown.T, preferred_element_type=jnp.float32)
    sigma = jax.nn.sigmoid(gate_pre)
    grad_gate_pre = (grad_hidden * up_pre * sigma * (1.0 + gate_pre * (1.0 - sigma))).astype(
        jnp.bfloat16
    )
    grad_up_pre = (grad_hidden * gate_pre * sigma).astype(jnp.bfloat16)
    grad_rows = (
        jnp.dot(grad_gate_pre, wgate.T, preferred_element_type=jnp.float32)
        + jnp.dot(grad_up_pre, wup.T, preferred_element_type=jnp.float32)
    ).astype(jnp.bfloat16)
    grad_wd = jnp.dot(hidden_units.T, grad_result, preferred_element_type=jnp.float32)
    grad_wg = jnp.dot(expert_rows.T, grad_gate_pre, preferred_element_type=jnp.float32)
    grad_wu = jnp.dot(expert_rows.T, grad_up_pre, preferred_element_type=jnp.float32)
    return (grad_rows, grad_wg, grad_wu, grad_wd)


def to_experts(buffer):
    return lax.all_to_all(buffer, ("dp", "tensor"), split_axis=0, concat_axis=0, tiled=True)


def to_sources(buffer):
    return lax.all_to_all(buffer, ("dp", "tensor"), split_axis=0, concat_axis=0, tiled=True)


def shards(
    hidden_in,
    segments,
    routes,
    query_weight,
    key_weight,
    value_weight,
    output_weight,
    gain_attn,
    gain_moe,
    query_gain,
    key_gain,
    router,
    gate_weight,
    up_weight,
    down_weight,
    cotangent,
):
    seg_ids = segments[0]
    rows_dev = hidden_in.shape[0]
    width = hidden_in.shape[1]
    top_count = routes.shape[1]
    experts = router.shape[1]
    capacity = 2 * rows_dev * top_count // experts
    full_query, full_key, full_value, full_output = (
        lax.all_gather(query_weight, "dp", axis=0, tiled=True),
        lax.all_gather(key_weight, "dp", axis=0, tiled=True),
        lax.all_gather(value_weight, "dp", axis=0, tiled=True),
        lax.all_gather(output_weight, "dp", axis=1, tiled=True),
    )
    inputs32 = hidden_in.astype(jnp.float32)
    factor_one = rms_scale(inputs32)
    normed_one = inputs32 * factor_one
    rows_one = (normed_one * gain_attn).astype(jnp.bfloat16)
    group_rows = lax.all_gather(rows_one, "tensor", axis=0, tiled=True)
    saved = attn_forward(
        group_rows, seg_ids, full_query, full_key, full_value, query_gain, key_gain
    )
    partial_add = jnp.dot(saved[0], full_output, preferred_element_type=jnp.float32)
    attn_add = lax.psum_scatter(partial_add, "tensor", scatter_dimension=0, tiled=True)
    residual = inputs32 + attn_add
    factor_two = rms_scale(residual)
    normed_two = residual * factor_two
    rows_two = (normed_two * gain_moe).astype(jnp.bfloat16)
    router_probs = softmax_rows(jnp.dot(rows_two, router, preferred_element_type=jnp.float32))
    route_hot = (routes[:, :, None] == jnp.arange(experts, dtype=jnp.int32)[None, None, :]).astype(
        jnp.float32
    )
    picked = jnp.sum(route_hot * router_probs[:, None, :], axis=-1)
    total = jnp.sum(picked, axis=1, keepdims=True)
    gates = picked / total
    flat_routes = routes.reshape(-1)
    onehot = (flat_routes[:, None] == jnp.arange(experts, dtype=jnp.int32)[None, :]).astype(
        jnp.int32
    )
    ranks = jnp.sum(onehot * jnp.cumsum(onehot, axis=0), axis=1) - 1
    slots = flat_routes * capacity + ranks
    send_rows = (
        jnp.zeros((experts * capacity, width), jnp.bfloat16)
        .at[slots]
        .set(jnp.repeat(rows_two, top_count, axis=0))
    )
    received = to_experts(send_rows.reshape(experts, capacity, width)).reshape(-1, width)
    result, gate_pre, up_pre, hidden_units = expert_forward(
        received, gate_weight[0], up_weight[0], down_weight[0]
    )
    returned = to_sources(result.reshape(-1, capacity, width)).reshape(experts * capacity, width)
    pair_out = returned[slots].astype(jnp.float32).reshape(rows_dev, top_count, width)
    moe_sum = jnp.sum(gates[:, :, None] * pair_out, axis=1)
    output = (residual + moe_sum).astype(jnp.bfloat16)
    cot32 = cotangent.astype(jnp.float32)
    grad_gates = jnp.sum(cot32[:, None, :] * pair_out, axis=-1)
    grad_result = (gates[:, :, None] * cot32[:, None, :]).astype(jnp.bfloat16).reshape(-1, width)
    send_grads = jnp.zeros((experts * capacity, width), jnp.bfloat16).at[slots].set(grad_result)
    received_grads = to_experts(send_grads.reshape(experts, capacity, width)).reshape(-1, width)
    grad_expert_rows, grad_wg, grad_wu, grad_wd = expert_backward(
        received,
        received_grads,
        gate_weight[0],
        up_weight[0],
        down_weight[0],
        gate_pre,
        up_pre,
        hidden_units,
    )
    returned_grads = to_sources(grad_expert_rows.reshape(-1, capacity, width)).reshape(
        experts * capacity, width
    )
    grad_pairs = returned_grads[slots].astype(jnp.float32).reshape(rows_dev, top_count, width)
    grad_picked = (grad_gates - jnp.sum(gates * grad_gates, axis=1, keepdims=True)) / total
    grad_probs = jnp.sum(route_hot * grad_picked[:, :, None], axis=1)
    grad_logits = (
        router_probs * (grad_probs - jnp.sum(grad_probs * router_probs, axis=-1, keepdims=True))
    ).astype(jnp.bfloat16)
    grad_router = jnp.dot(rows_two.T, grad_logits, preferred_element_type=jnp.float32)
    grad_rows_two = jnp.sum(grad_pairs, axis=1) + jnp.dot(
        grad_logits, router.T, preferred_element_type=jnp.float32
    )
    grad_res_norm, grad_gain_moe = row_norm_back(grad_rows_two, normed_two, factor_two, gain_moe)
    grad_residual = cot32 + grad_res_norm
    grad_attn = grad_residual.astype(jnp.bfloat16)
    group_grads = lax.all_gather(grad_attn, "tensor", axis=0, tiled=True)
    back_query, back_key, back_value, back_output = (
        lax.all_gather(query_weight, "dp", axis=0, tiled=True),
        lax.all_gather(key_weight, "dp", axis=0, tiled=True),
        lax.all_gather(value_weight, "dp", axis=0, tiled=True),
        lax.all_gather(output_weight, "dp", axis=1, tiled=True),
    )
    grad_group_rows, grad_wq, grad_wk, grad_wv, grad_wo, grad_qgain, grad_kgain = attn_backward(
        group_grads,
        group_rows,
        seg_ids,
        back_query,
        back_key,
        back_value,
        back_output,
        query_gain,
        key_gain,
        saved,
    )
    grad_rows_one = lax.psum_scatter(
        grad_group_rows.astype(jnp.bfloat16), "tensor", scatter_dimension=0, tiled=True
    ).astype(jnp.float32)
    grad_in_norm, grad_gain_attn = row_norm_back(grad_rows_one, normed_one, factor_one, gain_attn)
    grad_input = grad_residual + grad_in_norm
    grad_wq, grad_wk, grad_wv, grad_wo = (
        lax.psum_scatter(
            grad_wq.astype(jnp.bfloat16), "dp", scatter_dimension=0, tiled=True
        ).astype(jnp.float32),
        lax.psum_scatter(
            grad_wk.astype(jnp.bfloat16), "dp", scatter_dimension=0, tiled=True
        ).astype(jnp.float32),
        lax.psum_scatter(
            grad_wv.astype(jnp.bfloat16), "dp", scatter_dimension=0, tiled=True
        ).astype(jnp.float32),
        lax.psum_scatter(
            grad_wo.astype(jnp.bfloat16), "dp", scatter_dimension=1, tiled=True
        ).astype(jnp.float32),
    )
    grad_gain_attn, grad_gain_moe, grad_qgain, grad_kgain, grad_router = lax.psum(
        (grad_gain_attn, grad_gain_moe, grad_qgain, grad_kgain, grad_router), ("dp", "tensor")
    )
    return (
        output,
        grad_input,
        grad_wq,
        grad_wk,
        grad_wv,
        grad_wo,
        grad_gain_attn,
        grad_gain_moe,
        grad_qgain,
        grad_kgain,
        grad_router,
        grad_wg[None],
        grad_wu[None],
        grad_wd[None],
    )


AXES = ("dp", "tensor")


def gathered(
    hidden_in,
    segments,
    routes,
    query_weight,
    key_weight,
    value_weight,
    output_weight,
    gain_attn,
    gain_moe,
    query_gain,
    key_gain,
    router,
    gate_weight,
    up_weight,
    down_weight,
    cotangent,
):
    seg_ids = segments[0]
    rows_dev, width = hidden_in.shape
    top_count = routes.shape[1]
    expert_count = router.shape[1]
    capacity = 2 * rows_dev * top_count // expert_count
    length = lax.axis_size("tensor")
    query_cols, key_cols = query_weight.shape[1], key_weight.shape[1]

    inputs32 = hidden_in.astype(jnp.float32)
    factor_one = rms_scale(inputs32)
    normed_one = inputs32 * factor_one
    rows_one = (normed_one * gain_attn).astype(jnp.bfloat16)
    joint_weight = jnp.concatenate([query_weight, key_weight, value_weight], axis=1)
    cosine, sine_table = rope_tables(seg_ids, query_gain.shape[0])
    turns = (
        seg_ids[:, None],
        seg_ids[None, :],
        jnp.concatenate([cosine, cosine], axis=1),
        jnp.concatenate([-sine_table, sine_table], axis=1),
        query_gain[None, :],
        key_gain[None, :],
    )
    attn_add, group_rows, full_joint, full_output, all_cots, projected, attn_heads = attend(
        rows_one, joint_weight, output_weight, cotangent, *turns, length, 0
    )
    residual = inputs32 + attn_add
    factor_two = rms_scale(residual)
    normed_two = residual * factor_two
    rows_two = (normed_two * gain_moe).astype(jnp.bfloat16)
    router_probs = softmax_rows(jnp.dot(rows_two, router, preferred_element_type=jnp.float32))
    route_hot = (routes[:, :, None] == jnp.arange(expert_count, dtype=jnp.int32)[None, None, :]).astype(
        jnp.float32
    )
    picked = jnp.sum(route_hot * router_probs[:, None, :], axis=-1)
    total = jnp.sum(picked, axis=1, keepdims=True)
    gates = picked / total
    named = jnp.sum(route_hot, axis=1)
    gate_table = jnp.where(named > 0.5, jnp.sum(route_hot * gates[:, :, None], axis=1), -1.0)
    all_rows, partial_out, partial_rows, token_grads, *units = experts(
        rows_two,
        all_cots,
        jnp.broadcast_to(gate_table.T[:, None, :], (expert_count, 8, rows_dev)),
        gate_weight[0],
        up_weight[0],
        down_weight[0],
        length,
        capacity,
        1,
    )
    back_grads = token_grads[:, 0, :]
    cot32 = cotangent.astype(jnp.float32)
    grad_gates = jnp.sum(route_hot * back_grads.T[:, None, :], axis=-1)
    grad_picked = (grad_gates - jnp.sum(gates * grad_gates, axis=1, keepdims=True)) / total
    grad_probs = jnp.sum(route_hot * grad_picked[:, :, None], axis=1)
    grad_logits = (
        router_probs * (grad_probs - jnp.sum(grad_probs * router_probs, axis=-1, keepdims=True))
    ).astype(jnp.bfloat16)
    grad_sum, grad_router, grad_wg, grad_wu, grad_wd = reduce_rows(
        partial_rows,
        grad_logits.T,
        all_rows,
        *[unit.reshape(-1, unit.shape[-1]) for unit in units],
        length,
        2,
    )
    grad_rows_two = grad_sum + jnp.dot(grad_logits, router.T, preferred_element_type=jnp.float32)
    grad_res_norm, grad_gain_moe = row_norm_back(grad_rows_two, normed_two, factor_two, gain_moe)
    grad_residual = cot32 + grad_res_norm
    grad_attn = grad_residual.astype(jnp.bfloat16)
    grad_rows_one, grad_joint, grad_wo, moe_sum, grad_qgain, grad_kgain = attend_back(
        grad_attn,
        group_rows,
        full_joint,
        full_output,
        projected,
        attn_heads,
        partial_out,
        *turns,
        length,
        3,
    )
    output = (residual + moe_sum).astype(jnp.bfloat16)
    grad_in_norm, grad_gain_attn = row_norm_back(grad_rows_one, normed_one, factor_one, gain_attn)
    grad_input = grad_residual + grad_in_norm
    small = jnp.concatenate([grad_gain_attn, grad_gain_moe, grad_qgain[0], grad_kgain[0]]).reshape(-1, 128)
    small = jnp.pad(small, ((0, -small.shape[0] % 8), (0, 0)))
    sums = share_sum(small, length, 4).reshape(-1)
    head_dim = query_gain.shape[0]
    return (
        output,
        grad_input,
        grad_joint[:, :query_cols],
        grad_joint[:, query_cols : query_cols + key_cols],
        grad_joint[:, query_cols + key_cols :],
        grad_wo,
        sums[:width],
        sums[width : 2 * width],
        sums[2 * width : 2 * width + head_dim],
        sums[2 * width + head_dim : 2 * width + 2 * head_dim],
        grad_router.T,
        grad_wg[None],
        grad_wu[None],
        grad_wd[None],
    )


def solution(mesh):
    placed = (
        P(("dp", "tensor"), None),
        P("dp", None),
        P(("dp", "tensor"), None),
        P("dp", "tensor"),
        P("dp", "tensor"),
        P("dp", "tensor"),
        P("tensor", "dp"),
        P(),
        P(),
        P(),
        P(),
        P(),
        P(("dp", "tensor"), None, None),
        P(("dp", "tensor"), None, None),
        P(("dp", "tensor"), None, None),
        P(("dp", "tensor"), None),
    )
    program = gathered if mesh.shape["dp"] == 8 and mesh.shape["tensor"] <= 4 else shards
    return jax.shard_map(
        program,
        mesh=mesh,
        in_specs=placed,
        out_specs=(
            P(("dp", "tensor"), None),
            P(("dp", "tensor"), None),
            P("dp", "tensor"),
            P("dp", "tensor"),
            P("dp", "tensor"),
            P("tensor", "dp"),
            P(),
            P(),
            P(),
            P(),
            P(),
            P(("dp", "tensor"), None, None),
            P(("dp", "tensor"), None, None),
            P(("dp", "tensor"), None, None),
        ),
        check_vma=False,
    )
```

```python
import math

import jax
import jax.numpy as jnp
from jax import lax
from jax.experimental import pallas as pl
from jax.experimental.pallas import tpu as pltpu
from jax.sharding import PartitionSpec as P

EPSILON = 1e-06
THETA_BASE = 1000000.0
NEG_BIG = -1e30


MESH = pl.DeviceIdType.MESH


class Place:
    def __init__(self, length):
        self.length = length
        self.dp = lax.axis_index("dp")
        self.z = lax.axis_index("tensor")
        core, along_x, along_y = self.dp % 2, (self.dp // 2) % 2, self.dp // 4
        self.to_core = 1 - 2 * core
        self.core = self.dp + self.to_core
        self.x = self.dp + 2 - 4 * along_x
        self.y = self.dp + 4 - 8 * along_y
        self.columns = (self.dp, self.x, self.y, self.x + self.y - self.dp)

    def device(self, kind):
        if kind == "x":
            return (self.x, self.z)
        if kind == "y":
            return (self.y, self.z)
        if kind == "core":
            return (self.core, self.z)
        if kind == "up":
            return (self.dp, self.z + 1)
        return (self.dp, self.z - 1)

    @property
    def has_up(self):
        return self.z < self.length - 1

    @property
    def has_down(self):
        return self.z > 0

    def condition(self, kind):
        if kind == "up":
            return self.has_up
        return self.has_down if kind == "down" else None

    def nearest(self, turn):
        length = self.length

        def equal(left, right):
            far = 2 * length
            return (left - right + far) // far - (left - right - 1 + far) // far

        found = 0
        for mine in range(length):
            order = sorted(range(length), key=lambda other: (abs(other - mine), other))
            for step, other in enumerate(order):
                if other:
                    found = found + equal(self.z, mine) * equal(turn, step) * other
        return found

    def target(self, turn):
        length, z = self.length, self.z

        def at_least(left, right):
            return (left - right + 2 * length) // (2 * length)

        high = at_least(z, length // 2)
        mirrored = z + high * (length - 1 - 2 * z)
        above = length - 1 - mirrored
        first = at_least(above - 1, turn)
        if turn == length - 1:
            return z
        found = first * (length - 1 - turn) + (1 - first) * (turn - above)
        return found + high * (length - 1 - 2 * found)


def piece(rows, h):
    return pl.ds(0, rows) if h is None else pl.ds(h * (rows // 2), rows // 2)


def guarded(condition, action):
    if condition is None:
        action()
    else:
        pl.when(condition)(action)


def meet(place, over_z, over_dp):
    barrier = pltpu.get_barrier_semaphore()
    kinds = (("x", "y", "core") if over_dp else ()) + (("up", "down") if over_z else ())
    for kind in kinds:

        def greet(kind=kind):
            pl.semaphore_signal(
                barrier, 1, device_id=place.device(kind), device_id_type=MESH
            )

        guarded(place.condition(kind), greet)
    count = 3 if over_dp else 0
    if over_z:
        length = place.length
        count = count + (place.z + length - 1) // length + (2 * length - 2 - place.z) // length
    pl.semaphore_wait(barrier, count)


def other_device(place, distance):
    there = lax.rem(place.dp * place.length + place.z + distance, 8 * place.length)
    return (there // place.length, lax.rem(there, place.length)), there


def meet_all(place):
    barrier = pltpu.get_barrier_semaphore()
    others = 8 * place.length - 1

    def greet(n, carry):
        device, _ = other_device(place, n + 1)
        pl.semaphore_signal(barrier, 1, device_id=device, device_id_type=MESH)
        return carry

    lax.fori_loop(0, others, greet, 0)
    pl.semaphore_wait(barrier, others)


class Sends:
    def __init__(self, place):
        self.place = place
        self.started = []

    def start(self, kind, views, condition=lambda: None):
        def build():
            source, target, send_sem, recv_sem = views()
            return pltpu.make_async_remote_copy(
                src_ref=source,
                dst_ref=target,
                send_sem=send_sem,
                recv_sem=recv_sem,
                device_id=self.place.device(kind),
                device_id_type=MESH,
            )

        guarded(self.place.condition(kind), lambda: build().start())
        self.started.append((condition, kind, build))

    def drain(self):
        for condition, kind, build in self.started:

            def finish(kind=kind, build=build):
                guarded(self.place.condition(kind), lambda: build().wait_send())

            guarded(condition(), finish)


class GatherItem:
    def __init__(self, mode, place, own, slot, recv, send, local):
        self.mode, self.place = mode, place
        self.own, self.slot = own, slot
        self.recv, self.send, self.local = recv, send, local
        self.over_z = mode != "dp"
        self.over_dp = mode != "z"
        self.length = place.length if self.over_z else 1
        self.z = place.z if self.over_z else 0

    def index(self, column, z):
        if self.mode == "all":
            return column * self.length + z
        return column if self.mode == "dp" else z

    @staticmethod
    def semaphores(mode, length):
        blocks = {"all": 8 * length, "dp": 8, "z": length}[mode]
        turns = 2 * length - 1 if mode != "dp" else 1
        return [
            pltpu.SemaphoreType.DMA((blocks, 2)),
            pltpu.SemaphoreType.DMA((10, turns, 2)),
            pltpu.SemaphoreType.DMA((2,)),
        ]

    def turns(self, distance):
        if distance == 0:
            return [(0, 0, lambda: None, None)]
        place, length = self.place, self.length
        return [
            (2 * distance - 1, -distance, lambda: place.z >= distance, "up"),
            (2 * distance, distance, lambda: place.z < length - distance, "down"),
        ]

    def pass_on(self, sends, lane, kind, column, offset, turn, h, source=None, condition=lambda: None):
        at = 0 if h is None else h

        def views():
            z = self.z + offset
            view = self.slot(column, z, h)
            return (
                view if source is None else source(h),
                view,
                self.send.at[lane, turn, at],
                self.recv.at[self.index(column, z), at],
            )

        sends.start(kind, views, condition)

    def arrived(self, column, z, h):
        view = self.slot(column, z, h)
        at = 0 if h is None else h
        pltpu.make_async_copy(view, view, self.recv.at[self.index(column, z), at]).wait()

    def local_copy(self):
        return pltpu.make_async_copy(
            self.own(None), self.slot(self.place.dp, self.z, None), self.local.at[0]
        )

    def begin(self, sends):
        place = self.place
        if self.over_z:
            self.pass_on(sends, 0, "up", place.dp, 0, 0, None, self.own)
            self.pass_on(sends, 1, "down", place.dp, 0, 0, None, self.own)
        if self.over_dp:
            self.pass_on(sends, 2, "x", place.dp, 0, 0, None, self.own)
            self.pass_on(sends, 3, "y", place.dp, 0, 0, None, self.own)
            self.pass_on(sends, 4, "core", place.dp, 0, 0, None, self.own)
        self.local_copy().start()

    def along_z(self, sends, distance):
        if not self.over_z or distance >= self.length:
            return
        place = self.place
        for turn, offset, condition, onward in self.turns(distance):

            def step(turn=turn, offset=offset, condition=condition, onward=onward):
                self.arrived(place.dp, self.z + offset, None)
                lanes = []
                if distance < self.length - 1:
                    lanes.append((0 if onward == "up" else 1, onward))
                if self.over_dp:
                    lanes += [(2, "x"), (3, "y"), (4, "core")]
                for lane, kind in lanes:
                    self.pass_on(
                        sends, lane, kind, place.dp, offset, turn, None, condition=condition
                    )

            guarded(condition(), step)

    def across(self, sends, distance):
        if not self.over_dp or not 0 <= distance < self.length:
            return
        _, x, y, _ = self.place.columns
        for turn, offset, condition, _ in self.turns(distance):

            def step(turn=turn, offset=offset, condition=condition):
                self.arrived(x, self.z + offset, None)
                self.pass_on(sends, 5, "y", x, offset, turn, 0, condition=condition)
                self.pass_on(sends, 7, "core", x, offset, turn, None, condition=condition)
                self.arrived(y, self.z + offset, None)
                self.pass_on(sends, 6, "x", y, offset, turn, 1, condition=condition)
                self.pass_on(sends, 8, "core", y, offset, turn, None, condition=condition)

            guarded(condition(), step)

    def diagonal(self, sends, distance):
        if not self.over_dp or not 0 <= distance < self.length:
            return
        corner = self.place.columns[3]
        for turn, offset, condition, _ in self.turns(distance):

            def step(turn=turn, offset=offset, condition=condition):
                for h in range(2):
                    self.arrived(corner, self.z + offset, h)
                    self.pass_on(sends, 9, "core", corner, offset, turn, h, condition=condition)

            guarded(condition(), step)

    def settled(self):
        self.local_copy().wait()

    def from_core(self, z):
        for number, column in enumerate(self.place.columns):
            for h in (0, 1) if number == 3 else (None,):
                self.arrived(column + self.place.to_core, z, h)

    def finish(self):
        self.settled()
        if self.over_dp:
            for z in range(self.length):
                self.from_core(z)


class ReduceItem:
    def __init__(self, mode, place, block, bufs, out):
        self.mode, self.place, self.block, self.out = mode, place, block, out
        self.over_z = mode != "dp"
        self.over_dp = mode != "z"
        self.length = place.length if self.over_z else 1
        (self.acc, self.from_core, self.corner, self.from_xy, self.from_z,
         self.load, self.send, self.recv) = bufs

    @staticmethod
    def scratch(mode, length, rows, width, in_place=False):
        t = length if mode != "dp" else 1
        columns = 4 if mode != "z" else 1
        dp = mode != "z"
        small = (8, 128)
        return [
            pltpu.VMEM(small if in_place else (columns, t, rows, width), jnp.bfloat16),
            pltpu.VMEM((columns, t, rows, width) if dp else small, jnp.bfloat16),
            pltpu.VMEM((2, t, rows // 2, width) if dp else small, jnp.bfloat16),
            pltpu.VMEM((2, t, rows, width) if dp else small, jnp.bfloat16),
            pltpu.VMEM((t + 1, rows, width) if mode != "dp" else small, jnp.bfloat16),
            pltpu.SemaphoreType.DMA((columns, t)),
            pltpu.SemaphoreType.DMA((10, t, 2)),
            pltpu.SemaphoreType.DMA((9, t + 1, 2)),
        ]

    def z_of(self, turn):
        return self.place.target(turn) if self.over_z else 0

    def got(self, ref, lane, turn, h=0):
        pltpu.make_async_copy(ref, ref, self.recv.at[lane, turn, h]).wait()

    computed = False
    in_place = False

    def partial(self, column, turn, h):
        if self.in_place:
            return self.block(self.place.columns[column], self.z_of(turn), h)
        return self.acc.at[column, turn, piece(self.acc.shape[2], h)]

    def add(self, target, refs, out=None):
        rows = target.shape[0]
        step = 16 if rows % 16 == 0 else rows
        place = target if out is None else out

        def body(i, carry):
            at = pl.ds(pl.multiple_of(i * step, step), step)
            total = target[at, :].astype(jnp.float32)
            for ref in refs:
                total = total + ref[at, :].astype(jnp.float32)
            place[at, :] = total.astype(place.dtype)
            return carry

        lax.fori_loop(0, rows // step, body, 0, unroll=2 if (rows // step) % 2 == 0 else 1)

    def begin(self):
        place = self.place
        if self.over_z:

            @pl.when((place.z == 0) | (place.z == self.length - 1))
            def _():
                def clear(i, carry):
                    self.from_z[i] = jnp.zeros(self.from_z.shape[1:], jnp.bfloat16)
                    return carry

                lax.fori_loop(0, self.length + 1, clear, 0)

    def load_all(self):
        place = self.place
        for turn in range(self.length):
            for column in (3, 1, 2, 0) if self.over_dp else (0,):
                pltpu.make_async_copy(
                    self.block(place.columns[column], self.z_of(turn), None),
                    self.acc.at[column, turn],
                    self.load.at[column, turn],
                ).start()

    def hand_over(self, sends, turn):
        if not self.over_dp or turn >= self.length:
            return
        place = self.place
        for column in (3, 1, 2, 0):
            sends.start(
                "core",
                lambda column=column: (
                    self.block(place.columns[column] + place.to_core, self.z_of(turn), None),
                    self.from_core.at[column, turn],
                    self.send.at[column, turn, 0],
                    self.recv.at[column, turn, 0],
                ),
            )

    def ready(self, column, turn):
        if not (self.computed or self.in_place):
            ref = self.acc.at[column, turn]
            pltpu.make_async_copy(ref, ref, self.load.at[column, turn]).wait()
        if self.over_dp:
            self.got(self.from_core.at[column, turn], column, turn)

    def settle(self, column, turn, h, extra=(), out=None):
        refs = list(extra)
        if self.over_dp:
            rows = self.from_core.shape[2]
            refs.append(self.from_core.at[column, turn, piece(rows, h)])
        if refs or out is not None:
            self.add(self.partial(column, turn, h), refs, out)

    def corners(self, sends, turn):
        if not self.over_dp or not 0 <= turn < self.length:
            return
        self.ready(3, turn)
        for h, kind in ((0, "y"), (1, "x")):
            self.settle(3, turn, h)
            sends.start(
                kind,
                lambda h=h: (
                    self.partial(3, turn, h),
                    self.corner.at[h, turn],
                    self.send.at[4, turn, h],
                    self.recv.at[4, turn, h],
                ),
            )

    def straight(self, sends, turn, second):
        if not self.over_dp or not 0 <= turn < self.length:
            return
        rows = self.from_xy.shape[2]
        for column, kind in ((1, "x"), (2, "y")):
            h = (column - 1) if second else (2 - column)
            extra = ()
            if second:
                ref = self.corner.at[h, turn]
                self.got(ref, 4, turn, h)
                extra = (ref,)
            else:
                self.ready(column, turn)
            self.settle(column, turn, h, extra)
            sends.start(
                kind,
                lambda column=column, h=h: (
                    self.partial(column, turn, h),
                    self.from_xy.at[column - 1, turn, piece(rows, h)],
                    self.send.at[4 + column, turn, h],
                    self.recv.at[4 + column, turn, h],
                ),
            )

    def home(self, sends, turn):
        if not 0 <= turn < self.length:
            return
        place = self.place
        last = turn == self.length - 1
        z = self.z_of(turn)
        extra = []
        self.ready(0, turn)
        if self.over_dp:
            for lane in (0, 1):
                rows = self.from_xy.shape[2]
                for h in range(2):
                    self.got(self.from_xy.at[lane, turn, piece(rows, h)], 5 + lane, turn, h)
                extra.append(self.from_xy.at[lane, turn])
        if self.over_z:

            def got_slot():
                self.got(self.from_z.at[z], 7, z)

            def got_other():
                self.got(self.from_z.at[self.length], 7, self.length)

            extra.append(self.from_z.at[z])
            if last:
                guarded(place.has_down, got_slot)
                guarded(place.has_up, got_other)
                extra.append(self.from_z.at[self.length])
            else:
                guarded((z > place.z) & place.has_down, got_slot)
                guarded((z < place.z) & place.has_up, got_slot)
        self.settle(0, turn, None, extra, self.out(None) if last else None)
        if self.over_z and not last:

            def going_up():
                goal = self.z_of(turn)
                return (
                    self.partial(0, turn, None),
                    self.from_z.at[goal],
                    self.send.at[7, turn, 0],
                    self.recv.at[7, goal, 0],
                )

            def going_down():
                there = self.z_of(turn)
                arrives = (there - place.z + 1 + self.length) // self.length
                goal = there + arrives * (self.length - there)
                return (
                    self.partial(0, turn, None),
                    self.from_z.at[goal],
                    self.send.at[7, turn, 0],
                    self.recv.at[7, goal, 0],
                )

            def above():
                return self.z_of(turn) > place.z

            def below():
                return self.z_of(turn) < place.z

            pl.when(above())(lambda: sends.start("up", going_up, above))
            pl.when(below())(lambda: sends.start("down", going_down, below))


def advance(item, sends, step):
    item.corners(sends, step)
    item.straight(sends, step, False)
    item.hand_over(sends, step + 2)
    item.straight(sends, step - 1, True)
    item.home(sends, step - 2 if item.over_dp else step)


def reduce_rows(partials, small, all_rows, picked, gated, hid, dgate, dup, length, collective_id):
    devices, rows, width = partials.shape
    slots, hidden = dup.shape
    half, low = rows // 2, small.shape[0] // 2
    tile, narrow = width // 4, hidden // 3
    f32, bf16 = jnp.float32, jnp.bfloat16

    def kernel(
        source, small_ref, all_ref, picked_ref, gated_ref, hid_ref, dgate_ref, dup_ref,
        target, product, out_g, out_u, out_d,
        small_all, rows_v, rows_sem, hid_v, dgate_v, dup_v, picked_v, gated_v, tile_g, tile_u, tile_d, load_sem, tile_sem, store_sem,
        *rest,
    ):
        place = Place(length)
        item = ReduceItem(
            "all",
            place,
            lambda c, z, h: source.at[c * length + z, piece(2 * half, h)],
            rest[:8],
            lambda h: target.at[piece(2 * half, h)],
        )
        beside = GatherItem("all", place, None, None, *rest[8:])
        beside.own = lambda h: small_ref.at[piece(2 * low, h)]
        beside.slot = lambda c, z, h: small_all.at[c * length + z, piece(2 * low, h)]
        item.begin()
        meet(place, True, True)
        sends = Sends(place)
        beside.begin(sends)
        item.load_all()
        item.hand_over(sends, 0)
        item.hand_over(sends, 1)
        resident = [
            pltpu.make_async_copy(left, right, load_sem.at[n])
            for n, (left, right) in enumerate(
                ((hid_ref, hid_v), (dgate_ref, dgate_v), (dup_ref, dup_v))
            )
        ]
        for copy in resident:
            copy.start()

        def lanes_of(n):
            return pl.ds(pl.multiple_of(n * tile, tile), tile)

        def tiles(n, slot):
            return [
                pltpu.make_async_copy(picked_ref.at[:, lanes_of(n)], picked_v.at[slot], tile_sem.at[slot, 0]),
                pltpu.make_async_copy(gated_ref.at[:, lanes_of(n)], gated_v.at[slot], tile_sem.at[slot, 1]),
            ]

        def stores(n, slot):
            return [
                pltpu.make_async_copy(tile_g.at[slot], out_g.at[lanes_of(n)], store_sem.at[slot, 0]),
                pltpu.make_async_copy(tile_u.at[slot], out_u.at[lanes_of(n)], store_sem.at[slot, 1]),
                pltpu.make_async_copy(tile_d.at[slot], out_d.at[:, lanes_of(n)], store_sem.at[slot, 2]),
            ]

        for copy in tiles(0, 0):
            copy.start()

        def rows_load(group, part):
            return pltpu.make_async_copy(
                all_ref.at[pl.ds(group * length, length)], rows_v.at[part], rows_sem.at[part]
            )

        for part in range(2):
            rows_load(part, part).start()

        def narrow_of(m):
            return pl.ds(pl.multiple_of(m * narrow, narrow), narrow)

        def chunk(c, carry):
            n, kind = c // 3, c % 3
            slot = n % 2

            @pl.when((kind == 0) & (n < 4))
            def _():
                for copy in tiles(n, slot):
                    copy.wait()

                @pl.when(n < 3)
                def _():
                    for copy in tiles(n + 1, 1 - slot):
                        copy.start()

                @pl.when(n >= 2)
                def _():
                    for copy in stores(n, slot):
                        copy.wait()

                def body(m, carry):
                    tile_g[slot, :, narrow_of(m)] = dot(picked_v[slot], dgate_v[:, narrow_of(m)], 0, 0)
                    return carry

                lax.fori_loop(0, 3, body, 0)
                stores(n, slot)[0].start()

            @pl.when((kind == 1) & (n < 4))
            def _():
                def body(m, carry):
                    tile_u[slot, :, narrow_of(m)] = dot(picked_v[slot], dup_v[:, narrow_of(m)], 0, 0)
                    return carry

                lax.fori_loop(0, 3, body, 0)
                stores(n, slot)[1].start()

            @pl.when((kind == 2) & (n < 4))
            def _():
                def body(m, carry):
                    tile_d[slot, narrow_of(m), :] = dot(hid_v[:, narrow_of(m)], gated_v[slot], 0, 0)
                    return carry

                lax.fori_loop(0, 3, body, 0)
                stores(n, slot)[2].start()
            return carry

        def turn_of(i, carry):
            for step in range(length + 2):

                @pl.when(i == 2 * step)
                def _(step=step):
                    item.corners(sends, step)
                    item.straight(sends, step, False)
                    item.hand_over(sends, step + 2)

                @pl.when(i == 2 * step + 1)
                def _(step=step):
                    item.straight(sends, step - 1, True)
                    item.home(sends, step - 2)

            for step in range(length + 2):

                @pl.when(i == step)
                def _(step=step):
                    beside.along_z(sends, step + 1)
                    beside.across(sends, step)
                    beside.diagonal(sends, step - 1)

            @pl.when(i == length + 2)
            def _():
                beside.finish()
                product[...] = jnp.zeros(product.shape, f32)

            @pl.when((i >= length + 2) & (i < length + 6))
            def _():
                for part in range(2):
                    group = 2 * (i - length - 2) + part
                    rows_load(group, part).wait()
                    marks = [
                        small_all[group * length + z] for z in range(length)
                    ]
                    left = jnp.concatenate(marks, axis=1)

                    def body(m, carry, part=part, left=left):
                        lanes = pl.ds(pl.multiple_of(m * tile, tile), tile)
                        right = rows_v[part, :, :, lanes].reshape(length * rows, tile)
                        product[:, lanes] += dot(left, right)
                        return carry

                    lax.fori_loop(0, 4, body, 0)

                    @pl.when(group + 2 < 8)
                    def _(part=part, group=group):
                        rows_load(group + 2, part).start()

            @pl.when(i == 0)
            def _():
                for copy in resident:
                    copy.wait()

            @pl.when(i < 6)
            def _():
                lax.fori_loop(0, 2, lambda part, carry: chunk(2 * i + part, carry), 0)

            return carry

        lax.fori_loop(0, max(12, 2 * (length + 2), length + 6), turn_of, 0)
        for slot in range(2):
            for copy in stores(slot, slot):
                copy.wait()
        sends.drain()

    any_spec = pl.BlockSpec(memory_space=pl.ANY)
    shape = jax.ShapeDtypeStruct
    sems = pltpu.SemaphoreType.DMA
    return pl.pallas_call(
        kernel,
        name="reduce_rows",
        out_shape=[
            shape((rows, width), f32),
            shape((small.shape[0], width), f32),
            shape((width, hidden), f32),
            shape((width, hidden), f32),
            shape((hidden, width), f32),
        ],
        in_specs=[any_spec] * 8,
        out_specs=[pl.BlockSpec(memory_space=pltpu.VMEM)] * 2 + [any_spec] * 3,
        scratch_shapes=[
            pltpu.VMEM((devices,) + small.shape, small.dtype),
            pltpu.VMEM((2, length, rows, width), bf16),
            sems((2,)),
            pltpu.VMEM((slots, hidden), bf16),
            pltpu.VMEM((slots, hidden), bf16),
            pltpu.VMEM((slots, hidden), bf16),
            pltpu.VMEM((2, slots, tile), bf16),
            pltpu.VMEM((2, slots, tile), bf16),
            pltpu.VMEM((2, tile, hidden), f32),
            pltpu.VMEM((2, tile, hidden), f32),
            pltpu.VMEM((2, hidden, tile), f32),
            sems((3,)),
            sems((2, 2)),
            sems((2, 3)),
        ]
        + ReduceItem.scratch("all", length, rows, width)
        + GatherItem.semaphores("all", length),
        compiler_params=pltpu.CompilerParams(
            collective_id=collective_id, has_side_effects=True, vmem_limit_bytes=67043328
        ),
    )(partials, small, all_rows, picked, gated, hid, dgate, dup)


def dot(left, right, left_dim=1, right_dim=0):
    return lax.dot_general(
        left, right, (((left_dim,), (right_dim,)), ((), ())), preferred_element_type=jnp.float32
    )


def experts(rows_own, all_cots, gates_own, wgate, wup, wdown, length, capacity, collective_id):
    rows, width = rows_own.shape
    hidden = wgate.shape[1]
    devices = 8 * length
    count = 4 * capacity
    tile = 512 if width % 512 == 0 else width
    narrow = 256 if hidden % 256 == 0 else hidden
    f32, bf16 = jnp.float32, jnp.bfloat16

    def kernel(
        rows_ref, all_cots, gates_ref, wg_ref, wu_ref, wd_ref,
        all_rows, part_out, part_grad, token_in, picked_all, gated_all, hid_all, dgate_all, dup_all,
        wg, wu, wd, chosen_all, gates_all, rank_v, table, row_buf, cot_buf, picked, cotan, gated, hid, dgate, dup, scaled, back,
        chosen, slot_gate, slot_sum, stage_out, stage_grad, token_out,
        recv_r, send_r, local_r,
        load_sem, store_sem, save_sem, token_sem, gate_sem, weight_sem,
    ):
        place = Place(length)
        expert = place.dp * length + place.z

        def item_of(source, target, sems, half):
            item = GatherItem("all", place, None, None, *sems)
            item.own = lambda h: source.at[piece(2 * half, h)]
            item.slot = lambda column, z, h: target.at[
                column * length + z, piece(2 * half, h)
            ]
            return item

        big = [
            item_of(rows_ref, all_rows, (recv_r, send_r, local_r), rows // 2),
        ]
        items = big
        meet_all(place)
        sends = Sends(place)

        def gate_send(n):
            device, there = other_device(place, n + 1)
            return pltpu.make_async_remote_copy(
                src_ref=gates_ref.at[there],
                dst_ref=table.at[expert],
                send_sem=gate_sem.at[0],
                recv_sem=gate_sem.at[1],
                device_id=device,
                device_id_type=MESH,
            )

        def send_gates(n, carry):
            gate_send(n).start()
            return carry

        lax.fori_loop(0, devices - 1, send_gates, 0)
        pltpu.make_async_copy(gates_ref.at[expert], table.at[expert], gate_sem.at[1]).start()
        for item in items:
            item.begin(sends)

        weights = [
            pltpu.make_async_copy(source, target, weight_sem.at[n])
            for n, (source, target) in enumerate(((wg_ref, wg), (wu_ref, wu), (wd_ref, wd)))
        ]
        for copy in weights:
            copy.start()

        def along(distance):
            for item in items:
                item.along_z(sends, distance)

        def across(distance):
            for item in items:
                item.across(sends, distance)

        def corner(distance):
            for item in items:
                item.diagonal(sends, distance)

        across(0)
        along(1)
        pltpu.make_async_copy(table, table, gate_sem.at[1]).wait()
        order = lax.broadcasted_iota(jnp.int32, (rows, rows), 0)
        upto = (order <= lax.broadcasted_iota(jnp.int32, (rows, rows), 1)).astype(f32).astype(bf16)
        slots = lax.broadcasted_iota(jnp.int32, (capacity, rows), 0).astype(f32)
        lines = table[:, 0, :]
        rank_v[...] = dot((lines >= 0.0).astype(f32).astype(bf16), upto) - 1.0

        def choose(block, carry):
            line = table[block, 0:1, :]
            ranks = rank_v[pl.ds(block, 1), :]
            pick = jnp.where((line >= 0.0) & (ranks == slots), 1.0, 0.0)
            gate = jnp.sum(pick * line, axis=1, keepdims=True)
            chosen_all[block] = pick.astype(bf16)
            gates_all[block] = jnp.broadcast_to(gate, (capacity, 128))
            return carry

        lax.fori_loop(0, devices, choose, 0, unroll=4)
        for item in items:
            item.settled()

        def block_of(j, side, z):
            return (place.columns[j] + side * place.to_core) * length + z

        def load(j, side, z, slot):
            block = block_of(j, side, z)
            return [
                pltpu.make_async_copy(all_rows.at[block], row_buf.at[slot, j], load_sem.at[slot, 0, j]),
                pltpu.make_async_copy(all_cots.at[block], cot_buf.at[slot, j], load_sem.at[slot, 1, j]),
            ]

        def store(j, side, z, slot):
            block = block_of(j, side, z)
            return [
                pltpu.make_async_copy(stage_out.at[slot, j], part_out.at[block], store_sem.at[slot, 0, j]),
                pltpu.make_async_copy(stage_grad.at[slot, j], part_grad.at[block], store_sem.at[slot, 1, j]),
            ]

        def saved(i):
            first = [
                pltpu.make_async_copy(picked, picked_all.at[i], save_sem.at[0]),
                pltpu.make_async_copy(gated, gated_all.at[i], save_sem.at[1]),
            ]
            second = [
                pltpu.make_async_copy(hid, hid_all.at[i], save_sem.at[2]),
                pltpu.make_async_copy(dgate, dgate_all.at[i], save_sem.at[3]),
                pltpu.make_async_copy(dup, dup_all.at[i], save_sem.at[4]),
            ]
            return first, second

        def start_loads(step, side):
            for j in range(4):
                for copy in load(j, side, place.nearest(step), side):
                    copy.start()

        corner(0)
        for item in items:
            item.from_core(place.nearest(0))
        start_loads(0, 0)
        start_loads(0, 1)
        for copy in weights:
            copy.wait()

        def unit(i, carry):
            turn, side = i // 2, i % 2
            z = place.nearest(turn)

            @pl.when(i == 1)
            def _():
                along(2)
                across(1)

            for step in range(1, length):

                @pl.when(i == max(2, 2 * step - 1))
                def _(step=step):
                    corner(step)
                    along(step + 2)
                    across(step + 1)
                    for item in items:
                        item.from_core(place.nearest(step))
                    start_loads(step, 0)
                    if step == 1:
                        start_loads(step, 1)

            @pl.when(i >= 1)
            def _():
                for copy in saved(i)[0]:
                    copy.wait()

            for j in range(4):
                for copy in load(j, side, z, side):
                    copy.wait()
            for j in range(4):
                block = block_of(j, side, z)
                chosen[j] = chosen_all[block]
                slot_gate[pl.ds(j * capacity, capacity), :] = gates_all[block]

            def select(n, carry):
                lanes = pl.ds(pl.multiple_of(n * tile, tile), tile)
                for j in range(4):
                    at = pl.ds(j * capacity, capacity)
                    picked[at, lanes] = dot(chosen[j], row_buf[side, j, :, lanes]).astype(bf16)
                    cot = dot(chosen[j], cot_buf[side, j, :, lanes])
                    cotan[at, lanes] = cot.astype(bf16)
                    gated[at, lanes] = (slot_gate[at, 0:1] * cot).astype(bf16)
                return carry

            lax.fori_loop(0, width // tile, select, 0)

            for copy in saved(i)[0]:
                copy.start()
            for step in range(2, length):

                @pl.when(i == 2 * step - 1)
                def _(step=step):
                    start_loads(step, 1)

            @pl.when(i >= 1)
            def _():
                for copy in saved(i)[1]:
                    copy.wait()

            def middle(n, carry):
                lanes = pl.ds(pl.multiple_of(n * narrow, narrow), narrow)
                gate = dot(picked[...], wg[:, lanes])
                up = dot(picked[...], wu[:, lanes])
                grad = dot(gated[...], wd[lanes, :], 1, 1)
                sigma = jax.nn.sigmoid(gate)
                hid[:, lanes] = (gate * sigma * up).astype(bf16)
                dgate[:, lanes] = (grad * up * sigma * (1.0 + gate * (1.0 - sigma))).astype(bf16)
                dup[:, lanes] = (grad * gate * sigma).astype(bf16)
                return carry

            lax.fori_loop(0, hidden // narrow, middle, 0)
            for copy in saved(i)[1]:
                copy.start()
            slot_sum[...] = jnp.zeros(slot_sum.shape, f32)

            @pl.when(i >= 2)
            def _():
                for j in range(4):
                    for copy in store(j, side, z, side):
                        copy.wait()

            def outward(n, carry):
                lanes = pl.ds(pl.multiple_of(n * tile, tile), tile)
                result = dot(hid[...], wd[:, lanes]).astype(bf16).astype(f32)
                products = cotan[:, lanes].astype(f32) * result
                total = products[:, 0:128]
                for k in range(1, tile // 128):
                    total = total + products[:, 128 * k : 128 * (k + 1)]
                slot_sum[...] += total
                scaled[:, lanes] = (slot_gate[:, 0:1] * result).astype(bf16)
                back[:, lanes] = (
                    dot(dgate[...], wg[lanes, :], 1, 1) + dot(dup[...], wu[lanes, :], 1, 1)
                ).astype(bf16)
                for j in range(4):
                    at = pl.ds(j * capacity, capacity)
                    stage_out[side, j, :, lanes] = dot(chosen[j], scaled[at, lanes], 0, 0).astype(bf16)
                    stage_grad[side, j, :, lanes] = dot(chosen[j], back[at, lanes], 0, 0).astype(bf16)
                return carry

            lax.fori_loop(0, width // tile, outward, 0)
            for j in range(4):
                for copy in store(j, side, z, side):
                    copy.start()
            total = jnp.sum(slot_sum[...], axis=1, keepdims=True).reshape(4, capacity, 1)
            sums = jnp.sum(chosen[...].astype(f32) * total, axis=1)
            for j in range(4):
                token_out[block_of(j, side, z)] = jnp.broadcast_to(sums[j : j + 1], (8, rows))
            return carry

        lax.fori_loop(0, 2 * length, unit, 0)

        def token_send(n):
            device, there = other_device(place, n + 1)
            return pltpu.make_async_remote_copy(
                src_ref=token_out.at[there],
                dst_ref=token_in.at[expert],
                send_sem=token_sem.at[0],
                recv_sem=token_sem.at[1],
                device_id=device,
                device_id_type=MESH,
            )

        def send(n, carry):
            token_send(n).start()
            return carry

        lax.fori_loop(0, devices - 1, send, 0)
        pltpu.make_async_copy(token_out.at[expert], token_in.at[expert], token_sem.at[1]).start()
        for side in range(2):
            for j in range(4):
                for copy in store(j, side, 0, side):
                    copy.wait()
        for copies in saved(0):
            for copy in copies:
                copy.wait()
        sends.drain()
        pltpu.make_async_copy(token_out, token_in, token_sem.at[1]).wait()
        sent = token_out.at[pl.ds(0, devices - 1)]
        pltpu.make_async_copy(sent, sent, token_sem.at[0]).wait()
        pltpu.make_async_copy(sent, sent, gate_sem.at[0]).wait()

    any_spec = pl.BlockSpec(memory_space=pl.ANY)
    vmem = pl.BlockSpec(memory_space=pltpu.VMEM)
    big = (devices, rows, width)
    shape = jax.ShapeDtypeStruct
    sems = pltpu.SemaphoreType.DMA
    return pl.pallas_call(
        kernel,
        name="experts",
        out_shape=[
            shape(big, bf16), shape(big, bf16), shape(big, bf16),
            shape((devices, 8, rows), f32),
            shape((2 * length, count, width), bf16), shape((2 * length, count, width), bf16),
            shape((2 * length, count, hidden), bf16), shape((2 * length, count, hidden), bf16),
            shape((2 * length, count, hidden), bf16),
        ],
        in_specs=[any_spec] * 6,
        out_specs=[any_spec] * 3 + [vmem] + [any_spec] * 5,
        scratch_shapes=[
            pltpu.VMEM((width, hidden), bf16),
            pltpu.VMEM((width, hidden), bf16),
            pltpu.VMEM((hidden, width), bf16),
            pltpu.VMEM((devices, capacity, rows), bf16),
            pltpu.VMEM((devices, capacity, 128), f32),
            pltpu.VMEM((devices, rows), f32),
            pltpu.VMEM((devices, 8, rows), f32),
            pltpu.VMEM((2, 4, rows, width), bf16),
            pltpu.VMEM((2, 4, rows, width), bf16),
            pltpu.VMEM((count, width), bf16),
            pltpu.VMEM((count, width), bf16),
            pltpu.VMEM((count, width), bf16),
            pltpu.VMEM((count, hidden), bf16),
            pltpu.VMEM((count, hidden), bf16),
            pltpu.VMEM((count, hidden), bf16),
            pltpu.VMEM((count, width), bf16),
            pltpu.VMEM((count, width), bf16),
            pltpu.VMEM((4, capacity, rows), bf16),
            pltpu.VMEM((count, 128), f32),
            pltpu.VMEM((count, 128), f32),
            pltpu.VMEM((2, 4, rows, width), bf16),
            pltpu.VMEM((2, 4, rows, width), bf16),
            pltpu.VMEM((devices, 8, rows), f32),
        ]
        + GatherItem.semaphores("all", length)
        + [sems((2, 2, 4)), sems((2, 2, 4)), sems((5,)), sems((2,)), sems((2,)), sems((3,))],
        compiler_params=pltpu.CompilerParams(
            collective_id=collective_id, has_side_effects=True, vmem_limit_bytes=63 << 20
        ),
    )(rows_own, all_cots, gates_own, wgate, wup, wdown)


def rope(values, cosine, sine):
    return values * cosine + pltpu.roll(values, values.shape[-1] // 2, 1) * sine


def unrope(values, cosine, sine):
    return values * cosine - pltpu.roll(values, values.shape[-1] // 2, 1) * sine


def row_factor(values):
    return lax.rsqrt(jnp.mean(values * values, axis=-1, keepdims=True) + EPSILON)


def visible_pairs(seg_col, seg_row, start, stop, reach):
    shape = (stop - start, reach)
    query = lax.broadcasted_iota(jnp.int32, shape, 0) + start
    key = lax.broadcasted_iota(jnp.int32, shape, 1)
    return (seg_col[start:stop, :] == seg_row[:, 0:reach]) & (key <= query)


def attend(rows_own, joint_own, output_own, cots_own, seg_col, seg_row, cosine, sine, query_gain, key_gain, length, collective_id):
    rows, width = rows_own.shape
    depth, joint = joint_own.shape
    head_width, part = output_own.shape
    head = query_gain.shape[-1]
    heads = head_width // head
    tokens = rows * length
    block = tokens // 2
    tile = 512
    scale = 1.0 / math.sqrt(head)
    f32, bf16 = jnp.float32, jnp.bfloat16

    def kernel(
        rows_ref, joint_ref, output_ref, cots_ref, segc, segr, cos_ref, sin_ref, qgain, kgain,
        out_add, out_rows, out_joint, out_weight, out_cots, out_qkv, out_heads,
        rows_v, joint_v, weight_v, qkv, att, key_v, value_v,
        r0, r1, r2, r3, r4, r5, r6, r7,
        g0, g1, g2, j0, j1, j2, w0, w1, w2, c0, c1, c2, save_sem,
    ):
        place = Place(length)

        def item_of(mode, source, half, slot, sems):
            item = GatherItem(mode, place, None, None, *sems)
            item.own = lambda h: source.at[piece(2 * half, h)]
            item.slot = slot
            return item

        half, deep, tall = rows // 2, depth // 2, head_width // 2
        own_rows = item_of(
            "z", rows_ref, half, lambda c, z, h: rows_v.at[z, piece(2 * half, h)], (g0, g1, g2)
        )
        own_joint = item_of(
            "dp", joint_ref, deep, lambda c, z, h: joint_v.at[c, piece(2 * deep, h)], (j0, j1, j2)
        )
        own_weight = item_of(
            "dp",
            output_ref,
            tall,
            lambda c, z, h: weight_v.at[
                piece(2 * tall, h), pl.ds(pl.multiple_of(c * part, part), part)
            ],
            (w0, w1, w2),
        )
        cots = item_of(
            "all",
            cots_ref,
            half,
            lambda c, z, h: out_cots.at[c * length + z, piece(2 * half, h)],
            (c0, c1, c2),
        )
        total = ReduceItem(
            "z", place, None, (r0, r1, r2, r3, r4, r5, r6, r7),
            lambda h: out_add.at[piece(2 * half, h)],
        )
        total.computed = True
        total.begin()
        meet(place, True, True)
        sends = Sends(place)
        own_joint.begin(sends)
        own_rows.begin(sends)
        own_weight.begin(sends)
        own_joint.across(sends, 0)
        own_rows.along_z(sends, 1)
        own_weight.across(sends, 0)
        own_joint.diagonal(sends, 0)
        own_rows.along_z(sends, 2)
        cots.begin(sends)
        own_weight.diagonal(sends, 0)
        for distance in range(3, length):
            own_rows.along_z(sends, distance)
        own_joint.finish()
        own_rows.finish()

        def projection(n, carry):
            lanes = pl.ds(pl.multiple_of(n * 256, 256), 256)
            left = rows_v[...].reshape(tokens, width)
            right = joint_v[:, :, lanes].reshape(width, 256)
            qkv[:, lanes] = dot(left, right)
            return carry

        lax.fori_loop(0, joint // 256, projection, 0)
        saves = [
            pltpu.make_async_copy(source, target, save_sem.at[n])
            for n, (source, target) in enumerate(
                ((rows_v, out_rows), (joint_v, out_joint), (qkv, out_qkv), (weight_v, out_weight), (att, out_heads))
            )
        ]
        for copy in saves[:3]:
            copy.start()
        key = qkv[:, head_width : head_width + head]
        key_v[...] = rope(key * row_factor(key) * kgain[...], cos_ref[...], sin_ref[...]).astype(bf16)
        value_v[...] = qkv[:, head_width + head : head_width + 2 * head].astype(bf16)

        def one_head(n, carry):
            lanes = pl.ds(pl.multiple_of(n * head, head), head)
            for start in range(0, tokens, block):
                stop = start + block
                query = qkv[start:stop, lanes]
                turned = rope(
                    query * row_factor(query) * qgain[...], cos_ref[start:stop, :], sin_ref[start:stop, :]
                ).astype(bf16)
                scores = dot(turned, key_v[0:stop, :], 1, 1) * scale
                seen = visible_pairs(segc, segr, start, stop, stop)
                scores = jnp.where(seen, scores, NEG_BIG)
                top = jnp.max(scores, axis=-1, keepdims=True)
                powers = jnp.exp(scores - top)
                probs = (powers / jnp.sum(powers, axis=-1, keepdims=True)).astype(bf16)
                att[start:stop, lanes] = dot(probs, value_v[0:stop, :]).astype(bf16)
            return carry

        lax.fori_loop(0, heads // 2, one_head, 0)
        cots.across(sends, 0)
        cots.along_z(sends, 1)
        lax.fori_loop(heads // 2, heads, one_head, 0)
        saves[4].start()
        own_weight.finish()
        saves[3].start()

        def outward(turn):
            z = total.z_of(turn)

            def body(n, carry):
                lanes = pl.ds(pl.multiple_of(n * tile, tile), tile)
                left = att[pl.ds(pl.multiple_of(z * rows, rows), rows), :]
                found = dot(left, weight_v[:, lanes]).astype(bf16)
                total.acc[0, turn, :, lanes] = found
                return carry

            lax.fori_loop(0, width // tile, body, 0)

        for turn in range(length):
            outward(turn)
            total.home(sends, turn)
            cots.diagonal(sends, turn)
            cots.across(sends, turn + 1)
            cots.along_z(sends, turn + 2)
        cots.finish()
        for copy in saves:
            copy.wait()
        sends.drain()

    any_spec = pl.BlockSpec(memory_space=pl.ANY)
    vmem = pl.BlockSpec(memory_space=pltpu.VMEM)
    shape = jax.ShapeDtypeStruct
    return pl.pallas_call(
        kernel,
        name="attend",
        out_shape=[
            shape((rows, width), f32),
            shape((length, rows, width), bf16),
            shape((8, depth, joint), bf16),
            shape((head_width, 8 * part), bf16),
            shape((8 * length, rows, width), bf16),
            shape((tokens, joint), f32),
            shape((tokens, head_width), bf16),
        ],
        in_specs=[any_spec] * 4 + [vmem] * 6,
        out_specs=[vmem] + [any_spec] * 6,
        scratch_shapes=[
            pltpu.VMEM((length, rows, width), bf16),
            pltpu.VMEM((8, depth, joint), bf16),
            pltpu.VMEM((head_width, 8 * part), bf16),
            pltpu.VMEM((tokens, joint), f32),
            pltpu.VMEM((tokens, head_width), bf16),
            pltpu.VMEM((tokens, head), bf16),
            pltpu.VMEM((tokens, head), bf16),
        ]
        + ReduceItem.scratch("z", length, rows, width)
        + GatherItem.semaphores("z", length)
        + GatherItem.semaphores("dp", length) * 2
        + GatherItem.semaphores("all", length)
        + [pltpu.SemaphoreType.DMA((5,))],
        compiler_params=pltpu.CompilerParams(
            collective_id=collective_id, has_side_effects=True, vmem_limit_bytes=56 << 20
        ),
    )(rows_own, joint_own, output_own, cots_own, seg_col, seg_row, cosine, sine, query_gain, key_gain)


def attend_back(grad_own, rows_all, joint_all, output_all, qkv_all, heads_all, part_out, seg_col, seg_row, cosine, sine, query_gain, key_gain, length, collective_id):
    rows, width = grad_own.shape
    _, depth, joint = joint_all.shape
    head_width = output_all.shape[0]
    part = width // 8
    head = query_gain.shape[-1]
    heads = head_width // head
    tokens = rows * length
    block = tokens // 2
    scale = 1.0 / math.sqrt(head)
    f32, bf16 = jnp.float32, jnp.bfloat16
    half, deep, tall = rows // 2, depth // 2, head_width // 2

    def kernel(
        grad_ref, rows_ref, joint_ref, output_ref, qkv_ref, heads_ref, part_ref,
        segc, segr, cos_ref, sin_ref, qgain, kgain,
        out_rows, out_joint, out_weight, out_moe, out_qgain, out_kgain,
        grads, joint_v, weight_v, qkv, att, gatt, joint_b, part_w, key_v, value_v, dkey, dvalue,
        *rest,
    ):
        place = Place(length)
        o_bufs, z_bufs, j_bufs, w_bufs = (rest[8 * n : 8 * n + 8] for n in range(4))
        gather_sems, load_sem = rest[32:35], rest[35]

        outs = ReduceItem(
            "all",
            place,
            lambda c, z, h: part_ref.at[c * length + z, piece(2 * half, h)],
            o_bufs,
            lambda h: out_moe.at[piece(2 * half, h)],
        )
        back = ReduceItem(
            "z",
            place,
            lambda c, z, h: grads.at[z, piece(2 * half, h)],
            z_bufs,
            lambda h: out_rows.at[piece(2 * half, h)],
        )
        joints = ReduceItem(
            "dp",
            place,
            lambda c, z, h: joint_v.at[c, piece(2 * deep, h)],
            j_bufs,
            lambda h: out_joint.at[piece(2 * deep, h)],
        )
        weights = ReduceItem(
            "dp",
            place,
            lambda c, z, h: part_w.at[
                piece(2 * tall, h), pl.ds(pl.multiple_of(c * part, part), part)
            ],
            w_bufs,
            lambda h: out_weight.at[piece(2 * tall, h)],
        )
        for item in (back, joints, weights):
            item.in_place = True
        gathers = GatherItem("z", place, None, None, *gather_sems)
        gathers.own = lambda h: grad_ref.at[piece(2 * half, h)]
        gathers.slot = lambda c, z, h: grads.at[z, piece(2 * half, h)]

        outs.begin()
        back.begin()
        meet(place, True, True)
        first, sends = Sends(place), Sends(place)
        gathers.begin(first)
        outs.load_all()
        outs.hand_over(sends, 0)
        outs.hand_over(sends, 1)
        loads = [
            pltpu.make_async_copy(source, target, load_sem.at[n])
            for n, (source, target) in enumerate(
                ((output_ref, weight_v), (heads_ref, att), (qkv_ref, qkv), (joint_ref, joint_v))
            )
        ]
        for copy in loads:
            copy.start()
        advance(outs, sends, 0)
        for distance in range(1, length):
            gathers.along_z(first, distance)
            if distance < length - 1:
                advance(outs, sends, distance)
        gathers.finish()
        first.drain()
        for copy in loads[:3]:
            copy.wait()

        def to_heads(n, carry):
            lanes = pl.ds(pl.multiple_of(n * 256, 256), 256)
            left = grads[...].reshape(tokens, width)
            gatt[:, lanes] = dot(left, weight_v[lanes, :], 1, 1).astype(bf16)
            return carry

        def to_weight(n, carry):
            lanes = pl.ds(pl.multiple_of(n * 256, 256), 256)
            right = grads[:, :, lanes].reshape(tokens, 256)
            part_w[:, lanes] = dot(att[...], right, 0, 0).astype(bf16)
            return carry

        lax.fori_loop(0, width // 256, to_weight, 0)
        weights.hand_over(sends, 0)
        lax.fori_loop(0, head_width // 256, to_heads, 0)
        rows_v = weight_v.at[pl.ds(0, tokens)]
        rows_loads = [
            pltpu.make_async_copy(
                rows_ref.at[z], weight_v.at[pl.ds(z * rows, rows)], load_sem.at[4 + z]
            )
            for z in range(length)
        ]
        for copy in rows_loads:
            copy.start()
        advance(weights, sends, 0)
        key = qkv[:, head_width : head_width + head]
        key_v[...] = rope(key * row_factor(key) * kgain[...], cos_ref[...], sin_ref[...]).astype(bf16)
        value_v[...] = qkv[:, head_width + head : head_width + 2 * head].astype(bf16)
        dkey[...] = jnp.zeros((tokens, head), f32)
        dvalue[...] = jnp.zeros((tokens, head), f32)
        out_qgain[...] = jnp.zeros(out_qgain.shape, f32)

        def normed_back(grad, raw, gain, start, stop):
            factor = row_factor(raw)
            hat = raw * factor
            turned = unrope(grad, cos_ref[start:stop, :], sin_ref[start:stop, :])
            scaled = turned * gain
            found = factor * (scaled - hat * jnp.mean(scaled * hat, axis=-1, keepdims=True))
            return found, jnp.sum(turned * hat, axis=0, keepdims=True)

        def one_head(n, carry):
            lanes = pl.ds(pl.multiple_of(n * head, head), head)
            for start in range(0, tokens, block):
                stop = start + block
                raw = qkv[start:stop, lanes]
                turned = rope(
                    raw * row_factor(raw) * qgain[...], cos_ref[start:stop, :], sin_ref[start:stop, :]
                ).astype(bf16)
                grad = gatt[start:stop, lanes]
                delta = jnp.sum(
                    grad.astype(f32) * att[start:stop, lanes].astype(f32), axis=-1, keepdims=True
                )
                scores = dot(turned, key_v[0:stop, :], 1, 1) * scale
                seen = visible_pairs(segc, segr, start, stop, stop)
                scores = jnp.where(seen, scores, NEG_BIG)
                powers = jnp.exp(scores - jnp.max(scores, axis=-1, keepdims=True))
                probs = powers / jnp.sum(powers, axis=-1, keepdims=True)
                dprobs = dot(grad, value_v[0:stop, :], 1, 1)
                dscores = (probs * (dprobs - delta)).astype(bf16)
                dvalue[0:stop, :] += dot(probs.astype(bf16), grad, 0, 0)
                dkey[0:stop, :] += dot(dscores, turned, 0, 0) * scale
                dquery = dot(dscores, key_v[0:stop, :]) * scale
                found, gain_part = normed_back(dquery, raw, qgain[...], start, stop)
                joint_b[start:stop, lanes] = found.astype(bf16)
                out_qgain[...] += gain_part
            return carry

        lax.fori_loop(0, heads // 2, one_head, 0)
        advance(outs, sends, length - 1)
        advance(weights, sends, 1)
        lax.fori_loop(heads // 2, heads, one_head, 0)
        found, gain_part = normed_back(
            dkey[...], qkv[:, head_width : head_width + head], kgain[...], 0, tokens
        )
        out_kgain[...] = gain_part
        joint_b[:, head_width : head_width + head] = found.astype(bf16)
        joint_b[:, head_width + head : head_width + 2 * head] = dvalue[...].astype(bf16)
        loads[3].wait()

        def to_rows(n, carry):
            lanes = pl.ds(pl.multiple_of(n * depth, depth), depth)
            found = dot(joint_b[...], joint_v[n], 1, 1).astype(bf16)
            grads[:, :, lanes] = found.reshape(length, rows, depth)
            return carry

        lax.fori_loop(0, 8, to_rows, 0)
        back.home(sends, 0)
        for copy in rows_loads:
            copy.wait()

        def to_joint(n, carry):
            lanes = pl.ds(pl.multiple_of(n * depth, depth), depth)
            joint_v[n] = dot(weight_v[0:tokens, lanes], joint_b[...], 0, 0).astype(bf16)
            return carry

        lax.fori_loop(0, 8, to_joint, 0)
        joints.hand_over(sends, 0)
        advance(outs, sends, length)
        advance(joints, sends, 0)
        back.home(sends, 1)
        advance(weights, sends, 2)
        for turn in range(2, length - 1):
            back.home(sends, turn)
        advance(joints, sends, 1)
        advance(outs, sends, length + 1)
        back.home(sends, length - 1)
        advance(joints, sends, 2)
        sends.drain()

    any_spec = pl.BlockSpec(memory_space=pl.ANY)
    vmem = pl.BlockSpec(memory_space=pltpu.VMEM)
    shape = jax.ShapeDtypeStruct
    return pl.pallas_call(
        kernel,
        name="attend_back",
        out_shape=[
            shape((rows, width), f32),
            shape((depth, joint), f32),
            shape((head_width, part), f32),
            shape((rows, width), f32),
            shape((1, head), f32),
            shape((1, head), f32),
        ],
        in_specs=[any_spec] * 7 + [vmem] * 6,
        out_specs=[vmem] * 6,
        scratch_shapes=[
            pltpu.VMEM((length, rows, width), bf16),
            pltpu.VMEM((8, depth, joint), bf16),
            pltpu.VMEM((head_width, width), bf16),
            pltpu.VMEM((tokens, joint), f32),
            pltpu.VMEM((tokens, head_width), bf16),
            pltpu.VMEM((tokens, head_width), bf16),
            pltpu.VMEM((tokens, joint), bf16),
            pltpu.VMEM((head_width, width), bf16),
            pltpu.VMEM((tokens, head), bf16),
            pltpu.VMEM((tokens, head), bf16),
            pltpu.VMEM((tokens, head), f32),
            pltpu.VMEM((tokens, head), f32),
        ]
        + ReduceItem.scratch("all", length, rows, width)
        + ReduceItem.scratch("z", length, rows, width, True)
        + ReduceItem.scratch("dp", length, depth, joint, True)
        + ReduceItem.scratch("dp", length, head_width, part, True)
        + GatherItem.semaphores("z", length)
        + [pltpu.SemaphoreType.DMA((4 + length,))],
        compiler_params=pltpu.CompilerParams(
            collective_id=collective_id, has_side_effects=True, vmem_limit_bytes=67043328
        ),
    )(grad_own, rows_all, joint_all, output_all, qkv_all, heads_all, part_out, seg_col, seg_row, cosine, sine, query_gain, key_gain)


def share_sum(values, length, collective_id):
    rows, width = values.shape
    jumps = []
    while 2 ** len(jumps) < length:
        jumps.append(2 ** len(jumps))
    stages = 3 + len(jumps)

    def kernel(own, target, sums, land, send_sem, recv_sem):
        place = Place(length)
        z = place.z
        partners = [(place.core, z), (place.x, z), (place.y, z)] + [
            (place.dp, z + jump - 2 * jump * ((z // jump) % 2)) for jump in jumps
        ]
        barrier = pltpu.get_barrier_semaphore()
        for device in partners:
            pl.semaphore_signal(barrier, 1, device_id=device, device_id_type=MESH)
        pl.semaphore_wait(barrier, stages)
        sums[0] = own[...]
        copies = []
        for stage, device in enumerate(partners):
            copy = pltpu.make_async_remote_copy(
                src_ref=sums.at[stage],
                dst_ref=land.at[stage],
                send_sem=send_sem.at[stage],
                recv_sem=recv_sem.at[stage],
                device_id=device,
                device_id_type=MESH,
            )
            copy.start()
            copies.append(copy)
            copy.wait_recv()
            total = sums[stage] + land[stage]
            if stage + 1 < stages:
                sums[stage + 1] = total
            else:
                target[...] = total
        for copy in copies:
            copy.wait_send()

    vmem = pl.BlockSpec(memory_space=pltpu.VMEM)
    return pl.pallas_call(
        kernel,
        name="share_sum",
        out_shape=jax.ShapeDtypeStruct((rows, width), values.dtype),
        in_specs=[vmem],
        out_specs=vmem,
        scratch_shapes=[
            pltpu.VMEM((stages, rows, width), values.dtype),
            pltpu.VMEM((stages, rows, width), values.dtype),
            pltpu.SemaphoreType.DMA((stages,)),
            pltpu.SemaphoreType.DMA((stages,)),
        ],
        compiler_params=pltpu.CompilerParams(collective_id=collective_id, has_side_effects=True),
    )(values)


def mix(form, left, right):
    return jnp.einsum(form, left, right, preferred_element_type=jnp.float32)


def rms_scale(values):
    return lax.rsqrt(jnp.mean(values * values, axis=-1, keepdims=True) + EPSILON)


def rope_tables(seg_ids, head_dim):
    length = seg_ids.shape[0]
    row_index = jnp.arange(length, dtype=jnp.int32)
    starts = jnp.sum((seg_ids[None, :] < seg_ids[:, None]).astype(jnp.int32), axis=1)
    places = (row_index - starts).astype(jnp.float32)
    half_dim = head_dim // 2
    frequency = THETA_BASE ** (-(jnp.arange(half_dim, dtype=jnp.float32) * (2.0 / head_dim)))
    angles = places[:, None] * frequency[None, :]
    return (jnp.cos(angles), jnp.sin(angles))


def rotate(values, cosine, sine_table):
    half_dim = values.shape[-1] // 2
    front_part = values[..., :half_dim]
    back_part = values[..., half_dim:]
    cos_rows = cosine[:, None, :]
    sin_rows = sine_table[:, None, :]
    return jnp.concatenate(
        [
            front_part * cos_rows - back_part * sin_rows,
            back_part * cos_rows + front_part * sin_rows,
        ],
        axis=-1,
    )


def unrotate(values, cosine, sine_table):
    half_dim = values.shape[-1] // 2
    front_part = values[..., :half_dim]
    back_part = values[..., half_dim:]
    cos_rows = cosine[:, None, :]
    sin_rows = sine_table[:, None, :]
    return jnp.concatenate(
        [
            front_part * cos_rows + back_part * sin_rows,
            back_part * cos_rows - front_part * sin_rows,
        ],
        axis=-1,
    )


def head_norm_back(grad_out, normed, factor, gain):
    grad_normed = grad_out * gain
    grad_gain = jnp.sum(grad_out * normed, axis=(0, 1))
    grad_values = factor * (
        grad_normed - normed * jnp.mean(grad_normed * normed, axis=-1, keepdims=True)
    )
    return (grad_values, grad_gain)


def row_norm_back(grad_out, normed, factor, gain):
    grad_normed = grad_out * gain
    grad_gain = jnp.sum(grad_out * normed, axis=0)
    grad_values = factor * (
        grad_normed - normed * jnp.mean(grad_normed * normed, axis=-1, keepdims=True)
    )
    return (grad_values, grad_gain)


def softmax_rows(logits):
    top_value = jnp.max(logits, axis=-1, keepdims=True)
    expo = jnp.exp(logits - top_value)
    return expo / jnp.sum(expo, axis=-1, keepdims=True)


def attn_forward(rows, seg_ids, wq_full, wk_full, wv_full, query_gain, key_gain):
    length = rows.shape[0]
    head_dim = query_gain.shape[0]
    num_heads = wq_full.shape[1] // head_dim
    kv_heads = wk_full.shape[1] // head_dim
    per_group = num_heads // kv_heads
    inv_root = 1.0 / math.sqrt(head_dim)
    block_rows = math.gcd(length, 512)
    cosine, sine_table = rope_tables(seg_ids, head_dim)
    query = jnp.dot(rows, wq_full, preferred_element_type=jnp.float32).reshape(
        length, num_heads, head_dim
    )
    key_proj = jnp.dot(rows, wk_full, preferred_element_type=jnp.float32).reshape(
        length, kv_heads, head_dim
    )
    value_rows = (
        jnp.dot(rows, wv_full, preferred_element_type=jnp.float32)
        .astype(jnp.bfloat16)
        .reshape(length, kv_heads, head_dim)
    )
    query_factor = rms_scale(query)
    query_hat = query * query_factor
    key_factor = rms_scale(key_proj)
    key_hat = key_proj * key_factor
    query_rot = (
        rotate(query_hat * query_gain, cosine, sine_table)
        .astype(jnp.bfloat16)
        .reshape(length, kv_heads, per_group, head_dim)
    )
    key_rot = rotate(key_hat * key_gain, cosine, sine_table).astype(jnp.bfloat16)
    row_index = jnp.arange(length, dtype=jnp.int32)
    scores = mix("qgrd,kgd->grqk", query_rot, key_rot) * inv_root
    visible = (seg_ids[0:block_rows, None] == seg_ids[None, :]) & (
        row_index[None, :] <= row_index[0:block_rows, None]
    )
    scores = jnp.where(visible, scores, NEG_BIG)
    top_value = jnp.max(scores, axis=-1, keepdims=True)
    expo = jnp.exp(scores - top_value)
    totals = jnp.sum(expo, axis=-1, keepdims=True)
    prob_rows = (expo / totals).astype(jnp.bfloat16)
    outputs = mix("grqk,kgd->qgrd", prob_rows, value_rows).astype(jnp.bfloat16)
    lse_parts = top_value[..., 0] + jnp.log(totals[..., 0])
    attn_heads = outputs.reshape(length, num_heads * head_dim)
    return (
        attn_heads,
        lse_parts,
        query_rot,
        key_rot,
        value_rows,
        cosine,
        sine_table,
        query_hat,
        query_factor,
        key_hat,
        key_factor,
    )


def attn_backward(
    grad_attn, rows, seg_ids, wq_full, wk_full, wv_full, wo_full, query_gain, key_gain, saved
):
    (
        attn_heads,
        lse_all,
        query_rot,
        key_rot,
        value_rows,
        cosine,
        sine_table,
        query_hat,
        query_factor,
        key_hat,
        key_factor,
    ) = saved
    length = rows.shape[0]
    head_dim = query_gain.shape[0]
    num_heads = query_hat.shape[1]
    inv_root = 1.0 / math.sqrt(head_dim)
    block_rows = math.gcd(length, 512)
    grad_wo = jnp.dot(attn_heads.T, grad_attn, preferred_element_type=jnp.float32)
    grad_heads = (
        jnp.dot(grad_attn, wo_full.T, preferred_element_type=jnp.float32)
        .astype(jnp.bfloat16)
        .reshape(query_rot.shape)
    )
    heads_view = attn_heads.reshape(query_rot.shape)
    row_delta = jnp.transpose(
        jnp.sum(grad_heads.astype(jnp.float32) * heads_view.astype(jnp.float32), axis=-1), (1, 2, 0)
    )
    row_index = jnp.arange(length, dtype=jnp.int32)
    scores = mix("qgrd,kgd->grqk", query_rot, key_rot) * inv_root
    visible = (seg_ids[0:block_rows, None] == seg_ids[None, :]) & (
        row_index[None, :] <= row_index[0:block_rows, None]
    )
    scores = jnp.where(visible, scores, NEG_BIG)
    prob_f = jnp.where(visible, jnp.exp(scores - lse_all[:, :, 0:block_rows, None]), 0.0)
    prob_rows = prob_f.astype(jnp.bfloat16)
    grad_value = mix("grqk,qgrd->kgd", prob_rows, grad_heads)
    grad_probs = mix("qgrd,kgd->grqk", grad_heads, value_rows)
    grad_scores = (prob_f * (grad_probs - row_delta[:, :, 0:block_rows, None])).astype(jnp.bfloat16)
    pieces = mix("grqk,kgd->qgrd", grad_scores, key_rot) * inv_root
    grad_key_rot = mix("grqk,qgrd->kgd", grad_scores, query_rot) * inv_root
    grad_query_rot = pieces.reshape(length, num_heads, head_dim)
    grad_query, grad_qgain = head_norm_back(
        unrotate(grad_query_rot, cosine, sine_table), query_hat, query_factor, query_gain
    )
    grad_key, grad_kgain = head_norm_back(
        unrotate(grad_key_rot, cosine, sine_table), key_hat, key_factor, key_gain
    )
    query_b = grad_query.astype(jnp.bfloat16).reshape(length, -1)
    key_b = grad_key.astype(jnp.bfloat16).reshape(length, -1)
    value_b = grad_value.astype(jnp.bfloat16).reshape(length, -1)
    grad_rows = (
        jnp.dot(query_b, wq_full.T, preferred_element_type=jnp.float32)
        + jnp.dot(key_b, wk_full.T, preferred_element_type=jnp.float32)
        + jnp.dot(value_b, wv_full.T, preferred_element_type=jnp.float32)
    )
    grad_wq = jnp.dot(rows.T, query_b, preferred_element_type=jnp.float32)
    grad_wk = jnp.dot(rows.T, key_b, preferred_element_type=jnp.float32)
    grad_wv = jnp.dot(rows.T, value_b, preferred_element_type=jnp.float32)
    return (grad_rows, grad_wq, grad_wk, grad_wv, grad_wo, grad_qgain, grad_kgain)


def expert_forward(expert_rows, wgate, wup, wdown):
    gate_pre = jnp.dot(expert_rows, wgate, preferred_element_type=jnp.float32)
    up_pre = jnp.dot(expert_rows, wup, preferred_element_type=jnp.float32)
    hidden_units = (jax.nn.silu(gate_pre) * up_pre).astype(jnp.bfloat16)
    result = jnp.dot(hidden_units, wdown, preferred_element_type=jnp.float32).astype(jnp.bfloat16)
    return (result, gate_pre, up_pre, hidden_units)


def expert_backward(expert_rows, grad_result, wgate, wup, wdown, gate_pre, up_pre, hidden_units):
    grad_hidden = jnp.dot(grad_result, wdown.T, preferred_element_type=jnp.float32)
    sigma = jax.nn.sigmoid(gate_pre)
    grad_gate_pre = (grad_hidden * up_pre * sigma * (1.0 + gate_pre * (1.0 - sigma))).astype(
        jnp.bfloat16
    )
    grad_up_pre = (grad_hidden * gate_pre * sigma).astype(jnp.bfloat16)
    grad_rows = (
        jnp.dot(grad_gate_pre, wgate.T, preferred_element_type=jnp.float32)
        + jnp.dot(grad_up_pre, wup.T, preferred_element_type=jnp.float32)
    ).astype(jnp.bfloat16)
    grad_wd = jnp.dot(hidden_units.T, grad_result, preferred_element_type=jnp.float32)
    grad_wg = jnp.dot(expert_rows.T, grad_gate_pre, preferred_element_type=jnp.float32)
    grad_wu = jnp.dot(expert_rows.T, grad_up_pre, preferred_element_type=jnp.float32)
    return (grad_rows, grad_wg, grad_wu, grad_wd)


def to_experts(buffer):
    return lax.all_to_all(buffer, ("dp", "tensor"), split_axis=0, concat_axis=0, tiled=True)


def to_sources(buffer):
    return lax.all_to_all(buffer, ("dp", "tensor"), split_axis=0, concat_axis=0, tiled=True)


def shards(
    hidden_in,
    segments,
    routes,
    query_weight,
    key_weight,
    value_weight,
    output_weight,
    gain_attn,
    gain_moe,
    query_gain,
    key_gain,
    router,
    gate_weight,
    up_weight,
    down_weight,
    cotangent,
):
    seg_ids = segments[0]
    rows_dev = hidden_in.shape[0]
    width = hidden_in.shape[1]
    top_count = routes.shape[1]
    experts = router.shape[1]
    capacity = 2 * rows_dev * top_count // experts
    full_query, full_key, full_value, full_output = (
        lax.all_gather(query_weight, "dp", axis=0, tiled=True),
        lax.all_gather(key_weight, "dp", axis=0, tiled=True),
        lax.all_gather(value_weight, "dp", axis=0, tiled=True),
        lax.all_gather(output_weight, "dp", axis=1, tiled=True),
    )
    inputs32 = hidden_in.astype(jnp.float32)
    factor_one = rms_scale(inputs32)
    normed_one = inputs32 * factor_one
    rows_one = (normed_one * gain_attn).astype(jnp.bfloat16)
    group_rows = lax.all_gather(rows_one, "tensor", axis=0, tiled=True)
    saved = attn_forward(
        group_rows, seg_ids, full_query, full_key, full_value, query_gain, key_gain
    )
    partial_add = jnp.dot(saved[0], full_output, preferred_element_type=jnp.float32)
    attn_add = lax.psum_scatter(partial_add, "tensor", scatter_dimension=0, tiled=True)
    residual = inputs32 + attn_add
    factor_two = rms_scale(residual)
    normed_two = residual * factor_two
    rows_two = (normed_two * gain_moe).astype(jnp.bfloat16)
    router_probs = softmax_rows(jnp.dot(rows_two, router, preferred_element_type=jnp.float32))
    route_hot = (routes[:, :, None] == jnp.arange(experts, dtype=jnp.int32)[None, None, :]).astype(
        jnp.float32
    )
    picked = jnp.sum(route_hot * router_probs[:, None, :], axis=-1)
    total = jnp.sum(picked, axis=1, keepdims=True)
    gates = picked / total
    flat_routes = routes.reshape(-1)
    onehot = (flat_routes[:, None] == jnp.arange(experts, dtype=jnp.int32)[None, :]).astype(
        jnp.int32
    )
    ranks = jnp.sum(onehot * jnp.cumsum(onehot, axis=0), axis=1) - 1
    slots = flat_routes * capacity + ranks
    send_rows = (
        jnp.zeros((experts * capacity, width), jnp.bfloat16)
        .at[slots]
        .set(jnp.repeat(rows_two, top_count, axis=0))
    )
    received = to_experts(send_rows.reshape(experts, capacity, width)).reshape(-1, width)
    result, gate_pre, up_pre, hidden_units = expert_forward(
        received, gate_weight[0], up_weight[0], down_weight[0]
    )
    returned = to_sources(result.reshape(-1, capacity, width)).reshape(experts * capacity, width)
    pair_out = returned[slots].astype(jnp.float32).reshape(rows_dev, top_count, width)
    moe_sum = jnp.sum(gates[:, :, None] * pair_out, axis=1)
    output = (residual + moe_sum).astype(jnp.bfloat16)
    cot32 = cotangent.astype(jnp.float32)
    grad_gates = jnp.sum(cot32[:, None, :] * pair_out, axis=-1)
    grad_result = (gates[:, :, None] * cot32[:, None, :]).astype(jnp.bfloat16).reshape(-1, width)
    send_grads = jnp.zeros((experts * capacity, width), jnp.bfloat16).at[slots].set(grad_result)
    received_grads = to_experts(send_grads.reshape(experts, capacity, width)).reshape(-1, width)
    grad_expert_rows, grad_wg, grad_wu, grad_wd = expert_backward(
        received,
        received_grads,
        gate_weight[0],
        up_weight[0],
        down_weight[0],
        gate_pre,
        up_pre,
        hidden_units,
    )
    returned_grads = to_sources(grad_expert_rows.reshape(-1, capacity, width)).reshape(
        experts * capacity, width
    )
    grad_pairs = returned_grads[slots].astype(jnp.float32).reshape(rows_dev, top_count, width)
    grad_picked = (grad_gates - jnp.sum(gates * grad_gates, axis=1, keepdims=True)) / total
    grad_probs = jnp.sum(route_hot * grad_picked[:, :, None], axis=1)
    grad_logits = (
        router_probs * (grad_probs - jnp.sum(grad_probs * router_probs, axis=-1, keepdims=True))
    ).astype(jnp.bfloat16)
    grad_router = jnp.dot(rows_two.T, grad_logits, preferred_element_type=jnp.float32)
    grad_rows_two = jnp.sum(grad_pairs, axis=1) + jnp.dot(
        grad_logits, router.T, preferred_element_type=jnp.float32
    )
    grad_res_norm, grad_gain_moe = row_norm_back(grad_rows_two, normed_two, factor_two, gain_moe)
    grad_residual = cot32 + grad_res_norm
    grad_attn = grad_residual.astype(jnp.bfloat16)
    group_grads = lax.all_gather(grad_attn, "tensor", axis=0, tiled=True)
    back_query, back_key, back_value, back_output = (
        lax.all_gather(query_weight, "dp", axis=0, tiled=True),
        lax.all_gather(key_weight, "dp", axis=0, tiled=True),
        lax.all_gather(value_weight, "dp", axis=0, tiled=True),
        lax.all_gather(output_weight, "dp", axis=1, tiled=True),
    )
    grad_group_rows, grad_wq, grad_wk, grad_wv, grad_wo, grad_qgain, grad_kgain = attn_backward(
        group_grads,
        group_rows,
        seg_ids,
        back_query,
        back_key,
        back_value,
        back_output,
        query_gain,
        key_gain,
        saved,
    )
    grad_rows_one = lax.psum_scatter(
        grad_group_rows.astype(jnp.bfloat16), "tensor", scatter_dimension=0, tiled=True
    ).astype(jnp.float32)
    grad_in_norm, grad_gain_attn = row_norm_back(grad_rows_one, normed_one, factor_one, gain_attn)
    grad_input = grad_residual + grad_in_norm
    grad_wq, grad_wk, grad_wv, grad_wo = (
        lax.psum_scatter(
            grad_wq.astype(jnp.bfloat16), "dp", scatter_dimension=0, tiled=True
        ).astype(jnp.float32),
        lax.psum_scatter(
            grad_wk.astype(jnp.bfloat16), "dp", scatter_dimension=0, tiled=True
        ).astype(jnp.float32),
        lax.psum_scatter(
            grad_wv.astype(jnp.bfloat16), "dp", scatter_dimension=0, tiled=True
        ).astype(jnp.float32),
        lax.psum_scatter(
            grad_wo.astype(jnp.bfloat16), "dp", scatter_dimension=1, tiled=True
        ).astype(jnp.float32),
    )
    grad_gain_attn, grad_gain_moe, grad_qgain, grad_kgain, grad_router = lax.psum(
        (grad_gain_attn, grad_gain_moe, grad_qgain, grad_kgain, grad_router), ("dp", "tensor")
    )
    return (
        output,
        grad_input,
        grad_wq,
        grad_wk,
        grad_wv,
        grad_wo,
        grad_gain_attn,
        grad_gain_moe,
        grad_qgain,
        grad_kgain,
        grad_router,
        grad_wg[None],
        grad_wu[None],
        grad_wd[None],
    )


AXES = ("dp", "tensor")


def gathered(
    hidden_in,
    segments,
    routes,
    query_weight,
    key_weight,
    value_weight,
    output_weight,
    gain_attn,
    gain_moe,
    query_gain,
    key_gain,
    router,
    gate_weight,
    up_weight,
    down_weight,
    cotangent,
):
    seg_ids = segments[0]
    rows_dev, width = hidden_in.shape
    top_count = routes.shape[1]
    expert_count = router.shape[1]
    capacity = 2 * rows_dev * top_count // expert_count
    length = lax.axis_size("tensor")
    query_cols, key_cols = query_weight.shape[1], key_weight.shape[1]

    inputs32 = hidden_in.astype(jnp.float32)
    factor_one = rms_scale(inputs32)
    normed_one = inputs32 * factor_one
    rows_one = (normed_one * gain_attn).astype(jnp.bfloat16)
    joint_weight = jnp.concatenate([query_weight, key_weight, value_weight], axis=1)
    cosine, sine_table = rope_tables(seg_ids, query_gain.shape[0])
    turns = (
        seg_ids[:, None],
        seg_ids[None, :],
        jnp.concatenate([cosine, cosine], axis=1),
        jnp.concatenate([-sine_table, sine_table], axis=1),
        query_gain[None, :],
        key_gain[None, :],
    )
    attn_add, group_rows, full_joint, full_output, all_cots, projected, attn_heads = attend(
        rows_one, joint_weight, output_weight, cotangent, *turns, length, 0
    )
    residual = inputs32 + attn_add
    factor_two = rms_scale(residual)
    normed_two = residual * factor_two
    rows_two = (normed_two * gain_moe).astype(jnp.bfloat16)
    router_probs = softmax_rows(jnp.dot(rows_two, router, preferred_element_type=jnp.float32))
    route_hot = (routes[:, :, None] == jnp.arange(expert_count, dtype=jnp.int32)[None, None, :]).astype(
        jnp.float32
    )
    picked = jnp.sum(route_hot * router_probs[:, None, :], axis=-1)
    total = jnp.sum(picked, axis=1, keepdims=True)
    gates = picked / total
    named = jnp.sum(route_hot, axis=1)
    gate_table = jnp.where(named > 0.5, jnp.sum(route_hot * gates[:, :, None], axis=1), -1.0)
    all_rows, partial_out, partial_rows, token_grads, *units = experts(
        rows_two,
        all_cots,
        jnp.broadcast_to(gate_table.T[:, None, :], (expert_count, 8, rows_dev)),
        gate_weight[0],
        up_weight[0],
        down_weight[0],
        length,
        capacity,
        1,
    )
    back_grads = token_grads[:, 0, :]
    cot32 = cotangent.astype(jnp.float32)
    grad_gates = jnp.sum(route_hot * back_grads.T[:, None, :], axis=-1)
    grad_picked = (grad_gates - jnp.sum(gates * grad_gates, axis=1, keepdims=True)) / total
    grad_probs = jnp.sum(route_hot * grad_picked[:, :, None], axis=1)
    grad_logits = (
        router_probs * (grad_probs - jnp.sum(grad_probs * router_probs, axis=-1, keepdims=True))
    ).astype(jnp.bfloat16)
    grad_sum, grad_router, grad_wg, grad_wu, grad_wd = reduce_rows(
        partial_rows,
        grad_logits.T,
        all_rows,
        *[unit.reshape(-1, unit.shape[-1]) for unit in units],
        length,
        2,
    )
    grad_rows_two = grad_sum + jnp.dot(grad_logits, router.T, preferred_element_type=jnp.float32)
    grad_res_norm, grad_gain_moe = row_norm_back(grad_rows_two, normed_two, factor_two, gain_moe)
    grad_residual = cot32 + grad_res_norm
    grad_attn = grad_residual.astype(jnp.bfloat16)
    grad_rows_one, grad_joint, grad_wo, moe_sum, grad_qgain, grad_kgain = attend_back(
        grad_attn,
        group_rows,
        full_joint,
        full_output,
        projected,
        attn_heads,
        partial_out,
        *turns,
        length,
        3,
    )
    output = (residual + moe_sum).astype(jnp.bfloat16)
    grad_in_norm, grad_gain_attn = row_norm_back(grad_rows_one, normed_one, factor_one, gain_attn)
    grad_input = grad_residual + grad_in_norm
    small = jnp.concatenate([grad_gain_attn, grad_gain_moe, grad_qgain[0], grad_kgain[0]]).reshape(-1, 128)
    small = jnp.pad(small, ((0, -small.shape[0] % 8), (0, 0)))
    sums = share_sum(small, length, 4).reshape(-1)
    head_dim = query_gain.shape[0]
    return (
        output,
        grad_input,
        grad_joint[:, :query_cols],
        grad_joint[:, query_cols : query_cols + key_cols],
        grad_joint[:, query_cols + key_cols :],
        grad_wo,
        sums[:width],
        sums[width : 2 * width],
        sums[2 * width : 2 * width + head_dim],
        sums[2 * width + head_dim : 2 * width + 2 * head_dim],
        grad_router.T,
        grad_wg[None],
        grad_wu[None],
        grad_wd[None],
    )


def solution(mesh):
    placed = (
        P(("dp", "tensor"), None),
        P("dp", None),
        P(("dp", "tensor"), None),
        P("dp", "tensor"),
        P("dp", "tensor"),
        P("dp", "tensor"),
        P("tensor", "dp"),
        P(),
        P(),
        P(),
        P(),
        P(),
        P(("dp", "tensor"), None, None),
        P(("dp", "tensor"), None, None),
        P(("dp", "tensor"), None, None),
        P(("dp", "tensor"), None),
    )
    program = gathered if mesh.shape["dp"] == 8 and mesh.shape["tensor"] <= 4 else shards
    return jax.shard_map(
        program,
        mesh=mesh,
        in_specs=placed,
        out_specs=(
            P(("dp", "tensor"), None),
            P(("dp", "tensor"), None),
            P("dp", "tensor"),
            P("dp", "tensor"),
            P("dp", "tensor"),
            P("tensor", "dp"),
            P(),
            P(),
            P(),
            P(),
            P(),
            P(("dp", "tensor"), None, None),
            P(("dp", "tensor"), None, None),
            P(("dp", "tensor"), None, None),
        ),
        check_vma=False,
    )
```

```python
import math

import jax
import jax.numpy as jnp
from jax import lax
from jax.experimental import pallas as pl
from jax.experimental.pallas import tpu as pltpu
from jax.sharding import PartitionSpec as P

EPSILON = 1e-06
THETA_BASE = 1000000.0
NEG_BIG = -1e30


MESH = pl.DeviceIdType.MESH


class Place:
    def __init__(self, length):
        self.length = length
        self.dp = lax.axis_index("dp")
        self.z = lax.axis_index("tensor")
        core, along_x, along_y = self.dp % 2, (self.dp // 2) % 2, self.dp // 4
        self.to_core = 1 - 2 * core
        self.core = self.dp + self.to_core
        self.x = self.dp + 2 - 4 * along_x
        self.y = self.dp + 4 - 8 * along_y
        self.columns = (self.dp, self.x, self.y, self.x + self.y - self.dp)

    def device(self, kind):
        if kind == "x":
            return (self.x, self.z)
        if kind == "y":
            return (self.y, self.z)
        if kind == "core":
            return (self.core, self.z)
        if kind == "up":
            return (self.dp, self.z + 1)
        return (self.dp, self.z - 1)

    @property
    def has_up(self):
        return self.z < self.length - 1

    @property
    def has_down(self):
        return self.z > 0

    def condition(self, kind):
        if kind == "up":
            return self.has_up
        return self.has_down if kind == "down" else None

    def nearest(self, turn):
        length = self.length

        def equal(left, right):
            far = 2 * length
            return (left - right + far) // far - (left - right - 1 + far) // far

        found = 0
        for mine in range(length):
            order = sorted(range(length), key=lambda other: (abs(other - mine), other))
            for step, other in enumerate(order):
                if other:
                    found = found + equal(self.z, mine) * equal(turn, step) * other
        return found

    def target(self, turn):
        length, z = self.length, self.z

        def at_least(left, right):
            return (left - right + 2 * length) // (2 * length)

        high = at_least(z, length // 2)
        mirrored = z + high * (length - 1 - 2 * z)
        above = length - 1 - mirrored
        first = at_least(above - 1, turn)
        if turn == length - 1:
            return z
        found = first * (length - 1 - turn) + (1 - first) * (turn - above)
        return found + high * (length - 1 - 2 * found)


def piece(rows, h):
    return pl.ds(0, rows) if h is None else pl.ds(h * (rows // 2), rows // 2)


def guarded(condition, action):
    if condition is None:
        action()
    else:
        pl.when(condition)(action)


def meet(place, over_z, over_dp):
    barrier = pltpu.get_barrier_semaphore()
    kinds = (("x", "y", "core") if over_dp else ()) + (("up", "down") if over_z else ())
    for kind in kinds:

        def greet(kind=kind):
            pl.semaphore_signal(
                barrier, 1, device_id=place.device(kind), device_id_type=MESH
            )

        guarded(place.condition(kind), greet)
    count = 3 if over_dp else 0
    if over_z:
        length = place.length
        count = count + (place.z + length - 1) // length + (2 * length - 2 - place.z) // length
    pl.semaphore_wait(barrier, count)


def other_device(place, distance):
    there = lax.rem(place.dp * place.length + place.z + distance, 8 * place.length)
    return (there // place.length, lax.rem(there, place.length)), there


def meet_all(place):
    barrier = pltpu.get_barrier_semaphore()
    others = 8 * place.length - 1

    def greet(n, carry):
        device, _ = other_device(place, n + 1)
        pl.semaphore_signal(barrier, 1, device_id=device, device_id_type=MESH)
        return carry

    lax.fori_loop(0, others, greet, 0)
    pl.semaphore_wait(barrier, others)


class Sends:
    def __init__(self, place):
        self.place = place
        self.started = []

    def start(self, kind, views, condition=lambda: None):
        def build():
            source, target, send_sem, recv_sem = views()
            return pltpu.make_async_remote_copy(
                src_ref=source,
                dst_ref=target,
                send_sem=send_sem,
                recv_sem=recv_sem,
                device_id=self.place.device(kind),
                device_id_type=MESH,
            )

        guarded(self.place.condition(kind), lambda: build().start())
        self.started.append((condition, kind, build))

    def drain(self):
        for condition, kind, build in self.started:

            def finish(kind=kind, build=build):
                guarded(self.place.condition(kind), lambda: build().wait_send())

            guarded(condition(), finish)


class GatherItem:
    def __init__(self, mode, place, own, slot, recv, send, local):
        self.mode, self.place = mode, place
        self.own, self.slot = own, slot
        self.recv, self.send, self.local = recv, send, local
        self.over_z = mode != "dp"
        self.over_dp = mode != "z"
        self.length = place.length if self.over_z else 1
        self.z = place.z if self.over_z else 0

    def index(self, column, z):
        if self.mode == "all":
            return column * self.length + z
        return column if self.mode == "dp" else z

    @staticmethod
    def semaphores(mode, length):
        blocks = {"all": 8 * length, "dp": 8, "z": length}[mode]
        turns = 2 * length - 1 if mode != "dp" else 1
        return [
            pltpu.SemaphoreType.DMA((blocks, 2)),
            pltpu.SemaphoreType.DMA((10, turns, 2)),
            pltpu.SemaphoreType.DMA((2,)),
        ]

    def turns(self, distance):
        if distance == 0:
            return [(0, 0, lambda: None, None)]
        place, length = self.place, self.length
        return [
            (2 * distance - 1, -distance, lambda: place.z >= distance, "up"),
            (2 * distance, distance, lambda: place.z < length - distance, "down"),
        ]

    def pass_on(self, sends, lane, kind, column, offset, turn, h, source=None, condition=lambda: None):
        at = 0 if h is None else h

        def views():
            z = self.z + offset
            view = self.slot(column, z, h)
            return (
                view if source is None else source(h),
                view,
                self.send.at[lane, turn, at],
                self.recv.at[self.index(column, z), at],
            )

        sends.start(kind, views, condition)

    def arrived(self, column, z, h):
        view = self.slot(column, z, h)
        at = 0 if h is None else h
        pltpu.make_async_copy(view, view, self.recv.at[self.index(column, z), at]).wait()

    def local_copy(self):
        return pltpu.make_async_copy(
            self.own(None), self.slot(self.place.dp, self.z, None), self.local.at[0]
        )

    def begin(self, sends):
        place = self.place
        if self.over_z:
            self.pass_on(sends, 0, "up", place.dp, 0, 0, None, self.own)
            self.pass_on(sends, 1, "down", place.dp, 0, 0, None, self.own)
        if self.over_dp:
            self.pass_on(sends, 2, "x", place.dp, 0, 0, None, self.own)
            self.pass_on(sends, 3, "y", place.dp, 0, 0, None, self.own)
            self.pass_on(sends, 4, "core", place.dp, 0, 0, None, self.own)
        self.local_copy().start()

    def along_z(self, sends, distance):
        if not self.over_z or distance >= self.length:
            return
        place = self.place
        for turn, offset, condition, onward in self.turns(distance):

            def step(turn=turn, offset=offset, condition=condition, onward=onward):
                self.arrived(place.dp, self.z + offset, None)
                lanes = []
                if distance < self.length - 1:
                    lanes.append((0 if onward == "up" else 1, onward))
                if self.over_dp:
                    lanes += [(2, "x"), (3, "y"), (4, "core")]
                for lane, kind in lanes:
                    self.pass_on(
                        sends, lane, kind, place.dp, offset, turn, None, condition=condition
                    )

            guarded(condition(), step)

    def across(self, sends, distance):
        if not self.over_dp or not 0 <= distance < self.length:
            return
        _, x, y, _ = self.place.columns
        for turn, offset, condition, _ in self.turns(distance):

            def step(turn=turn, offset=offset, condition=condition):
                self.arrived(x, self.z + offset, None)
                self.pass_on(sends, 5, "y", x, offset, turn, 0, condition=condition)
                self.pass_on(sends, 7, "core", x, offset, turn, None, condition=condition)
                self.arrived(y, self.z + offset, None)
                self.pass_on(sends, 6, "x", y, offset, turn, 1, condition=condition)
                self.pass_on(sends, 8, "core", y, offset, turn, None, condition=condition)

            guarded(condition(), step)

    def diagonal(self, sends, distance):
        if not self.over_dp or not 0 <= distance < self.length:
            return
        corner = self.place.columns[3]
        for turn, offset, condition, _ in self.turns(distance):

            def step(turn=turn, offset=offset, condition=condition):
                for h in range(2):
                    self.arrived(corner, self.z + offset, h)
                    self.pass_on(sends, 9, "core", corner, offset, turn, h, condition=condition)

            guarded(condition(), step)

    def settled(self):
        self.local_copy().wait()

    def from_core(self, z):
        for number, column in enumerate(self.place.columns):
            for h in (0, 1) if number == 3 else (None,):
                self.arrived(column + self.place.to_core, z, h)

    def finish(self):
        self.settled()
        if self.over_dp:
            for z in range(self.length):
                self.from_core(z)


class ReduceItem:
    def __init__(self, mode, place, block, bufs, out):
        self.mode, self.place, self.block, self.out = mode, place, block, out
        self.over_z = mode != "dp"
        self.over_dp = mode != "z"
        self.length = place.length if self.over_z else 1
        (self.acc, self.from_core, self.corner, self.from_xy, self.from_z,
         self.load, self.send, self.recv) = bufs

    @staticmethod
    def scratch(mode, length, rows, width, in_place=False):
        t = length if mode != "dp" else 1
        columns = 4 if mode != "z" else 1
        dp = mode != "z"
        small = (8, 128)
        return [
            pltpu.VMEM(small if in_place else (columns, t, rows, width), jnp.bfloat16),
            pltpu.VMEM((columns, t, rows, width) if dp else small, jnp.bfloat16),
            pltpu.VMEM((2, t, rows // 2, width) if dp else small, jnp.bfloat16),
            pltpu.VMEM((2, t, rows, width) if dp else small, jnp.bfloat16),
            pltpu.VMEM((t + 1, rows, width) if mode != "dp" else small, jnp.bfloat16),
            pltpu.SemaphoreType.DMA((columns, t)),
            pltpu.SemaphoreType.DMA((10, t, 2)),
            pltpu.SemaphoreType.DMA((9, t + 1, 2)),
        ]

    def z_of(self, turn):
        return self.place.target(turn) if self.over_z else 0

    def got(self, ref, lane, turn, h=0):
        pltpu.make_async_copy(ref, ref, self.recv.at[lane, turn, h]).wait()

    computed = False
    in_place = False

    def partial(self, column, turn, h):
        if self.in_place:
            return self.block(self.place.columns[column], self.z_of(turn), h)
        return self.acc.at[column, turn, piece(self.acc.shape[2], h)]

    def add(self, target, refs, out=None):
        rows = target.shape[0]
        step = 16 if rows % 16 == 0 else rows
        place = target if out is None else out

        def body(i, carry):
            at = pl.ds(pl.multiple_of(i * step, step), step)
            total = target[at, :].astype(jnp.float32)
            for ref in refs:
                total = total + ref[at, :].astype(jnp.float32)
            place[at, :] = total.astype(place.dtype)
            return carry

        lax.fori_loop(0, rows // step, body, 0, unroll=2 if (rows // step) % 2 == 0 else 1)

    def begin(self):
        place = self.place
        if self.over_z:

            @pl.when((place.z == 0) | (place.z == self.length - 1))
            def _():
                def clear(i, carry):
                    self.from_z[i] = jnp.zeros(self.from_z.shape[1:], jnp.bfloat16)
                    return carry

                lax.fori_loop(0, self.length + 1, clear, 0)

    def load_all(self):
        place = self.place
        for turn in range(self.length):
            for column in (3, 1, 2, 0) if self.over_dp else (0,):
                pltpu.make_async_copy(
                    self.block(place.columns[column], self.z_of(turn), None),
                    self.acc.at[column, turn],
                    self.load.at[column, turn],
                ).start()

    def hand_over(self, sends, turn):
        if not self.over_dp or turn >= self.length:
            return
        place = self.place
        for column in (3, 1, 2, 0):
            sends.start(
                "core",
                lambda column=column: (
                    self.block(place.columns[column] + place.to_core, self.z_of(turn), None),
                    self.from_core.at[column, turn],
                    self.send.at[column, turn, 0],
                    self.recv.at[column, turn, 0],
                ),
            )

    def ready(self, column, turn):
        if not (self.computed or self.in_place):
            ref = self.acc.at[column, turn]
            pltpu.make_async_copy(ref, ref, self.load.at[column, turn]).wait()
        if self.over_dp:
            self.got(self.from_core.at[column, turn], column, turn)

    def settle(self, column, turn, h, extra=(), out=None):
        refs = list(extra)
        if self.over_dp:
            rows = self.from_core.shape[2]
            refs.append(self.from_core.at[column, turn, piece(rows, h)])
        if refs or out is not None:
            self.add(self.partial(column, turn, h), refs, out)

    def corners(self, sends, turn):
        if not self.over_dp or not 0 <= turn < self.length:
            return
        self.ready(3, turn)
        for h, kind in ((0, "y"), (1, "x")):
            self.settle(3, turn, h)
            sends.start(
                kind,
                lambda h=h: (
                    self.partial(3, turn, h),
                    self.corner.at[h, turn],
                    self.send.at[4, turn, h],
                    self.recv.at[4, turn, h],
                ),
            )

    def straight(self, sends, turn, second):
        if not self.over_dp or not 0 <= turn < self.length:
            return
        rows = self.from_xy.shape[2]
        for column, kind in ((1, "x"), (2, "y")):
            h = (column - 1) if second else (2 - column)
            extra = ()
            if second:
                ref = self.corner.at[h, turn]
                self.got(ref, 4, turn, h)
                extra = (ref,)
            else:
                self.ready(column, turn)
            self.settle(column, turn, h, extra)
            sends.start(
                kind,
                lambda column=column, h=h: (
                    self.partial(column, turn, h),
                    self.from_xy.at[column - 1, turn, piece(rows, h)],
                    self.send.at[4 + column, turn, h],
                    self.recv.at[4 + column, turn, h],
                ),
            )

    def home(self, sends, turn):
        if not 0 <= turn < self.length:
            return
        place = self.place
        last = turn == self.length - 1
        z = self.z_of(turn)
        extra = []
        self.ready(0, turn)
        if self.over_dp:
            for lane in (0, 1):
                rows = self.from_xy.shape[2]
                for h in range(2):
                    self.got(self.from_xy.at[lane, turn, piece(rows, h)], 5 + lane, turn, h)
                extra.append(self.from_xy.at[lane, turn])
        if self.over_z:

            def got_slot():
                self.got(self.from_z.at[z], 7, z)

            def got_other():
                self.got(self.from_z.at[self.length], 7, self.length)

            extra.append(self.from_z.at[z])
            if last:
                guarded(place.has_down, got_slot)
                guarded(place.has_up, got_other)
                extra.append(self.from_z.at[self.length])
            else:
                guarded((z > place.z) & place.has_down, got_slot)
                guarded((z < place.z) & place.has_up, got_slot)
        self.settle(0, turn, None, extra, self.out(None) if last else None)
        if self.over_z and not last:

            def going_up():
                goal = self.z_of(turn)
                return (
                    self.partial(0, turn, None),
                    self.from_z.at[goal],
                    self.send.at[7, turn, 0],
                    self.recv.at[7, goal, 0],
                )

            def going_down():
                there = self.z_of(turn)
                arrives = (there - place.z + 1 + self.length) // self.length
                goal = there + arrives * (self.length - there)
                return (
                    self.partial(0, turn, None),
                    self.from_z.at[goal],
                    self.send.at[7, turn, 0],
                    self.recv.at[7, goal, 0],
                )

            def above():
                return self.z_of(turn) > place.z

            def below():
                return self.z_of(turn) < place.z

            pl.when(above())(lambda: sends.start("up", going_up, above))
            pl.when(below())(lambda: sends.start("down", going_down, below))


def advance(item, sends, step):
    item.corners(sends, step)
    item.straight(sends, step, False)
    item.hand_over(sends, step + 2)
    item.straight(sends, step - 1, True)
    item.home(sends, step - 2 if item.over_dp else step)


def reduce_rows(partials, small, all_rows, picked, gated, hid, dgate, dup, length, collective_id):
    devices, rows, width = partials.shape
    slots, hidden = dup.shape
    half, low = rows // 2, small.shape[0] // 2
    tile, narrow = width // 4, hidden // 3
    f32, bf16 = jnp.float32, jnp.bfloat16

    def kernel(
        source, small_ref, all_ref, picked_ref, gated_ref, hid_ref, dgate_ref, dup_ref,
        target, product, out_g, out_u, out_d,
        small_all, rows_v, rows_sem, hid_v, dgate_v, dup_v, picked_v, gated_v, tile_g, tile_u, tile_d, load_sem, tile_sem, store_sem,
        *rest,
    ):
        place = Place(length)
        item = ReduceItem(
            "all",
            place,
            lambda c, z, h: source.at[c * length + z, piece(2 * half, h)],
            rest[:8],
            lambda h: target.at[piece(2 * half, h)],
        )
        beside = GatherItem("all", place, None, None, *rest[8:])
        beside.own = lambda h: small_ref.at[piece(2 * low, h)]
        beside.slot = lambda c, z, h: small_all.at[c * length + z, piece(2 * low, h)]
        item.begin()
        meet(place, True, True)
        sends = Sends(place)
        beside.begin(sends)
        item.load_all()
        item.hand_over(sends, 0)
        item.hand_over(sends, 1)
        resident = [
            pltpu.make_async_copy(left, right, load_sem.at[n])
            for n, (left, right) in enumerate(
                ((hid_ref, hid_v), (dgate_ref, dgate_v), (dup_ref, dup_v))
            )
        ]
        for copy in resident:
            copy.start()

        def lanes_of(n):
            return pl.ds(pl.multiple_of(n * tile, tile), tile)

        def tiles(n, slot):
            return [
                pltpu.make_async_copy(picked_ref.at[:, lanes_of(n)], picked_v.at[slot], tile_sem.at[slot, 0]),
                pltpu.make_async_copy(gated_ref.at[:, lanes_of(n)], gated_v.at[slot], tile_sem.at[slot, 1]),
            ]

        def stores(n, slot):
            return [
                pltpu.make_async_copy(tile_g.at[slot], out_g.at[lanes_of(n)], store_sem.at[slot, 0]),
                pltpu.make_async_copy(tile_u.at[slot], out_u.at[lanes_of(n)], store_sem.at[slot, 1]),
                pltpu.make_async_copy(tile_d.at[slot], out_d.at[:, lanes_of(n)], store_sem.at[slot, 2]),
            ]

        for copy in tiles(0, 0):
            copy.start()

        def rows_load(group, part):
            return pltpu.make_async_copy(
                all_ref.at[pl.ds(group * length, length)], rows_v.at[part], rows_sem.at[part]
            )

        for part in range(2):
            rows_load(part, part).start()

        def narrow_of(m):
            return pl.ds(pl.multiple_of(m * narrow, narrow), narrow)

        def chunk(c, carry):
            n, kind = c // 3, c % 3
            slot = n % 2

            @pl.when((kind == 0) & (n < 4))
            def _():
                for copy in tiles(n, slot):
                    copy.wait()

                @pl.when(n < 3)
                def _():
                    for copy in tiles(n + 1, 1 - slot):
                        copy.start()

                @pl.when(n >= 2)
                def _():
                    for copy in stores(n, slot):
                        copy.wait()

                def body(m, carry):
                    tile_g[slot, :, narrow_of(m)] = dot(picked_v[slot], dgate_v[:, narrow_of(m)], 0, 0)
                    return carry

                lax.fori_loop(0, 3, body, 0)
                stores(n, slot)[0].start()

            @pl.when((kind == 1) & (n < 4))
            def _():
                def body(m, carry):
                    tile_u[slot, :, narrow_of(m)] = dot(picked_v[slot], dup_v[:, narrow_of(m)], 0, 0)
                    return carry

                lax.fori_loop(0, 3, body, 0)
                stores(n, slot)[1].start()

            @pl.when((kind == 2) & (n < 4))
            def _():
                def body(m, carry):
                    tile_d[slot, narrow_of(m), :] = dot(hid_v[:, narrow_of(m)], gated_v[slot], 0, 0)
                    return carry

                lax.fori_loop(0, 3, body, 0)
                stores(n, slot)[2].start()
            return carry

        def turn_of(i, carry):
            for step in range(length + 2):

                @pl.when(i == 2 * step)
                def _(step=step):
                    item.corners(sends, step)
                    item.straight(sends, step, False)
                    item.hand_over(sends, step + 2)

                @pl.when(i == 2 * step + 1)
                def _(step=step):
                    item.straight(sends, step - 1, True)
                    item.home(sends, step - 2)

            for step in range(length + 2):

                @pl.when(i == step)
                def _(step=step):
                    beside.along_z(sends, step + 1)
                    beside.across(sends, step)
                    beside.diagonal(sends, step - 1)

            @pl.when(i == length + 2)
            def _():
                beside.finish()
                product[...] = jnp.zeros(product.shape, f32)

            @pl.when((i >= length + 2) & (i < length + 6))
            def _():
                for part in range(2):
                    group = 2 * (i - length - 2) + part
                    rows_load(group, part).wait()
                    marks = [
                        small_all[group * length + z] for z in range(length)
                    ]
                    left = jnp.concatenate(marks, axis=1)

                    def body(m, carry, part=part, left=left):
                        lanes = pl.ds(pl.multiple_of(m * tile, tile), tile)
                        right = rows_v[part, :, :, lanes].reshape(length * rows, tile)
                        product[:, lanes] += dot(left, right)
                        return carry

                    lax.fori_loop(0, 4, body, 0)

                    @pl.when(group + 2 < 8)
                    def _(part=part, group=group):
                        rows_load(group + 2, part).start()

            @pl.when(i == 0)
            def _():
                for copy in resident:
                    copy.wait()

            @pl.when(i < 6)
            def _():
                lax.fori_loop(0, 2, lambda part, carry: chunk(2 * i + part, carry), 0)

            return carry

        lax.fori_loop(0, max(12, 2 * (length + 2), length + 6), turn_of, 0)
        for slot in range(2):
            for copy in stores(slot, slot):
                copy.wait()
        sends.drain()

    any_spec = pl.BlockSpec(memory_space=pl.ANY)
    shape = jax.ShapeDtypeStruct
    sems = pltpu.SemaphoreType.DMA
    return pl.pallas_call(
        kernel,
        name="reduce_rows",
        out_shape=[
            shape((rows, width), f32),
            shape((small.shape[0], width), f32),
            shape((width, hidden), f32),
            shape((width, hidden), f32),
            shape((hidden, width), f32),
        ],
        in_specs=[any_spec] * 8,
        out_specs=[pl.BlockSpec(memory_space=pltpu.VMEM)] * 2 + [any_spec] * 3,
        scratch_shapes=[
            pltpu.VMEM((devices,) + small.shape, small.dtype),
            pltpu.VMEM((2, length, rows, width), bf16),
            sems((2,)),
            pltpu.VMEM((slots, hidden), bf16),
            pltpu.VMEM((slots, hidden), bf16),
            pltpu.VMEM((slots, hidden), bf16),
            pltpu.VMEM((2, slots, tile), bf16),
            pltpu.VMEM((2, slots, tile), bf16),
            pltpu.VMEM((2, tile, hidden), f32),
            pltpu.VMEM((2, tile, hidden), f32),
            pltpu.VMEM((2, hidden, tile), f32),
            sems((3,)),
            sems((2, 2)),
            sems((2, 3)),
        ]
        + ReduceItem.scratch("all", length, rows, width)
        + GatherItem.semaphores("all", length),
        compiler_params=pltpu.CompilerParams(
            collective_id=collective_id, has_side_effects=True, vmem_limit_bytes=67043328
        ),
    )(partials, small, all_rows, picked, gated, hid, dgate, dup)


def dot(left, right, left_dim=1, right_dim=0):
    return lax.dot_general(
        left, right, (((left_dim,), (right_dim,)), ((), ())), preferred_element_type=jnp.float32
    )


def experts(rows_own, all_cots, gates_own, wgate, wup, wdown, length, capacity, collective_id):
    rows, width = rows_own.shape
    hidden = wgate.shape[1]
    devices = 8 * length
    count = 4 * capacity
    tile = 512 if width % 512 == 0 else width
    narrow = 256 if hidden % 256 == 0 else hidden
    f32, bf16 = jnp.float32, jnp.bfloat16

    def kernel(
        rows_ref, all_cots, gates_ref, wg_ref, wu_ref, wd_ref,
        all_rows, part_out, part_grad, token_in, picked_all, gated_all, hid_all, dgate_all, dup_all,
        wg, wu, wd, chosen_all, gates_all, rank_v, table, row_buf, cot_buf, picked, cotan, gated, hid, dgate, dup, scaled, back,
        chosen, slot_gate, slot_sum, stage_out, stage_grad, token_out,
        recv_r, send_r, local_r,
        load_sem, store_sem, save_sem, token_sem, gate_sem, weight_sem,
    ):
        place = Place(length)
        expert = place.dp * length + place.z

        def item_of(source, target, sems, half):
            item = GatherItem("all", place, None, None, *sems)
            item.own = lambda h: source.at[piece(2 * half, h)]
            item.slot = lambda column, z, h: target.at[
                column * length + z, piece(2 * half, h)
            ]
            return item

        big = [
            item_of(rows_ref, all_rows, (recv_r, send_r, local_r), rows // 2),
        ]
        items = big
        meet_all(place)
        sends = Sends(place)

        def gate_send(n):
            device, there = other_device(place, n + 1)
            return pltpu.make_async_remote_copy(
                src_ref=gates_ref.at[there],
                dst_ref=table.at[expert],
                send_sem=gate_sem.at[0],
                recv_sem=gate_sem.at[1],
                device_id=device,
                device_id_type=MESH,
            )

        def send_gates(n, carry):
            gate_send(n).start()
            return carry

        lax.fori_loop(0, devices - 1, send_gates, 0)
        pltpu.make_async_copy(gates_ref.at[expert], table.at[expert], gate_sem.at[1]).start()
        for item in items:
            item.begin(sends)

        weights = [
            pltpu.make_async_copy(source, target, weight_sem.at[n])
            for n, (source, target) in enumerate(((wg_ref, wg), (wu_ref, wu), (wd_ref, wd)))
        ]
        for copy in weights:
            copy.start()

        def along(distance):
            for item in items:
                item.along_z(sends, distance)

        def across(distance):
            for item in items:
                item.across(sends, distance)

        def corner(distance):
            for item in items:
                item.diagonal(sends, distance)

        across(0)
        along(1)
        pltpu.make_async_copy(table, table, gate_sem.at[1]).wait()
        order = lax.broadcasted_iota(jnp.int32, (rows, rows), 0)
        upto = (order <= lax.broadcasted_iota(jnp.int32, (rows, rows), 1)).astype(f32).astype(bf16)
        slots = lax.broadcasted_iota(jnp.int32, (capacity, rows), 0).astype(f32)
        lines = table[:, 0, :]
        rank_v[...] = dot((lines >= 0.0).astype(f32).astype(bf16), upto) - 1.0

        def choose(block, carry):
            line = table[block, 0:1, :]
            ranks = rank_v[pl.ds(block, 1), :]
            pick = jnp.where((line >= 0.0) & (ranks == slots), 1.0, 0.0)
            gate = jnp.sum(pick * line, axis=1, keepdims=True)
            chosen_all[block] = pick.astype(bf16)
            gates_all[block] = jnp.broadcast_to(gate, (capacity, 128))
            return carry

        lax.fori_loop(0, devices, choose, 0, unroll=4)
        for item in items:
            item.settled()

        def block_of(j, side, z):
            return (place.columns[j] + side * place.to_core) * length + z

        def load(j, side, z, slot):
            block = block_of(j, side, z)
            return [
                pltpu.make_async_copy(all_rows.at[block], row_buf.at[slot, j], load_sem.at[slot, 0, j]),
                pltpu.make_async_copy(all_cots.at[block], cot_buf.at[slot, j], load_sem.at[slot, 1, j]),
            ]

        def store(j, side, z, slot):
            block = block_of(j, side, z)
            return [
                pltpu.make_async_copy(stage_out.at[slot, j], part_out.at[block], store_sem.at[slot, 0, j]),
                pltpu.make_async_copy(stage_grad.at[slot, j], part_grad.at[block], store_sem.at[slot, 1, j]),
            ]

        def saved(i):
            first = [
                pltpu.make_async_copy(picked, picked_all.at[i], save_sem.at[0]),
                pltpu.make_async_copy(gated, gated_all.at[i], save_sem.at[1]),
            ]
            second = [
                pltpu.make_async_copy(hid, hid_all.at[i], save_sem.at[2]),
                pltpu.make_async_copy(dgate, dgate_all.at[i], save_sem.at[3]),
                pltpu.make_async_copy(dup, dup_all.at[i], save_sem.at[4]),
            ]
            return first, second

        def start_loads(step, side):
            for j in range(4):
                for copy in load(j, side, place.nearest(step), side):
                    copy.start()

        corner(0)
        for item in items:
            item.from_core(place.nearest(0))
        start_loads(0, 0)
        start_loads(0, 1)
        for copy in weights:
            copy.wait()

        def unit(i, carry):
            turn, side = i // 2, i % 2
            z = place.nearest(turn)

            @pl.when(i == 1)
            def _():
                along(2)
                across(1)

            for step in range(1, length):

                @pl.when(i == max(2, 2 * step - 1))
                def _(step=step):
                    corner(step)
                    along(step + 2)
                    across(step + 1)
                    for item in items:
                        item.from_core(place.nearest(step))
                    start_loads(step, 0)
                    if step == 1:
                        start_loads(step, 1)

            @pl.when(i >= 1)
            def _():
                for copy in saved(i)[0]:
                    copy.wait()

            for j in range(4):
                for copy in load(j, side, z, side):
                    copy.wait()
            for j in range(4):
                block = block_of(j, side, z)
                chosen[j] = chosen_all[block]
                slot_gate[pl.ds(j * capacity, capacity), :] = gates_all[block]

            def select(n, carry):
                lanes = pl.ds(pl.multiple_of(n * tile, tile), tile)
                for j in range(4):
                    at = pl.ds(j * capacity, capacity)
                    picked[at, lanes] = dot(chosen[j], row_buf[side, j, :, lanes]).astype(bf16)
                    cot = dot(chosen[j], cot_buf[side, j, :, lanes])
                    cotan[at, lanes] = cot.astype(bf16)
                    gated[at, lanes] = (slot_gate[at, 0:1] * cot).astype(bf16)
                return carry

            lax.fori_loop(0, width // tile, select, 0)

            for copy in saved(i)[0]:
                copy.start()
            for step in range(2, length):

                @pl.when(i == 2 * step - 1)
                def _(step=step):
                    start_loads(step, 1)

            @pl.when(i >= 1)
            def _():
                for copy in saved(i)[1]:
                    copy.wait()

            def middle(n, carry):
                lanes = pl.ds(pl.multiple_of(n * narrow, narrow), narrow)
                gate = dot(picked[...], wg[:, lanes])
                up = dot(picked[...], wu[:, lanes])
                grad = dot(gated[...], wd[lanes, :], 1, 1)
                sigma = jax.nn.sigmoid(gate)
                hid[:, lanes] = (gate * sigma * up).astype(bf16)
                dgate[:, lanes] = (grad * up * sigma * (1.0 + gate * (1.0 - sigma))).astype(bf16)
                dup[:, lanes] = (grad * gate * sigma).astype(bf16)
                return carry

            lax.fori_loop(0, hidden // narrow, middle, 0)
            for copy in saved(i)[1]:
                copy.start()
            slot_sum[...] = jnp.zeros(slot_sum.shape, f32)

            @pl.when(i >= 2)
            def _():
                for j in range(4):
                    for copy in store(j, side, z, side):
                        copy.wait()

            def outward(n, carry):
                lanes = pl.ds(pl.multiple_of(n * tile, tile), tile)
                result = dot(hid[...], wd[:, lanes]).astype(bf16).astype(f32)
                products = cotan[:, lanes].astype(f32) * result
                total = products[:, 0:128]
                for k in range(1, tile // 128):
                    total = total + products[:, 128 * k : 128 * (k + 1)]
                slot_sum[...] += total
                scaled[:, lanes] = (slot_gate[:, 0:1] * result).astype(bf16)
                back[:, lanes] = (
                    dot(dgate[...], wg[lanes, :], 1, 1) + dot(dup[...], wu[lanes, :], 1, 1)
                ).astype(bf16)
                for j in range(4):
                    at = pl.ds(j * capacity, capacity)
                    stage_out[side, j, :, lanes] = dot(chosen[j], scaled[at, lanes], 0, 0).astype(bf16)
                    stage_grad[side, j, :, lanes] = dot(chosen[j], back[at, lanes], 0, 0).astype(bf16)
                return carry

            lax.fori_loop(0, width // tile, outward, 0)
            for j in range(4):
                for copy in store(j, side, z, side):
                    copy.start()
            total = jnp.sum(slot_sum[...], axis=1, keepdims=True).reshape(4, capacity, 1)
            sums = jnp.sum(chosen[...].astype(f32) * total, axis=1)
            for j in range(4):
                token_out[block_of(j, side, z)] = jnp.broadcast_to(sums[j : j + 1], (8, rows))
            return carry

        lax.fori_loop(0, 2 * length, unit, 0)

        def token_send(n):
            device, there = other_device(place, n + 1)
            return pltpu.make_async_remote_copy(
                src_ref=token_out.at[there],
                dst_ref=token_in.at[expert],
                send_sem=token_sem.at[0],
                recv_sem=token_sem.at[1],
                device_id=device,
                device_id_type=MESH,
            )

        def send(n, carry):
            token_send(n).start()
            return carry

        lax.fori_loop(0, devices - 1, send, 0)
        pltpu.make_async_copy(token_out.at[expert], token_in.at[expert], token_sem.at[1]).start()
        for side in range(2):
            for j in range(4):
                for copy in store(j, side, 0, side):
                    copy.wait()
        for copies in saved(0):
            for copy in copies:
                copy.wait()
        sends.drain()
        pltpu.make_async_copy(token_out, token_in, token_sem.at[1]).wait()
        sent = token_out.at[pl.ds(0, devices - 1)]
        pltpu.make_async_copy(sent, sent, token_sem.at[0]).wait()
        pltpu.make_async_copy(sent, sent, gate_sem.at[0]).wait()

    any_spec = pl.BlockSpec(memory_space=pl.ANY)
    vmem = pl.BlockSpec(memory_space=pltpu.VMEM)
    big = (devices, rows, width)
    shape = jax.ShapeDtypeStruct
    sems = pltpu.SemaphoreType.DMA
    return pl.pallas_call(
        kernel,
        name="experts",
        out_shape=[
            shape(big, bf16), shape(big, bf16), shape(big, bf16),
            shape((devices, 8, rows), f32),
            shape((2 * length, count, width), bf16), shape((2 * length, count, width), bf16),
            shape((2 * length, count, hidden), bf16), shape((2 * length, count, hidden), bf16),
            shape((2 * length, count, hidden), bf16),
        ],
        in_specs=[any_spec] * 6,
        out_specs=[any_spec] * 3 + [vmem] + [any_spec] * 5,
        scratch_shapes=[
            pltpu.VMEM((width, hidden), bf16),
            pltpu.VMEM((width, hidden), bf16),
            pltpu.VMEM((hidden, width), bf16),
            pltpu.VMEM((devices, capacity, rows), bf16),
            pltpu.VMEM((devices, capacity, 128), f32),
            pltpu.VMEM((devices, rows), f32),
            pltpu.VMEM((devices, 8, rows), f32),
            pltpu.VMEM((2, 4, rows, width), bf16),
            pltpu.VMEM((2, 4, rows, width), bf16),
            pltpu.VMEM((count, width), bf16),
            pltpu.VMEM((count, width), bf16),
            pltpu.VMEM((count, width), bf16),
            pltpu.VMEM((count, hidden), bf16),
            pltpu.VMEM((count, hidden), bf16),
            pltpu.VMEM((count, hidden), bf16),
            pltpu.VMEM((count, width), bf16),
            pltpu.VMEM((count, width), bf16),
            pltpu.VMEM((4, capacity, rows), bf16),
            pltpu.VMEM((count, 128), f32),
            pltpu.VMEM((count, 128), f32),
            pltpu.VMEM((2, 4, rows, width), bf16),
            pltpu.VMEM((2, 4, rows, width), bf16),
            pltpu.VMEM((devices, 8, rows), f32),
        ]
        + GatherItem.semaphores("all", length)
        + [sems((2, 2, 4)), sems((2, 2, 4)), sems((5,)), sems((2,)), sems((2,)), sems((3,))],
        compiler_params=pltpu.CompilerParams(
            collective_id=collective_id, has_side_effects=True, vmem_limit_bytes=63 << 20
        ),
    )(rows_own, all_cots, gates_own, wgate, wup, wdown)


def rope(values, cosine, sine):
    return values * cosine + pltpu.roll(values, values.shape[-1] // 2, 1) * sine


def unrope(values, cosine, sine):
    return values * cosine - pltpu.roll(values, values.shape[-1] // 2, 1) * sine


def row_factor(values):
    return lax.rsqrt(jnp.mean(values * values, axis=-1, keepdims=True) + EPSILON)


def visible_pairs(seg_col, seg_row, start, stop, reach):
    shape = (stop - start, reach)
    query = lax.broadcasted_iota(jnp.int32, shape, 0) + start
    key = lax.broadcasted_iota(jnp.int32, shape, 1)
    return (seg_col[start:stop, :] == seg_row[:, 0:reach]) & (key <= query)


def fill_turns(seg_row, cos_half, sin_half, seg_col, cosine, sine):
    spread = jnp.broadcast_to(seg_row[...].astype(jnp.float32), (128, seg_row.shape[1]))
    seg_col[...] = spread.T[:, 0:1].astype(jnp.int32)
    cosine[...] = jnp.concatenate([cos_half[...], cos_half[...]], axis=1)
    sine[...] = jnp.concatenate([-sin_half[...], sin_half[...]], axis=1)


def attend(rows_own, joint_own, output_own, cots_own, segments, cosine, sine, query_gain, key_gain, length, collective_id):
    rows, width = rows_own.shape
    depth, joint = joint_own.shape
    head_width, part = output_own.shape
    head = query_gain.shape[-1]
    heads = head_width // head
    tokens = rows * length
    block = tokens // 2
    tile = 512
    scale = 1.0 / math.sqrt(head)
    f32, bf16 = jnp.float32, jnp.bfloat16

    def kernel(
        rows_ref, joint_ref, output_ref, cots_ref, segr, cos_half, sin_half, qgain, kgain,
        out_add, out_rows, out_joint, out_weight, out_cots, out_qkv, out_heads,
        segc, cos_ref, sin_ref,
        rows_v, joint_v, weight_v, qkv, att, key_v, value_v,
        r0, r1, r2, r3, r4, r5, r6, r7,
        g0, g1, g2, j0, j1, j2, w0, w1, w2, c0, c1, c2, save_sem,
    ):
        place = Place(length)

        def item_of(mode, source, half, slot, sems):
            item = GatherItem(mode, place, None, None, *sems)
            item.own = lambda h: source.at[piece(2 * half, h)]
            item.slot = slot
            return item

        half, deep, tall = rows // 2, depth // 2, head_width // 2
        own_rows = item_of(
            "z", rows_ref, half, lambda c, z, h: rows_v.at[z, piece(2 * half, h)], (g0, g1, g2)
        )
        own_joint = item_of(
            "dp", joint_ref, deep, lambda c, z, h: joint_v.at[c, piece(2 * deep, h)], (j0, j1, j2)
        )
        own_weight = item_of(
            "dp",
            output_ref,
            tall,
            lambda c, z, h: weight_v.at[
                piece(2 * tall, h), pl.ds(pl.multiple_of(c * part, part), part)
            ],
            (w0, w1, w2),
        )
        cots = item_of(
            "all",
            cots_ref,
            half,
            lambda c, z, h: out_cots.at[c * length + z, piece(2 * half, h)],
            (c0, c1, c2),
        )
        total = ReduceItem(
            "z", place, None, (r0, r1, r2, r3, r4, r5, r6, r7),
            lambda h: out_add.at[piece(2 * half, h)],
        )
        total.computed = True
        total.begin()
        meet(place, True, True)
        sends = Sends(place)
        own_joint.begin(sends)
        own_rows.begin(sends)
        own_weight.begin(sends)
        fill_turns(segr, cos_half, sin_half, segc, cos_ref, sin_ref)
        own_joint.across(sends, 0)
        own_rows.along_z(sends, 1)
        own_weight.across(sends, 0)
        own_joint.diagonal(sends, 0)
        own_rows.along_z(sends, 2)
        cots.begin(sends)
        own_weight.diagonal(sends, 0)
        for distance in range(3, length):
            own_rows.along_z(sends, distance)
        own_joint.finish()
        own_rows.finish()

        def projection(n, carry):
            lanes = pl.ds(pl.multiple_of(n * 256, 256), 256)
            left = rows_v[...].reshape(tokens, width)
            right = joint_v[:, :, lanes].reshape(width, 256)
            qkv[:, lanes] = dot(left, right)
            return carry

        lax.fori_loop(0, joint // 256, projection, 0)
        saves = [
            pltpu.make_async_copy(source, target, save_sem.at[n])
            for n, (source, target) in enumerate(
                ((rows_v, out_rows), (joint_v, out_joint), (qkv, out_qkv), (weight_v, out_weight), (att, out_heads))
            )
        ]
        for copy in saves[:3]:
            copy.start()
        key = qkv[:, head_width : head_width + head]
        key_v[...] = rope(key * row_factor(key) * kgain[...], cos_ref[...], sin_ref[...]).astype(bf16)
        value_v[...] = qkv[:, head_width + head : head_width + 2 * head].astype(bf16)

        def one_head(n, carry):
            lanes = pl.ds(pl.multiple_of(n * head, head), head)
            for start in range(0, tokens, block):
                stop = start + block
                query = qkv[start:stop, lanes]
                turned = rope(
                    query * row_factor(query) * qgain[...], cos_ref[start:stop, :], sin_ref[start:stop, :]
                ).astype(bf16)
                scores = dot(turned, key_v[0:stop, :], 1, 1) * scale
                seen = visible_pairs(segc, segr, start, stop, stop)
                scores = jnp.where(seen, scores, NEG_BIG)
                top = jnp.max(scores, axis=-1, keepdims=True)
                powers = jnp.exp(scores - top)
                probs = (powers / jnp.sum(powers, axis=-1, keepdims=True)).astype(bf16)
                att[start:stop, lanes] = dot(probs, value_v[0:stop, :]).astype(bf16)
            return carry

        lax.fori_loop(0, heads // 2, one_head, 0)
        cots.across(sends, 0)
        cots.along_z(sends, 1)
        lax.fori_loop(heads // 2, heads, one_head, 0)
        saves[4].start()
        own_weight.finish()
        saves[3].start()

        def outward(turn):
            z = total.z_of(turn)

            def body(n, carry):
                lanes = pl.ds(pl.multiple_of(n * tile, tile), tile)
                left = att[pl.ds(pl.multiple_of(z * rows, rows), rows), :]
                found = dot(left, weight_v[:, lanes]).astype(bf16)
                total.acc[0, turn, :, lanes] = found
                return carry

            lax.fori_loop(0, width // tile, body, 0)

        for turn in range(length):
            outward(turn)
            total.home(sends, turn)
            cots.diagonal(sends, turn)
            cots.across(sends, turn + 1)
            cots.along_z(sends, turn + 2)
        cots.finish()
        for copy in saves:
            copy.wait()
        sends.drain()

    any_spec = pl.BlockSpec(memory_space=pl.ANY)
    vmem = pl.BlockSpec(memory_space=pltpu.VMEM)
    shape = jax.ShapeDtypeStruct
    return pl.pallas_call(
        kernel,
        name="attend",
        out_shape=[
            shape((rows, width), f32),
            shape((length, rows, width), bf16),
            shape((8, depth, joint), bf16),
            shape((head_width, 8 * part), bf16),
            shape((8 * length, rows, width), bf16),
            shape((tokens, joint), f32),
            shape((tokens, head_width), bf16),
            shape((tokens, 1), jnp.int32),
            shape((tokens, head), f32),
            shape((tokens, head), f32),
        ],
        in_specs=[any_spec] * 4 + [vmem] * 5,
        out_specs=[vmem] + [any_spec] * 6 + [vmem] * 3,
        scratch_shapes=[
            pltpu.VMEM((length, rows, width), bf16),
            pltpu.VMEM((8, depth, joint), bf16),
            pltpu.VMEM((head_width, 8 * part), bf16),
            pltpu.VMEM((tokens, joint), f32),
            pltpu.VMEM((tokens, head_width), bf16),
            pltpu.VMEM((tokens, head), bf16),
            pltpu.VMEM((tokens, head), bf16),
        ]
        + ReduceItem.scratch("z", length, rows, width)
        + GatherItem.semaphores("z", length)
        + GatherItem.semaphores("dp", length) * 2
        + GatherItem.semaphores("all", length)
        + [pltpu.SemaphoreType.DMA((5,))],
        compiler_params=pltpu.CompilerParams(
            collective_id=collective_id, has_side_effects=True, vmem_limit_bytes=56 << 20
        ),
    )(rows_own, joint_own, output_own, cots_own, segments, cosine, sine, query_gain, key_gain)


def attend_back(grad_own, rows_all, joint_all, output_all, qkv_all, heads_all, part_out, seg_col, seg_row, cosine, sine, query_gain, key_gain, length, collective_id):
    rows, width = grad_own.shape
    _, depth, joint = joint_all.shape
    head_width = output_all.shape[0]
    part = width // 8
    head = query_gain.shape[-1]
    heads = head_width // head
    tokens = rows * length
    block = tokens // 2
    scale = 1.0 / math.sqrt(head)
    f32, bf16 = jnp.float32, jnp.bfloat16
    half, deep, tall = rows // 2, depth // 2, head_width // 2

    def kernel(
        grad_ref, rows_ref, joint_ref, output_ref, qkv_ref, heads_ref, part_ref,
        segc, segr, cos_ref, sin_ref, qgain, kgain,
        out_rows, out_joint, out_weight, out_moe, out_qgain, out_kgain,
        grads, joint_v, weight_v, qkv, att, gatt, joint_b, part_w, key_v, value_v, dkey, dvalue,
        *rest,
    ):
        place = Place(length)
        o_bufs, z_bufs, j_bufs, w_bufs = (rest[8 * n : 8 * n + 8] for n in range(4))
        gather_sems, load_sem = rest[32:35], rest[35]

        outs = ReduceItem(
            "all",
            place,
            lambda c, z, h: part_ref.at[c * length + z, piece(2 * half, h)],
            o_bufs,
            lambda h: out_moe.at[piece(2 * half, h)],
        )
        back = ReduceItem(
            "z",
            place,
            lambda c, z, h: grads.at[z, piece(2 * half, h)],
            z_bufs,
            lambda h: out_rows.at[piece(2 * half, h)],
        )
        joints = ReduceItem(
            "dp",
            place,
            lambda c, z, h: joint_v.at[c, piece(2 * deep, h)],
            j_bufs,
            lambda h: out_joint.at[piece(2 * deep, h)],
        )
        weights = ReduceItem(
            "dp",
            place,
            lambda c, z, h: part_w.at[
                piece(2 * tall, h), pl.ds(pl.multiple_of(c * part, part), part)
            ],
            w_bufs,
            lambda h: out_weight.at[piece(2 * tall, h)],
        )
        for item in (back, joints, weights):
            item.in_place = True
        gathers = GatherItem("z", place, None, None, *gather_sems)
        gathers.own = lambda h: grad_ref.at[piece(2 * half, h)]
        gathers.slot = lambda c, z, h: grads.at[z, piece(2 * half, h)]

        outs.begin()
        back.begin()
        meet(place, True, True)
        first, sends = Sends(place), Sends(place)
        gathers.begin(first)
        outs.load_all()
        outs.hand_over(sends, 0)
        outs.hand_over(sends, 1)
        loads = [
            pltpu.make_async_copy(source, target, load_sem.at[n])
            for n, (source, target) in enumerate(
                ((output_ref, weight_v), (heads_ref, att), (qkv_ref, qkv), (joint_ref, joint_v))
            )
        ]
        for copy in loads:
            copy.start()
        advance(outs, sends, 0)
        for distance in range(1, length):
            gathers.along_z(first, distance)
            if distance < length - 1:
                advance(outs, sends, distance)
        gathers.finish()
        first.drain()
        for copy in loads[:3]:
            copy.wait()

        def to_heads(n, carry):
            lanes = pl.ds(pl.multiple_of(n * 256, 256), 256)
            left = grads[...].reshape(tokens, width)
            gatt[:, lanes] = dot(left, weight_v[lanes, :], 1, 1).astype(bf16)
            return carry

        def to_weight(n, carry):
            lanes = pl.ds(pl.multiple_of(n * 256, 256), 256)
            right = grads[:, :, lanes].reshape(tokens, 256)
            part_w[:, lanes] = dot(att[...], right, 0, 0).astype(bf16)
            return carry

        lax.fori_loop(0, width // 256, to_weight, 0)
        weights.hand_over(sends, 0)
        lax.fori_loop(0, head_width // 256, to_heads, 0)
        rows_v = weight_v.at[pl.ds(0, tokens)]
        rows_loads = [
            pltpu.make_async_copy(
                rows_ref.at[z], weight_v.at[pl.ds(z * rows, rows)], load_sem.at[4 + z]
            )
            for z in range(length)
        ]
        for copy in rows_loads:
            copy.start()
        advance(weights, sends, 0)
        key = qkv[:, head_width : head_width + head]
        key_v[...] = rope(key * row_factor(key) * kgain[...], cos_ref[...], sin_ref[...]).astype(bf16)
        value_v[...] = qkv[:, head_width + head : head_width + 2 * head].astype(bf16)
        dkey[...] = jnp.zeros((tokens, head), f32)
        dvalue[...] = jnp.zeros((tokens, head), f32)
        out_qgain[...] = jnp.zeros(out_qgain.shape, f32)

        def normed_back(grad, raw, gain, start, stop):
            factor = row_factor(raw)
            hat = raw * factor
            turned = unrope(grad, cos_ref[start:stop, :], sin_ref[start:stop, :])
            scaled = turned * gain
            found = factor * (scaled - hat * jnp.mean(scaled * hat, axis=-1, keepdims=True))
            return found, jnp.sum(turned * hat, axis=0, keepdims=True)

        def one_head(n, carry):
            lanes = pl.ds(pl.multiple_of(n * head, head), head)
            for start in range(0, tokens, block):
                stop = start + block
                raw = qkv[start:stop, lanes]
                turned = rope(
                    raw * row_factor(raw) * qgain[...], cos_ref[start:stop, :], sin_ref[start:stop, :]
                ).astype(bf16)
                grad = gatt[start:stop, lanes]
                delta = jnp.sum(
                    grad.astype(f32) * att[start:stop, lanes].astype(f32), axis=-1, keepdims=True
                )
                scores = dot(turned, key_v[0:stop, :], 1, 1) * scale
                seen = visible_pairs(segc, segr, start, stop, stop)
                scores = jnp.where(seen, scores, NEG_BIG)
                powers = jnp.exp(scores - jnp.max(scores, axis=-1, keepdims=True))
                probs = powers / jnp.sum(powers, axis=-1, keepdims=True)
                dprobs = dot(grad, value_v[0:stop, :], 1, 1)
                dscores = (probs * (dprobs - delta)).astype(bf16)
                dvalue[0:stop, :] += dot(probs.astype(bf16), grad, 0, 0)
                dkey[0:stop, :] += dot(dscores, turned, 0, 0) * scale
                dquery = dot(dscores, key_v[0:stop, :]) * scale
                found, gain_part = normed_back(dquery, raw, qgain[...], start, stop)
                joint_b[start:stop, lanes] = found.astype(bf16)
                out_qgain[...] += gain_part
            return carry

        lax.fori_loop(0, heads // 2, one_head, 0)
        advance(outs, sends, length - 1)
        advance(weights, sends, 1)
        lax.fori_loop(heads // 2, heads, one_head, 0)
        found, gain_part = normed_back(
            dkey[...], qkv[:, head_width : head_width + head], kgain[...], 0, tokens
        )
        out_kgain[...] = gain_part
        joint_b[:, head_width : head_width + head] = found.astype(bf16)
        joint_b[:, head_width + head : head_width + 2 * head] = dvalue[...].astype(bf16)
        loads[3].wait()

        def to_rows(n, carry):
            lanes = pl.ds(pl.multiple_of(n * depth, depth), depth)
            found = dot(joint_b[...], joint_v[n], 1, 1).astype(bf16)
            grads[:, :, lanes] = found.reshape(length, rows, depth)
            return carry

        lax.fori_loop(0, 8, to_rows, 0)
        back.home(sends, 0)
        for copy in rows_loads:
            copy.wait()

        def to_joint(n, carry):
            lanes = pl.ds(pl.multiple_of(n * depth, depth), depth)
            joint_v[n] = dot(weight_v[0:tokens, lanes], joint_b[...], 0, 0).astype(bf16)
            return carry

        lax.fori_loop(0, 8, to_joint, 0)
        joints.hand_over(sends, 0)
        advance(outs, sends, length)
        advance(joints, sends, 0)
        back.home(sends, 1)
        advance(weights, sends, 2)
        for turn in range(2, length - 1):
            back.home(sends, turn)
        advance(joints, sends, 1)
        advance(outs, sends, length + 1)
        back.home(sends, length - 1)
        advance(joints, sends, 2)
        sends.drain()

    any_spec = pl.BlockSpec(memory_space=pl.ANY)
    vmem = pl.BlockSpec(memory_space=pltpu.VMEM)
    shape = jax.ShapeDtypeStruct
    return pl.pallas_call(
        kernel,
        name="attend_back",
        out_shape=[
            shape((rows, width), f32),
            shape((depth, joint), f32),
            shape((head_width, part), f32),
            shape((rows, width), f32),
            shape((1, head), f32),
            shape((1, head), f32),
        ],
        in_specs=[any_spec] * 7 + [vmem] * 6,
        out_specs=[vmem] * 6,
        scratch_shapes=[
            pltpu.VMEM((length, rows, width), bf16),
            pltpu.VMEM((8, depth, joint), bf16),
            pltpu.VMEM((head_width, width), bf16),
            pltpu.VMEM((tokens, joint), f32),
            pltpu.VMEM((tokens, head_width), bf16),
            pltpu.VMEM((tokens, head_width), bf16),
            pltpu.VMEM((tokens, joint), bf16),
            pltpu.VMEM((head_width, width), bf16),
            pltpu.VMEM((tokens, head), bf16),
            pltpu.VMEM((tokens, head), bf16),
            pltpu.VMEM((tokens, head), f32),
            pltpu.VMEM((tokens, head), f32),
        ]
        + ReduceItem.scratch("all", length, rows, width)
        + ReduceItem.scratch("z", length, rows, width, True)
        + ReduceItem.scratch("dp", length, depth, joint, True)
        + ReduceItem.scratch("dp", length, head_width, part, True)
        + GatherItem.semaphores("z", length)
        + [pltpu.SemaphoreType.DMA((4 + length,))],
        compiler_params=pltpu.CompilerParams(
            collective_id=collective_id, has_side_effects=True, vmem_limit_bytes=67043328
        ),
    )(grad_own, rows_all, joint_all, output_all, qkv_all, heads_all, part_out, seg_col, seg_row, cosine, sine, query_gain, key_gain)


def share_sum(values, length, collective_id):
    rows, width = values.shape

    def kernel(own, target, middle, group, line, send_sem, recv_sem):
        place = Place(length)

        def dp_peer(n):
            return lax.rem(place.dp + n, 8), place.z

        def z_peer(n):
            return place.dp, lax.rem(place.z + n, length)

        peers = [dp_peer(n) for n in range(1, 8)] + [z_peer(n) for n in range(1, length)]
        barrier = pltpu.get_barrier_semaphore()
        for device in peers:
            pl.semaphore_signal(barrier, 1, device_id=device, device_id_type=MESH)
        pl.semaphore_wait(barrier, len(peers))

        def exchange(source, land, mine, devices, at):
            for device in devices:
                pltpu.make_async_remote_copy(
                    src_ref=source,
                    dst_ref=land.at[mine],
                    send_sem=send_sem.at[at],
                    recv_sem=recv_sem.at[at],
                    device_id=device,
                    device_id_type=MESH,
                ).start()
            pltpu.make_async_copy(source, land.at[mine], recv_sem.at[at]).start()
            pltpu.make_async_copy(land, land, recv_sem.at[at]).wait()
            total = land[0]
            for n in range(1, land.shape[0]):
                total = total + land[n]
            return total

        middle[...] = exchange(own, group, place.dp, peers[:7], 0)
        target[...] = exchange(middle, line, place.z, peers[7:], 1)
        for at, land in ((0, group), (1, line)):
            sent = land.at[pl.ds(0, land.shape[0] - 1)]
            pltpu.make_async_copy(sent, sent, send_sem.at[at]).wait()

    vmem = pl.BlockSpec(memory_space=pltpu.VMEM)
    return pl.pallas_call(
        kernel,
        name="share_sum",
        out_shape=jax.ShapeDtypeStruct((rows, width), values.dtype),
        in_specs=[vmem],
        out_specs=vmem,
        scratch_shapes=[
            pltpu.VMEM((rows, width), values.dtype),
            pltpu.VMEM((8, rows, width), values.dtype),
            pltpu.VMEM((length, rows, width), values.dtype),
            pltpu.SemaphoreType.DMA((2,)),
            pltpu.SemaphoreType.DMA((2,)),
        ],
        compiler_params=pltpu.CompilerParams(collective_id=collective_id, has_side_effects=True),
    )(values)


def mix(form, left, right):
    return jnp.einsum(form, left, right, preferred_element_type=jnp.float32)


def rms_scale(values):
    return lax.rsqrt(jnp.mean(values * values, axis=-1, keepdims=True) + EPSILON)


def rope_tables(seg_ids, head_dim):
    length = seg_ids.shape[0]
    row_index = jnp.arange(length, dtype=jnp.int32)
    starts = jnp.sum((seg_ids[None, :] < seg_ids[:, None]).astype(jnp.int32), axis=1)
    places = (row_index - starts).astype(jnp.float32)
    half_dim = head_dim // 2
    frequency = THETA_BASE ** (-(jnp.arange(half_dim, dtype=jnp.float32) * (2.0 / head_dim)))
    angles = places[:, None] * frequency[None, :]
    return (jnp.cos(angles), jnp.sin(angles))


def rotate(values, cosine, sine_table):
    half_dim = values.shape[-1] // 2
    front_part = values[..., :half_dim]
    back_part = values[..., half_dim:]
    cos_rows = cosine[:, None, :]
    sin_rows = sine_table[:, None, :]
    return jnp.concatenate(
        [
            front_part * cos_rows - back_part * sin_rows,
            back_part * cos_rows + front_part * sin_rows,
        ],
        axis=-1,
    )


def unrotate(values, cosine, sine_table):
    half_dim = values.shape[-1] // 2
    front_part = values[..., :half_dim]
    back_part = values[..., half_dim:]
    cos_rows = cosine[:, None, :]
    sin_rows = sine_table[:, None, :]
    return jnp.concatenate(
        [
            front_part * cos_rows + back_part * sin_rows,
            back_part * cos_rows - front_part * sin_rows,
        ],
        axis=-1,
    )


def head_norm_back(grad_out, normed, factor, gain):
    grad_normed = grad_out * gain
    grad_gain = jnp.sum(grad_out * normed, axis=(0, 1))
    grad_values = factor * (
        grad_normed - normed * jnp.mean(grad_normed * normed, axis=-1, keepdims=True)
    )
    return (grad_values, grad_gain)


def row_norm_back(grad_out, normed, factor, gain):
    grad_normed = grad_out * gain
    grad_gain = jnp.sum(grad_out * normed, axis=0)
    grad_values = factor * (
        grad_normed - normed * jnp.mean(grad_normed * normed, axis=-1, keepdims=True)
    )
    return (grad_values, grad_gain)


def softmax_rows(logits):
    top_value = jnp.max(logits, axis=-1, keepdims=True)
    expo = jnp.exp(logits - top_value)
    return expo / jnp.sum(expo, axis=-1, keepdims=True)


def attn_forward(rows, seg_ids, wq_full, wk_full, wv_full, query_gain, key_gain):
    length = rows.shape[0]
    head_dim = query_gain.shape[0]
    num_heads = wq_full.shape[1] // head_dim
    kv_heads = wk_full.shape[1] // head_dim
    per_group = num_heads // kv_heads
    inv_root = 1.0 / math.sqrt(head_dim)
    block_rows = math.gcd(length, 512)
    cosine, sine_table = rope_tables(seg_ids, head_dim)
    query = jnp.dot(rows, wq_full, preferred_element_type=jnp.float32).reshape(
        length, num_heads, head_dim
    )
    key_proj = jnp.dot(rows, wk_full, preferred_element_type=jnp.float32).reshape(
        length, kv_heads, head_dim
    )
    value_rows = (
        jnp.dot(rows, wv_full, preferred_element_type=jnp.float32)
        .astype(jnp.bfloat16)
        .reshape(length, kv_heads, head_dim)
    )
    query_factor = rms_scale(query)
    query_hat = query * query_factor
    key_factor = rms_scale(key_proj)
    key_hat = key_proj * key_factor
    query_rot = (
        rotate(query_hat * query_gain, cosine, sine_table)
        .astype(jnp.bfloat16)
        .reshape(length, kv_heads, per_group, head_dim)
    )
    key_rot = rotate(key_hat * key_gain, cosine, sine_table).astype(jnp.bfloat16)
    row_index = jnp.arange(length, dtype=jnp.int32)
    scores = mix("qgrd,kgd->grqk", query_rot, key_rot) * inv_root
    visible = (seg_ids[0:block_rows, None] == seg_ids[None, :]) & (
        row_index[None, :] <= row_index[0:block_rows, None]
    )
    scores = jnp.where(visible, scores, NEG_BIG)
    top_value = jnp.max(scores, axis=-1, keepdims=True)
    expo = jnp.exp(scores - top_value)
    totals = jnp.sum(expo, axis=-1, keepdims=True)
    prob_rows = (expo / totals).astype(jnp.bfloat16)
    outputs = mix("grqk,kgd->qgrd", prob_rows, value_rows).astype(jnp.bfloat16)
    lse_parts = top_value[..., 0] + jnp.log(totals[..., 0])
    attn_heads = outputs.reshape(length, num_heads * head_dim)
    return (
        attn_heads,
        lse_parts,
        query_rot,
        key_rot,
        value_rows,
        cosine,
        sine_table,
        query_hat,
        query_factor,
        key_hat,
        key_factor,
    )


def attn_backward(
    grad_attn, rows, seg_ids, wq_full, wk_full, wv_full, wo_full, query_gain, key_gain, saved
):
    (
        attn_heads,
        lse_all,
        query_rot,
        key_rot,
        value_rows,
        cosine,
        sine_table,
        query_hat,
        query_factor,
        key_hat,
        key_factor,
    ) = saved
    length = rows.shape[0]
    head_dim = query_gain.shape[0]
    num_heads = query_hat.shape[1]
    inv_root = 1.0 / math.sqrt(head_dim)
    block_rows = math.gcd(length, 512)
    grad_wo = jnp.dot(attn_heads.T, grad_attn, preferred_element_type=jnp.float32)
    grad_heads = (
        jnp.dot(grad_attn, wo_full.T, preferred_element_type=jnp.float32)
        .astype(jnp.bfloat16)
        .reshape(query_rot.shape)
    )
    heads_view = attn_heads.reshape(query_rot.shape)
    row_delta = jnp.transpose(
        jnp.sum(grad_heads.astype(jnp.float32) * heads_view.astype(jnp.float32), axis=-1), (1, 2, 0)
    )
    row_index = jnp.arange(length, dtype=jnp.int32)
    scores = mix("qgrd,kgd->grqk", query_rot, key_rot) * inv_root
    visible = (seg_ids[0:block_rows, None] == seg_ids[None, :]) & (
        row_index[None, :] <= row_index[0:block_rows, None]
    )
    scores = jnp.where(visible, scores, NEG_BIG)
    prob_f = jnp.where(visible, jnp.exp(scores - lse_all[:, :, 0:block_rows, None]), 0.0)
    prob_rows = prob_f.astype(jnp.bfloat16)
    grad_value = mix("grqk,qgrd->kgd", prob_rows, grad_heads)
    grad_probs = mix("qgrd,kgd->grqk", grad_heads, value_rows)
    grad_scores = (prob_f * (grad_probs - row_delta[:, :, 0:block_rows, None])).astype(jnp.bfloat16)
    pieces = mix("grqk,kgd->qgrd", grad_scores, key_rot) * inv_root
    grad_key_rot = mix("grqk,qgrd->kgd", grad_scores, query_rot) * inv_root
    grad_query_rot = pieces.reshape(length, num_heads, head_dim)
    grad_query, grad_qgain = head_norm_back(
        unrotate(grad_query_rot, cosine, sine_table), query_hat, query_factor, query_gain
    )
    grad_key, grad_kgain = head_norm_back(
        unrotate(grad_key_rot, cosine, sine_table), key_hat, key_factor, key_gain
    )
    query_b = grad_query.astype(jnp.bfloat16).reshape(length, -1)
    key_b = grad_key.astype(jnp.bfloat16).reshape(length, -1)
    value_b = grad_value.astype(jnp.bfloat16).reshape(length, -1)
    grad_rows = (
        jnp.dot(query_b, wq_full.T, preferred_element_type=jnp.float32)
        + jnp.dot(key_b, wk_full.T, preferred_element_type=jnp.float32)
        + jnp.dot(value_b, wv_full.T, preferred_element_type=jnp.float32)
    )
    grad_wq = jnp.dot(rows.T, query_b, preferred_element_type=jnp.float32)
    grad_wk = jnp.dot(rows.T, key_b, preferred_element_type=jnp.float32)
    grad_wv = jnp.dot(rows.T, value_b, preferred_element_type=jnp.float32)
    return (grad_rows, grad_wq, grad_wk, grad_wv, grad_wo, grad_qgain, grad_kgain)


def expert_forward(expert_rows, wgate, wup, wdown):
    gate_pre = jnp.dot(expert_rows, wgate, preferred_element_type=jnp.float32)
    up_pre = jnp.dot(expert_rows, wup, preferred_element_type=jnp.float32)
    hidden_units = (jax.nn.silu(gate_pre) * up_pre).astype(jnp.bfloat16)
    result = jnp.dot(hidden_units, wdown, preferred_element_type=jnp.float32).astype(jnp.bfloat16)
    return (result, gate_pre, up_pre, hidden_units)


def expert_backward(expert_rows, grad_result, wgate, wup, wdown, gate_pre, up_pre, hidden_units):
    grad_hidden = jnp.dot(grad_result, wdown.T, preferred_element_type=jnp.float32)
    sigma = jax.nn.sigmoid(gate_pre)
    grad_gate_pre = (grad_hidden * up_pre * sigma * (1.0 + gate_pre * (1.0 - sigma))).astype(
        jnp.bfloat16
    )
    grad_up_pre = (grad_hidden * gate_pre * sigma).astype(jnp.bfloat16)
    grad_rows = (
        jnp.dot(grad_gate_pre, wgate.T, preferred_element_type=jnp.float32)
        + jnp.dot(grad_up_pre, wup.T, preferred_element_type=jnp.float32)
    ).astype(jnp.bfloat16)
    grad_wd = jnp.dot(hidden_units.T, grad_result, preferred_element_type=jnp.float32)
    grad_wg = jnp.dot(expert_rows.T, grad_gate_pre, preferred_element_type=jnp.float32)
    grad_wu = jnp.dot(expert_rows.T, grad_up_pre, preferred_element_type=jnp.float32)
    return (grad_rows, grad_wg, grad_wu, grad_wd)


def to_experts(buffer):
    return lax.all_to_all(buffer, ("dp", "tensor"), split_axis=0, concat_axis=0, tiled=True)


def to_sources(buffer):
    return lax.all_to_all(buffer, ("dp", "tensor"), split_axis=0, concat_axis=0, tiled=True)


def shards(
    hidden_in,
    segments,
    routes,
    query_weight,
    key_weight,
    value_weight,
    output_weight,
    gain_attn,
    gain_moe,
    query_gain,
    key_gain,
    router,
    gate_weight,
    up_weight,
    down_weight,
    cotangent,
):
    seg_ids = segments[0]
    rows_dev = hidden_in.shape[0]
    width = hidden_in.shape[1]
    top_count = routes.shape[1]
    experts = router.shape[1]
    capacity = 2 * rows_dev * top_count // experts
    full_query, full_key, full_value, full_output = (
        lax.all_gather(query_weight, "dp", axis=0, tiled=True),
        lax.all_gather(key_weight, "dp", axis=0, tiled=True),
        lax.all_gather(value_weight, "dp", axis=0, tiled=True),
        lax.all_gather(output_weight, "dp", axis=1, tiled=True),
    )
    inputs32 = hidden_in.astype(jnp.float32)
    factor_one = rms_scale(inputs32)
    normed_one = inputs32 * factor_one
    rows_one = (normed_one * gain_attn).astype(jnp.bfloat16)
    group_rows = lax.all_gather(rows_one, "tensor", axis=0, tiled=True)
    saved = attn_forward(
        group_rows, seg_ids, full_query, full_key, full_value, query_gain, key_gain
    )
    partial_add = jnp.dot(saved[0], full_output, preferred_element_type=jnp.float32)
    attn_add = lax.psum_scatter(partial_add, "tensor", scatter_dimension=0, tiled=True)
    residual = inputs32 + attn_add
    factor_two = rms_scale(residual)
    normed_two = residual * factor_two
    rows_two = (normed_two * gain_moe).astype(jnp.bfloat16)
    router_probs = softmax_rows(jnp.dot(rows_two, router, preferred_element_type=jnp.float32))
    route_hot = (routes[:, :, None] == jnp.arange(experts, dtype=jnp.int32)[None, None, :]).astype(
        jnp.float32
    )
    picked = jnp.sum(route_hot * router_probs[:, None, :], axis=-1)
    total = jnp.sum(picked, axis=1, keepdims=True)
    gates = picked / total
    flat_routes = routes.reshape(-1)
    onehot = (flat_routes[:, None] == jnp.arange(experts, dtype=jnp.int32)[None, :]).astype(
        jnp.int32
    )
    ranks = jnp.sum(onehot * jnp.cumsum(onehot, axis=0), axis=1) - 1
    slots = flat_routes * capacity + ranks
    send_rows = (
        jnp.zeros((experts * capacity, width), jnp.bfloat16)
        .at[slots]
        .set(jnp.repeat(rows_two, top_count, axis=0))
    )
    received = to_experts(send_rows.reshape(experts, capacity, width)).reshape(-1, width)
    result, gate_pre, up_pre, hidden_units = expert_forward(
        received, gate_weight[0], up_weight[0], down_weight[0]
    )
    returned = to_sources(result.reshape(-1, capacity, width)).reshape(experts * capacity, width)
    pair_out = returned[slots].astype(jnp.float32).reshape(rows_dev, top_count, width)
    moe_sum = jnp.sum(gates[:, :, None] * pair_out, axis=1)
    output = (residual + moe_sum).astype(jnp.bfloat16)
    cot32 = cotangent.astype(jnp.float32)
    grad_gates = jnp.sum(cot32[:, None, :] * pair_out, axis=-1)
    grad_result = (gates[:, :, None] * cot32[:, None, :]).astype(jnp.bfloat16).reshape(-1, width)
    send_grads = jnp.zeros((experts * capacity, width), jnp.bfloat16).at[slots].set(grad_result)
    received_grads = to_experts(send_grads.reshape(experts, capacity, width)).reshape(-1, width)
    grad_expert_rows, grad_wg, grad_wu, grad_wd = expert_backward(
        received,
        received_grads,
        gate_weight[0],
        up_weight[0],
        down_weight[0],
        gate_pre,
        up_pre,
        hidden_units,
    )
    returned_grads = to_sources(grad_expert_rows.reshape(-1, capacity, width)).reshape(
        experts * capacity, width
    )
    grad_pairs = returned_grads[slots].astype(jnp.float32).reshape(rows_dev, top_count, width)
    grad_picked = (grad_gates - jnp.sum(gates * grad_gates, axis=1, keepdims=True)) / total
    grad_probs = jnp.sum(route_hot * grad_picked[:, :, None], axis=1)
    grad_logits = (
        router_probs * (grad_probs - jnp.sum(grad_probs * router_probs, axis=-1, keepdims=True))
    ).astype(jnp.bfloat16)
    grad_router = jnp.dot(rows_two.T, grad_logits, preferred_element_type=jnp.float32)
    grad_rows_two = jnp.sum(grad_pairs, axis=1) + jnp.dot(
        grad_logits, router.T, preferred_element_type=jnp.float32
    )
    grad_res_norm, grad_gain_moe = row_norm_back(grad_rows_two, normed_two, factor_two, gain_moe)
    grad_residual = cot32 + grad_res_norm
    grad_attn = grad_residual.astype(jnp.bfloat16)
    group_grads = lax.all_gather(grad_attn, "tensor", axis=0, tiled=True)
    back_query, back_key, back_value, back_output = (
        lax.all_gather(query_weight, "dp", axis=0, tiled=True),
        lax.all_gather(key_weight, "dp", axis=0, tiled=True),
        lax.all_gather(value_weight, "dp", axis=0, tiled=True),
        lax.all_gather(output_weight, "dp", axis=1, tiled=True),
    )
    grad_group_rows, grad_wq, grad_wk, grad_wv, grad_wo, grad_qgain, grad_kgain = attn_backward(
        group_grads,
        group_rows,
        seg_ids,
        back_query,
        back_key,
        back_value,
        back_output,
        query_gain,
        key_gain,
        saved,
    )
    grad_rows_one = lax.psum_scatter(
        grad_group_rows.astype(jnp.bfloat16), "tensor", scatter_dimension=0, tiled=True
    ).astype(jnp.float32)
    grad_in_norm, grad_gain_attn = row_norm_back(grad_rows_one, normed_one, factor_one, gain_attn)
    grad_input = grad_residual + grad_in_norm
    grad_wq, grad_wk, grad_wv, grad_wo = (
        lax.psum_scatter(
            grad_wq.astype(jnp.bfloat16), "dp", scatter_dimension=0, tiled=True
        ).astype(jnp.float32),
        lax.psum_scatter(
            grad_wk.astype(jnp.bfloat16), "dp", scatter_dimension=0, tiled=True
        ).astype(jnp.float32),
        lax.psum_scatter(
            grad_wv.astype(jnp.bfloat16), "dp", scatter_dimension=0, tiled=True
        ).astype(jnp.float32),
        lax.psum_scatter(
            grad_wo.astype(jnp.bfloat16), "dp", scatter_dimension=1, tiled=True
        ).astype(jnp.float32),
    )
    grad_gain_attn, grad_gain_moe, grad_qgain, grad_kgain, grad_router = lax.psum(
        (grad_gain_attn, grad_gain_moe, grad_qgain, grad_kgain, grad_router), ("dp", "tensor")
    )
    return (
        output,
        grad_input,
        grad_wq,
        grad_wk,
        grad_wv,
        grad_wo,
        grad_gain_attn,
        grad_gain_moe,
        grad_qgain,
        grad_kgain,
        grad_router,
        grad_wg[None],
        grad_wu[None],
        grad_wd[None],
    )


AXES = ("dp", "tensor")


def gathered(
    hidden_in,
    segments,
    routes,
    query_weight,
    key_weight,
    value_weight,
    output_weight,
    gain_attn,
    gain_moe,
    query_gain,
    key_gain,
    router,
    gate_weight,
    up_weight,
    down_weight,
    cotangent,
):
    seg_ids = segments[0]
    rows_dev, width = hidden_in.shape
    top_count = routes.shape[1]
    expert_count = router.shape[1]
    capacity = 2 * rows_dev * top_count // expert_count
    length = lax.axis_size("tensor")
    query_cols, key_cols = query_weight.shape[1], key_weight.shape[1]

    inputs32 = hidden_in.astype(jnp.float32)
    factor_one = rms_scale(inputs32)
    normed_one = inputs32 * factor_one
    rows_one = (normed_one * gain_attn).astype(jnp.bfloat16)
    joint_weight = jnp.concatenate([query_weight, key_weight, value_weight], axis=1)
    cosine, sine_table = rope_tables(seg_ids, query_gain.shape[0])
    turns = (
        seg_ids[None, :],
        cosine,
        sine_table,
        query_gain[None, :],
        key_gain[None, :],
    )
    attn_add, group_rows, full_joint, full_output, all_cots, projected, attn_heads, *laid = attend(
        rows_one, joint_weight, output_weight, cotangent, *turns, length, 0
    )
    residual = inputs32 + attn_add
    factor_two = rms_scale(residual)
    normed_two = residual * factor_two
    rows_two = (normed_two * gain_moe).astype(jnp.bfloat16)
    router_probs = softmax_rows(jnp.dot(rows_two, router, preferred_element_type=jnp.float32))
    route_hot = (routes[:, :, None] == jnp.arange(expert_count, dtype=jnp.int32)[None, None, :]).astype(
        jnp.float32
    )
    picked = jnp.sum(route_hot * router_probs[:, None, :], axis=-1)
    total = jnp.sum(picked, axis=1, keepdims=True)
    gates = picked / total
    named = jnp.sum(route_hot, axis=1)
    gate_table = jnp.where(named > 0.5, jnp.sum(route_hot * gates[:, :, None], axis=1), -1.0)
    all_rows, partial_out, partial_rows, token_grads, *units = experts(
        rows_two,
        all_cots,
        jnp.broadcast_to(gate_table.T[:, None, :], (expert_count, 8, rows_dev)),
        gate_weight[0],
        up_weight[0],
        down_weight[0],
        length,
        capacity,
        1,
    )
    back_grads = token_grads[:, 0, :]
    cot32 = cotangent.astype(jnp.float32)
    grad_gates = jnp.sum(route_hot * back_grads.T[:, None, :], axis=-1)
    grad_picked = (grad_gates - jnp.sum(gates * grad_gates, axis=1, keepdims=True)) / total
    grad_probs = jnp.sum(route_hot * grad_picked[:, :, None], axis=1)
    grad_logits = (
        router_probs * (grad_probs - jnp.sum(grad_probs * router_probs, axis=-1, keepdims=True))
    ).astype(jnp.bfloat16)
    grad_sum, grad_router, grad_wg, grad_wu, grad_wd = reduce_rows(
        partial_rows,
        grad_logits.T,
        all_rows,
        *[unit.reshape(-1, unit.shape[-1]) for unit in units],
        length,
        2,
    )
    grad_rows_two = grad_sum + jnp.dot(grad_logits, router.T, preferred_element_type=jnp.float32)
    grad_res_norm, grad_gain_moe = row_norm_back(grad_rows_two, normed_two, factor_two, gain_moe)
    grad_residual = cot32 + grad_res_norm
    grad_attn = grad_residual.astype(jnp.bfloat16)
    grad_rows_one, grad_joint, grad_wo, moe_sum, grad_qgain, grad_kgain = attend_back(
        grad_attn,
        group_rows,
        full_joint,
        full_output,
        projected,
        attn_heads,
        partial_out,
        laid[0],
        turns[0],
        *laid[1:],
        *turns[3:],
        length,
        3,
    )
    output = (residual + moe_sum).astype(jnp.bfloat16)
    grad_in_norm, grad_gain_attn = row_norm_back(grad_rows_one, normed_one, factor_one, gain_attn)
    grad_input = grad_residual + grad_in_norm
    small = jnp.concatenate([grad_gain_attn, grad_gain_moe, grad_qgain[0], grad_kgain[0]]).reshape(-1, 128)
    small = jnp.pad(small, ((0, -small.shape[0] % 8), (0, 0)))
    sums = share_sum(small, length, 4).reshape(-1)
    head_dim = query_gain.shape[0]
    return (
        output,
        grad_input,
        grad_joint[:, :query_cols],
        grad_joint[:, query_cols : query_cols + key_cols],
        grad_joint[:, query_cols + key_cols :],
        grad_wo,
        sums[:width],
        sums[width : 2 * width],
        sums[2 * width : 2 * width + head_dim],
        sums[2 * width + head_dim : 2 * width + 2 * head_dim],
        grad_router.T,
        grad_wg[None],
        grad_wu[None],
        grad_wd[None],
    )


def solution(mesh):
    placed = (
        P(("dp", "tensor"), None),
        P("dp", None),
        P(("dp", "tensor"), None),
        P("dp", "tensor"),
        P("dp", "tensor"),
        P("dp", "tensor"),
        P("tensor", "dp"),
        P(),
        P(),
        P(),
        P(),
        P(),
        P(("dp", "tensor"), None, None),
        P(("dp", "tensor"), None, None),
        P(("dp", "tensor"), None, None),
        P(("dp", "tensor"), None),
    )
    program = gathered if mesh.shape["dp"] == 8 and mesh.shape["tensor"] <= 4 else shards
    return jax.shard_map(
        program,
        mesh=mesh,
        in_specs=placed,
        out_specs=(
            P(("dp", "tensor"), None),
            P(("dp", "tensor"), None),
            P("dp", "tensor"),
            P("dp", "tensor"),
            P("dp", "tensor"),
            P("tensor", "dp"),
            P(),
            P(),
            P(),
            P(),
            P(),
            P(("dp", "tensor"), None, None),
            P(("dp", "tensor"), None, None),
            P(("dp", "tensor"), None, None),
        ),
        check_vma=False,
    )
```

```python
import math

import jax
import jax.numpy as jnp
from jax import lax
from jax.experimental import pallas as pl
from jax.experimental.pallas import tpu as pltpu
from jax.sharding import PartitionSpec as P

EPSILON = 1e-06
THETA_BASE = 1000000.0
NEG_BIG = -1e30


MESH = pl.DeviceIdType.MESH


class Place:
    def __init__(self, length):
        self.length = length
        self.dp = lax.axis_index("dp")
        self.z = lax.axis_index("tensor")
        core, along_x, along_y = self.dp % 2, (self.dp // 2) % 2, self.dp // 4
        self.to_core = 1 - 2 * core
        self.core = self.dp + self.to_core
        self.x = self.dp + 2 - 4 * along_x
        self.y = self.dp + 4 - 8 * along_y
        self.columns = (self.dp, self.x, self.y, self.x + self.y - self.dp)

    def device(self, kind):
        if kind == "x":
            return (self.x, self.z)
        if kind == "y":
            return (self.y, self.z)
        if kind == "core":
            return (self.core, self.z)
        if kind == "up":
            return (self.dp, self.z + 1)
        return (self.dp, self.z - 1)

    @property
    def has_up(self):
        return self.z < self.length - 1

    @property
    def has_down(self):
        return self.z > 0

    def condition(self, kind):
        if kind == "up":
            return self.has_up
        return self.has_down if kind == "down" else None

    def nearest(self, turn):
        length = self.length

        def equal(left, right):
            far = 2 * length
            return (left - right + far) // far - (left - right - 1 + far) // far

        found = 0
        for mine in range(length):
            order = sorted(range(length), key=lambda other: (abs(other - mine), other))
            for step, other in enumerate(order):
                if other:
                    found = found + equal(self.z, mine) * equal(turn, step) * other
        return found

    def target(self, turn):
        length, z = self.length, self.z

        def at_least(left, right):
            return (left - right + 2 * length) // (2 * length)

        high = at_least(z, length // 2)
        mirrored = z + high * (length - 1 - 2 * z)
        above = length - 1 - mirrored
        first = at_least(above - 1, turn)
        if turn == length - 1:
            return z
        found = first * (length - 1 - turn) + (1 - first) * (turn - above)
        return found + high * (length - 1 - 2 * found)


def piece(rows, h):
    return pl.ds(0, rows) if h is None else pl.ds(h * (rows // 2), rows // 2)


def guarded(condition, action):
    if condition is None:
        action()
    else:
        pl.when(condition)(action)


def meet(place, over_z, over_dp):
    barrier = pltpu.get_barrier_semaphore()
    kinds = (("x", "y", "core") if over_dp else ()) + (("up", "down") if over_z else ())
    for kind in kinds:

        def greet(kind=kind):
            pl.semaphore_signal(
                barrier, 1, device_id=place.device(kind), device_id_type=MESH
            )

        guarded(place.condition(kind), greet)
    count = 3 if over_dp else 0
    if over_z:
        length = place.length
        count = count + (place.z + length - 1) // length + (2 * length - 2 - place.z) // length
    pl.semaphore_wait(barrier, count)


def other_device(place, distance):
    there = lax.rem(place.dp * place.length + place.z + distance, 8 * place.length)
    return (there // place.length, lax.rem(there, place.length)), there


def meet_all(place):
    barrier = pltpu.get_barrier_semaphore()
    others = 8 * place.length - 1

    def greet(n, carry):
        device, _ = other_device(place, n + 1)
        pl.semaphore_signal(barrier, 1, device_id=device, device_id_type=MESH)
        return carry

    lax.fori_loop(0, others, greet, 0)
    pl.semaphore_wait(barrier, others)


class Sends:
    def __init__(self, place):
        self.place = place
        self.started = []

    def start(self, kind, views, condition=lambda: None):
        def build():
            source, target, send_sem, recv_sem = views()
            return pltpu.make_async_remote_copy(
                src_ref=source,
                dst_ref=target,
                send_sem=send_sem,
                recv_sem=recv_sem,
                device_id=self.place.device(kind),
                device_id_type=MESH,
            )

        guarded(self.place.condition(kind), lambda: build().start())
        self.started.append((condition, kind, build))

    def drain(self):
        for condition, kind, build in self.started:

            def finish(kind=kind, build=build):
                guarded(self.place.condition(kind), lambda: build().wait_send())

            guarded(condition(), finish)


class GatherItem:
    def __init__(self, mode, place, own, slot, recv, send, local):
        self.mode, self.place = mode, place
        self.own, self.slot = own, slot
        self.recv, self.send, self.local = recv, send, local
        self.over_z = mode != "dp"
        self.over_dp = mode != "z"
        self.length = place.length if self.over_z else 1
        self.z = place.z if self.over_z else 0

    def index(self, column, z):
        if self.mode == "all":
            return column * self.length + z
        return column if self.mode == "dp" else z

    @staticmethod
    def semaphores(mode, length):
        blocks = {"all": 8 * length, "dp": 8, "z": length}[mode]
        turns = 2 * length - 1 if mode != "dp" else 1
        return [
            pltpu.SemaphoreType.DMA((blocks, 2)),
            pltpu.SemaphoreType.DMA((10, turns, 2)),
            pltpu.SemaphoreType.DMA((2,)),
        ]

    def turns(self, distance):
        if distance == 0:
            return [(0, 0, lambda: None, None)]
        place, length = self.place, self.length
        return [
            (2 * distance - 1, -distance, lambda: place.z >= distance, "up"),
            (2 * distance, distance, lambda: place.z < length - distance, "down"),
        ]

    def pass_on(self, sends, lane, kind, column, offset, turn, h, source=None, condition=lambda: None):
        at = 0 if h is None else h

        def views():
            z = self.z + offset
            view = self.slot(column, z, h)
            return (
                view if source is None else source(h),
                view,
                self.send.at[lane, turn, at],
                self.recv.at[self.index(column, z), at],
            )

        sends.start(kind, views, condition)

    def arrived(self, column, z, h):
        view = self.slot(column, z, h)
        at = 0 if h is None else h
        pltpu.make_async_copy(view, view, self.recv.at[self.index(column, z), at]).wait()

    def local_copy(self):
        return pltpu.make_async_copy(
            self.own(None), self.slot(self.place.dp, self.z, None), self.local.at[0]
        )

    def begin(self, sends):
        place = self.place
        if self.over_z:
            self.pass_on(sends, 0, "up", place.dp, 0, 0, None, self.own)
            self.pass_on(sends, 1, "down", place.dp, 0, 0, None, self.own)
        if self.over_dp:
            self.pass_on(sends, 2, "x", place.dp, 0, 0, None, self.own)
            self.pass_on(sends, 3, "y", place.dp, 0, 0, None, self.own)
            self.pass_on(sends, 4, "core", place.dp, 0, 0, None, self.own)
        self.local_copy().start()

    def along_z(self, sends, distance):
        if not self.over_z or distance >= self.length:
            return
        place = self.place
        for turn, offset, condition, onward in self.turns(distance):

            def step(turn=turn, offset=offset, condition=condition, onward=onward):
                self.arrived(place.dp, self.z + offset, None)
                lanes = []
                if distance < self.length - 1:
                    lanes.append((0 if onward == "up" else 1, onward))
                if self.over_dp:
                    lanes += [(2, "x"), (3, "y"), (4, "core")]
                for lane, kind in lanes:
                    self.pass_on(
                        sends, lane, kind, place.dp, offset, turn, None, condition=condition
                    )

            guarded(condition(), step)

    def across(self, sends, distance):
        if not self.over_dp or not 0 <= distance < self.length:
            return
        _, x, y, _ = self.place.columns
        for turn, offset, condition, _ in self.turns(distance):

            def step(turn=turn, offset=offset, condition=condition):
                self.arrived(x, self.z + offset, None)
                self.pass_on(sends, 5, "y", x, offset, turn, 0, condition=condition)
                self.pass_on(sends, 7, "core", x, offset, turn, None, condition=condition)
                self.arrived(y, self.z + offset, None)
                self.pass_on(sends, 6, "x", y, offset, turn, 1, condition=condition)
                self.pass_on(sends, 8, "core", y, offset, turn, None, condition=condition)

            guarded(condition(), step)

    def diagonal(self, sends, distance):
        if not self.over_dp or not 0 <= distance < self.length:
            return
        corner = self.place.columns[3]
        for turn, offset, condition, _ in self.turns(distance):

            def step(turn=turn, offset=offset, condition=condition):
                for h in range(2):
                    self.arrived(corner, self.z + offset, h)
                    self.pass_on(sends, 9, "core", corner, offset, turn, h, condition=condition)

            guarded(condition(), step)

    def settled(self):
        self.local_copy().wait()

    def from_core(self, z):
        for number, column in enumerate(self.place.columns):
            for h in (0, 1) if number == 3 else (None,):
                self.arrived(column + self.place.to_core, z, h)

    def finish(self):
        self.settled()
        if self.over_dp:
            for z in range(self.length):
                self.from_core(z)


class ReduceItem:
    def __init__(self, mode, place, block, bufs, out):
        self.mode, self.place, self.block, self.out = mode, place, block, out
        self.over_z = mode != "dp"
        self.over_dp = mode != "z"
        self.length = place.length if self.over_z else 1
        (self.acc, self.from_core, self.corner, self.from_xy, self.from_z,
         self.load, self.send, self.recv) = bufs

    @staticmethod
    def scratch(mode, length, rows, width, in_place=False):
        t = length if mode != "dp" else 1
        columns = 4 if mode != "z" else 1
        dp = mode != "z"
        small = (8, 128)
        return [
            pltpu.VMEM(small if in_place else (columns, t, rows, width), jnp.bfloat16),
            pltpu.VMEM((columns, t, rows, width) if dp else small, jnp.bfloat16),
            pltpu.VMEM((2, t, rows // 2, width) if dp else small, jnp.bfloat16),
            pltpu.VMEM((2, t, rows, width) if dp else small, jnp.bfloat16),
            pltpu.VMEM((t + 1, rows, width) if mode != "dp" else small, jnp.bfloat16),
            pltpu.SemaphoreType.DMA((columns, t)),
            pltpu.SemaphoreType.DMA((10, t, 2)),
            pltpu.SemaphoreType.DMA((9, t + 1, 2)),
        ]

    def z_of(self, turn):
        return self.place.target(turn) if self.over_z else 0

    def got(self, ref, lane, turn, h=0):
        pltpu.make_async_copy(ref, ref, self.recv.at[lane, turn, h]).wait()

    computed = False
    in_place = False

    def partial(self, column, turn, h):
        if self.in_place:
            return self.block(self.place.columns[column], self.z_of(turn), h)
        return self.acc.at[column, turn, piece(self.acc.shape[2], h)]

    def add(self, target, refs, out=None):
        rows = target.shape[0]
        step = 16 if rows % 16 == 0 else rows
        place = target if out is None else out

        def body(i, carry):
            at = pl.ds(pl.multiple_of(i * step, step), step)
            total = target[at, :].astype(jnp.float32)
            for ref in refs:
                total = total + ref[at, :].astype(jnp.float32)
            place[at, :] = total.astype(place.dtype)
            return carry

        lax.fori_loop(0, rows // step, body, 0, unroll=2 if (rows // step) % 2 == 0 else 1)

    def begin(self):
        place = self.place
        if self.over_z:

            @pl.when((place.z == 0) | (place.z == self.length - 1))
            def _():
                def clear(i, carry):
                    self.from_z[i] = jnp.zeros(self.from_z.shape[1:], jnp.bfloat16)
                    return carry

                lax.fori_loop(0, self.length + 1, clear, 0)

    def load_all(self):
        place = self.place
        for turn in range(self.length):
            for column in (3, 1, 2, 0) if self.over_dp else (0,):
                pltpu.make_async_copy(
                    self.block(place.columns[column], self.z_of(turn), None),
                    self.acc.at[column, turn],
                    self.load.at[column, turn],
                ).start()

    def hand_over(self, sends, turn):
        if not self.over_dp or turn >= self.length:
            return
        place = self.place
        for column in (3, 1, 2, 0):
            sends.start(
                "core",
                lambda column=column: (
                    self.block(place.columns[column] + place.to_core, self.z_of(turn), None),
                    self.from_core.at[column, turn],
                    self.send.at[column, turn, 0],
                    self.recv.at[column, turn, 0],
                ),
            )

    def ready(self, column, turn):
        if not (self.computed or self.in_place):
            ref = self.acc.at[column, turn]
            pltpu.make_async_copy(ref, ref, self.load.at[column, turn]).wait()
        if self.over_dp:
            self.got(self.from_core.at[column, turn], column, turn)

    def settle(self, column, turn, h, extra=(), out=None):
        refs = list(extra)
        if self.over_dp:
            rows = self.from_core.shape[2]
            refs.append(self.from_core.at[column, turn, piece(rows, h)])
        if refs or out is not None:
            self.add(self.partial(column, turn, h), refs, out)

    def corners(self, sends, turn):
        if not self.over_dp or not 0 <= turn < self.length:
            return
        self.ready(3, turn)
        for h, kind in ((0, "y"), (1, "x")):
            self.settle(3, turn, h)
            sends.start(
                kind,
                lambda h=h: (
                    self.partial(3, turn, h),
                    self.corner.at[h, turn],
                    self.send.at[4, turn, h],
                    self.recv.at[4, turn, h],
                ),
            )

    def straight(self, sends, turn, second):
        if not self.over_dp or not 0 <= turn < self.length:
            return
        rows = self.from_xy.shape[2]
        for column, kind in ((1, "x"), (2, "y")):
            h = (column - 1) if second else (2 - column)
            extra = ()
            if second:
                ref = self.corner.at[h, turn]
                self.got(ref, 4, turn, h)
                extra = (ref,)
            else:
                self.ready(column, turn)
            self.settle(column, turn, h, extra)
            sends.start(
                kind,
                lambda column=column, h=h: (
                    self.partial(column, turn, h),
                    self.from_xy.at[column - 1, turn, piece(rows, h)],
                    self.send.at[4 + column, turn, h],
                    self.recv.at[4 + column, turn, h],
                ),
            )

    def home(self, sends, turn):
        if not 0 <= turn < self.length:
            return
        place = self.place
        last = turn == self.length - 1
        z = self.z_of(turn)
        extra = []
        self.ready(0, turn)
        if self.over_dp:
            for lane in (0, 1):
                rows = self.from_xy.shape[2]
                for h in range(2):
                    self.got(self.from_xy.at[lane, turn, piece(rows, h)], 5 + lane, turn, h)
                extra.append(self.from_xy.at[lane, turn])
        if self.over_z:

            def got_slot():
                self.got(self.from_z.at[z], 7, z)

            def got_other():
                self.got(self.from_z.at[self.length], 7, self.length)

            extra.append(self.from_z.at[z])
            if last:
                guarded(place.has_down, got_slot)
                guarded(place.has_up, got_other)
                extra.append(self.from_z.at[self.length])
            else:
                guarded((z > place.z) & place.has_down, got_slot)
                guarded((z < place.z) & place.has_up, got_slot)
        self.settle(0, turn, None, extra, self.out(None) if last else None)
        if self.over_z and not last:

            def going_up():
                goal = self.z_of(turn)
                return (
                    self.partial(0, turn, None),
                    self.from_z.at[goal],
                    self.send.at[7, turn, 0],
                    self.recv.at[7, goal, 0],
                )

            def going_down():
                there = self.z_of(turn)
                arrives = (there - place.z + 1 + self.length) // self.length
                goal = there + arrives * (self.length - there)
                return (
                    self.partial(0, turn, None),
                    self.from_z.at[goal],
                    self.send.at[7, turn, 0],
                    self.recv.at[7, goal, 0],
                )

            def above():
                return self.z_of(turn) > place.z

            def below():
                return self.z_of(turn) < place.z

            pl.when(above())(lambda: sends.start("up", going_up, above))
            pl.when(below())(lambda: sends.start("down", going_down, below))


def advance(item, sends, step):
    item.corners(sends, step)
    item.straight(sends, step, False)
    item.hand_over(sends, step + 2)
    item.straight(sends, step - 1, True)
    item.home(sends, step - 2 if item.over_dp else step)


def reduce_rows(partials, small, all_rows, picked, gated, hid, dgate, dup, length, collective_id):
    devices, rows, width = partials.shape
    slots, hidden = dup.shape
    half, low = rows // 2, small.shape[0] // 2
    tile, narrow = width // 4, hidden // 3
    f32, bf16 = jnp.float32, jnp.bfloat16

    def kernel(
        source, small_ref, all_ref, picked_ref, gated_ref, hid_ref, dgate_ref, dup_ref,
        target, product, out_g, out_u, out_d,
        small_all, rows_v, rows_sem, hid_v, dgate_v, dup_v, picked_v, gated_v, tile_g, tile_u, tile_d, load_sem, tile_sem, store_sem,
        *rest,
    ):
        place = Place(length)
        item = ReduceItem(
            "all",
            place,
            lambda c, z, h: source.at[c * length + z, piece(2 * half, h)],
            rest[:8],
            lambda h: target.at[piece(2 * half, h)],
        )
        beside = GatherItem("all", place, None, None, *rest[8:])
        beside.own = lambda h: small_ref.at[piece(2 * low, h)]
        beside.slot = lambda c, z, h: small_all.at[c * length + z, piece(2 * low, h)]
        item.begin()
        meet(place, True, True)
        sends = Sends(place)
        beside.begin(sends)
        item.hand_over(sends, 0)
        item.load_all()
        item.hand_over(sends, 1)
        resident = [
            pltpu.make_async_copy(left, right, load_sem.at[n])
            for n, (left, right) in enumerate(
                ((hid_ref, hid_v), (dgate_ref, dgate_v), (dup_ref, dup_v))
            )
        ]
        for copy in resident:
            copy.start()

        def lanes_of(n):
            return pl.ds(pl.multiple_of(n * tile, tile), tile)

        def tiles(n, slot):
            return [
                pltpu.make_async_copy(picked_ref.at[:, lanes_of(n)], picked_v.at[slot], tile_sem.at[slot, 0]),
                pltpu.make_async_copy(gated_ref.at[:, lanes_of(n)], gated_v.at[slot], tile_sem.at[slot, 1]),
            ]

        def stores(n, slot):
            return [
                pltpu.make_async_copy(tile_g.at[slot], out_g.at[lanes_of(n)], store_sem.at[slot, 0]),
                pltpu.make_async_copy(tile_u.at[slot], out_u.at[lanes_of(n)], store_sem.at[slot, 1]),
                pltpu.make_async_copy(tile_d.at[slot], out_d.at[:, lanes_of(n)], store_sem.at[slot, 2]),
            ]

        for copy in tiles(0, 0):
            copy.start()

        def rows_load(group, part):
            return pltpu.make_async_copy(
                all_ref.at[pl.ds(group * length, length)], rows_v.at[part], rows_sem.at[part]
            )

        for part in range(2):
            rows_load(part, part).start()

        def narrow_of(m):
            return pl.ds(pl.multiple_of(m * narrow, narrow), narrow)

        def chunk(c, carry):
            n, kind = c // 3, c % 3
            slot = n % 2

            @pl.when((kind == 0) & (n < 4))
            def _():
                for copy in tiles(n, slot):
                    copy.wait()

                @pl.when(n < 3)
                def _():
                    for copy in tiles(n + 1, 1 - slot):
                        copy.start()

                @pl.when(n >= 2)
                def _():
                    for copy in stores(n, slot):
                        copy.wait()

                def body(m, carry):
                    tile_g[slot, :, narrow_of(m)] = dot(picked_v[slot], dgate_v[:, narrow_of(m)], 0, 0)
                    return carry

                lax.fori_loop(0, 3, body, 0)
                stores(n, slot)[0].start()

            @pl.when((kind == 1) & (n < 4))
            def _():
                def body(m, carry):
                    tile_u[slot, :, narrow_of(m)] = dot(picked_v[slot], dup_v[:, narrow_of(m)], 0, 0)
                    return carry

                lax.fori_loop(0, 3, body, 0)
                stores(n, slot)[1].start()

            @pl.when((kind == 2) & (n < 4))
            def _():
                def body(m, carry):
                    tile_d[slot, narrow_of(m), :] = dot(hid_v[:, narrow_of(m)], gated_v[slot], 0, 0)
                    return carry

                lax.fori_loop(0, 3, body, 0)
                stores(n, slot)[2].start()
            return carry

        def turn_of(i, carry):
            for step in range(length + 2):

                @pl.when(i == 2 * step)
                def _(step=step):
                    item.corners(sends, step)
                    item.straight(sends, step, False)
                    item.hand_over(sends, step + 2)

                @pl.when(i == 2 * step + 1)
                def _(step=step):
                    item.straight(sends, step - 1, True)
                    item.home(sends, step - 2)

            for step in range(length + 2):

                @pl.when(i == step)
                def _(step=step):
                    beside.along_z(sends, step + 1)
                    beside.across(sends, step)
                    beside.diagonal(sends, step - 1)

            @pl.when(i == length + 2)
            def _():
                beside.finish()
                product[...] = jnp.zeros(product.shape, f32)

            @pl.when((i >= length + 2) & (i < length + 6))
            def _():
                for part in range(2):
                    group = 2 * (i - length - 2) + part
                    rows_load(group, part).wait()
                    marks = [
                        small_all[group * length + z] for z in range(length)
                    ]
                    left = jnp.concatenate(marks, axis=1)

                    def body(m, carry, part=part, left=left):
                        lanes = pl.ds(pl.multiple_of(m * tile, tile), tile)
                        right = rows_v[part, :, :, lanes].reshape(length * rows, tile)
                        product[:, lanes] += dot(left, right)
                        return carry

                    lax.fori_loop(0, 4, body, 0)

                    @pl.when(group + 2 < 8)
                    def _(part=part, group=group):
                        rows_load(group + 2, part).start()

            @pl.when(i == 0)
            def _():
                for copy in resident:
                    copy.wait()

            @pl.when(i < 6)
            def _():
                lax.fori_loop(0, 2, lambda part, carry: chunk(2 * i + part, carry), 0)

            return carry

        lax.fori_loop(0, max(12, 2 * (length + 2), length + 6), turn_of, 0)
        for slot in range(2):
            for copy in stores(slot, slot):
                copy.wait()
        sends.drain()

    any_spec = pl.BlockSpec(memory_space=pl.ANY)
    shape = jax.ShapeDtypeStruct
    sems = pltpu.SemaphoreType.DMA
    return pl.pallas_call(
        kernel,
        name="reduce_rows",
        out_shape=[
            shape((rows, width), f32),
            shape((small.shape[0], width), f32),
            shape((width, hidden), f32),
            shape((width, hidden), f32),
            shape((hidden, width), f32),
        ],
        in_specs=[any_spec] * 8,
        out_specs=[pl.BlockSpec(memory_space=pltpu.VMEM)] * 2 + [any_spec] * 3,
        scratch_shapes=[
            pltpu.VMEM((devices,) + small.shape, small.dtype),
            pltpu.VMEM((2, length, rows, width), bf16),
            sems((2,)),
            pltpu.VMEM((slots, hidden), bf16),
            pltpu.VMEM((slots, hidden), bf16),
            pltpu.VMEM((slots, hidden), bf16),
            pltpu.VMEM((2, slots, tile), bf16),
            pltpu.VMEM((2, slots, tile), bf16),
            pltpu.VMEM((2, tile, hidden), f32),
            pltpu.VMEM((2, tile, hidden), f32),
            pltpu.VMEM((2, hidden, tile), f32),
            sems((3,)),
            sems((2, 2)),
            sems((2, 3)),
        ]
        + ReduceItem.scratch("all", length, rows, width)
        + GatherItem.semaphores("all", length),
        compiler_params=pltpu.CompilerParams(
            collective_id=collective_id, has_side_effects=True, vmem_limit_bytes=67043328
        ),
    )(partials, small, all_rows, picked, gated, hid, dgate, dup)


def dot(left, right, left_dim=1, right_dim=0):
    return lax.dot_general(
        left, right, (((left_dim,), (right_dim,)), ((), ())), preferred_element_type=jnp.float32
    )


def experts(rows_own, all_cots, gates_own, wgate, wup, wdown, length, capacity, collective_id):
    rows, width = rows_own.shape
    hidden = wgate.shape[1]
    devices = 8 * length
    count = 4 * capacity
    tile = 512 if width % 512 == 0 else width
    narrow = 256 if hidden % 256 == 0 else hidden
    f32, bf16 = jnp.float32, jnp.bfloat16

    def kernel(
        rows_ref, all_cots, gates_ref, wg_ref, wu_ref, wd_ref,
        all_rows, part_out, part_grad, token_in, picked_all, gated_all, hid_all, dgate_all, dup_all,
        wg, wu, wd, chosen_all, gates_all, rank_v, table, row_buf, cot_buf, picked, cotan, gated, hid, dgate, dup, scaled, back,
        chosen, slot_gate, slot_sum, stage_out, stage_grad, token_out,
        recv_r, send_r, local_r,
        load_sem, store_sem, save_sem, token_sem, gate_sem, weight_sem,
    ):
        place = Place(length)
        expert = place.dp * length + place.z

        def item_of(source, target, sems, half):
            item = GatherItem("all", place, None, None, *sems)
            item.own = lambda h: source.at[piece(2 * half, h)]
            item.slot = lambda column, z, h: target.at[
                column * length + z, piece(2 * half, h)
            ]
            return item

        big = [
            item_of(rows_ref, all_rows, (recv_r, send_r, local_r), rows // 2),
        ]
        items = big
        meet_all(place)
        sends = Sends(place)

        def gate_send(n):
            device, there = other_device(place, n + 1)
            return pltpu.make_async_remote_copy(
                src_ref=gates_ref.at[there],
                dst_ref=table.at[expert],
                send_sem=gate_sem.at[0],
                recv_sem=gate_sem.at[1],
                device_id=device,
                device_id_type=MESH,
            )

        def send_gates(n, carry):
            gate_send(n).start()
            return carry

        lax.fori_loop(0, devices - 1, send_gates, 0)
        pltpu.make_async_copy(gates_ref.at[expert], table.at[expert], gate_sem.at[1]).start()
        for item in items:
            item.begin(sends)

        weights = [
            pltpu.make_async_copy(source, target, weight_sem.at[n])
            for n, (source, target) in enumerate(((wg_ref, wg), (wu_ref, wu), (wd_ref, wd)))
        ]
        for copy in weights:
            copy.start()

        def along(distance):
            for item in items:
                item.along_z(sends, distance)

        def across(distance):
            for item in items:
                item.across(sends, distance)

        def corner(distance):
            for item in items:
                item.diagonal(sends, distance)

        across(0)
        along(1)
        pltpu.make_async_copy(table, table, gate_sem.at[1]).wait()
        order = lax.broadcasted_iota(jnp.int32, (rows, rows), 0)
        upto = (order <= lax.broadcasted_iota(jnp.int32, (rows, rows), 1)).astype(f32).astype(bf16)
        slots = lax.broadcasted_iota(jnp.int32, (capacity, rows), 0).astype(f32)
        lines = table[:, 0, :]
        rank_v[...] = dot((lines >= 0.0).astype(f32).astype(bf16), upto) - 1.0

        def choose(block, carry):
            line = table[block, 0:1, :]
            ranks = rank_v[pl.ds(block, 1), :]
            pick = jnp.where((line >= 0.0) & (ranks == slots), 1.0, 0.0)
            gate = jnp.sum(pick * line, axis=1, keepdims=True)
            chosen_all[block] = pick.astype(bf16)
            gates_all[block] = jnp.broadcast_to(gate, (capacity, 128))
            return carry

        lax.fori_loop(0, devices, choose, 0, unroll=4)
        for item in items:
            item.settled()

        def block_of(j, side, z):
            return (place.columns[j] + side * place.to_core) * length + z

        def load(j, side, z, slot):
            block = block_of(j, side, z)
            return [
                pltpu.make_async_copy(all_rows.at[block], row_buf.at[slot, j], load_sem.at[slot, 0, j]),
                pltpu.make_async_copy(all_cots.at[block], cot_buf.at[slot, j], load_sem.at[slot, 1, j]),
            ]

        def store(j, side, z, slot):
            block = block_of(j, side, z)
            return [
                pltpu.make_async_copy(stage_out.at[slot, j], part_out.at[block], store_sem.at[slot, 0, j]),
                pltpu.make_async_copy(stage_grad.at[slot, j], part_grad.at[block], store_sem.at[slot, 1, j]),
            ]

        def saved(i):
            first = [
                pltpu.make_async_copy(picked, picked_all.at[i], save_sem.at[0]),
                pltpu.make_async_copy(gated, gated_all.at[i], save_sem.at[1]),
            ]
            second = [
                pltpu.make_async_copy(hid, hid_all.at[i], save_sem.at[2]),
                pltpu.make_async_copy(dgate, dgate_all.at[i], save_sem.at[3]),
                pltpu.make_async_copy(dup, dup_all.at[i], save_sem.at[4]),
            ]
            return first, second

        def start_loads(step, side):
            for j in range(4):
                for copy in load(j, side, place.nearest(step), side):
                    copy.start()

        corner(0)
        for item in items:
            item.from_core(place.nearest(0))
        start_loads(0, 0)
        start_loads(0, 1)
        for copy in weights:
            copy.wait()

        def unit(i, carry):
            turn, side = i // 2, i % 2
            z = place.nearest(turn)

            @pl.when(i == 1)
            def _():
                along(2)
                across(1)

            for step in range(1, length):

                @pl.when(i == max(2, 2 * step - 1))
                def _(step=step):
                    corner(step)
                    along(step + 2)
                    across(step + 1)
                    for item in items:
                        item.from_core(place.nearest(step))
                    start_loads(step, 0)
                    if step == 1:
                        start_loads(step, 1)

            @pl.when(i >= 1)
            def _():
                for copy in saved(i)[0]:
                    copy.wait()

            for j in range(4):
                for copy in load(j, side, z, side):
                    copy.wait()
            for j in range(4):
                block = block_of(j, side, z)
                chosen[j] = chosen_all[block]
                slot_gate[pl.ds(j * capacity, capacity), :] = gates_all[block]

            def select(n, carry):
                lanes = pl.ds(pl.multiple_of(n * tile, tile), tile)
                for j in range(4):
                    at = pl.ds(j * capacity, capacity)
                    picked[at, lanes] = dot(chosen[j], row_buf[side, j, :, lanes]).astype(bf16)
                    cot = dot(chosen[j], cot_buf[side, j, :, lanes])
                    cotan[at, lanes] = cot.astype(bf16)
                    gated[at, lanes] = (slot_gate[at, 0:1] * cot).astype(bf16)
                return carry

            lax.fori_loop(0, width // tile, select, 0)

            for copy in saved(i)[0]:
                copy.start()
            for step in range(2, length):

                @pl.when(i == 2 * step - 1)
                def _(step=step):
                    start_loads(step, 1)

            @pl.when(i >= 1)
            def _():
                for copy in saved(i)[1]:
                    copy.wait()

            def middle(n, carry):
                lanes = pl.ds(pl.multiple_of(n * narrow, narrow), narrow)
                gate = dot(picked[...], wg[:, lanes])
                up = dot(picked[...], wu[:, lanes])
                grad = dot(gated[...], wd[lanes, :], 1, 1)
                sigma = jax.nn.sigmoid(gate)
                hid[:, lanes] = (gate * sigma * up).astype(bf16)
                dgate[:, lanes] = (grad * up * sigma * (1.0 + gate * (1.0 - sigma))).astype(bf16)
                dup[:, lanes] = (grad * gate * sigma).astype(bf16)
                return carry

            lax.fori_loop(0, hidden // narrow, middle, 0)
            for copy in saved(i)[1]:
                copy.start()
            slot_sum[...] = jnp.zeros(slot_sum.shape, f32)

            @pl.when(i >= 2)
            def _():
                for j in range(4):
                    for copy in store(j, side, z, side):
                        copy.wait()

            def outward(n, carry):
                lanes = pl.ds(pl.multiple_of(n * tile, tile), tile)
                result = dot(hid[...], wd[:, lanes]).astype(bf16).astype(f32)
                products = cotan[:, lanes].astype(f32) * result
                total = products[:, 0:128]
                for k in range(1, tile // 128):
                    total = total + products[:, 128 * k : 128 * (k + 1)]
                slot_sum[...] += total
                scaled[:, lanes] = (slot_gate[:, 0:1] * result).astype(bf16)
                back[:, lanes] = (
                    dot(dgate[...], wg[lanes, :], 1, 1) + dot(dup[...], wu[lanes, :], 1, 1)
                ).astype(bf16)
                for j in range(4):
                    at = pl.ds(j * capacity, capacity)
                    stage_out[side, j, :, lanes] = dot(chosen[j], scaled[at, lanes], 0, 0).astype(bf16)
                    stage_grad[side, j, :, lanes] = dot(chosen[j], back[at, lanes], 0, 0).astype(bf16)
                return carry

            lax.fori_loop(0, width // tile, outward, 0)
            for j in range(4):
                for copy in store(j, side, z, side):
                    copy.start()
            total = jnp.sum(slot_sum[...], axis=1, keepdims=True).reshape(4, capacity, 1)
            sums = jnp.sum(chosen[...].astype(f32) * total, axis=1)
            for j in range(4):
                token_out[block_of(j, side, z)] = jnp.broadcast_to(sums[j : j + 1], (8, rows))
            return carry

        lax.fori_loop(0, 2 * length, unit, 0)

        def token_send(n):
            device, there = other_device(place, n + 1)
            return pltpu.make_async_remote_copy(
                src_ref=token_out.at[there],
                dst_ref=token_in.at[expert],
                send_sem=token_sem.at[0],
                recv_sem=token_sem.at[1],
                device_id=device,
                device_id_type=MESH,
            )

        def send(n, carry):
            token_send(n).start()
            return carry

        lax.fori_loop(0, devices - 1, send, 0)
        pltpu.make_async_copy(token_out.at[expert], token_in.at[expert], token_sem.at[1]).start()
        for side in range(2):
            for j in range(4):
                for copy in store(j, side, 0, side):
                    copy.wait()
        for copies in saved(0):
            for copy in copies:
                copy.wait()
        sends.drain()
        pltpu.make_async_copy(token_out, token_in, token_sem.at[1]).wait()
        sent = token_out.at[pl.ds(0, devices - 1)]
        pltpu.make_async_copy(sent, sent, token_sem.at[0]).wait()
        pltpu.make_async_copy(sent, sent, gate_sem.at[0]).wait()

    any_spec = pl.BlockSpec(memory_space=pl.ANY)
    vmem = pl.BlockSpec(memory_space=pltpu.VMEM)
    big = (devices, rows, width)
    shape = jax.ShapeDtypeStruct
    sems = pltpu.SemaphoreType.DMA
    return pl.pallas_call(
        kernel,
        name="experts",
        out_shape=[
            shape(big, bf16), shape(big, bf16), shape(big, bf16),
            shape((devices, 8, rows), f32),
            shape((2 * length, count, width), bf16), shape((2 * length, count, width), bf16),
            shape((2 * length, count, hidden), bf16), shape((2 * length, count, hidden), bf16),
            shape((2 * length, count, hidden), bf16),
        ],
        in_specs=[any_spec] * 6,
        out_specs=[any_spec] * 3 + [vmem] + [any_spec] * 5,
        scratch_shapes=[
            pltpu.VMEM((width, hidden), bf16),
            pltpu.VMEM((width, hidden), bf16),
            pltpu.VMEM((hidden, width), bf16),
            pltpu.VMEM((devices, capacity, rows), bf16),
            pltpu.VMEM((devices, capacity, 128), f32),
            pltpu.VMEM((devices, rows), f32),
            pltpu.VMEM((devices, 8, rows), f32),
            pltpu.VMEM((2, 4, rows, width), bf16),
            pltpu.VMEM((2, 4, rows, width), bf16),
            pltpu.VMEM((count, width), bf16),
            pltpu.VMEM((count, width), bf16),
            pltpu.VMEM((count, width), bf16),
            pltpu.VMEM((count, hidden), bf16),
            pltpu.VMEM((count, hidden), bf16),
            pltpu.VMEM((count, hidden), bf16),
            pltpu.VMEM((count, width), bf16),
            pltpu.VMEM((count, width), bf16),
            pltpu.VMEM((4, capacity, rows), bf16),
            pltpu.VMEM((count, 128), f32),
            pltpu.VMEM((count, 128), f32),
            pltpu.VMEM((2, 4, rows, width), bf16),
            pltpu.VMEM((2, 4, rows, width), bf16),
            pltpu.VMEM((devices, 8, rows), f32),
        ]
        + GatherItem.semaphores("all", length)
        + [sems((2, 2, 4)), sems((2, 2, 4)), sems((5,)), sems((2,)), sems((2,)), sems((3,))],
        compiler_params=pltpu.CompilerParams(
            collective_id=collective_id, has_side_effects=True, vmem_limit_bytes=63 << 20
        ),
    )(rows_own, all_cots, gates_own, wgate, wup, wdown)


def rope(values, cosine, sine):
    return values * cosine + pltpu.roll(values, values.shape[-1] // 2, 1) * sine


def unrope(values, cosine, sine):
    return values * cosine - pltpu.roll(values, values.shape[-1] // 2, 1) * sine


def row_factor(values):
    return lax.rsqrt(jnp.mean(values * values, axis=-1, keepdims=True) + EPSILON)


def visible_pairs(seg_col, seg_row, start, stop, reach):
    shape = (stop - start, reach)
    query = lax.broadcasted_iota(jnp.int32, shape, 0) + start
    key = lax.broadcasted_iota(jnp.int32, shape, 1)
    return (seg_col[start:stop, :] == seg_row[:, 0:reach]) & (key <= query)


def fill_turns(seg_row, cos_half, sin_half, seg_col, cosine, sine):
    spread = jnp.broadcast_to(seg_row[...].astype(jnp.float32), (128, seg_row.shape[1]))
    seg_col[...] = spread.T[:, 0:1].astype(jnp.int32)
    cosine[...] = jnp.concatenate([cos_half[...], cos_half[...]], axis=1)
    sine[...] = jnp.concatenate([-sin_half[...], sin_half[...]], axis=1)


def attend(rows_own, joint_own, output_own, cots_own, segments, cosine, sine, query_gain, key_gain, length, collective_id):
    rows, width = rows_own.shape
    depth, joint = joint_own.shape
    head_width, part = output_own.shape
    head = query_gain.shape[-1]
    heads = head_width // head
    tokens = rows * length
    block = tokens // 2
    tile = 512
    scale = 1.0 / math.sqrt(head)
    f32, bf16 = jnp.float32, jnp.bfloat16

    def kernel(
        rows_ref, joint_ref, output_ref, cots_ref, segr, cos_half, sin_half, qgain, kgain,
        out_add, out_rows, out_joint, out_weight, out_cots, out_qkv, out_heads,
        segc, cos_ref, sin_ref,
        rows_v, joint_v, weight_v, qkv, att, key_v, value_v,
        r0, r1, r2, r3, r4, r5, r6, r7,
        g0, g1, g2, j0, j1, j2, w0, w1, w2, c0, c1, c2, save_sem,
    ):
        place = Place(length)

        def item_of(mode, source, half, slot, sems):
            item = GatherItem(mode, place, None, None, *sems)
            item.own = lambda h: source.at[piece(2 * half, h)]
            item.slot = slot
            return item

        half, deep, tall = rows // 2, depth // 2, head_width // 2
        own_rows = item_of(
            "z", rows_ref, half, lambda c, z, h: rows_v.at[z, piece(2 * half, h)], (g0, g1, g2)
        )
        own_joint = item_of(
            "dp", joint_ref, deep, lambda c, z, h: joint_v.at[c, piece(2 * deep, h)], (j0, j1, j2)
        )
        own_weight = item_of(
            "dp",
            output_ref,
            tall,
            lambda c, z, h: weight_v.at[
                piece(2 * tall, h), pl.ds(pl.multiple_of(c * part, part), part)
            ],
            (w0, w1, w2),
        )
        cots = item_of(
            "all",
            cots_ref,
            half,
            lambda c, z, h: out_cots.at[c * length + z, piece(2 * half, h)],
            (c0, c1, c2),
        )
        total = ReduceItem(
            "z", place, None, (r0, r1, r2, r3, r4, r5, r6, r7),
            lambda h: out_add.at[piece(2 * half, h)],
        )
        total.computed = True
        total.begin()
        meet(place, True, True)
        sends = Sends(place)
        own_joint.begin(sends)
        own_rows.begin(sends)
        own_weight.begin(sends)
        fill_turns(segr, cos_half, sin_half, segc, cos_ref, sin_ref)
        own_joint.across(sends, 0)
        own_rows.along_z(sends, 1)
        own_weight.across(sends, 0)
        own_joint.diagonal(sends, 0)
        own_rows.along_z(sends, 2)
        cots.begin(sends)
        own_weight.diagonal(sends, 0)
        for distance in range(3, length):
            own_rows.along_z(sends, distance)
        own_joint.finish()
        own_rows.finish()

        def projection(n, carry):
            lanes = pl.ds(pl.multiple_of(n * 256, 256), 256)
            left = rows_v[...].reshape(tokens, width)
            right = joint_v[:, :, lanes].reshape(width, 256)
            qkv[:, lanes] = dot(left, right)
            return carry

        lax.fori_loop(0, joint // 256, projection, 0)
        saves = [
            pltpu.make_async_copy(source, target, save_sem.at[n])
            for n, (source, target) in enumerate(
                ((rows_v, out_rows), (joint_v, out_joint), (qkv, out_qkv), (weight_v, out_weight), (att, out_heads))
            )
        ]
        for copy in saves[:3]:
            copy.start()
        key = qkv[:, head_width : head_width + head]
        key_v[...] = rope(key * row_factor(key) * kgain[...], cos_ref[...], sin_ref[...]).astype(bf16)
        value_v[...] = qkv[:, head_width + head : head_width + 2 * head].astype(bf16)

        def one_head(n, carry):
            lanes = pl.ds(pl.multiple_of(n * head, head), head)
            for start in range(0, tokens, block):
                stop = start + block
                query = qkv[start:stop, lanes]
                turned = rope(
                    query * row_factor(query) * qgain[...], cos_ref[start:stop, :], sin_ref[start:stop, :]
                ).astype(bf16)
                scores = dot(turned, key_v[0:stop, :], 1, 1) * scale
                seen = visible_pairs(segc, segr, start, stop, stop)
                scores = jnp.where(seen, scores, NEG_BIG)
                top = jnp.max(scores, axis=-1, keepdims=True)
                powers = jnp.exp(scores - top)
                probs = (powers / jnp.sum(powers, axis=-1, keepdims=True)).astype(bf16)
                att[start:stop, lanes] = dot(probs, value_v[0:stop, :]).astype(bf16)
            return carry

        lax.fori_loop(0, heads // 2, one_head, 0)
        cots.across(sends, 0)
        cots.along_z(sends, 1)
        lax.fori_loop(heads // 2, heads, one_head, 0)
        saves[4].start()
        own_weight.finish()
        saves[3].start()

        def outward(turn):
            z = total.z_of(turn)

            def body(n, carry):
                lanes = pl.ds(pl.multiple_of(n * tile, tile), tile)
                left = att[pl.ds(pl.multiple_of(z * rows, rows), rows), :]
                found = dot(left, weight_v[:, lanes]).astype(bf16)
                total.acc[0, turn, :, lanes] = found
                return carry

            lax.fori_loop(0, width // tile, body, 0)

        for turn in range(length):
            outward(turn)
            total.home(sends, turn)
            cots.diagonal(sends, turn)
            cots.across(sends, turn + 1)
            cots.along_z(sends, turn + 2)
        cots.finish()
        for copy in saves:
            copy.wait()
        sends.drain()

    any_spec = pl.BlockSpec(memory_space=pl.ANY)
    vmem = pl.BlockSpec(memory_space=pltpu.VMEM)
    shape = jax.ShapeDtypeStruct
    return pl.pallas_call(
        kernel,
        name="attend",
        out_shape=[
            shape((rows, width), f32),
            shape((length, rows, width), bf16),
            shape((8, depth, joint), bf16),
            shape((head_width, 8 * part), bf16),
            shape((8 * length, rows, width), bf16),
            shape((tokens, joint), f32),
            shape((tokens, head_width), bf16),
            shape((tokens, 1), jnp.int32),
            shape((tokens, head), f32),
            shape((tokens, head), f32),
        ],
        in_specs=[any_spec] * 4 + [vmem] * 5,
        out_specs=[vmem] + [any_spec] * 6 + [vmem] * 3,
        scratch_shapes=[
            pltpu.VMEM((length, rows, width), bf16),
            pltpu.VMEM((8, depth, joint), bf16),
            pltpu.VMEM((head_width, 8 * part), bf16),
            pltpu.VMEM((tokens, joint), f32),
            pltpu.VMEM((tokens, head_width), bf16),
            pltpu.VMEM((tokens, head), bf16),
            pltpu.VMEM((tokens, head), bf16),
        ]
        + ReduceItem.scratch("z", length, rows, width)
        + GatherItem.semaphores("z", length)
        + GatherItem.semaphores("dp", length) * 2
        + GatherItem.semaphores("all", length)
        + [pltpu.SemaphoreType.DMA((5,))],
        compiler_params=pltpu.CompilerParams(
            collective_id=collective_id, has_side_effects=True, vmem_limit_bytes=56 << 20
        ),
    )(rows_own, joint_own, output_own, cots_own, segments, cosine, sine, query_gain, key_gain)


def attend_back(grad_own, rows_all, joint_all, output_all, qkv_all, heads_all, part_out, seg_col, seg_row, cosine, sine, query_gain, key_gain, length, collective_id):
    rows, width = grad_own.shape
    _, depth, joint = joint_all.shape
    head_width = output_all.shape[0]
    part = width // 8
    head = query_gain.shape[-1]
    heads = head_width // head
    tokens = rows * length
    block = tokens // 2
    scale = 1.0 / math.sqrt(head)
    f32, bf16 = jnp.float32, jnp.bfloat16
    half, deep, tall = rows // 2, depth // 2, head_width // 2

    def kernel(
        grad_ref, rows_ref, joint_ref, output_ref, qkv_ref, heads_ref, part_ref,
        segc, segr, cos_ref, sin_ref, qgain, kgain,
        out_rows, out_joint, out_weight, out_moe, out_qgain, out_kgain,
        grads, joint_v, weight_v, qkv, att, gatt, joint_b, part_w, key_v, value_v, dkey, dvalue,
        *rest,
    ):
        place = Place(length)
        o_bufs, z_bufs, j_bufs, w_bufs = (rest[8 * n : 8 * n + 8] for n in range(4))
        gather_sems, load_sem = rest[32:35], rest[35]

        outs = ReduceItem(
            "all",
            place,
            lambda c, z, h: part_ref.at[c * length + z, piece(2 * half, h)],
            o_bufs,
            lambda h: out_moe.at[piece(2 * half, h)],
        )
        back = ReduceItem(
            "z",
            place,
            lambda c, z, h: grads.at[z, piece(2 * half, h)],
            z_bufs,
            lambda h: out_rows.at[piece(2 * half, h)],
        )
        joints = ReduceItem(
            "dp",
            place,
            lambda c, z, h: joint_v.at[c, piece(2 * deep, h)],
            j_bufs,
            lambda h: out_joint.at[piece(2 * deep, h)],
        )
        weights = ReduceItem(
            "dp",
            place,
            lambda c, z, h: part_w.at[
                piece(2 * tall, h), pl.ds(pl.multiple_of(c * part, part), part)
            ],
            w_bufs,
            lambda h: out_weight.at[piece(2 * tall, h)],
        )
        for item in (back, joints, weights):
            item.in_place = True
        gathers = GatherItem("z", place, None, None, *gather_sems)
        gathers.own = lambda h: grad_ref.at[piece(2 * half, h)]
        gathers.slot = lambda c, z, h: grads.at[z, piece(2 * half, h)]

        outs.begin()
        back.begin()
        meet(place, True, True)
        first, sends = Sends(place), Sends(place)
        gathers.begin(first)
        outs.hand_over(sends, 0)
        outs.load_all()
        outs.hand_over(sends, 1)
        loads = [
            pltpu.make_async_copy(source, target, load_sem.at[n])
            for n, (source, target) in enumerate(
                ((output_ref, weight_v), (heads_ref, att), (qkv_ref, qkv), (joint_ref, joint_v))
            )
        ]
        for copy in loads:
            copy.start()
        advance(outs, sends, 0)
        for distance in range(1, length):
            gathers.along_z(first, distance)
            if distance < length - 1:
                advance(outs, sends, distance)
        gathers.finish()
        first.drain()
        for copy in loads[:3]:
            copy.wait()

        def to_heads(n, carry):
            lanes = pl.ds(pl.multiple_of(n * 256, 256), 256)
            left = grads[...].reshape(tokens, width)
            gatt[:, lanes] = dot(left, weight_v[lanes, :], 1, 1).astype(bf16)
            return carry

        def to_weight(n, carry):
            lanes = pl.ds(pl.multiple_of(n * 256, 256), 256)
            right = grads[:, :, lanes].reshape(tokens, 256)
            part_w[:, lanes] = dot(att[...], right, 0, 0).astype(bf16)
            return carry

        lax.fori_loop(0, width // 256, to_weight, 0)
        weights.hand_over(sends, 0)
        lax.fori_loop(0, head_width // 256, to_heads, 0)
        rows_v = weight_v.at[pl.ds(0, tokens)]
        rows_loads = [
            pltpu.make_async_copy(
                rows_ref.at[z], weight_v.at[pl.ds(z * rows, rows)], load_sem.at[4 + z]
            )
            for z in range(length)
        ]
        for copy in rows_loads:
            copy.start()
        advance(weights, sends, 0)
        key = qkv[:, head_width : head_width + head]
        key_v[...] = rope(key * row_factor(key) * kgain[...], cos_ref[...], sin_ref[...]).astype(bf16)
        value_v[...] = qkv[:, head_width + head : head_width + 2 * head].astype(bf16)
        dkey[...] = jnp.zeros((tokens, head), f32)
        dvalue[...] = jnp.zeros((tokens, head), f32)
        out_qgain[...] = jnp.zeros(out_qgain.shape, f32)

        def normed_back(grad, raw, gain, start, stop):
            factor = row_factor(raw)
            hat = raw * factor
            turned = unrope(grad, cos_ref[start:stop, :], sin_ref[start:stop, :])
            scaled = turned * gain
            found = factor * (scaled - hat * jnp.mean(scaled * hat, axis=-1, keepdims=True))
            return found, jnp.sum(turned * hat, axis=0, keepdims=True)

        def one_head(n, carry):
            lanes = pl.ds(pl.multiple_of(n * head, head), head)
            for start in range(0, tokens, block):
                stop = start + block
                raw = qkv[start:stop, lanes]
                turned = rope(
                    raw * row_factor(raw) * qgain[...], cos_ref[start:stop, :], sin_ref[start:stop, :]
                ).astype(bf16)
                grad = gatt[start:stop, lanes]
                delta = jnp.sum(
                    grad.astype(f32) * att[start:stop, lanes].astype(f32), axis=-1, keepdims=True
                )
                scores = dot(turned, key_v[0:stop, :], 1, 1) * scale
                seen = visible_pairs(segc, segr, start, stop, stop)
                scores = jnp.where(seen, scores, NEG_BIG)
                powers = jnp.exp(scores - jnp.max(scores, axis=-1, keepdims=True))
                probs = powers / jnp.sum(powers, axis=-1, keepdims=True)
                dprobs = dot(grad, value_v[0:stop, :], 1, 1)
                dscores = (probs * (dprobs - delta)).astype(bf16)
                dvalue[0:stop, :] += dot(probs.astype(bf16), grad, 0, 0)
                dkey[0:stop, :] += dot(dscores, turned, 0, 0) * scale
                dquery = dot(dscores, key_v[0:stop, :]) * scale
                found, gain_part = normed_back(dquery, raw, qgain[...], start, stop)
                joint_b[start:stop, lanes] = found.astype(bf16)
                out_qgain[...] += gain_part
            return carry

        lax.fori_loop(0, heads // 2, one_head, 0)
        advance(outs, sends, length - 1)
        advance(weights, sends, 1)
        lax.fori_loop(heads // 2, heads, one_head, 0)
        found, gain_part = normed_back(
            dkey[...], qkv[:, head_width : head_width + head], kgain[...], 0, tokens
        )
        out_kgain[...] = gain_part
        joint_b[:, head_width : head_width + head] = found.astype(bf16)
        joint_b[:, head_width + head : head_width + 2 * head] = dvalue[...].astype(bf16)
        loads[3].wait()

        def to_rows(n, carry):
            lanes = pl.ds(pl.multiple_of(n * depth, depth), depth)
            found = dot(joint_b[...], joint_v[n], 1, 1).astype(bf16)
            grads[:, :, lanes] = found.reshape(length, rows, depth)
            return carry

        lax.fori_loop(0, 8, to_rows, 0)
        back.home(sends, 0)
        for copy in rows_loads:
            copy.wait()

        def to_joint(n, carry):
            lanes = pl.ds(pl.multiple_of(n * depth, depth), depth)
            joint_v[n] = dot(weight_v[0:tokens, lanes], joint_b[...], 0, 0).astype(bf16)
            return carry

        lax.fori_loop(0, 8, to_joint, 0)
        joints.hand_over(sends, 0)
        advance(outs, sends, length)
        advance(joints, sends, 0)
        back.home(sends, 1)
        advance(weights, sends, 2)
        for turn in range(2, length - 1):
            back.home(sends, turn)
        advance(joints, sends, 1)
        advance(outs, sends, length + 1)
        back.home(sends, length - 1)
        advance(joints, sends, 2)
        sends.drain()

    any_spec = pl.BlockSpec(memory_space=pl.ANY)
    vmem = pl.BlockSpec(memory_space=pltpu.VMEM)
    shape = jax.ShapeDtypeStruct
    return pl.pallas_call(
        kernel,
        name="attend_back",
        out_shape=[
            shape((rows, width), f32),
            shape((depth, joint), f32),
            shape((head_width, part), f32),
            shape((rows, width), f32),
            shape((1, head), f32),
            shape((1, head), f32),
        ],
        in_specs=[any_spec] * 7 + [vmem] * 6,
        out_specs=[vmem] * 6,
        scratch_shapes=[
            pltpu.VMEM((length, rows, width), bf16),
            pltpu.VMEM((8, depth, joint), bf16),
            pltpu.VMEM((head_width, width), bf16),
            pltpu.VMEM((tokens, joint), f32),
            pltpu.VMEM((tokens, head_width), bf16),
            pltpu.VMEM((tokens, head_width), bf16),
            pltpu.VMEM((tokens, joint), bf16),
            pltpu.VMEM((head_width, width), bf16),
            pltpu.VMEM((tokens, head), bf16),
            pltpu.VMEM((tokens, head), bf16),
            pltpu.VMEM((tokens, head), f32),
            pltpu.VMEM((tokens, head), f32),
        ]
        + ReduceItem.scratch("all", length, rows, width)
        + ReduceItem.scratch("z", length, rows, width, True)
        + ReduceItem.scratch("dp", length, depth, joint, True)
        + ReduceItem.scratch("dp", length, head_width, part, True)
        + GatherItem.semaphores("z", length)
        + [pltpu.SemaphoreType.DMA((4 + length,))],
        compiler_params=pltpu.CompilerParams(
            collective_id=collective_id, has_side_effects=True, vmem_limit_bytes=67043328
        ),
    )(grad_own, rows_all, joint_all, output_all, qkv_all, heads_all, part_out, seg_col, seg_row, cosine, sine, query_gain, key_gain)


def share_sum(values, length, collective_id):
    rows, width = values.shape

    def kernel(own, target, middle, group, line, send_sem, recv_sem):
        place = Place(length)

        def dp_peer(n):
            return lax.rem(place.dp + n, 8), place.z

        def z_peer(n):
            return place.dp, lax.rem(place.z + n, length)

        peers = [dp_peer(n) for n in range(1, 8)] + [z_peer(n) for n in range(1, length)]
        barrier = pltpu.get_barrier_semaphore()
        for device in peers:
            pl.semaphore_signal(barrier, 1, device_id=device, device_id_type=MESH)
        pl.semaphore_wait(barrier, len(peers))

        def exchange(source, land, mine, devices, at):
            for device in devices:
                pltpu.make_async_remote_copy(
                    src_ref=source,
                    dst_ref=land.at[mine],
                    send_sem=send_sem.at[at],
                    recv_sem=recv_sem.at[at],
                    device_id=device,
                    device_id_type=MESH,
                ).start()
            pltpu.make_async_copy(source, land.at[mine], recv_sem.at[at]).start()
            pltpu.make_async_copy(land, land, recv_sem.at[at]).wait()
            total = land[0]
            for n in range(1, land.shape[0]):
                total = total + land[n]
            return total

        middle[...] = exchange(own, group, place.dp, peers[:7], 0)
        target[...] = exchange(middle, line, place.z, peers[7:], 1)
        for at, land in ((0, group), (1, line)):
            sent = land.at[pl.ds(0, land.shape[0] - 1)]
            pltpu.make_async_copy(sent, sent, send_sem.at[at]).wait()

    vmem = pl.BlockSpec(memory_space=pltpu.VMEM)
    return pl.pallas_call(
        kernel,
        name="share_sum",
        out_shape=jax.ShapeDtypeStruct((rows, width), values.dtype),
        in_specs=[vmem],
        out_specs=vmem,
        scratch_shapes=[
            pltpu.VMEM((rows, width), values.dtype),
            pltpu.VMEM((8, rows, width), values.dtype),
            pltpu.VMEM((length, rows, width), values.dtype),
            pltpu.SemaphoreType.DMA((2,)),
            pltpu.SemaphoreType.DMA((2,)),
        ],
        compiler_params=pltpu.CompilerParams(collective_id=collective_id, has_side_effects=True),
    )(values)


def mix(form, left, right):
    return jnp.einsum(form, left, right, preferred_element_type=jnp.float32)


def rms_scale(values):
    return lax.rsqrt(jnp.mean(values * values, axis=-1, keepdims=True) + EPSILON)


def rope_tables(seg_ids, head_dim):
    length = seg_ids.shape[0]
    row_index = jnp.arange(length, dtype=jnp.int32)
    starts = jnp.sum((seg_ids[None, :] < seg_ids[:, None]).astype(jnp.int32), axis=1)
    places = (row_index - starts).astype(jnp.float32)
    half_dim = head_dim // 2
    frequency = THETA_BASE ** (-(jnp.arange(half_dim, dtype=jnp.float32) * (2.0 / head_dim)))
    angles = places[:, None] * frequency[None, :]
    return (jnp.cos(angles), jnp.sin(angles))


def rotate(values, cosine, sine_table):
    half_dim = values.shape[-1] // 2
    front_part = values[..., :half_dim]
    back_part = values[..., half_dim:]
    cos_rows = cosine[:, None, :]
    sin_rows = sine_table[:, None, :]
    return jnp.concatenate(
        [
            front_part * cos_rows - back_part * sin_rows,
            back_part * cos_rows + front_part * sin_rows,
        ],
        axis=-1,
    )


def unrotate(values, cosine, sine_table):
    half_dim = values.shape[-1] // 2
    front_part = values[..., :half_dim]
    back_part = values[..., half_dim:]
    cos_rows = cosine[:, None, :]
    sin_rows = sine_table[:, None, :]
    return jnp.concatenate(
        [
            front_part * cos_rows + back_part * sin_rows,
            back_part * cos_rows - front_part * sin_rows,
        ],
        axis=-1,
    )


def head_norm_back(grad_out, normed, factor, gain):
    grad_normed = grad_out * gain
    grad_gain = jnp.sum(grad_out * normed, axis=(0, 1))
    grad_values = factor * (
        grad_normed - normed * jnp.mean(grad_normed * normed, axis=-1, keepdims=True)
    )
    return (grad_values, grad_gain)


def row_norm_back(grad_out, normed, factor, gain):
    grad_normed = grad_out * gain
    grad_gain = jnp.sum(grad_out * normed, axis=0)
    grad_values = factor * (
        grad_normed - normed * jnp.mean(grad_normed * normed, axis=-1, keepdims=True)
    )
    return (grad_values, grad_gain)


def softmax_rows(logits):
    top_value = jnp.max(logits, axis=-1, keepdims=True)
    expo = jnp.exp(logits - top_value)
    return expo / jnp.sum(expo, axis=-1, keepdims=True)


def attn_forward(rows, seg_ids, wq_full, wk_full, wv_full, query_gain, key_gain):
    length = rows.shape[0]
    head_dim = query_gain.shape[0]
    num_heads = wq_full.shape[1] // head_dim
    kv_heads = wk_full.shape[1] // head_dim
    per_group = num_heads // kv_heads
    inv_root = 1.0 / math.sqrt(head_dim)
    block_rows = math.gcd(length, 512)
    cosine, sine_table = rope_tables(seg_ids, head_dim)
    query = jnp.dot(rows, wq_full, preferred_element_type=jnp.float32).reshape(
        length, num_heads, head_dim
    )
    key_proj = jnp.dot(rows, wk_full, preferred_element_type=jnp.float32).reshape(
        length, kv_heads, head_dim
    )
    value_rows = (
        jnp.dot(rows, wv_full, preferred_element_type=jnp.float32)
        .astype(jnp.bfloat16)
        .reshape(length, kv_heads, head_dim)
    )
    query_factor = rms_scale(query)
    query_hat = query * query_factor
    key_factor = rms_scale(key_proj)
    key_hat = key_proj * key_factor
    query_rot = (
        rotate(query_hat * query_gain, cosine, sine_table)
        .astype(jnp.bfloat16)
        .reshape(length, kv_heads, per_group, head_dim)
    )
    key_rot = rotate(key_hat * key_gain, cosine, sine_table).astype(jnp.bfloat16)
    row_index = jnp.arange(length, dtype=jnp.int32)
    scores = mix("qgrd,kgd->grqk", query_rot, key_rot) * inv_root
    visible = (seg_ids[0:block_rows, None] == seg_ids[None, :]) & (
        row_index[None, :] <= row_index[0:block_rows, None]
    )
    scores = jnp.where(visible, scores, NEG_BIG)
    top_value = jnp.max(scores, axis=-1, keepdims=True)
    expo = jnp.exp(scores - top_value)
    totals = jnp.sum(expo, axis=-1, keepdims=True)
    prob_rows = (expo / totals).astype(jnp.bfloat16)
    outputs = mix("grqk,kgd->qgrd", prob_rows, value_rows).astype(jnp.bfloat16)
    lse_parts = top_value[..., 0] + jnp.log(totals[..., 0])
    attn_heads = outputs.reshape(length, num_heads * head_dim)
    return (
        attn_heads,
        lse_parts,
        query_rot,
        key_rot,
        value_rows,
        cosine,
        sine_table,
        query_hat,
        query_factor,
        key_hat,
        key_factor,
    )


def attn_backward(
    grad_attn, rows, seg_ids, wq_full, wk_full, wv_full, wo_full, query_gain, key_gain, saved
):
    (
        attn_heads,
        lse_all,
        query_rot,
        key_rot,
        value_rows,
        cosine,
        sine_table,
        query_hat,
        query_factor,
        key_hat,
        key_factor,
    ) = saved
    length = rows.shape[0]
    head_dim = query_gain.shape[0]
    num_heads = query_hat.shape[1]
    inv_root = 1.0 / math.sqrt(head_dim)
    block_rows = math.gcd(length, 512)
    grad_wo = jnp.dot(attn_heads.T, grad_attn, preferred_element_type=jnp.float32)
    grad_heads = (
        jnp.dot(grad_attn, wo_full.T, preferred_element_type=jnp.float32)
        .astype(jnp.bfloat16)
        .reshape(query_rot.shape)
    )
    heads_view = attn_heads.reshape(query_rot.shape)
    row_delta = jnp.transpose(
        jnp.sum(grad_heads.astype(jnp.float32) * heads_view.astype(jnp.float32), axis=-1), (1, 2, 0)
    )
    row_index = jnp.arange(length, dtype=jnp.int32)
    scores = mix("qgrd,kgd->grqk", query_rot, key_rot) * inv_root
    visible = (seg_ids[0:block_rows, None] == seg_ids[None, :]) & (
        row_index[None, :] <= row_index[0:block_rows, None]
    )
    scores = jnp.where(visible, scores, NEG_BIG)
    prob_f = jnp.where(visible, jnp.exp(scores - lse_all[:, :, 0:block_rows, None]), 0.0)
    prob_rows = prob_f.astype(jnp.bfloat16)
    grad_value = mix("grqk,qgrd->kgd", prob_rows, grad_heads)
    grad_probs = mix("qgrd,kgd->grqk", grad_heads, value_rows)
    grad_scores = (prob_f * (grad_probs - row_delta[:, :, 0:block_rows, None])).astype(jnp.bfloat16)
    pieces = mix("grqk,kgd->qgrd", grad_scores, key_rot) * inv_root
    grad_key_rot = mix("grqk,qgrd->kgd", grad_scores, query_rot) * inv_root
    grad_query_rot = pieces.reshape(length, num_heads, head_dim)
    grad_query, grad_qgain = head_norm_back(
        unrotate(grad_query_rot, cosine, sine_table), query_hat, query_factor, query_gain
    )
    grad_key, grad_kgain = head_norm_back(
        unrotate(grad_key_rot, cosine, sine_table), key_hat, key_factor, key_gain
    )
    query_b = grad_query.astype(jnp.bfloat16).reshape(length, -1)
    key_b = grad_key.astype(jnp.bfloat16).reshape(length, -1)
    value_b = grad_value.astype(jnp.bfloat16).reshape(length, -1)
    grad_rows = (
        jnp.dot(query_b, wq_full.T, preferred_element_type=jnp.float32)
        + jnp.dot(key_b, wk_full.T, preferred_element_type=jnp.float32)
        + jnp.dot(value_b, wv_full.T, preferred_element_type=jnp.float32)
    )
    grad_wq = jnp.dot(rows.T, query_b, preferred_element_type=jnp.float32)
    grad_wk = jnp.dot(rows.T, key_b, preferred_element_type=jnp.float32)
    grad_wv = jnp.dot(rows.T, value_b, preferred_element_type=jnp.float32)
    return (grad_rows, grad_wq, grad_wk, grad_wv, grad_wo, grad_qgain, grad_kgain)


def expert_forward(expert_rows, wgate, wup, wdown):
    gate_pre = jnp.dot(expert_rows, wgate, preferred_element_type=jnp.float32)
    up_pre = jnp.dot(expert_rows, wup, preferred_element_type=jnp.float32)
    hidden_units = (jax.nn.silu(gate_pre) * up_pre).astype(jnp.bfloat16)
    result = jnp.dot(hidden_units, wdown, preferred_element_type=jnp.float32).astype(jnp.bfloat16)
    return (result, gate_pre, up_pre, hidden_units)


def expert_backward(expert_rows, grad_result, wgate, wup, wdown, gate_pre, up_pre, hidden_units):
    grad_hidden = jnp.dot(grad_result, wdown.T, preferred_element_type=jnp.float32)
    sigma = jax.nn.sigmoid(gate_pre)
    grad_gate_pre = (grad_hidden * up_pre * sigma * (1.0 + gate_pre * (1.0 - sigma))).astype(
        jnp.bfloat16
    )
    grad_up_pre = (grad_hidden * gate_pre * sigma).astype(jnp.bfloat16)
    grad_rows = (
        jnp.dot(grad_gate_pre, wgate.T, preferred_element_type=jnp.float32)
        + jnp.dot(grad_up_pre, wup.T, preferred_element_type=jnp.float32)
    ).astype(jnp.bfloat16)
    grad_wd = jnp.dot(hidden_units.T, grad_result, preferred_element_type=jnp.float32)
    grad_wg = jnp.dot(expert_rows.T, grad_gate_pre, preferred_element_type=jnp.float32)
    grad_wu = jnp.dot(expert_rows.T, grad_up_pre, preferred_element_type=jnp.float32)
    return (grad_rows, grad_wg, grad_wu, grad_wd)


def to_experts(buffer):
    return lax.all_to_all(buffer, ("dp", "tensor"), split_axis=0, concat_axis=0, tiled=True)


def to_sources(buffer):
    return lax.all_to_all(buffer, ("dp", "tensor"), split_axis=0, concat_axis=0, tiled=True)


def shards(
    hidden_in,
    segments,
    routes,
    query_weight,
    key_weight,
    value_weight,
    output_weight,
    gain_attn,
    gain_moe,
    query_gain,
    key_gain,
    router,
    gate_weight,
    up_weight,
    down_weight,
    cotangent,
):
    seg_ids = segments[0]
    rows_dev = hidden_in.shape[0]
    width = hidden_in.shape[1]
    top_count = routes.shape[1]
    experts = router.shape[1]
    capacity = 2 * rows_dev * top_count // experts
    full_query, full_key, full_value, full_output = (
        lax.all_gather(query_weight, "dp", axis=0, tiled=True),
        lax.all_gather(key_weight, "dp", axis=0, tiled=True),
        lax.all_gather(value_weight, "dp", axis=0, tiled=True),
        lax.all_gather(output_weight, "dp", axis=1, tiled=True),
    )
    inputs32 = hidden_in.astype(jnp.float32)
    factor_one = rms_scale(inputs32)
    normed_one = inputs32 * factor_one
    rows_one = (normed_one * gain_attn).astype(jnp.bfloat16)
    group_rows = lax.all_gather(rows_one, "tensor", axis=0, tiled=True)
    saved = attn_forward(
        group_rows, seg_ids, full_query, full_key, full_value, query_gain, key_gain
    )
    partial_add = jnp.dot(saved[0], full_output, preferred_element_type=jnp.float32)
    attn_add = lax.psum_scatter(partial_add, "tensor", scatter_dimension=0, tiled=True)
    residual = inputs32 + attn_add
    factor_two = rms_scale(residual)
    normed_two = residual * factor_two
    rows_two = (normed_two * gain_moe).astype(jnp.bfloat16)
    router_probs = softmax_rows(jnp.dot(rows_two, router, preferred_element_type=jnp.float32))
    route_hot = (routes[:, :, None] == jnp.arange(experts, dtype=jnp.int32)[None, None, :]).astype(
        jnp.float32
    )
    picked = jnp.sum(route_hot * router_probs[:, None, :], axis=-1)
    total = jnp.sum(picked, axis=1, keepdims=True)
    gates = picked / total
    flat_routes = routes.reshape(-1)
    onehot = (flat_routes[:, None] == jnp.arange(experts, dtype=jnp.int32)[None, :]).astype(
        jnp.int32
    )
    ranks = jnp.sum(onehot * jnp.cumsum(onehot, axis=0), axis=1) - 1
    slots = flat_routes * capacity + ranks
    send_rows = (
        jnp.zeros((experts * capacity, width), jnp.bfloat16)
        .at[slots]
        .set(jnp.repeat(rows_two, top_count, axis=0))
    )
    received = to_experts(send_rows.reshape(experts, capacity, width)).reshape(-1, width)
    result, gate_pre, up_pre, hidden_units = expert_forward(
        received, gate_weight[0], up_weight[0], down_weight[0]
    )
    returned = to_sources(result.reshape(-1, capacity, width)).reshape(experts * capacity, width)
    pair_out = returned[slots].astype(jnp.float32).reshape(rows_dev, top_count, width)
    moe_sum = jnp.sum(gates[:, :, None] * pair_out, axis=1)
    output = (residual + moe_sum).astype(jnp.bfloat16)
    cot32 = cotangent.astype(jnp.float32)
    grad_gates = jnp.sum(cot32[:, None, :] * pair_out, axis=-1)
    grad_result = (gates[:, :, None] * cot32[:, None, :]).astype(jnp.bfloat16).reshape(-1, width)
    send_grads = jnp.zeros((experts * capacity, width), jnp.bfloat16).at[slots].set(grad_result)
    received_grads = to_experts(send_grads.reshape(experts, capacity, width)).reshape(-1, width)
    grad_expert_rows, grad_wg, grad_wu, grad_wd = expert_backward(
        received,
        received_grads,
        gate_weight[0],
        up_weight[0],
        down_weight[0],
        gate_pre,
        up_pre,
        hidden_units,
    )
    returned_grads = to_sources(grad_expert_rows.reshape(-1, capacity, width)).reshape(
        experts * capacity, width
    )
    grad_pairs = returned_grads[slots].astype(jnp.float32).reshape(rows_dev, top_count, width)
    grad_picked = (grad_gates - jnp.sum(gates * grad_gates, axis=1, keepdims=True)) / total
    grad_probs = jnp.sum(route_hot * grad_picked[:, :, None], axis=1)
    grad_logits = (
        router_probs * (grad_probs - jnp.sum(grad_probs * router_probs, axis=-1, keepdims=True))
    ).astype(jnp.bfloat16)
    grad_router = jnp.dot(rows_two.T, grad_logits, preferred_element_type=jnp.float32)
    grad_rows_two = jnp.sum(grad_pairs, axis=1) + jnp.dot(
        grad_logits, router.T, preferred_element_type=jnp.float32
    )
    grad_res_norm, grad_gain_moe = row_norm_back(grad_rows_two, normed_two, factor_two, gain_moe)
    grad_residual = cot32 + grad_res_norm
    grad_attn = grad_residual.astype(jnp.bfloat16)
    group_grads = lax.all_gather(grad_attn, "tensor", axis=0, tiled=True)
    back_query, back_key, back_value, back_output = (
        lax.all_gather(query_weight, "dp", axis=0, tiled=True),
        lax.all_gather(key_weight, "dp", axis=0, tiled=True),
        lax.all_gather(value_weight, "dp", axis=0, tiled=True),
        lax.all_gather(output_weight, "dp", axis=1, tiled=True),
    )
    grad_group_rows, grad_wq, grad_wk, grad_wv, grad_wo, grad_qgain, grad_kgain = attn_backward(
        group_grads,
        group_rows,
        seg_ids,
        back_query,
        back_key,
        back_value,
        back_output,
        query_gain,
        key_gain,
        saved,
    )
    grad_rows_one = lax.psum_scatter(
        grad_group_rows.astype(jnp.bfloat16), "tensor", scatter_dimension=0, tiled=True
    ).astype(jnp.float32)
    grad_in_norm, grad_gain_attn = row_norm_back(grad_rows_one, normed_one, factor_one, gain_attn)
    grad_input = grad_residual + grad_in_norm
    grad_wq, grad_wk, grad_wv, grad_wo = (
        lax.psum_scatter(
            grad_wq.astype(jnp.bfloat16), "dp", scatter_dimension=0, tiled=True
        ).astype(jnp.float32),
        lax.psum_scatter(
            grad_wk.astype(jnp.bfloat16), "dp", scatter_dimension=0, tiled=True
        ).astype(jnp.float32),
        lax.psum_scatter(
            grad_wv.astype(jnp.bfloat16), "dp", scatter_dimension=0, tiled=True
        ).astype(jnp.float32),
        lax.psum_scatter(
            grad_wo.astype(jnp.bfloat16), "dp", scatter_dimension=1, tiled=True
        ).astype(jnp.float32),
    )
    grad_gain_attn, grad_gain_moe, grad_qgain, grad_kgain, grad_router = lax.psum(
        (grad_gain_attn, grad_gain_moe, grad_qgain, grad_kgain, grad_router), ("dp", "tensor")
    )
    return (
        output,
        grad_input,
        grad_wq,
        grad_wk,
        grad_wv,
        grad_wo,
        grad_gain_attn,
        grad_gain_moe,
        grad_qgain,
        grad_kgain,
        grad_router,
        grad_wg[None],
        grad_wu[None],
        grad_wd[None],
    )


AXES = ("dp", "tensor")


def gathered(
    hidden_in,
    segments,
    routes,
    query_weight,
    key_weight,
    value_weight,
    output_weight,
    gain_attn,
    gain_moe,
    query_gain,
    key_gain,
    router,
    gate_weight,
    up_weight,
    down_weight,
    cotangent,
):
    seg_ids = segments[0]
    rows_dev, width = hidden_in.shape
    top_count = routes.shape[1]
    expert_count = router.shape[1]
    capacity = 2 * rows_dev * top_count // expert_count
    length = lax.axis_size("tensor")
    query_cols, key_cols = query_weight.shape[1], key_weight.shape[1]

    inputs32 = hidden_in.astype(jnp.float32)
    factor_one = rms_scale(inputs32)
    normed_one = inputs32 * factor_one
    rows_one = (normed_one * gain_attn).astype(jnp.bfloat16)
    joint_weight = jnp.concatenate([query_weight, key_weight, value_weight], axis=1)
    cosine, sine_table = rope_tables(seg_ids, query_gain.shape[0])
    turns = (
        seg_ids[None, :],
        cosine,
        sine_table,
        query_gain[None, :],
        key_gain[None, :],
    )
    attn_add, group_rows, full_joint, full_output, all_cots, projected, attn_heads, *laid = attend(
        rows_one, joint_weight, output_weight, cotangent, *turns, length, 0
    )
    residual = inputs32 + attn_add
    factor_two = rms_scale(residual)
    normed_two = residual * factor_two
    rows_two = (normed_two * gain_moe).astype(jnp.bfloat16)
    router_probs = softmax_rows(jnp.dot(rows_two, router, preferred_element_type=jnp.float32))
    route_hot = (routes[:, :, None] == jnp.arange(expert_count, dtype=jnp.int32)[None, None, :]).astype(
        jnp.float32
    )
    picked = jnp.sum(route_hot * router_probs[:, None, :], axis=-1)
    total = jnp.sum(picked, axis=1, keepdims=True)
    gates = picked / total
    named = jnp.sum(route_hot, axis=1)
    gate_table = jnp.where(named > 0.5, jnp.sum(route_hot * gates[:, :, None], axis=1), -1.0)
    all_rows, partial_out, partial_rows, token_grads, *units = experts(
        rows_two,
        all_cots,
        jnp.broadcast_to(gate_table.T[:, None, :], (expert_count, 8, rows_dev)),
        gate_weight[0],
        up_weight[0],
        down_weight[0],
        length,
        capacity,
        1,
    )
    back_grads = token_grads[:, 0, :]
    cot32 = cotangent.astype(jnp.float32)
    grad_gates = jnp.sum(route_hot * back_grads.T[:, None, :], axis=-1)
    grad_picked = (grad_gates - jnp.sum(gates * grad_gates, axis=1, keepdims=True)) / total
    grad_probs = jnp.sum(route_hot * grad_picked[:, :, None], axis=1)
    grad_logits = (
        router_probs * (grad_probs - jnp.sum(grad_probs * router_probs, axis=-1, keepdims=True))
    ).astype(jnp.bfloat16)
    grad_sum, grad_router, grad_wg, grad_wu, grad_wd = reduce_rows(
        partial_rows,
        grad_logits.T,
        all_rows,
        *[unit.reshape(-1, unit.shape[-1]) for unit in units],
        length,
        2,
    )
    grad_rows_two = grad_sum + jnp.dot(grad_logits, router.T, preferred_element_type=jnp.float32)
    grad_res_norm, grad_gain_moe = row_norm_back(grad_rows_two, normed_two, factor_two, gain_moe)
    grad_residual = cot32 + grad_res_norm
    grad_attn = grad_residual.astype(jnp.bfloat16)
    grad_rows_one, grad_joint, grad_wo, moe_sum, grad_qgain, grad_kgain = attend_back(
        grad_attn,
        group_rows,
        full_joint,
        full_output,
        projected,
        attn_heads,
        partial_out,
        laid[0],
        turns[0],
        *laid[1:],
        *turns[3:],
        length,
        3,
    )
    output = (residual + moe_sum).astype(jnp.bfloat16)
    grad_in_norm, grad_gain_attn = row_norm_back(grad_rows_one, normed_one, factor_one, gain_attn)
    grad_input = grad_residual + grad_in_norm
    small = jnp.concatenate([grad_gain_attn, grad_gain_moe, grad_qgain[0], grad_kgain[0]]).reshape(-1, 128)
    small = jnp.pad(small, ((0, -small.shape[0] % 8), (0, 0)))
    sums = share_sum(small, length, 4).reshape(-1)
    head_dim = query_gain.shape[0]
    return (
        output,
        grad_input,
        grad_joint[:, :query_cols],
        grad_joint[:, query_cols : query_cols + key_cols],
        grad_joint[:, query_cols + key_cols :],
        grad_wo,
        sums[:width],
        sums[width : 2 * width],
        sums[2 * width : 2 * width + head_dim],
        sums[2 * width + head_dim : 2 * width + 2 * head_dim],
        grad_router.T,
        grad_wg[None],
        grad_wu[None],
        grad_wd[None],
    )


def solution(mesh):
    placed = (
        P(("dp", "tensor"), None),
        P("dp", None),
        P(("dp", "tensor"), None),
        P("dp", "tensor"),
        P("dp", "tensor"),
        P("dp", "tensor"),
        P("tensor", "dp"),
        P(),
        P(),
        P(),
        P(),
        P(),
        P(("dp", "tensor"), None, None),
        P(("dp", "tensor"), None, None),
        P(("dp", "tensor"), None, None),
        P(("dp", "tensor"), None),
    )
    program = gathered if mesh.shape["dp"] == 8 and mesh.shape["tensor"] <= 4 else shards
    return jax.shard_map(
        program,
        mesh=mesh,
        in_specs=placed,
        out_specs=(
            P(("dp", "tensor"), None),
            P(("dp", "tensor"), None),
            P("dp", "tensor"),
            P("dp", "tensor"),
            P("dp", "tensor"),
            P("tensor", "dp"),
            P(),
            P(),
            P(),
            P(),
            P(),
            P(("dp", "tensor"), None, None),
            P(("dp", "tensor"), None, None),
            P(("dp", "tensor"), None, None),
        ),
        check_vma=False,
    )
```
